32 devices in a mesh: ma: 16 (over z, y, core), freq: 2 (over x).
Axes of the slice: x: 2, y: 2, z: 4, core: 2. Of those that a mesh axis runs over, the one named last changes fastest.
Arguments:
- right_side: float32 [128, 8, 2, 512], P('ma', 'freq'), may hold values from -60 to 60
- start_field: float32 [128, 8, 2, 512], P('ma', 'freq'), may hold values from -6 to 6
- beam: float32 [128, 8, 2, 16, 512], P('ma', 'freq'), may hold values from -0.75 to 0.75
- noise: float32 [128, 8, 16], P('ma', 'freq'), may hold values from 0.3 to 3
- inv_power: float32 [512], replicated, may hold values from 0.5 to 2
- smooth: float32 [512], replicated, may hold values from 0.5 to 4
Outputs:
- solution_field: float32 [128, 8, 2, 512], P('ma', 'freq')
- residual: float32 [128, 8, 2, 512], P('ma', 'freq')
The draws below stay inside these ranges and needn't reach their ends.
All inputs are finite; a program needn't handle non-finite values.
Results may differ from the reference program's by a relative error of at most 0.0003.
Values sent between devices are 32-bit elements; how exact they have to be, the bound alone decides.
A program may use at most 64 MiB of HBM per device.

```python
import math
import jax
import jax.numpy as jnp
from jax import lax

ELL = 512
RANK = 16
ITERS = 2
M = 128
FREQ = 8


def draw_right_side(key, part):
    key_values = jax.random.fold_in(key, 0)
    position = jnp.arange(M, dtype=jnp.float32) / M
    row_scale = jnp.power(10.0, position)
    values = jnp.clip(jax.random.normal(key_values, (M, FREQ, 2, ELL), jnp.float32), -6.0, 6.0)
    return jnp.clip(values * row_scale[:, None, None, None], -60.0, 60.0)


def block_scale(own_key, dims, pieces, low, largest):
    loudness, own = 1.0, jax.random.fold_in(own_key, 6)
    for axis_at, shards_of in pieces:
        draws = jnp.exp(jax.random.uniform(jax.random.fold_in(own, axis_at), (shards_of,), jnp.float32, low / len(pieces), largest / len(pieces)))
        loudness = loudness * jnp.repeat(draws, dims[axis_at] // shards_of).reshape([-1 if axis == axis_at else 1 for axis in range(len(dims))])
    return loudness


def gaussian(own_key, dims, spread, reach, cuts=(), held_as=jnp.bfloat16):
    drawn = spread * jax.random.normal(own_key, dims, jnp.float32)
    if cuts:
        drawn = drawn * block_scale(own_key, dims, cuts, -0.22, 0.18)
    return jnp.clip(drawn, -reach, reach).astype(held_as)


def setup_inputs(seed: int = 0) -> dict:
    splits = jax.random.split(jax.random.key(seed), 7)
    return {
        "right_side": draw_right_side(jax.random.fold_in(splits[6], 71), 0),
        "start_field": gaussian(splits[1], (M, FREQ, 2, ELL), 1.0, 6.0, ((0, 16), (1, 2)), jnp.float32),
        "beam": gaussian(splits[2], (M, FREQ, 2, RANK, ELL), (4 * RANK) ** -0.5, 0.75, ((0, 16), (1, 2)), jnp.float32),
        "noise": jnp.clip(jnp.exp(math.log(3.0) - 2.3025851 * jax.random.uniform(splits[3], (M, FREQ, RANK), jnp.float32) ** block_scale(splits[3], (M, FREQ, RANK), ((0, 16), (1, 2)), -0.2, 0.2)), 0.3, 3.0),
        "inv_power": jnp.clip(jnp.exp(jax.random.uniform(splits[4], (ELL,), jnp.float32, math.log(0.5), math.log(2.0))), 0.5, 2.0),
        "smooth": jnp.clip(jnp.exp(jax.random.uniform(splits[5], (ELL,), jnp.float32, math.log(0.5), math.log(4.0))), 0.5, 4.0),
    }


def beam_image(field, beam, noise):
    projected = jnp.einsum('mfakl,mfbl->mfabk', beam, field, precision=lax.Precision.HIGHEST)
    real_part = projected[:, :, 0, 0] + projected[:, :, 1, 1]
    imaginary = projected[:, :, 0, 1] - projected[:, :, 1, 0]
    weighted = jnp.stack([real_part, imaginary], axis=2) * noise[:, :, None, :]
    back = jnp.einsum('mfakl,mfbk->mfabl', beam, weighted, precision=lax.Precision.HIGHEST)
    return jnp.stack([back[:, :, 0, 0] - back[:, :, 1, 1], back[:, :, 0, 1] + back[:, :, 1, 0]], axis=2)


def operate(field, beam, noise, inv_power, smooth):
    padded = jnp.pad(field, ((0, 0), (1, 1), (0, 0), (0, 0)))
    channel = jnp.arange(field.shape[1], dtype=jnp.int32)
    weight = (channel > 0).astype(jnp.float32) + (channel < field.shape[1] - 1).astype(jnp.float32)
    prior = smooth * (weight[None, :, None, None] * field - padded[:, :-2] - padded[:, 2:])
    return beam_image(field, beam, noise) + inv_power * field + prior


def reference(right_side, start_field, beam, noise, inv_power, smooth):
    solution_field = start_field
    resid_now = right_side - operate(start_field, beam, noise, inv_power, smooth)
    direction = resid_now
    norm_now = jnp.sum(resid_now * resid_now)
    for turn in range(ITERS):
        applied = operate(direction, beam, noise, inv_power, smooth)
        step_size = norm_now / jnp.sum(direction * applied)
        solution_field = solution_field + step_size * direction
        resid_now = resid_now - step_size * applied
        norm_next = jnp.sum(resid_now * resid_now)
        direction = resid_now + (norm_next / norm_now) * direction
        norm_now = norm_next
    return solution_field, resid_now
```

```python
import functools

import jax
import jax.numpy as jnp
from jax import lax
from jax.experimental import pallas as pl
from jax.experimental.pallas import tpu as pltpu
from jax.sharding import PartitionSpec as P

MESH = pl.DeviceIdType.MESH
F32, BF16 = jnp.float32, jnp.bfloat16


def split(x):
    high = x.astype(BF16)
    return high, (x - high.astype(F32)).astype(BF16)


def times(x, high, low, transposed):
    dims = (((1,), (1 if transposed else 0,)), ((), ()))
    rows = x.shape[0]
    x_high, x_low = split(x)
    both = jnp.concatenate([x_high, x_low], axis=0)
    main = lax.dot_general(both, high, dims, preferred_element_type=F32)
    rest = lax.dot_general(x_high, low, dims, preferred_element_type=F32)
    return main[:rows] + (main[rows:] + rest)


def total_of(x):
    return jnp.sum(jnp.sum(x, axis=0, keepdims=True), axis=1, keepdims=True)


def kernel(
    nma, nf, rhs_in, x0_in, beam_in, noise_in, power_in, smooth_in, sol_s, res_s,
    rhs_s, x0_s, edge_s, beam_s, noise_s, power_s, smooth_s,
    high_s, low_s, x_s, y_s, r_s, v_s, u_s, w_s, mask_s, first_s, halo_s,
    sol_move_s, res_move_s, message_s, early_s, late_s,
    in_sem, beam_sem, halo_send, halo_recv, sum_send, sum_recv, word_sem,
):
    modes, freqs, _, ell = rhs_in.shape
    rank = beam_in.shape[3]
    width = modes * rank
    n = nma * nf
    my_ma, my_f = lax.axis_index("ma"), lax.axis_index("freq")
    me = my_ma * nf + my_f
    last = freqs - 1
    two_sided = nf > 2
    edges = [0, last][:min(nf - 1, 2)]
    inner = [f for f in range(freqs) if f not in edges]

    def at(g):
        return jnp.where(my_f == 0, last - g, g)

    edge_copies = [
        pltpu.make_async_copy(x0_in.at[:, at(f)], edge_s.at[i], in_sem.at[i])
        for i, f in enumerate(edges)
    ]
    x0_copy = pltpu.make_async_copy(x0_in, x0_s, in_sem.at[2])
    rhs_copy = pltpu.make_async_copy(rhs_in, rhs_s, in_sem.at[3])
    small = [
        pltpu.make_async_copy(power_in, power_s, in_sem.at[4]),
        pltpu.make_async_copy(smooth_in, smooth_s, in_sem.at[5]),
        pltpu.make_async_copy(noise_in, noise_s, in_sem.at[6]),
    ]
    beam_copies = [
        pltpu.make_async_copy(beam_in.at[:, at(f)], beam_s.at[f], beam_sem.at[f])
        for f in range(freqs)
    ]
    for copy in edge_copies + [x0_copy] + small + [beam_copies[0], rhs_copy] + beam_copies[1:]:
        copy.start()

    def partners(size, place):
        distances = [1 << bit for bit in range(size.bit_length() - 1)]
        return [place + d * (1 - 2 * (place // d % 2)) for d in distances]

    word = [(my_ma, other) for other in partners(nf, my_f)]
    word += [(other, my_f) for other in partners(nma, my_ma)]
    words = max(len(word) - 1, 0)
    barrier = pltpu.get_barrier_semaphore()
    near = jnp.where(my_f == 0, 1, my_f - 1)
    has_far = (my_f > 0) & (my_f < nf - 1)

    def greet(device):
        pl.semaphore_signal(barrier, inc=1, device_id=device, device_id_type=MESH)

    for device in word:
        greet(device)
    expected = len(word)
    if nf > 2:
        pl.when(my_f > 0)(lambda: greet((my_ma, my_f - 1)))
        pl.when(my_f < nf - 1)(lambda: greet((my_ma, my_f + 1)))
        expected = expected + jnp.minimum(my_f, 1) + jnp.minimum(nf - 1 - my_f, 1)

    steps = list(range(words + 1))

    def advance():
        if steps:
            step = steps.pop(0)
            if step > 0:
                pl.semaphore_wait(word_sem.at[step - 1], 1)
            if step < words:
                pl.semaphore_signal(
                    word_sem.at[step], inc=1, device_id=word[step], device_id_type=MESH
                )

    slots = [(edge_s, first_s), (y_s, halo_s.at[0]), (v_s, halo_s.at[1])]

    def near_copy(kind):
        source, target = slots[kind]
        side = jnp.minimum(my_f // 2, 1) if two_sided else 0
        return pltpu.make_async_remote_copy(
            src_ref=source.at[0], dst_ref=target.at[side],
            send_sem=halo_send.at[kind, 0], recv_sem=halo_recv.at[kind, side],
            device_id=(my_ma, near), device_id_type=MESH,
        )

    def far_copy(kind):
        source, target = slots[kind]
        return pltpu.make_async_remote_copy(
            src_ref=source.at[1], dst_ref=target.at[0],
            send_sem=halo_send.at[kind, 1], recv_sem=halo_recv.at[kind, 0],
            device_id=(my_ma, my_f + 1), device_id_type=MESH,
        )

    def arrival(kind, side):
        slot = slots[kind][1].at[side]
        return pltpu.make_async_copy(slot, slot, halo_recv.at[kind, side])

    def send(kind):
        if nf > 1:
            near_copy(kind).start()
        if two_sided:
            pl.when(has_far)(lambda: far_copy(kind).start())

    def arrive(kind):
        if nf > 1:
            arrival(kind, 0).wait()
        if two_sided:
            pl.when(has_far)(lambda: arrival(kind, 1).wait())

    def sent(kind):
        if nf > 1:
            near_copy(kind).wait_send()
        if two_sided:
            pl.when(has_far)(lambda: far_copy(kind).wait_send())

    def beside(i, value):
        return jnp.where(has_far, value, 0.0) if i else value

    if two_sided:
        @pl.when(jnp.logical_not(has_far))
        def _():
            first_s[1] = jnp.zeros_like(first_s[1])
            halo_s[:, 1] = jnp.zeros_like(halo_s[:, 1])

    for copy in edge_copies:
        copy.wait()
    pl.semaphore_wait(barrier, expected)
    send(0)
    advance()

    x0_copy.wait()
    for copy in small:
        copy.wait()
    for f in range(freqs):
        for b in range(2):
            x_s[f, b * modes:(b + 1) * modes, :] = x0_s[:, at(f), b, :]
    power, smooth = power_s[...], smooth_s[...]
    own = (
        lax.broadcasted_iota(jnp.int32, (modes, width), 1) // rank
        == lax.broadcasted_iota(jnp.int32, (modes, width), 0)
    )
    for f in range(freqs):
        mask_s[f] = jnp.where(own, jnp.concatenate([noise_s[:, at(f), :]] * modes, axis=1), 0.0)

    def project(f, field):
        seen = times(field, high_s[f], low_s[f], True)
        real = seen[:modes, :width] + seen[modes:, width:]
        imaginary = seen[modes:, :width] - seen[:modes, width:]
        return real, imaginary, mask_s[f] * real, mask_s[f] * imaginary

    def back(f, real, imaginary):
        weighted = jnp.concatenate(
            [
                jnp.concatenate([real, -imaginary], axis=1),
                jnp.concatenate([imaginary, real], axis=1),
            ],
            axis=0,
        )
        return times(weighted, high_s[f], low_s[f], False)

    def apply_beam(fs, fields):
        parts = [project(f, field) for f, field in zip(fs, fields)]
        return [back(f, *part[2:]) for f, part in zip(fs, parts)]

    def count(f):
        value = float(f > 0) + float(f < last) + float(nf > 1 and f == 0)
        if two_sided and f == last:
            value = value + jnp.where(has_far, 1.0, 0.0)
        return value

    def local_prior(f, ref):
        value = count(f) * ref[f]
        if f > 0:
            value = value - ref[f - 1]
        if f < last:
            value = value - ref[f + 1]
        return power * ref[f] + smooth * value

    for copy in beam_copies:
        copy.wait()
    rhs_copy.wait()
    for f in range(freqs):
        for a in range(2):
            rows = slice(a * width, (a + 1) * width)
            high, low = split(beam_s[f, :, a].reshape(width, ell))
            high_s[f, rows] = high
            low_s[f, rows] = low
    order = edges + inner
    images = apply_beam(order, [x_s[f] for f in order])
    for f, image in zip(order, images):
        rhs = jnp.concatenate([rhs_s[:, at(f), 0, :], rhs_s[:, at(f), 1, :]], axis=0)
        value = rhs - image - local_prior(f, x_s)
        if f in edges:
            y_s[edges.index(f)] = value
        else:
            r_s[f] = value
    send(1)
    advance()

    for f, image in zip(inner, apply_beam(inner, [r_s[f] for f in inner])):
        u_s[f] = image
    advance()

    arrive(0)
    for i, f in enumerate(edges):
        halo = jnp.concatenate([first_s[i, :, 0, :], first_s[i, :, 1, :]], axis=0)
        r_s[f] = y_s[i] + smooth * halo
    for i, (f, image) in enumerate(zip(edges, apply_beam(edges, [r_s[f] for f in edges]))):
        v_s[i] = image + local_prior(f, r_s)
    send(2)
    advance()

    for f in inner:
        u_s[f] = u_s[f] + local_prior(f, r_s)
    seen = {f: project(f, u_s[f]) for f in inner}
    advance()

    arrive(1)
    for i, f in enumerate(edges):
        u_s[f] = v_s[i] - beside(i, smooth * (halo_s[0, i] + smooth * x_s[f]))
    for f in edges:
        seen[f] = project(f, u_s[f])
    norm = jnp.zeros((2 * modes, ell), F32)
    curve, square, cube = norm, norm, norm
    beam_part = jnp.zeros((modes, width), F32)
    for f in inner + edges:
        real, imaginary, real_weighted, imaginary_weighted = seen[f]
        beam_part = beam_part + (real * real_weighted + imaginary * imaginary_weighted)
        w_s[f] = local_prior(f, u_s)
        norm = norm + r_s[f] * r_s[f]
        curve = curve + r_s[f] * u_s[f]
        square = square + u_s[f] * u_s[f]
        cube = cube + u_s[f] * w_s[f]
    lane = lax.broadcasted_iota(jnp.int32, (1, 128), 1)
    message = jnp.zeros((1, 128), F32)
    for i, part in enumerate((norm, curve, square, cube)):
        total = total_of(part)
        if i == 3:
            total = total + total_of(beam_part)
        message = jnp.where(lane == i, total, message)
    message_s[0] = message
    early_s[me] = message

    while steps:
        advance()

    def share(source, target, turn, offset):
        slot = my_ma if turn and nf == 2 else me
        pltpu.make_async_remote_copy(
            src_ref=message_s.at[source], dst_ref=target.at[slot],
            send_sem=sum_send.at[turn], recv_sem=sum_recv.at[turn],
            device_id=(lax.rem(my_ma + offset // nf, nma), lax.rem(my_f + offset % nf, nf)),
            device_id_type=MESH,
        ).start()

    def share_all(source, target, turn):
        stride = nf if turn and nf == 2 else 1
        if n > 64:
            def body(i, carry):
                share(source, target, turn, i * stride)
                return carry

            lax.fori_loop(1, n // stride, body, 0)
        else:
            offsets = range(stride, n, stride)
            for offset in sorted(offsets, key=lambda o: abs(2 * (o // nf) - nma)):
                share(source, target, turn, offset)

    def landed(target, sem):
        count_in = target.shape[0] - 1
        if count_in:
            rows = target.at[pl.ds(0, count_in)]
            pltpu.make_async_copy(rows, rows, sem).wait()

    share_all(0, early_s, 0)
    for f in inner + edges:
        w_s[f] = w_s[f] + back(f, *seen[f][2:])

    arrive(2)
    cross = jnp.zeros((2 * modes, ell), F32)
    nexts = []
    for i, f in enumerate(edges):
        pull = beside(i, smooth * (halo_s[1, i] - smooth * r_s[f]))
        nexts.append(pull)
        cross = cross + pull * u_s[f]
    message = jnp.sum(cross, axis=0, keepdims=True)
    message = sum(message[:, i:i + 128] for i in range(0, ell, 128))
    late_s[my_ma if nf == 2 else me] = message
    message_s[1] = message
    share_all(1, late_s, 1)
    for f, pull in zip(edges, nexts):
        w_s[f] = w_s[f] - pull

    for kind in range(3):
        sent(kind)
    landed(early_s, sum_recv.at[0])
    total = jnp.sum(early_s[...], axis=0)
    m0, m1, m2, m3 = (
        jnp.sum(jnp.where(lane == i, total, 0.0), axis=1, keepdims=True) for i in range(4)
    )
    step = m0 / m1
    norm_next = step * (step * m2 - m1)
    growth = norm_next / m0
    curve_part = m1 - 2.0 * step * m2 + step * step * m3 - growth * norm_next / step
    cross_scale = step * step * (2.0 if nf == 2 else 1.0)
    for f in range(freqs):
        x, r, u, w = x_s[f], r_s[f], u_s[f], w_s[f]
        for b in range(2):
            rows = slice(b * modes, (b + 1) * modes)
            sol_s[:, at(f), b, :] = x[rows] + step * r[rows]
            res_s[:, at(f), b, :] = r[rows] - step * u[rows]
            sol_move_s[:, at(f), b, :] = (1.0 + growth) * r[rows] - step * u[rows]
            res_move_s[:, at(f), b, :] = (1.0 + growth) * u[rows] - step * w[rows]
    landed(early_s, sum_send.at[0])
    landed(late_s, sum_send.at[1])

    landed(late_s, sum_recv.at[1])
    crossed = jnp.sum(jnp.sum(late_s[...], axis=0), axis=1, keepdims=True)
    step_next = norm_next / (curve_part - cross_scale * crossed)
    sol_s[...] = sol_s[...] + step_next * sol_move_s[...]
    res_s[...] = res_s[...] - step_next * res_move_s[...]


def write_out(sol_in, res_in, sol_out, res_out, sem):
    copies = [
        pltpu.make_async_copy(sol_in, sol_out, sem.at[0]),
        pltpu.make_async_copy(res_in, res_out, sem.at[1]),
    ]
    for copy in copies:
        copy.start()
    for copy in copies:
        copy.wait()


def shards(right_side, start_field, beam, noise, inv_power, smooth):
    nma, nf = lax.axis_size("ma"), lax.axis_size("freq")
    modes, freqs, _, ell = right_side.shape
    rank = beam.shape[3]
    width = modes * rank
    sides = 2 if nf > 2 else 1
    vmem_spec = pl.BlockSpec(memory_space=pltpu.VMEM)
    any_spec = pl.BlockSpec(memory_space=pl.ANY)
    field = pltpu.VMEM(right_side.shape, F32)
    edge = pltpu.VMEM((sides, modes, 2, ell), F32)
    slab = pltpu.VMEM((freqs, 2 * modes, ell), F32)
    edge_slab = pltpu.VMEM((sides, 2 * modes, ell), F32)
    half = pltpu.VMEM((freqs, 2 * width, ell), BF16)
    outs = pl.pallas_call(
        functools.partial(kernel, nma, nf),
        out_shape=[field] * 2,
        in_specs=[any_spec] * 6,
        out_specs=[vmem_spec] * 2,
        scratch_shapes=[
            field, field, edge,
            pltpu.VMEM((freqs, modes, 2, rank, ell), F32),
            pltpu.VMEM(noise.shape, F32),
            pltpu.VMEM((1, ell), F32), pltpu.VMEM((1, ell), F32),
            half, half,
            slab, edge_slab, slab, edge_slab, slab, slab,
            pltpu.VMEM((freqs, modes, width), F32),
            edge,
            pltpu.VMEM((2, sides, 2 * modes, ell), F32),
            field, field,
            pltpu.VMEM((2, 1, 128), F32),
            pltpu.VMEM((nma * nf, 1, 128), F32),
            pltpu.VMEM((nma if nf == 2 else nma * nf, 1, 128), F32),
            pltpu.SemaphoreType.DMA((7,)),
            pltpu.SemaphoreType.DMA((freqs,)),
            pltpu.SemaphoreType.DMA((3, sides)),
            pltpu.SemaphoreType.DMA((3, sides)),
            pltpu.SemaphoreType.DMA((2,)),
            pltpu.SemaphoreType.DMA((2,)),
            pltpu.SemaphoreType.REGULAR((max((nma * nf).bit_length() - 2, 1),)),
        ],
        compiler_params=pltpu.CompilerParams(
            collective_id=0, has_side_effects=True, vmem_limit_bytes=67043328 - 2 * right_side.size * 4
        ),
        name="solve",
    )(right_side, start_field, beam, noise, inv_power[None], smooth[None])
    return pl.pallas_call(
        write_out,
        out_shape=[jax.ShapeDtypeStruct(right_side.shape, F32)] * 2,
        in_specs=[vmem_spec] * 2,
        out_specs=[any_spec] * 2,
        scratch_shapes=[pltpu.SemaphoreType.DMA((2,))],
        compiler_params=pltpu.CompilerParams(vmem_limit_bytes=1024 * 1024),
        name="write_out",
    )(*outs)


def solution(mesh):
    in_specs = (
        P("ma", "freq", None, None),
        P("ma", "freq", None, None),
        P("ma", "freq", None, None, None),
        P("ma", "freq", None),
        P(),
        P(),
    )
    out_specs = (P("ma", "freq", None, None), P("ma", "freq", None, None))
    return jax.shard_map(shards, mesh=mesh, in_specs=in_specs, out_specs=out_specs, check_vma=False)
```

```python
import functools

import jax
import jax.numpy as jnp
from jax import lax
from jax.experimental import pallas as pl
from jax.experimental.pallas import tpu as pltpu
from jax.sharding import PartitionSpec as P

MESH = pl.DeviceIdType.MESH
F32, BF16 = jnp.float32, jnp.bfloat16


def split(x):
    high = x.astype(BF16)
    return high, (x - high.astype(F32)).astype(BF16)


def times(x, high, low, transposed):
    dims = (((1,), (1 if transposed else 0,)), ((), ()))
    rows = x.shape[0]
    x_high, x_low = split(x)
    both = jnp.concatenate([x_high, x_low], axis=0)
    main = lax.dot_general(both, high, dims, preferred_element_type=F32)
    rest = lax.dot_general(x_high, low, dims, preferred_element_type=F32)
    return main[:rows] + (main[rows:] + rest)


def folded(parts):
    row = lax.broadcasted_iota(jnp.int32, parts[0].shape, 0)
    upper = row < 4
    fours = [
        jnp.where(upper, parts[s], parts[s + 4])
        + pltpu.roll(jnp.where(upper, parts[s + 4], parts[s]), 4, 0)
        for s in range(4)
    ]
    even = row // 2 % 2 == 0
    twos = [
        jnp.where(
            even, fours[s] + pltpu.roll(fours[s], 6, 0), fours[s + 2] + pltpu.roll(fours[s + 2], 2, 0)
        )
        for s in range(2)
    ]
    return jnp.where(
        row % 2 == 0, twos[0] + pltpu.roll(twos[0], 7, 0), twos[1] + pltpu.roll(twos[1], 1, 0)
    )


def total_of(x):
    return jnp.sum(jnp.sum(x, axis=0, keepdims=True), axis=1, keepdims=True)


def kernel(
    nma, nf, rhs_in, x0_in, beam_in, noise_in, power_in, smooth_in, sol_s, res_s,
    rhs_s, x0_s, edge_s, beam_s, noise_s, power_s, smooth_s,
    high_s, low_s, x_s, y_s, r_s, v_s, u_s, w_s, mask_s, column_s, first_s, halo_s,
    sol_move_s, res_move_s, message_s, early_s, late_s,
    in_sem, beam_sem, halo_send, halo_recv, sum_send, sum_recv, word_sem,
):
    modes, freqs, _, ell = rhs_in.shape
    rank = beam_in.shape[3]
    width = modes * rank
    n = nma * nf
    my_ma, my_f = lax.axis_index("ma"), lax.axis_index("freq")
    me = my_ma * nf + my_f
    last = freqs - 1
    two_sided = nf > 2
    groups = modes // 4
    edges = [0, last][:min(nf - 1, 2)]
    inner = [f for f in range(freqs) if f not in edges]

    def at(g):
        return jnp.where(my_f == 0, last - g, g)

    edge_copies = [
        pltpu.make_async_copy(x0_in.at[:, at(f)], edge_s.at[i], in_sem.at[i])
        for i, f in enumerate(edges)
    ]
    x0_copy = pltpu.make_async_copy(x0_in, x0_s, in_sem.at[2])
    rhs_copy = pltpu.make_async_copy(rhs_in, rhs_s, in_sem.at[3])
    small = [
        pltpu.make_async_copy(power_in, power_s, in_sem.at[4]),
        pltpu.make_async_copy(smooth_in, smooth_s, in_sem.at[5]),
        pltpu.make_async_copy(noise_in, noise_s, in_sem.at[6]),
    ]
    beam_copies = [
        pltpu.make_async_copy(beam_in.at[:, at(f)], beam_s.at[f], beam_sem.at[f])
        for f in range(freqs)
    ]
    for copy in edge_copies + [x0_copy] + small + [beam_copies[0], rhs_copy] + beam_copies[1:]:
        copy.start()

    def partners(size, place):
        distances = [1 << bit for bit in range(size.bit_length() - 1)]
        return [place + d * (1 - 2 * (place // d % 2)) for d in distances]

    word = [(my_ma, other) for other in partners(nf, my_f)]
    word += [(other, my_f) for other in partners(nma, my_ma)]
    words = max(len(word) - 1, 0)
    barrier = pltpu.get_barrier_semaphore()
    near = jnp.where(my_f == 0, 1, my_f - 1)
    has_far = (my_f > 0) & (my_f < nf - 1)

    def greet(device):
        pl.semaphore_signal(barrier, inc=1, device_id=device, device_id_type=MESH)

    for device in word:
        greet(device)
    expected = len(word)
    if nf > 2:
        pl.when(my_f > 0)(lambda: greet((my_ma, my_f - 1)))
        pl.when(my_f < nf - 1)(lambda: greet((my_ma, my_f + 1)))
        expected = expected + jnp.minimum(my_f, 1) + jnp.minimum(nf - 1 - my_f, 1)

    steps = list(range(words + 1))

    def advance():
        if steps:
            step = steps.pop(0)
            if step > 0:
                pl.semaphore_wait(word_sem.at[step - 1], 1)
            if step < words:
                pl.semaphore_signal(
                    word_sem.at[step], inc=1, device_id=word[step], device_id_type=MESH
                )

    def piece(kind, g):
        if kind == 0:
            rows = pl.ds(4 * g, 4)
            return (lambda i: edge_s.at[i, rows]), (lambda i: first_s.at[i, rows])
        source = (y_s, v_s)[kind - 1]
        rows = pl.ds(8 * g, 8)
        return (lambda i: source.at[i, rows]), (lambda i: halo_s.at[kind - 1, i, rows])

    def near_copy(kind, g):
        source, target = piece(kind, g)
        side = jnp.minimum(my_f // 2, 1) if two_sided else 0
        return pltpu.make_async_remote_copy(
            src_ref=source(0), dst_ref=target(side),
            send_sem=halo_send.at[kind, g, 0], recv_sem=halo_recv.at[kind, g, side],
            device_id=(my_ma, near), device_id_type=MESH,
        )

    def far_copy(kind, g):
        source, target = piece(kind, g)
        return pltpu.make_async_remote_copy(
            src_ref=source(1), dst_ref=target(0),
            send_sem=halo_send.at[kind, g, 1], recv_sem=halo_recv.at[kind, g, 0],
            device_id=(my_ma, my_f + 1), device_id_type=MESH,
        )

    def arrival(kind, g, side):
        slot = piece(kind, g)[1](side)
        return pltpu.make_async_copy(slot, slot, halo_recv.at[kind, g, side])

    def send(kind, g):
        if nf > 1:
            near_copy(kind, g).start()
        if two_sided:
            pl.when(has_far)(lambda: far_copy(kind, g).start())

    def arrive(kind, g):
        if nf > 1:
            arrival(kind, g, 0).wait()
        if two_sided:
            pl.when(has_far)(lambda: arrival(kind, g, 1).wait())

    def sent(kind, g):
        if nf > 1:
            near_copy(kind, g).wait_send()
        if two_sided:
            pl.when(has_far)(lambda: far_copy(kind, g).wait_send())

    def beside(i, value):
        return jnp.where(has_far, value, 0.0) if i else value

    if two_sided:
        @pl.when(jnp.logical_not(has_far))
        def _():
            first_s[1] = jnp.zeros_like(first_s[1])
            halo_s[:, 1] = jnp.zeros_like(halo_s[:, 1])

    for copy in edge_copies:
        copy.wait()
    pl.semaphore_wait(barrier, expected)
    for g in range(groups):
        send(0, g)
    advance()

    x0_copy.wait()
    for copy in small:
        copy.wait()
    def rows_of(ref, *at_f):
        place = (slice(None), *at_f)
        return jnp.concatenate(
            [ref[(slice(4 * g, 4 * g + 4), *place[1:], b)] for g in range(groups) for b in range(2)],
            axis=0,
        )

    def group(g):
        return slice(8 * g, 8 * g + 8)

    for f in range(freqs):
        x_s[f] = rows_of(x0_s, at(f))
    power, smooth = power_s[...], smooth_s[...]
    row = lax.broadcasted_iota(jnp.int32, (2 * modes, width), 0)
    own = lax.broadcasted_iota(jnp.int32, (2 * modes, width), 1) // rank == row // 8 * 4 + row % 4
    sign = jnp.where(row % 8 < 4, 1.0, -1.0)
    for i, f in enumerate(inner):
        levels = noise_s[:, at(f), :]
        levels = jnp.concatenate(
            [levels[4 * g:4 * g + 4] for g in range(groups) for _ in range(2)], axis=0
        )
        mask_s[i] = jnp.where(own, jnp.concatenate([levels] * modes, axis=1), 0.0)
    unit = (
        lax.broadcasted_iota(jnp.int32, (rank, rank), 0)
        == lax.broadcasted_iota(jnp.int32, (rank, rank), 1)
    )
    for i, f in enumerate(edges):
        levels = noise_s[:, at(f), :]
        for m in range(modes):
            column = jnp.sum(jnp.where(unit, levels[m:m + 1], 0.0), axis=1, keepdims=True)
            column_s[i, m] = jnp.broadcast_to(column, (rank, 128))

    def swapped(x):
        return jnp.concatenate([pltpu.roll(x[group(g)], 4, 0) for g in range(groups)], axis=0)

    def project(f, field):
        i = inner.index(f)
        seen = times(field, high_s[i], low_s[i], True)
        parts = seen[:, :width] + sign * swapped(seen[:, width:])
        return parts, mask_s[i] * parts

    def back(f, weighted):
        i = inner.index(f)
        weighted = jnp.concatenate([weighted, -sign * swapped(weighted)], axis=1)
        return times(weighted, high_s[i], low_s[i], False)

    def apply_beam(fs, fields):
        parts = [project(f, field) for f, field in zip(fs, fields)]
        return [back(f, part[1]) for f, part in zip(fs, parts)]

    def wide(x):
        return jnp.concatenate([x] * (ell // 128), axis=1)

    def edge_project(f, g, field):
        parts = []
        for j in range(4):
            m = 4 * g + j
            real_beam, imaginary_beam = beam_s[f, m, 0], beam_s[f, m, 1]
            real_field, imaginary_field = field[j:j + 1], field[4 + j:5 + j]
            levels = column_s[edges.index(f), m]
            real = jnp.sum(
                real_beam * real_field + imaginary_beam * imaginary_field, axis=1, keepdims=True
            )
            imaginary = jnp.sum(
                real_beam * imaginary_field - imaginary_beam * real_field, axis=1, keepdims=True
            )
            parts.append((real, imaginary, levels * real, levels * imaginary))
        return parts

    def edge_back(f, g, parts):
        reals, imaginaries = [], []
        for j, (_, _, real, imaginary) in enumerate(parts):
            m = 4 * g + j
            real, imaginary = wide(real), wide(imaginary)
            real_beam, imaginary_beam = beam_s[f, m, 0], beam_s[f, m, 1]
            for found, value in (
                (reals, real_beam * real - imaginary_beam * imaginary),
                (imaginaries, real_beam * imaginary + imaginary_beam * real),
            ):
                found.append(sum(value[k:k + 8] for k in range(0, rank, 8)))
        return folded(reals + imaginaries)

    def edge_beam(f, g, field):
        return edge_back(f, g, edge_project(f, g, field))

    def count(f):
        value = float(f > 0) + float(f < last) + float(nf > 1 and f == 0)
        if two_sided and f == last:
            value = value + jnp.where(has_far, 1.0, 0.0)
        return value

    def local_prior(f, ref, rows=slice(None)):
        value = count(f) * ref[f, rows]
        if f > 0:
            value = value - ref[f - 1, rows]
        if f < last:
            value = value - ref[f + 1, rows]
        return power * ref[f, rows] + smooth * value

    for copy in beam_copies:
        copy.wait()
    rhs_copy.wait()
    for i, f in enumerate(inner):
        for a in range(2):
            rows = slice(a * width, (a + 1) * width)
            high, low = split(beam_s[f, :, a].reshape(width, ell))
            high_s[i, rows] = high
            low_s[i, rows] = low
    images = apply_beam(inner, [x_s[f] for f in inner])
    for i, f in enumerate(edges):
        for g in range(groups):
            rows = group(g)
            image = edge_beam(f, g, x_s[f, rows])
            y_s[i, rows] = rows_of(rhs_s, at(f))[rows] - image - local_prior(f, x_s, rows)
    for g in range(groups):
        send(1, g)
    for f, image in zip(inner, images):
        r_s[f] = rows_of(rhs_s, at(f)) - image - local_prior(f, x_s)
    advance()

    for f, image in zip(inner, apply_beam(inner, [r_s[f] for f in inner])):
        u_s[f] = image
    advance()

    for g in range(groups):
        arrive(0, g)
        rows = group(g)
        for i, f in enumerate(edges):
            halo = jnp.concatenate([first_s[i, 4 * g:4 * g + 4, b, :] for b in range(2)], axis=0)
            r_s[f, rows] = y_s[i, rows] + smooth * halo
        for i, f in enumerate(edges):
            v_s[i, rows] = edge_beam(f, g, r_s[f, rows]) + local_prior(f, r_s, rows)
        send(2, g)
    advance()

    for f in inner:
        u_s[f] = u_s[f] + local_prior(f, r_s)
    seen = {f: project(f, u_s[f]) for f in inner}
    advance()

    for g in range(groups):
        arrive(1, g)
    for i, f in enumerate(edges):
        u_s[f] = v_s[i] - beside(i, smooth * (halo_s[0, i] + smooth * x_s[f]))
    edge_seen = {f: [edge_project(f, g, u_s[f, group(g)]) for g in range(groups)] for f in edges}
    norm = jnp.zeros((2 * modes, ell), F32)
    curve, square, cube = norm, norm, norm
    beam_part = jnp.zeros((2 * modes, width), F32)
    column_part = jnp.zeros((rank, 128), F32)
    for f in inner + edges:
        if f in inner:
            beam_part = beam_part + seen[f][0] * seen[f][1]
        else:
            for parts in edge_seen[f]:
                for real, imaginary, real_weighted, imaginary_weighted in parts:
                    column_part = column_part + (real * real_weighted + imaginary * imaginary_weighted)
        w_s[f] = local_prior(f, u_s)
        norm = norm + r_s[f] * r_s[f]
        curve = curve + r_s[f] * u_s[f]
        square = square + u_s[f] * u_s[f]
        cube = cube + u_s[f] * w_s[f]
    lane = lax.broadcasted_iota(jnp.int32, (1, 128), 1)
    message = jnp.zeros((1, 128), F32)
    for i, part in enumerate((norm, curve, square, cube)):
        total = total_of(part)
        if i == 3:
            total = total + total_of(beam_part) + jnp.sum(column_part, axis=0, keepdims=True)
        message = jnp.where(lane == i, total, message)
    message_s[0] = message
    early_s[me] = message

    while steps:
        advance()

    def share(source, target, turn, offset):
        slot = my_ma if turn and nf == 2 else me
        pltpu.make_async_remote_copy(
            src_ref=message_s.at[source], dst_ref=target.at[slot],
            send_sem=sum_send.at[turn], recv_sem=sum_recv.at[turn],
            device_id=(lax.rem(my_ma + offset // nf, nma), lax.rem(my_f + offset % nf, nf)),
            device_id_type=MESH,
        ).start()

    def share_all(source, target, turn):
        stride = nf if turn and nf == 2 else 1
        if n > 64:
            def body(i, carry):
                share(source, target, turn, i * stride)
                return carry

            lax.fori_loop(1, n // stride, body, 0)
        else:
            offsets = range(stride, n, stride)
            for offset in sorted(offsets, key=lambda o: abs(2 * (o // nf) - nma)):
                share(source, target, turn, offset)

    def landed(target, sem):
        count_in = target.shape[0] - 1
        if count_in:
            rows = target.at[pl.ds(0, count_in)]
            pltpu.make_async_copy(rows, rows, sem).wait()

    share_all(0, early_s, 0)
    for f in inner:
        w_s[f] = w_s[f] + back(f, seen[f][1])
    for f in edges:
        for g in range(groups):
            w_s[f, group(g)] = w_s[f, group(g)] + edge_back(f, g, edge_seen[f][g])

    cross = jnp.zeros((8, ell), F32)
    nexts = []
    for g in range(groups):
        arrive(2, g)
        rows = group(g)
        for i, f in enumerate(edges):
            pull = beside(i, smooth * (halo_s[1, i, rows] - smooth * r_s[f, rows]))
            nexts.append((f, rows, pull))
            cross = cross + pull * u_s[f, rows]
    message = jnp.sum(cross, axis=0, keepdims=True)
    message = sum(message[:, i:i + 128] for i in range(0, ell, 128))
    late_s[my_ma if nf == 2 else me] = message
    message_s[1] = message
    share_all(1, late_s, 1)
    for f, rows, pull in nexts:
        w_s[f, rows] = w_s[f, rows] - pull

    for kind in range(3):
        for g in range(groups):
            sent(kind, g)
    landed(early_s, sum_recv.at[0])
    total = jnp.sum(early_s[...], axis=0)
    m0, m1, m2, m3 = (
        jnp.sum(jnp.where(lane == i, total, 0.0), axis=1, keepdims=True) for i in range(4)
    )
    step = m0 / m1
    norm_next = step * (step * m2 - m1)
    growth = norm_next / m0
    curve_part = m1 - 2.0 * step * m2 + step * step * m3 - growth * norm_next / step
    cross_scale = step * step * (2.0 if nf == 2 else 1.0)
    for f in range(freqs):
        x, r, u, w = x_s[f], r_s[f], u_s[f], w_s[f]
        for target, value in (
            (sol_s, x + step * r),
            (res_s, r - step * u),
            (sol_move_s, (1.0 + growth) * r - step * u),
            (res_move_s, (1.0 + growth) * u - step * w),
        ):
            for g in range(groups):
                for b in range(2):
                    start = 8 * g + 4 * b
                    target[4 * g:4 * g + 4, at(f), b, :] = value[start:start + 4]
    landed(early_s, sum_send.at[0])
    landed(late_s, sum_send.at[1])

    landed(late_s, sum_recv.at[1])
    crossed = jnp.sum(jnp.sum(late_s[...], axis=0), axis=1, keepdims=True)
    step_next = norm_next / (curve_part - cross_scale * crossed)
    sol_s[...] = sol_s[...] + step_next * sol_move_s[...]
    res_s[...] = res_s[...] - step_next * res_move_s[...]


def write_out(sol_in, res_in, sol_out, res_out, sem):
    copies = [
        pltpu.make_async_copy(sol_in, sol_out, sem.at[0]),
        pltpu.make_async_copy(res_in, res_out, sem.at[1]),
    ]
    for copy in copies:
        copy.start()
    for copy in copies:
        copy.wait()


def shards(right_side, start_field, beam, noise, inv_power, smooth):
    nma, nf = lax.axis_size("ma"), lax.axis_size("freq")
    modes, freqs, _, ell = right_side.shape
    rank = beam.shape[3]
    width = modes * rank
    sides = 2 if nf > 2 else 1
    vmem_spec = pl.BlockSpec(memory_space=pltpu.VMEM)
    any_spec = pl.BlockSpec(memory_space=pl.ANY)
    field = pltpu.VMEM(right_side.shape, F32)
    edge = pltpu.VMEM((sides, modes, 2, ell), F32)
    slab = pltpu.VMEM((freqs, 2 * modes, ell), F32)
    edge_slab = pltpu.VMEM((sides, 2 * modes, ell), F32)
    inner = max(freqs - min(nf - 1, 2), 1)
    half = pltpu.VMEM((inner, 2 * width, ell), BF16)
    outs = pl.pallas_call(
        functools.partial(kernel, nma, nf),
        out_shape=[field] * 2,
        in_specs=[any_spec] * 6,
        out_specs=[vmem_spec] * 2,
        scratch_shapes=[
            field, field, edge,
            pltpu.VMEM((freqs, modes, 2, rank, ell), F32),
            pltpu.VMEM(noise.shape, F32),
            pltpu.VMEM((1, ell), F32), pltpu.VMEM((1, ell), F32),
            half, half,
            slab, edge_slab, slab, edge_slab, slab, slab,
            pltpu.VMEM((inner, 2 * modes, width), F32),
            pltpu.VMEM((sides, modes, rank, 128), F32),
            edge,
            pltpu.VMEM((2, sides, 2 * modes, ell), F32),
            field, field,
            pltpu.VMEM((2, 1, 128), F32),
            pltpu.VMEM((nma * nf, 1, 128), F32),
            pltpu.VMEM((nma if nf == 2 else nma * nf, 1, 128), F32),
            pltpu.SemaphoreType.DMA((7,)),
            pltpu.SemaphoreType.DMA((freqs,)),
            pltpu.SemaphoreType.DMA((3, modes // 4, sides)),
            pltpu.SemaphoreType.DMA((3, modes // 4, sides)),
            pltpu.SemaphoreType.DMA((2,)),
            pltpu.SemaphoreType.DMA((2,)),
            pltpu.SemaphoreType.REGULAR((max((nma * nf).bit_length() - 2, 1),)),
        ],
        compiler_params=pltpu.CompilerParams(
            collective_id=0, has_side_effects=True, vmem_limit_bytes=67043328 - 2 * right_side.size * 4
        ),
        name="solve",
    )(right_side, start_field, beam, noise, inv_power[None], smooth[None])
    return pl.pallas_call(
        write_out,
        out_shape=[jax.ShapeDtypeStruct(right_side.shape, F32)] * 2,
        in_specs=[vmem_spec] * 2,
        out_specs=[any_spec] * 2,
        scratch_shapes=[pltpu.SemaphoreType.DMA((2,))],
        compiler_params=pltpu.CompilerParams(vmem_limit_bytes=1024 * 1024),
        name="write_out",
    )(*outs)


def solution(mesh):
    in_specs = (
        P("ma", "freq", None, None),
        P("ma", "freq", None, None),
        P("ma", "freq", None, None, None),
        P("ma", "freq", None),
        P(),
        P(),
    )
    out_specs = (P("ma", "freq", None, None), P("ma", "freq", None, None))
    return jax.shard_map(shards, mesh=mesh, in_specs=in_specs, out_specs=out_specs, check_vma=False)
```

```python
import functools

import jax
import jax.numpy as jnp
from jax import lax
from jax.experimental import pallas as pl
from jax.experimental.pallas import tpu as pltpu
from jax.sharding import PartitionSpec as P

MESH = pl.DeviceIdType.MESH
F32, BF16 = jnp.float32, jnp.bfloat16


def split(x):
    high = x.astype(BF16)
    return high, (x - high.astype(F32)).astype(BF16)


def times(x, high, low, transposed):
    dims = (((1,), (1 if transposed else 0,)), ((), ()))
    rows = x.shape[0]
    x_high, x_low = split(x)
    both = jnp.concatenate([x_high, x_low], axis=0)
    main = lax.dot_general(both, high, dims, preferred_element_type=F32)
    rest = lax.dot_general(x_high, low, dims, preferred_element_type=F32)
    return main[:rows] + (main[rows:] + rest)


def folded(parts):
    row = lax.broadcasted_iota(jnp.int32, parts[0].shape, 0)
    upper = row < 4
    fours = [
        jnp.where(upper, parts[s], parts[s + 4])
        + pltpu.roll(jnp.where(upper, parts[s + 4], parts[s]), 4, 0)
        for s in range(4)
    ]
    even = row // 2 % 2 == 0
    twos = [
        jnp.where(
            even, fours[s] + pltpu.roll(fours[s], 6, 0), fours[s + 2] + pltpu.roll(fours[s + 2], 2, 0)
        )
        for s in range(2)
    ]
    return jnp.where(
        row % 2 == 0, twos[0] + pltpu.roll(twos[0], 7, 0), twos[1] + pltpu.roll(twos[1], 1, 0)
    )


def total_of(x):
    return jnp.sum(jnp.sum(x, axis=0, keepdims=True), axis=1, keepdims=True)


def kernel(
    nma, nf, rhs_in, x0_in, beam_in, noise_in, power_in, smooth_in, sol_s, res_s,
    rhs_s, x0_s, edge_s, beam_s, noise_s, power_s, smooth_s,
    high_s, low_s, x_s, y_s, r_s, v_s, u_s, w_s, mask_s, column_s, first_s, halo_s,
    sol_move_s, res_move_s, pull_s, partner_s, cross_s, message_s, early_s, late_s,
    in_sem, beam_sem, halo_send, halo_recv, pair_sem, sum_send, sum_recv, word_sem,
):
    modes, freqs, _, ell = rhs_in.shape
    rank = beam_in.shape[3]
    width = modes * rank
    n = nma * nf
    my_ma, my_f = lax.axis_index("ma"), lax.axis_index("freq")
    me = my_ma * nf + my_f
    last = freqs - 1
    two_sided = nf > 2
    paired = nf == 2 and nma % 2 == 0
    helper = my_ma % 2 == 1
    groups = modes // 4
    edges = [0, last][:min(nf - 1, 2)]
    inner = [f for f in range(freqs) if f not in edges]

    def at(g):
        return jnp.where(my_f == 0, last - g, g)

    edge_copies = [
        pltpu.make_async_copy(x0_in.at[:, at(f)], edge_s.at[i], in_sem.at[i])
        for i, f in enumerate(edges)
    ]
    x0_copy = pltpu.make_async_copy(x0_in, x0_s, in_sem.at[2])
    rhs_copy = pltpu.make_async_copy(rhs_in, rhs_s, in_sem.at[3])
    small = [
        pltpu.make_async_copy(power_in, power_s, in_sem.at[4]),
        pltpu.make_async_copy(smooth_in, smooth_s, in_sem.at[5]),
        pltpu.make_async_copy(noise_in, noise_s, in_sem.at[6]),
    ]
    beam_copies = [
        pltpu.make_async_copy(beam_in.at[:, at(f)], beam_s.at[f], beam_sem.at[f])
        for f in range(freqs)
    ]
    for copy in edge_copies:
        copy.start()

    def partners(size, place):
        distances = [1 << bit for bit in range(size.bit_length() - 1)]
        return [place + d * (1 - 2 * (place // d % 2)) for d in distances]

    word = [(my_ma, other) for other in partners(nf, my_f)]
    word += [(other, my_f) for other in partners(nma, my_ma)]
    words = max(len(word) - 1, 0)
    barrier = pltpu.get_barrier_semaphore()
    near = jnp.where(my_f == 0, 1, my_f - 1)
    has_far = (my_f > 0) & (my_f < nf - 1)

    def greet(device):
        pl.semaphore_signal(barrier, inc=1, device_id=device, device_id_type=MESH)

    greeted = list(word)
    if paired:
        greeted.append((my_ma + 1 - 2 * (my_ma % 2), 1 - my_f))
    for i, device in enumerate(greeted):
        greet(device)
        if i == 0:
            for copy in [x0_copy] + small + [beam_copies[0], rhs_copy] + beam_copies[1:]:
                copy.start()
    expected = len(greeted)
    if nf > 2:
        pl.when(my_f > 0)(lambda: greet((my_ma, my_f - 1)))
        pl.when(my_f < nf - 1)(lambda: greet((my_ma, my_f + 1)))
        expected = expected + jnp.minimum(my_f, 1) + jnp.minimum(nf - 1 - my_f, 1)

    steps = list(range(words + 1))

    def advance():
        if steps:
            step = steps.pop(0)
            if step > 0:
                pl.semaphore_wait(word_sem.at[step - 1], 1)
            if step < words:
                pl.semaphore_signal(
                    word_sem.at[step], inc=1, device_id=word[step], device_id_type=MESH
                )

    def piece(kind, g):
        if kind == 0:
            rows = pl.ds(4 * g, 4)
            return (lambda i: edge_s.at[i, rows]), (lambda i: first_s.at[i, rows])
        source = (y_s, v_s)[kind - 1]
        rows = pl.ds(8 * g, 8)
        return (lambda i: source.at[i, rows]), (lambda i: halo_s.at[kind - 1, i, rows])

    def near_copy(kind, g):
        source, target = piece(kind, g)
        side = jnp.minimum(my_f // 2, 1) if two_sided else 0
        return pltpu.make_async_remote_copy(
            src_ref=source(0), dst_ref=target(side),
            send_sem=halo_send.at[kind, g, 0], recv_sem=halo_recv.at[kind, g, side],
            device_id=(my_ma, near), device_id_type=MESH,
        )

    def far_copy(kind, g):
        source, target = piece(kind, g)
        return pltpu.make_async_remote_copy(
            src_ref=source(1), dst_ref=target(0),
            send_sem=halo_send.at[kind, g, 1], recv_sem=halo_recv.at[kind, g, 0],
            device_id=(my_ma, my_f + 1), device_id_type=MESH,
        )

    def arrival(kind, g, side):
        slot = piece(kind, g)[1](side)
        return pltpu.make_async_copy(slot, slot, halo_recv.at[kind, g, side])

    def send(kind, g):
        if nf > 1:
            near_copy(kind, g).start()
        if two_sided:
            pl.when(has_far)(lambda: far_copy(kind, g).start())

    def arrive(kind, g):
        if nf > 1:
            arrival(kind, g, 0).wait()
        if two_sided:
            pl.when(has_far)(lambda: arrival(kind, g, 1).wait())

    def sent(kind, g):
        if nf > 1:
            near_copy(kind, g).wait_send()
        if two_sided:
            pl.when(has_far)(lambda: far_copy(kind, g).wait_send())

    def cross_copy(g):
        rows = pl.ds(8 * g, 8)
        return pltpu.make_async_remote_copy(
            src_ref=v_s.at[0, rows], dst_ref=cross_s.at[rows],
            send_sem=pair_sem.at[g], recv_sem=pair_sem.at[groups + g],
            device_id=(my_ma + 1, 1 - my_f), device_id_type=MESH,
        )

    def pull_copy():
        return pltpu.make_async_remote_copy(
            src_ref=pull_s, dst_ref=partner_s,
            send_sem=pair_sem.at[2 * groups], recv_sem=pair_sem.at[2 * groups + 1],
            device_id=(my_ma + 1, my_f), device_id_type=MESH,
        )

    def beside(i, value):
        return jnp.where(has_far, value, 0.0) if i else value

    if two_sided:
        @pl.when(jnp.logical_not(has_far))
        def _():
            first_s[1] = jnp.zeros_like(first_s[1])
            halo_s[:, 1] = jnp.zeros_like(halo_s[:, 1])

    for copy in edge_copies:
        copy.wait()
    pl.semaphore_wait(barrier, expected)
    for g in range(groups):
        send(0, g)
    advance()

    x0_copy.wait()
    for copy in small:
        copy.wait()
    def rows_of(ref, *at_f):
        place = (slice(None), *at_f)
        return jnp.concatenate(
            [ref[(slice(4 * g, 4 * g + 4), *place[1:], b)] for g in range(groups) for b in range(2)],
            axis=0,
        )

    def group(g):
        return slice(8 * g, 8 * g + 8)

    for f in range(freqs):
        x_s[f] = rows_of(x0_s, at(f))
    power, smooth = power_s[...], smooth_s[...]
    row = lax.broadcasted_iota(jnp.int32, (2 * modes, width), 0)
    own = lax.broadcasted_iota(jnp.int32, (2 * modes, width), 1) // rank == row // 8 * 4 + row % 4
    sign = jnp.where(row % 8 < 4, 1.0, -1.0)
    for i, f in enumerate(inner):
        levels = noise_s[:, at(f), :]
        levels = jnp.concatenate(
            [levels[4 * g:4 * g + 4] for g in range(groups) for _ in range(2)], axis=0
        )
        mask_s[i] = jnp.where(own, jnp.concatenate([levels] * modes, axis=1), 0.0)
    unit = (
        lax.broadcasted_iota(jnp.int32, (rank, rank), 0)
        == lax.broadcasted_iota(jnp.int32, (rank, rank), 1)
    )
    for i, f in enumerate(edges):
        levels = noise_s[:, at(f), :]
        for m in range(modes):
            column = jnp.sum(jnp.where(unit, levels[m:m + 1], 0.0), axis=1, keepdims=True)
            column_s[i, m] = jnp.broadcast_to(column, (rank, 128))

    def swapped(x):
        return jnp.concatenate([pltpu.roll(x[group(g)], 4, 0) for g in range(groups)], axis=0)

    def project(f, field):
        i = inner.index(f)
        seen = times(field, high_s[i], low_s[i], True)
        parts = seen[:, :width] + sign * swapped(seen[:, width:])
        return parts, mask_s[i] * parts

    def back(f, weighted):
        i = inner.index(f)
        weighted = jnp.concatenate([weighted, -sign * swapped(weighted)], axis=1)
        return times(weighted, high_s[i], low_s[i], False)

    def apply_beam(fs, fields):
        parts = [project(f, field) for f, field in zip(fs, fields)]
        return [back(f, part[1]) for f, part in zip(fs, parts)]

    def wide(x):
        return jnp.concatenate([x] * (ell // 128), axis=1)

    def edge_project(f, g, field):
        parts = []
        for j in range(4):
            m = 4 * g + j
            real_beam, imaginary_beam = beam_s[f, m, 0], beam_s[f, m, 1]
            real_field, imaginary_field = field[j:j + 1], field[4 + j:5 + j]
            levels = column_s[edges.index(f), m]
            real = jnp.sum(
                real_beam * real_field + imaginary_beam * imaginary_field, axis=1, keepdims=True
            )
            imaginary = jnp.sum(
                real_beam * imaginary_field - imaginary_beam * real_field, axis=1, keepdims=True
            )
            parts.append((real, imaginary, levels * real, levels * imaginary))
        return parts

    def edge_back(f, g, parts):
        reals, imaginaries = [], []
        for j, (_, _, real, imaginary) in enumerate(parts):
            m = 4 * g + j
            real, imaginary = wide(real), wide(imaginary)
            real_beam, imaginary_beam = beam_s[f, m, 0], beam_s[f, m, 1]
            for found, value in (
                (reals, real_beam * real - imaginary_beam * imaginary),
                (imaginaries, real_beam * imaginary + imaginary_beam * real),
            ):
                found.append(sum(value[k:k + 8] for k in range(0, rank, 8)))
        return folded(reals + imaginaries)

    def edge_beam(f, g, field):
        return edge_back(f, g, edge_project(f, g, field))

    def count(f):
        value = float(f > 0) + float(f < last) + float(nf > 1 and f == 0)
        if two_sided and f == last:
            value = value + jnp.where(has_far, 1.0, 0.0)
        return value

    def local_prior(f, ref, rows=slice(None)):
        value = count(f) * ref[f, rows]
        if f > 0:
            value = value - ref[f - 1, rows]
        if f < last:
            value = value - ref[f + 1, rows]
        return power * ref[f, rows] + smooth * value

    for copy in beam_copies:
        copy.wait()
    rhs_copy.wait()
    for i, f in enumerate(inner):
        for a in range(2):
            rows = slice(a * width, (a + 1) * width)
            high, low = split(beam_s[f, :, a].reshape(width, ell))
            high_s[i, rows] = high
            low_s[i, rows] = low
    images = apply_beam(inner, [x_s[f] for f in inner])
    for i, f in enumerate(edges):
        for g in range(groups):
            rows = group(g)
            image = edge_beam(f, g, x_s[f, rows])
            y_s[i, rows] = rows_of(rhs_s, at(f))[rows] - image - local_prior(f, x_s, rows)
    for g in range(groups):
        send(1, g)
    for f, image in zip(inner, images):
        r_s[f] = rows_of(rhs_s, at(f)) - image - local_prior(f, x_s)
    advance()

    for f, image in zip(inner, apply_beam(inner, [r_s[f] for f in inner])):
        u_s[f] = image
    advance()

    for g in range(groups):
        arrive(0, g)
        rows = group(g)
        for i, f in enumerate(edges):
            halo = jnp.concatenate([first_s[i, 4 * g:4 * g + 4, b, :] for b in range(2)], axis=0)
            r_s[f, rows] = y_s[i, rows] + smooth * halo
        for i, f in enumerate(edges):
            v_s[i, rows] = edge_beam(f, g, r_s[f, rows]) + local_prior(f, r_s, rows)
        if paired:
            pl.when(jnp.logical_not(helper))(lambda: cross_copy(g).start())
        else:
            send(2, g)
    if paired:
        for g in range(groups):
            send(2, g)
    advance()

    for f in inner:
        u_s[f] = u_s[f] + local_prior(f, r_s)
    seen = {f: project(f, u_s[f]) for f in inner}
    advance()

    for g in range(groups):
        arrive(1, g)
    for i, f in enumerate(edges):
        u_s[f] = v_s[i] - beside(i, smooth * (halo_s[0, i] + smooth * x_s[f]))
    if paired:
        pull_s[...] = smooth * u_s[0]
        pl.when(jnp.logical_not(helper))(lambda: pull_copy().start())
    edge_seen = {f: [edge_project(f, g, u_s[f, group(g)]) for g in range(groups)] for f in edges}
    norm = jnp.zeros((2 * modes, ell), F32)
    curve, square, cube = norm, norm, norm
    beam_part = jnp.zeros((2 * modes, width), F32)
    column_part = jnp.zeros((rank, 128), F32)
    for f in inner + edges:
        if f in inner:
            beam_part = beam_part + seen[f][0] * seen[f][1]
        else:
            for parts in edge_seen[f]:
                for real, imaginary, real_weighted, imaginary_weighted in parts:
                    column_part = column_part + (real * real_weighted + imaginary * imaginary_weighted)
        w_s[f] = local_prior(f, u_s)
        norm = norm + r_s[f] * r_s[f]
        curve = curve + r_s[f] * u_s[f]
        square = square + u_s[f] * u_s[f]
        cube = cube + u_s[f] * w_s[f]
    lane = lax.broadcasted_iota(jnp.int32, (1, 128), 1)
    message = jnp.zeros((1, 128), F32)
    for i, part in enumerate((norm, curve, square, cube)):
        total = total_of(part)
        if i == 3:
            total = total + total_of(beam_part) + jnp.sum(column_part, axis=0, keepdims=True)
        message = jnp.where(lane == i, total, message)
    if paired:
        message = jnp.where(lane == 4 + my_f, total_of(smooth * r_s[0] * pull_s[...]), message)
    message_s[0] = message
    early_s[me] = message

    while steps:
        advance()

    def share(source, target, slot, turn, offset):
        pltpu.make_async_remote_copy(
            src_ref=message_s.at[source], dst_ref=target.at[slot],
            send_sem=sum_send.at[turn], recv_sem=sum_recv.at[turn],
            device_id=(lax.rem(my_ma + offset // nf, nma), lax.rem(my_f + offset % nf, nf)),
            device_id_type=MESH,
        ).start()

    def share_all(source, target, slot, turn, stride):
        if n > 64:
            def body(i, carry):
                share(source, target, slot, turn, i * stride)
                return carry

            lax.fori_loop(1, n // stride, body, 0)
        else:
            offsets = range(stride, n, stride)
            for offset in sorted(offsets, key=lambda o: abs(2 * (o // nf) - nma) - 4 * (o // nf % 2)):
                share(source, target, slot, turn, offset)

    def landed(target, sem, rows):
        if rows:
            rows = target.at[pl.ds(0, rows)]
            pltpu.make_async_copy(rows, rows, sem).wait()

    def lanes_of(x):
        x = jnp.sum(x, axis=0, keepdims=True)
        return sum(x[:, i:i + 128] for i in range(0, ell, 128))

    share_all(0, early_s, me, 0, 1)
    for f in inner:
        w_s[f] = w_s[f] + back(f, seen[f][1])
    for f in edges:
        for g in range(groups):
            w_s[f, group(g)] = w_s[f, group(g)] + edge_back(f, g, edge_seen[f][g])

    late_rows = late_s.shape[0]
    if paired:
        @pl.when(helper)
        def _():
            cross = jnp.zeros((8, ell), F32)
            for g in range(groups):
                arrive(2, g)
                cross = cross + pull_s[group(g)] * halo_s[1, 0, group(g)]
            pull_copy().wait_recv()
            for g in range(groups):
                cross_copy(g).wait_recv()
                cross = cross + partner_s[group(g)] * cross_s[group(g)]
            message = lanes_of(cross)
            late_s[my_ma // 2] = message
            message_s[1] = message
            share_all(1, late_s, my_ma // 2, 1, nf)

        @pl.when(jnp.logical_not(helper))
        def _():
            for g in range(groups):
                arrive(2, g)
            pull_copy().wait_send()
            for g in range(groups):
                cross_copy(g).wait_send()

        w_s[0] = w_s[0] - smooth * (halo_s[1, 0] - smooth * r_s[0])
    else:
        cross = jnp.zeros((8, ell), F32)
        nexts = []
        for g in range(groups):
            arrive(2, g)
            rows = group(g)
            for i, f in enumerate(edges):
                pull = beside(i, smooth * (halo_s[1, i, rows] - smooth * r_s[f, rows]))
                nexts.append((f, rows, pull))
                cross = cross + pull * u_s[f, rows]
        message = lanes_of(cross)
        late_s[me] = message
        message_s[1] = message
        share_all(1, late_s, me, 1, 1)
        for f, rows, pull in nexts:
            w_s[f, rows] = w_s[f, rows] - pull

    for kind in range(3):
        for g in range(groups):
            sent(kind, g)
    landed(early_s, sum_recv.at[0], n - 1)
    total = jnp.sum(early_s[...], axis=0)
    m0, m1, m2, m3, known = (
        jnp.sum(jnp.where(lane == i, total, 0.0), axis=1, keepdims=True)
        for i in (0, 1, 2, 3, 4 + my_f)
    )
    if paired:
        m3 = m3 + 2.0 * known
    step = m0 / m1
    norm_next = step * (step * m2 - m1)
    growth = norm_next / m0
    curve_part = m1 - 2.0 * step * m2 + step * step * m3 - growth * norm_next / step
    cross_scale = step * step * (2.0 if paired else 1.0)
    for f in range(freqs):
        x, r, u, w = x_s[f], r_s[f], u_s[f], w_s[f]
        for target, value in (
            (sol_s, x + step * r),
            (res_s, r - step * u),
            (sol_move_s, (1.0 + growth) * r - step * u),
            (res_move_s, (1.0 + growth) * u - step * w),
        ):
            for g in range(groups):
                for b in range(2):
                    start = 8 * g + 4 * b
                    target[4 * g:4 * g + 4, at(f), b, :] = value[start:start + 4]
    landed(early_s, sum_send.at[0], n - 1)
    if paired:
        @pl.when(helper)
        def _():
            rows = early_s.at[pl.ds(0, nma - 1)]
            pltpu.make_async_copy(rows, rows, sum_send.at[1]).wait()
            landed(late_s, sum_recv.at[1], late_rows - 1)

        pl.when(jnp.logical_not(helper))(lambda: landed(late_s, sum_recv.at[1], late_rows))
    else:
        landed(late_s, sum_send.at[1], late_rows - 1)
        landed(late_s, sum_recv.at[1], late_rows - 1)
    crossed = jnp.sum(jnp.sum(late_s[...], axis=0), axis=1, keepdims=True)
    step_next = norm_next / (curve_part - cross_scale * crossed)
    sol_s[...] = sol_s[...] + step_next * sol_move_s[...]
    res_s[...] = res_s[...] - step_next * res_move_s[...]


def write_out(sol_in, res_in, sol_out, res_out, sem):
    copies = [
        pltpu.make_async_copy(sol_in, sol_out, sem.at[0]),
        pltpu.make_async_copy(res_in, res_out, sem.at[1]),
    ]
    for copy in copies:
        copy.start()
    for copy in copies:
        copy.wait()


def shards(right_side, start_field, beam, noise, inv_power, smooth):
    nma, nf = lax.axis_size("ma"), lax.axis_size("freq")
    modes, freqs, _, ell = right_side.shape
    rank = beam.shape[3]
    width = modes * rank
    sides = 2 if nf > 2 else 1
    vmem_spec = pl.BlockSpec(memory_space=pltpu.VMEM)
    any_spec = pl.BlockSpec(memory_space=pl.ANY)
    field = pltpu.VMEM(right_side.shape, F32)
    edge = pltpu.VMEM((sides, modes, 2, ell), F32)
    slab = pltpu.VMEM((freqs, 2 * modes, ell), F32)
    edge_slab = pltpu.VMEM((sides, 2 * modes, ell), F32)
    inner = max(freqs - min(nf - 1, 2), 1)
    half = pltpu.VMEM((inner, 2 * width, ell), BF16)
    outs = pl.pallas_call(
        functools.partial(kernel, nma, nf),
        out_shape=[field] * 2,
        in_specs=[any_spec] * 6,
        out_specs=[vmem_spec] * 2,
        scratch_shapes=[
            field, field, edge,
            pltpu.VMEM((freqs, modes, 2, rank, ell), F32),
            pltpu.VMEM(noise.shape, F32),
            pltpu.VMEM((1, ell), F32), pltpu.VMEM((1, ell), F32),
            half, half,
            slab, edge_slab, slab, edge_slab, slab, slab,
            pltpu.VMEM((inner, 2 * modes, width), F32),
            pltpu.VMEM((sides, modes, rank, 128), F32),
            edge,
            pltpu.VMEM((2, sides, 2 * modes, ell), F32),
            field, field,
            pltpu.VMEM((2 * modes, ell), F32), pltpu.VMEM((2 * modes, ell), F32),
            pltpu.VMEM((2 * modes, ell), F32),
            pltpu.VMEM((2, 1, 128), F32),
            pltpu.VMEM((nma * nf, 1, 128), F32),
            pltpu.VMEM((nma // 2 if nf == 2 and nma % 2 == 0 else nma * nf, 1, 128), F32),
            pltpu.SemaphoreType.DMA((7,)),
            pltpu.SemaphoreType.DMA((freqs,)),
            pltpu.SemaphoreType.DMA((3, modes // 4, sides)),
            pltpu.SemaphoreType.DMA((3, modes // 4, sides)),
            pltpu.SemaphoreType.DMA((2 * (modes // 4) + 2,)),
            pltpu.SemaphoreType.DMA((2,)),
            pltpu.SemaphoreType.DMA((2,)),
            pltpu.SemaphoreType.REGULAR((max((nma * nf).bit_length() - 2, 1),)),
        ],
        compiler_params=pltpu.CompilerParams(
            collective_id=0, has_side_effects=True, vmem_limit_bytes=67043328 - 2 * right_side.size * 4
        ),
        name="solve",
    )(right_side, start_field, beam, noise, inv_power[None], smooth[None])
    return pl.pallas_call(
        write_out,
        out_shape=[jax.ShapeDtypeStruct(right_side.shape, F32)] * 2,
        in_specs=[vmem_spec] * 2,
        out_specs=[any_spec] * 2,
        scratch_shapes=[pltpu.SemaphoreType.DMA((2,))],
        compiler_params=pltpu.CompilerParams(vmem_limit_bytes=1024 * 1024),
        name="write_out",
    )(*outs)


def solution(mesh):
    in_specs = (
        P("ma", "freq", None, None),
        P("ma", "freq", None, None),
        P("ma", "freq", None, None, None),
        P("ma", "freq", None),
        P(),
        P(),
    )
    out_specs = (P("ma", "freq", None, None), P("ma", "freq", None, None))
    return jax.shard_map(shards, mesh=mesh, in_specs=in_specs, out_specs=out_specs, check_vma=False)
```

```python
import functools

import jax
import jax.numpy as jnp
from jax import lax
from jax.experimental import pallas as pl
from jax.experimental.pallas import tpu as pltpu
from jax.sharding import PartitionSpec as P

MESH = pl.DeviceIdType.MESH
F32, BF16 = jnp.float32, jnp.bfloat16


def split(x):
    high = x.astype(BF16)
    return high, (x - high.astype(F32)).astype(BF16)


def times(x, high, low, transposed):
    dims = (((1,), (1 if transposed else 0,)), ((), ()))
    rows = x.shape[0]
    x_high, x_low = split(x)
    both = jnp.concatenate([x_high, x_low], axis=0)
    main = lax.dot_general(both, high, dims, preferred_element_type=F32)
    rest = lax.dot_general(x_high, low, dims, preferred_element_type=F32)
    return main[:rows] + (main[rows:] + rest)


def folded(parts):
    row = lax.broadcasted_iota(jnp.int32, parts[0].shape, 0)
    upper = row < 4
    fours = [
        jnp.where(upper, parts[s], parts[s + 4])
        + pltpu.roll(jnp.where(upper, parts[s + 4], parts[s]), 4, 0)
        for s in range(4)
    ]
    even = row // 2 % 2 == 0
    twos = [
        jnp.where(
            even, fours[s] + pltpu.roll(fours[s], 6, 0), fours[s + 2] + pltpu.roll(fours[s + 2], 2, 0)
        )
        for s in range(2)
    ]
    return jnp.where(
        row % 2 == 0, twos[0] + pltpu.roll(twos[0], 7, 0), twos[1] + pltpu.roll(twos[1], 1, 0)
    )


def total_of(x):
    return jnp.sum(jnp.sum(x, axis=0, keepdims=True), axis=1, keepdims=True)


def kernel(
    nma, nf, rhs_in, x0_in, beam_in, noise_in, power_in, smooth_in, sol_s, res_s,
    rhs_s, x0_s, edge_s, beam_s, noise_s, power_s, smooth_s,
    high_s, low_s, x_s, y_s, r_s, v_s, u_s, w_s, mask_s, column_s, first_s, halo_s,
    sol_move_s, res_move_s, pull_s, partner_s, cross_s, message_s, early_s, late_s,
    halo_recv, pair_sem, sum_recv, word_sem, in_sem, beam_sem, halo_send, sum_send,
):
    modes, freqs, _, ell = rhs_in.shape
    rank = beam_in.shape[3]
    width = modes * rank
    n = nma * nf
    my_ma, my_f = lax.axis_index("ma"), lax.axis_index("freq")
    me = my_ma * nf + my_f
    last = freqs - 1
    two_sided = nf > 2
    paired = nf == 2 and nma % 2 == 0
    helper = my_ma % 2 == 1
    groups = modes // 4
    edges = [0, last][:min(nf - 1, 2)]
    inner = [f for f in range(freqs) if f not in edges]
    beside_edge = [f for f in inner if f - 1 in edges or f + 1 in edges]
    apart = [f for f in inner if f not in beside_edge]
    vector = edges + inner[:max(freqs // 2 - len(edges), 0)]
    matrix = [f for f in range(freqs) if f not in vector]

    def at(g):
        return jnp.where(my_f == 0, last - g, g)

    edge_copies = [
        pltpu.make_async_copy(x0_in.at[:, at(f)], edge_s.at[i], in_sem.at[i])
        for i, f in enumerate(edges)
    ]
    x0_copy = pltpu.make_async_copy(x0_in, x0_s, in_sem.at[2])
    rhs_copy = pltpu.make_async_copy(rhs_in, rhs_s, in_sem.at[3])
    small = [
        pltpu.make_async_copy(power_in, power_s, in_sem.at[4]),
        pltpu.make_async_copy(smooth_in, smooth_s, in_sem.at[5]),
        pltpu.make_async_copy(noise_in, noise_s, in_sem.at[6]),
    ]
    beam_copies = [
        pltpu.make_async_copy(beam_in.at[:, at(f)], beam_s.at[f], beam_sem.at[f])
        for f in range(freqs)
    ]
    for copy in edge_copies:
        copy.start()

    def flip(bit):
        d = 1 << (bit if bit < freq_bits else bit - freq_bits)
        place = my_f if bit < freq_bits else my_ma
        return d * (1 - 2 * (place // d % 2))

    def partner(bits):
        return (
            my_ma + sum(flip(bit) for bit in bits if bit >= freq_bits),
            my_f + sum(flip(bit) for bit in bits if bit < freq_bits),
        )

    freq_bits = nf.bit_length() - 1
    bits = freq_bits + nma.bit_length() - 1
    close = min(bits, 3)
    greeted = [
        partner([bit for bit in range(close) if mask >> bit & 1]) for mask in range(1, 1 << close)
    ]
    word = [partner([bit]) for bit in range(close, bits)]
    greeted += word
    words = len(word)
    barrier = pltpu.get_barrier_semaphore()
    near = jnp.where(my_f == 0, 1, my_f - 1)
    has_far = (my_f > 0) & (my_f < nf - 1)

    def greet(device):
        pl.semaphore_signal(barrier, inc=1, device_id=device, device_id_type=MESH)

    for i, device in enumerate(greeted):
        greet(device)
        if i == 0:
            others = [beam_copies[f] for f in edges] + [rhs_copy] + [beam_copies[f] for f in inner]
            for copy in [x0_copy] + small + others:
                copy.start()
    expected = len(greeted)
    if nf > 2:
        pl.when(my_f > 0)(lambda: greet((my_ma, my_f - 1)))
        pl.when(my_f < nf - 1)(lambda: greet((my_ma, my_f + 1)))
        expected = expected + jnp.minimum(my_f, 1) + jnp.minimum(nf - 1 - my_f, 1)

    steps = list(range(words + 1))

    def advance():
        if steps:
            step = steps.pop(0)
            if step > 0:
                pl.semaphore_wait(word_sem.at[step - 1], 1)
            if step < words:
                pl.semaphore_signal(
                    word_sem.at[step], inc=1, device_id=word[step], device_id_type=MESH
                )

    def piece(kind, g):
        if kind == 0:
            rows = pl.ds(4 * g, 4)
            return (lambda i: edge_s.at[i, rows]), (lambda i: first_s.at[i, rows])
        source = (y_s, v_s)[kind - 1]
        rows = pl.ds(8 * g, 8)
        return (lambda i: source.at[i, rows]), (lambda i: halo_s.at[kind - 1, i, rows])

    def near_copy(kind, g):
        source, target = piece(kind, g)
        side = jnp.minimum(my_f // 2, 1) if two_sided else 0
        return pltpu.make_async_remote_copy(
            src_ref=source(0), dst_ref=target(side),
            send_sem=halo_send.at[kind, g, 0], recv_sem=halo_recv.at[kind, g, side],
            device_id=(my_ma, near), device_id_type=MESH,
        )

    def far_copy(kind, g):
        source, target = piece(kind, g)
        return pltpu.make_async_remote_copy(
            src_ref=source(1), dst_ref=target(0),
            send_sem=halo_send.at[kind, g, 1], recv_sem=halo_recv.at[kind, g, 0],
            device_id=(my_ma, my_f + 1), device_id_type=MESH,
        )

    def arrival(kind, g, side):
        slot = piece(kind, g)[1](side)
        return pltpu.make_async_copy(slot, slot, halo_recv.at[kind, g, side])

    def send(kind, g):
        if nf > 1:
            near_copy(kind, g).start()
        if two_sided:
            pl.when(has_far)(lambda: far_copy(kind, g).start())

    def arrive(kind, g):
        if nf > 1:
            arrival(kind, g, 0).wait()
        if two_sided:
            pl.when(has_far)(lambda: arrival(kind, g, 1).wait())

    def sent(kind, g):
        if nf > 1:
            near_copy(kind, g).wait_send()
        if two_sided:
            pl.when(has_far)(lambda: far_copy(kind, g).wait_send())

    def cross_copy(g):
        rows = pl.ds(8 * g, 8)
        return pltpu.make_async_remote_copy(
            src_ref=v_s.at[0, rows], dst_ref=cross_s.at[rows],
            send_sem=pair_sem.at[g], recv_sem=pair_sem.at[groups + g],
            device_id=(my_ma + 1, 1 - my_f), device_id_type=MESH,
        )

    def pull_copy():
        return pltpu.make_async_remote_copy(
            src_ref=pull_s, dst_ref=partner_s,
            send_sem=pair_sem.at[2 * groups], recv_sem=pair_sem.at[2 * groups + 1],
            device_id=(my_ma + 1, my_f), device_id_type=MESH,
        )

    def beside(i, value):
        return jnp.where(has_far, value, 0.0) if i else value

    if two_sided:
        @pl.when(jnp.logical_not(has_far))
        def _():
            first_s[1] = jnp.zeros_like(first_s[1])
            halo_s[:, 1] = jnp.zeros_like(halo_s[:, 1])

    for copy in edge_copies:
        copy.wait()
    pl.semaphore_wait(barrier, expected)
    for g in range(groups):
        send(0, g)
    advance()

    x0_copy.wait()
    for copy in small:
        copy.wait()
    def rows_of(ref, *at_f):
        place = (slice(None), *at_f)
        return jnp.concatenate(
            [ref[(slice(4 * g, 4 * g + 4), *place[1:], b)] for g in range(groups) for b in range(2)],
            axis=0,
        )

    def group(g):
        return slice(8 * g, 8 * g + 8)

    for f in range(freqs):
        x_s[f] = rows_of(x0_s, at(f))
    power, smooth = power_s[...], smooth_s[...]
    row = lax.broadcasted_iota(jnp.int32, (2 * modes, width), 0)
    own = lax.broadcasted_iota(jnp.int32, (2 * modes, width), 1) // rank == row // 8 * 4 + row % 4
    sign = jnp.where(row % 8 < 4, 1.0, -1.0)
    for i, f in enumerate(matrix):
        levels = noise_s[:, at(f), :]
        levels = jnp.concatenate(
            [levels[4 * g:4 * g + 4] for g in range(groups) for _ in range(2)], axis=0
        )
        mask_s[i] = jnp.where(own, jnp.concatenate([levels] * modes, axis=1), 0.0)
    unit = (
        lax.broadcasted_iota(jnp.int32, (rank, rank), 0)
        == lax.broadcasted_iota(jnp.int32, (rank, rank), 1)
    )
    for i, f in enumerate(vector):
        levels = noise_s[:, at(f), :]
        for m in range(modes):
            column = jnp.sum(jnp.where(unit, levels[m:m + 1], 0.0), axis=1, keepdims=True)
            column_s[i, m] = jnp.broadcast_to(column, (rank, 128))

    def swapped(x):
        return jnp.concatenate([pltpu.roll(x[group(g)], 4, 0) for g in range(groups)], axis=0)

    def matrix_project(f, field):
        i = matrix.index(f)
        seen = times(field, high_s[i], low_s[i], True)
        parts = seen[:, :width] + sign * swapped(seen[:, width:])
        return parts, mask_s[i] * parts

    def matrix_back(f, seen):
        i = matrix.index(f)
        weighted = jnp.concatenate([seen[1], -sign * swapped(seen[1])], axis=1)
        return times(weighted, high_s[i], low_s[i], False)

    def wide(x):
        return jnp.concatenate([x] * (ell // 128), axis=1)

    def group_project(f, g, field):
        parts = []
        for j in range(4):
            m = 4 * g + j
            real_beam, imaginary_beam = beam_s[f, m, 0], beam_s[f, m, 1]
            real_field, imaginary_field = field[j:j + 1], field[4 + j:5 + j]
            levels = column_s[vector.index(f), m]
            real = jnp.sum(
                real_beam * real_field + imaginary_beam * imaginary_field, axis=1, keepdims=True
            )
            imaginary = jnp.sum(
                real_beam * imaginary_field - imaginary_beam * real_field, axis=1, keepdims=True
            )
            parts.append((real, imaginary, levels * real, levels * imaginary))
        return parts

    def group_back(f, g, parts):
        reals, imaginaries = [], []
        for j, (_, _, real, imaginary) in enumerate(parts):
            m = 4 * g + j
            real, imaginary = wide(real), wide(imaginary)
            real_beam, imaginary_beam = beam_s[f, m, 0], beam_s[f, m, 1]
            for found, value in (
                (reals, real_beam * real - imaginary_beam * imaginary),
                (imaginaries, real_beam * imaginary + imaginary_beam * real),
            ):
                found.append(sum(value[k:k + 8] for k in range(0, rank, 8)))
        return folded(reals + imaginaries)

    def group_beam(f, g, field):
        return group_back(f, g, group_project(f, g, field))

    def project(f, ref):
        if f in matrix:
            return matrix_project(f, ref[f])
        return [group_project(f, g, ref[f, group(g)]) for g in range(groups)]

    def back(f, seen):
        if f in matrix:
            return matrix_back(f, seen)
        return jnp.concatenate([group_back(f, g, seen[g]) for g in range(groups)], axis=0)

    def apply_beam(fs, ref):
        fs = [f for f in fs if f in matrix] + [f for f in fs if f in vector]
        seen = [project(f, ref) for f in fs]
        return {f: back(f, found) for f, found in zip(fs, seen)}

    def count(f):
        value = float(f > 0) + float(f < last) + float(nf > 1 and f == 0)
        if two_sided and f == last:
            value = value + jnp.where(has_far, 1.0, 0.0)
        return value

    def local_prior(f, ref, rows=slice(None)):
        value = count(f) * ref[f, rows]
        if f > 0:
            value = value - ref[f - 1, rows]
        if f < last:
            value = value - ref[f + 1, rows]
        return power * ref[f, rows] + smooth * value

    for f in edges:
        beam_copies[f].wait()
    rhs_copy.wait()
    for i, f in enumerate(edges):
        for g in range(groups):
            rows = group(g)
            image = group_beam(f, g, x_s[f, rows])
            y_s[i, rows] = rows_of(rhs_s, at(f))[rows] - image - local_prior(f, x_s, rows)
    for g in range(groups):
        send(1, g)

    for f in inner:
        beam_copies[f].wait()
    for i, f in enumerate(matrix):
        for a in range(2):
            rows = slice(a * width, (a + 1) * width)
            high, low = split(beam_s[f, :, a].reshape(width, ell))
            high_s[i, rows] = high
            low_s[i, rows] = low
    for f, image in apply_beam(inner, x_s).items():
        r_s[f] = rows_of(rhs_s, at(f)) - image - local_prior(f, x_s)
    for f, image in apply_beam(inner, r_s).items():
        u_s[f] = image + local_prior(f, r_s) if f in apart else image
    seen = {f: project(f, u_s) for f in apart}
    advance()

    for g in range(groups):
        arrive(0, g)
        rows = group(g)
        for i, f in enumerate(edges):
            halo = jnp.concatenate([first_s[i, 4 * g:4 * g + 4, b, :] for b in range(2)], axis=0)
            r_s[f, rows] = y_s[i, rows] + smooth * halo
        for i, f in enumerate(edges):
            v_s[i, rows] = group_beam(f, g, r_s[f, rows]) + local_prior(f, r_s, rows)
        if paired:
            pl.when(jnp.logical_not(helper))(lambda: cross_copy(g).start())
        else:
            send(2, g)
    if paired:
        for g in range(groups):
            send(2, g)

    for f in beside_edge:
        u_s[f] = u_s[f] + local_prior(f, r_s)
    seen |= {f: project(f, u_s) for f in beside_edge}

    for g in range(groups):
        arrive(1, g)
    for i, f in enumerate(edges):
        u_s[f] = v_s[i] - beside(i, smooth * (halo_s[0, i] + smooth * x_s[f]))
    if paired:
        pull_s[...] = smooth * u_s[0]
        pl.when(jnp.logical_not(helper))(lambda: pull_copy().start())
    seen |= {f: project(f, u_s) for f in edges}
    norm = jnp.zeros((2 * modes, ell), F32)
    curve, square, cube = norm, norm, norm
    beam_part = jnp.zeros((2 * modes, width), F32)
    column_part = jnp.zeros((rank, 128), F32)
    for f in inner + edges:
        if f in matrix:
            beam_part = beam_part + seen[f][0] * seen[f][1]
        else:
            for parts in seen[f]:
                for real, imaginary, real_weighted, imaginary_weighted in parts:
                    column_part = column_part + (real * real_weighted + imaginary * imaginary_weighted)
        w_s[f] = local_prior(f, u_s)
        norm = norm + r_s[f] * r_s[f]
        curve = curve + r_s[f] * u_s[f]
        square = square + u_s[f] * u_s[f]
        cube = cube + u_s[f] * w_s[f]
    lane = lax.broadcasted_iota(jnp.int32, (1, 128), 1)
    message = jnp.zeros((1, 128), F32)
    for i, part in enumerate((norm, curve, square, cube)):
        total = total_of(part)
        if i == 3:
            total = total + total_of(beam_part) + jnp.sum(column_part, axis=0, keepdims=True)
        message = jnp.where(lane == i, total, message)
    if paired:
        message = jnp.where(lane == 4 + my_f, total_of(smooth * r_s[0] * pull_s[...]), message)
    message_s[0] = message
    early_s[me] = message

    while steps:
        advance()

    def share(source, target, slot, turn, offset):
        pltpu.make_async_remote_copy(
            src_ref=message_s.at[source], dst_ref=target.at[slot],
            send_sem=sum_send.at[turn], recv_sem=sum_recv.at[turn],
            device_id=(lax.rem(my_ma + offset // nf, nma), lax.rem(my_f + offset % nf, nf)),
            device_id_type=MESH,
        ).start()

    def share_all(source, target, slot, turn, stride):
        if n > 64:
            def body(i, carry):
                share(source, target, slot, turn, i * stride)
                return carry

            lax.fori_loop(1, n // stride, body, 0)
        else:
            offsets = range(stride, n, stride)
            for offset in sorted(offsets, key=lambda o: abs(2 * (o // nf) - nma) - 4 * (o // nf % 2)):
                share(source, target, slot, turn, offset)

    def landed(target, sem, rows):
        if rows:
            rows = target.at[pl.ds(0, rows)]
            pltpu.make_async_copy(rows, rows, sem).wait()

    def lanes_of(x):
        x = jnp.sum(x, axis=0, keepdims=True)
        return sum(x[:, i:i + 128] for i in range(0, ell, 128))

    share_all(0, early_s, me, 0, 1)
    for f in matrix + vector:
        w_s[f] = w_s[f] + back(f, seen[f])

    late_rows = late_s.shape[0]
    if paired:
        @pl.when(helper)
        def _():
            cross = jnp.zeros((8, ell), F32)
            for g in range(groups):
                arrive(2, g)
                cross = cross + pull_s[group(g)] * halo_s[1, 0, group(g)]
            pull_copy().wait_recv()
            for g in range(groups):
                cross_copy(g).wait_recv()
                cross = cross + partner_s[group(g)] * cross_s[group(g)]
            message = lanes_of(cross)
            late_s[my_ma // 2] = message
            message_s[1] = message
            share_all(1, late_s, my_ma // 2, 1, nf)

        @pl.when(jnp.logical_not(helper))
        def _():
            for g in range(groups):
                arrive(2, g)
            pull_copy().wait_send()
            for g in range(groups):
                cross_copy(g).wait_send()

        w_s[0] = w_s[0] - smooth * (halo_s[1, 0] - smooth * r_s[0])
    else:
        cross = jnp.zeros((8, ell), F32)
        nexts = []
        for g in range(groups):
            arrive(2, g)
            rows = group(g)
            for i, f in enumerate(edges):
                pull = beside(i, smooth * (halo_s[1, i, rows] - smooth * r_s[f, rows]))
                nexts.append((f, rows, pull))
                cross = cross + pull * u_s[f, rows]
        message = lanes_of(cross)
        late_s[me] = message
        message_s[1] = message
        share_all(1, late_s, me, 1, 1)
        for f, rows, pull in nexts:
            w_s[f, rows] = w_s[f, rows] - pull

    for kind in range(3):
        for g in range(groups):
            sent(kind, g)
    landed(early_s, sum_recv.at[0], n - 1)
    total = jnp.sum(early_s[...], axis=0)
    m0, m1, m2, m3, known = (
        jnp.sum(jnp.where(lane == i, total, 0.0), axis=1, keepdims=True)
        for i in (0, 1, 2, 3, 4 + my_f)
    )
    if paired:
        m3 = m3 + 2.0 * known
    step = m0 / m1
    norm_next = step * (step * m2 - m1)
    growth = norm_next / m0
    curve_part = m1 - 2.0 * step * m2 + step * step * m3 - growth * norm_next / step
    cross_scale = step * step * (2.0 if paired else 1.0)
    for f in range(freqs):
        x, r, u, w = x_s[f], r_s[f], u_s[f], w_s[f]
        for target, value in (
            (sol_s, x + step * r),
            (res_s, r - step * u),
            (sol_move_s, (1.0 + growth) * r - step * u),
            (res_move_s, (1.0 + growth) * u - step * w),
        ):
            for g in range(groups):
                for b in range(2):
                    start = 8 * g + 4 * b
                    target[4 * g:4 * g + 4, at(f), b, :] = value[start:start + 4]
    landed(early_s, sum_send.at[0], n - 1)
    if paired:
        @pl.when(helper)
        def _():
            rows = early_s.at[pl.ds(0, nma - 1)]
            pltpu.make_async_copy(rows, rows, sum_send.at[1]).wait()
            landed(late_s, sum_recv.at[1], late_rows - 1)

        pl.when(jnp.logical_not(helper))(lambda: landed(late_s, sum_recv.at[1], late_rows))
    else:
        landed(late_s, sum_send.at[1], late_rows - 1)
        landed(late_s, sum_recv.at[1], late_rows - 1)
    crossed = jnp.sum(jnp.sum(late_s[...], axis=0), axis=1, keepdims=True)
    step_next = norm_next / (curve_part - cross_scale * crossed)
    sol_s[...] = sol_s[...] + step_next * sol_move_s[...]
    res_s[...] = res_s[...] - step_next * res_move_s[...]


def scoped_kernel(nma, nf, sides, *refs):
    modes, freqs = refs[0].shape[:2]
    dma = pltpu.SemaphoreType.DMA
    pl.run_scoped(
        functools.partial(kernel, nma, nf, *refs),
        dma((7,)), dma((freqs,)), dma((3, modes // 4, sides)), dma((2,)),
    )


def write_out(sol_in, res_in, sol_out, res_out, sem):
    copies = [
        pltpu.make_async_copy(sol_in, sol_out, sem.at[0]),
        pltpu.make_async_copy(res_in, res_out, sem.at[1]),
    ]
    for copy in copies:
        copy.start()
    for copy in copies:
        copy.wait()


def shards(right_side, start_field, beam, noise, inv_power, smooth):
    nma, nf = lax.axis_size("ma"), lax.axis_size("freq")
    modes, freqs, _, ell = right_side.shape
    rank = beam.shape[3]
    width = modes * rank
    sides = 2 if nf > 2 else 1
    vmem_spec = pl.BlockSpec(memory_space=pltpu.VMEM)
    any_spec = pl.BlockSpec(memory_space=pl.ANY)
    field = pltpu.VMEM(right_side.shape, F32)
    edge = pltpu.VMEM((sides, modes, 2, ell), F32)
    slab = pltpu.VMEM((freqs, 2 * modes, ell), F32)
    edge_slab = pltpu.VMEM((sides, 2 * modes, ell), F32)
    vector = max(min(nf - 1, 2), freqs // 2)
    matrix = max(freqs - vector, 1)
    half = pltpu.VMEM((matrix, 2 * width, ell), BF16)
    outs = pl.pallas_call(
        functools.partial(scoped_kernel, nma, nf, sides),
        out_shape=[field] * 2,
        in_specs=[any_spec] * 6,
        out_specs=[vmem_spec] * 2,
        scratch_shapes=[
            field, field, edge,
            pltpu.VMEM((freqs, modes, 2, rank, ell), F32),
            pltpu.VMEM(noise.shape, F32),
            pltpu.VMEM((1, ell), F32), pltpu.VMEM((1, ell), F32),
            half, half,
            slab, edge_slab, slab, edge_slab, slab, slab,
            pltpu.VMEM((matrix, 2 * modes, width), F32),
            pltpu.VMEM((vector, modes, rank, 128), F32),
            edge,
            pltpu.VMEM((2, sides, 2 * modes, ell), F32),
            field, field,
            pltpu.VMEM((2 * modes, ell), F32), pltpu.VMEM((2 * modes, ell), F32),
            pltpu.VMEM((2 * modes, ell), F32),
            pltpu.VMEM((2, 1, 128), F32),
            pltpu.VMEM((nma * nf, 1, 128), F32),
            pltpu.VMEM((nma // 2 if nf == 2 and nma % 2 == 0 else nma * nf, 1, 128), F32),
            pltpu.SemaphoreType.DMA((3, modes // 4, sides)),
            pltpu.SemaphoreType.DMA((2 * (modes // 4) + 2,)),
            pltpu.SemaphoreType.DMA((2,)),
            pltpu.SemaphoreType.REGULAR((max((nma * nf).bit_length() - 4, 1),)),
        ],
        compiler_params=pltpu.CompilerParams(
            collective_id=0, has_side_effects=True, vmem_limit_bytes=67043328 - 2 * right_side.size * 4
        ),
        name="solve",
    )(right_side, start_field, beam, noise, inv_power[None], smooth[None])
    return pl.pallas_call(
        write_out,
        out_shape=[jax.ShapeDtypeStruct(right_side.shape, F32)] * 2,
        in_specs=[vmem_spec] * 2,
        out_specs=[any_spec] * 2,
        scratch_shapes=[pltpu.SemaphoreType.DMA((2,))],
        compiler_params=pltpu.CompilerParams(vmem_limit_bytes=1024 * 1024),
        name="write_out",
    )(*outs)


def solution(mesh):
    in_specs = (
        P("ma", "freq", None, None),
        P("ma", "freq", None, None),
        P("ma", "freq", None, None, None),
        P("ma", "freq", None),
        P(),
        P(),
    )
    out_specs = (P("ma", "freq", None, None), P("ma", "freq", None, None))
    return jax.shard_map(shards, mesh=mesh, in_specs=in_specs, out_specs=out_specs, check_vma=False)
```

```python
import functools

import jax
import jax.numpy as jnp
from jax import lax
from jax.experimental import pallas as pl
from jax.experimental.pallas import tpu as pltpu
from jax.sharding import PartitionSpec as P

MESH = pl.DeviceIdType.MESH
F32, BF16 = jnp.float32, jnp.bfloat16


def split(x):
    high = x.astype(BF16)
    return high, (x - high.astype(F32)).astype(BF16)


def times(x, high, low, transposed):
    dims = (((1,), (1 if transposed else 0,)), ((), ()))
    rows = x.shape[0]
    x_high, x_low = split(x)
    both = jnp.concatenate([x_high, x_low], axis=0)
    main = lax.dot_general(both, high, dims, preferred_element_type=F32)
    rest = lax.dot_general(x_high, low, dims, preferred_element_type=F32)
    return main[:rows] + (main[rows:] + rest)


def folded(parts):
    row = lax.broadcasted_iota(jnp.int32, parts[0].shape, 0)
    upper = row < 4
    fours = [
        jnp.where(upper, parts[s], parts[s + 4])
        + pltpu.roll(jnp.where(upper, parts[s + 4], parts[s]), 4, 0)
        for s in range(4)
    ]
    even = row // 2 % 2 == 0
    twos = [
        jnp.where(
            even, fours[s] + pltpu.roll(fours[s], 6, 0), fours[s + 2] + pltpu.roll(fours[s + 2], 2, 0)
        )
        for s in range(2)
    ]
    return jnp.where(
        row % 2 == 0, twos[0] + pltpu.roll(twos[0], 7, 0), twos[1] + pltpu.roll(twos[1], 1, 0)
    )


def total_of(x):
    return jnp.sum(jnp.sum(x, axis=0, keepdims=True), axis=1, keepdims=True)


def kernel(
    nma, nf, rhs_in, x0_in, beam_in, noise_in, power_in, smooth_in, sol_s, res_s,
    rhs_s, x0_s, edge_s, beam_s, noise_s, power_s, smooth_s,
    high_s, low_s, x_s, y_s, r_s, v_s, u_s, w_s, mask_s, column_s, first_s, halo_s,
    sol_move_s, res_move_s, pull_s, partner_s, cross_s, message_s, early_s, late_s,
    halo_recv, pair_sem, sum_recv, word_sem, in_sem, beam_sem, halo_send, sum_send,
):
    modes, freqs, _, ell = rhs_in.shape
    rank = beam_in.shape[3]
    width = modes * rank
    n = nma * nf
    my_ma, my_f = lax.axis_index("ma"), lax.axis_index("freq")
    me = my_ma * nf + my_f
    last = freqs - 1
    two_sided = nf > 2
    paired = nf == 2 and nma % 2 == 0
    helper = my_ma % 2 == 1
    groups = modes // 4
    edges = [0, last][:min(nf - 1, 2)]
    inner = [f for f in range(freqs) if f not in edges]
    beside_edge = [f for f in inner if f - 1 in edges or f + 1 in edges]
    apart = [f for f in inner if f not in beside_edge]
    vector = edges + inner[:max(freqs // 2 - len(edges), 0)]
    matrix = [f for f in range(freqs) if f not in vector]

    def at(g):
        return jnp.where(my_f == 0, last - g, g)

    edge_copies = [
        pltpu.make_async_copy(x0_in.at[:, at(f)], edge_s.at[i], in_sem.at[i])
        for i, f in enumerate(edges)
    ]
    x0_copy = pltpu.make_async_copy(x0_in, x0_s, in_sem.at[2])
    rhs_copy = pltpu.make_async_copy(rhs_in, rhs_s, in_sem.at[3])
    small = [
        pltpu.make_async_copy(power_in, power_s, in_sem.at[4]),
        pltpu.make_async_copy(smooth_in, smooth_s, in_sem.at[5]),
        pltpu.make_async_copy(noise_in, noise_s, in_sem.at[6]),
    ]
    beam_copies = [
        pltpu.make_async_copy(beam_in.at[:, at(f)], beam_s.at[f], beam_sem.at[f])
        for f in range(freqs)
    ]
    for copy in edge_copies:
        copy.start()

    def flip(bit):
        d = 1 << (bit if bit < freq_bits else bit - freq_bits)
        place = my_f if bit < freq_bits else my_ma
        return d * (1 - 2 * (place // d % 2))

    def partner(bits):
        return (
            my_ma + sum(flip(bit) for bit in bits if bit >= freq_bits),
            my_f + sum(flip(bit) for bit in bits if bit < freq_bits),
        )

    freq_bits = nf.bit_length() - 1
    bits = freq_bits + nma.bit_length() - 1
    close = min(bits, 3)
    greeted = [
        partner([bit for bit in range(close) if mask >> bit & 1]) for mask in range(1, 1 << close)
    ]
    word = [partner([bit]) for bit in range(close, bits)]
    greeted += word
    words = len(word)
    barrier = pltpu.get_barrier_semaphore()
    near = jnp.where(my_f == 0, 1, my_f - 1)
    has_far = (my_f > 0) & (my_f < nf - 1)

    def greet(device):
        pl.semaphore_signal(barrier, inc=1, device_id=device, device_id_type=MESH)

    for i, device in enumerate(greeted):
        greet(device)
        if i == 0:
            others = [beam_copies[f] for f in edges] + [rhs_copy] + [beam_copies[f] for f in inner]
            for copy in [x0_copy] + small + others:
                copy.start()
    expected = len(greeted)
    if nf > 2:
        pl.when(my_f > 0)(lambda: greet((my_ma, my_f - 1)))
        pl.when(my_f < nf - 1)(lambda: greet((my_ma, my_f + 1)))
        expected = expected + jnp.minimum(my_f, 1) + jnp.minimum(nf - 1 - my_f, 1)

    steps = list(range(words + 1))

    def advance():
        if steps:
            step = steps.pop(0)
            if step > 0:
                pl.semaphore_wait(word_sem.at[step - 1], 1)
            if step < words:
                pl.semaphore_signal(
                    word_sem.at[step], inc=1, device_id=word[step], device_id_type=MESH
                )

    def piece(kind, g):
        if kind == 0:
            rows = pl.ds(4 * g, 4)
            return (lambda i: edge_s.at[i, rows]), (lambda i: first_s.at[i, rows])
        source = (y_s, v_s)[kind - 1]
        rows = pl.ds(8 * g, 8)
        return (lambda i: source.at[i, rows]), (lambda i: halo_s.at[kind - 1, i, rows])

    def near_copy(kind, g):
        source, target = piece(kind, g)
        side = jnp.minimum(my_f // 2, 1) if two_sided else 0
        return pltpu.make_async_remote_copy(
            src_ref=source(0), dst_ref=target(side),
            send_sem=halo_send.at[kind, g, 0], recv_sem=halo_recv.at[kind, g, side],
            device_id=(my_ma, near), device_id_type=MESH,
        )

    def far_copy(kind, g):
        source, target = piece(kind, g)
        return pltpu.make_async_remote_copy(
            src_ref=source(1), dst_ref=target(0),
            send_sem=halo_send.at[kind, g, 1], recv_sem=halo_recv.at[kind, g, 0],
            device_id=(my_ma, my_f + 1), device_id_type=MESH,
        )

    def arrival(kind, g, side):
        slot = piece(kind, g)[1](side)
        return pltpu.make_async_copy(slot, slot, halo_recv.at[kind, g, side])

    def send(kind, g):
        if nf > 1:
            near_copy(kind, g).start()
        if two_sided:
            pl.when(has_far)(lambda: far_copy(kind, g).start())

    def arrive(kind, g):
        if nf > 1:
            arrival(kind, g, 0).wait()
        if two_sided:
            pl.when(has_far)(lambda: arrival(kind, g, 1).wait())

    def sent(kind, g):
        if nf > 1:
            near_copy(kind, g).wait_send()
        if two_sided:
            pl.when(has_far)(lambda: far_copy(kind, g).wait_send())

    def cross_copy(g):
        rows = pl.ds(8 * g, 8)
        return pltpu.make_async_remote_copy(
            src_ref=v_s.at[0, rows], dst_ref=cross_s.at[rows],
            send_sem=pair_sem.at[g], recv_sem=pair_sem.at[groups + g],
            device_id=(my_ma + 1, 1 - my_f), device_id_type=MESH,
        )

    def pull_copy():
        return pltpu.make_async_remote_copy(
            src_ref=pull_s, dst_ref=partner_s,
            send_sem=pair_sem.at[2 * groups], recv_sem=pair_sem.at[2 * groups + 1],
            device_id=(my_ma + 1, my_f), device_id_type=MESH,
        )

    def beside(i, value):
        return jnp.where(has_far, value, 0.0) if i else value

    if two_sided:
        @pl.when(jnp.logical_not(has_far))
        def _():
            first_s[1] = jnp.zeros_like(first_s[1])
            halo_s[:, 1] = jnp.zeros_like(halo_s[:, 1])

    for copy in edge_copies:
        copy.wait()
    pl.semaphore_wait(barrier, expected)
    for g in range(groups):
        send(0, g)
    advance()

    x0_copy.wait()
    for copy in small:
        copy.wait()
    def rows_of(ref, *at_f):
        place = (slice(None), *at_f)
        return jnp.concatenate(
            [ref[(slice(4 * g, 4 * g + 4), *place[1:], b)] for g in range(groups) for b in range(2)],
            axis=0,
        )

    def group(g):
        return slice(8 * g, 8 * g + 8)

    for f in range(freqs):
        x_s[f] = rows_of(x0_s, at(f))
    power, smooth = power_s[...], smooth_s[...]
    row = lax.broadcasted_iota(jnp.int32, (2 * modes, width), 0)
    own = lax.broadcasted_iota(jnp.int32, (2 * modes, width), 1) // rank == row // 8 * 4 + row % 4
    sign = jnp.where(row % 8 < 4, 1.0, -1.0)
    for i, f in enumerate(matrix):
        levels = noise_s[:, at(f), :]
        levels = jnp.concatenate(
            [levels[4 * g:4 * g + 4] for g in range(groups) for _ in range(2)], axis=0
        )
        mask_s[i] = jnp.where(own, jnp.concatenate([levels] * modes, axis=1), 0.0)
    unit = (
        lax.broadcasted_iota(jnp.int32, (rank, rank), 0)
        == lax.broadcasted_iota(jnp.int32, (rank, rank), 1)
    )
    for i, f in enumerate(vector):
        levels = noise_s[:, at(f), :]
        for m in range(modes):
            column = jnp.sum(jnp.where(unit, levels[m:m + 1], 0.0), axis=1, keepdims=True)
            column_s[i, m] = jnp.broadcast_to(column, (rank, 128))

    def swapped(x):
        return jnp.concatenate([pltpu.roll(x[group(g)], 4, 0) for g in range(groups)], axis=0)

    def matrix_project(f, field):
        i = matrix.index(f)
        seen = times(field, high_s[i], low_s[i], True)
        parts = seen[:, :width] + sign * swapped(seen[:, width:])
        return parts, mask_s[i] * parts

    def matrix_back(f, seen):
        i = matrix.index(f)
        weighted = jnp.concatenate([seen[1], -sign * swapped(seen[1])], axis=1)
        return times(weighted, high_s[i], low_s[i], False)

    def wide(x):
        return jnp.concatenate([x] * (ell // 128), axis=1)

    def group_project(f, g, field):
        parts = []
        for j in range(4):
            m = 4 * g + j
            real_beam, imaginary_beam = beam_s[f, m, 0], beam_s[f, m, 1]
            real_field, imaginary_field = field[j:j + 1], field[4 + j:5 + j]
            levels = column_s[vector.index(f), m]
            real = jnp.sum(
                real_beam * real_field + imaginary_beam * imaginary_field, axis=1, keepdims=True
            )
            imaginary = jnp.sum(
                real_beam * imaginary_field - imaginary_beam * real_field, axis=1, keepdims=True
            )
            parts.append((real, imaginary, levels * real, levels * imaginary))
        return parts

    def group_back(f, g, parts):
        reals, imaginaries = [], []
        for j, (_, _, real, imaginary) in enumerate(parts):
            m = 4 * g + j
            real, imaginary = wide(real), wide(imaginary)
            real_beam, imaginary_beam = beam_s[f, m, 0], beam_s[f, m, 1]
            for found, value in (
                (reals, real_beam * real - imaginary_beam * imaginary),
                (imaginaries, real_beam * imaginary + imaginary_beam * real),
            ):
                found.append(sum(value[k:k + 8] for k in range(0, rank, 8)))
        return folded(reals + imaginaries)

    def group_beam(f, g, field):
        return group_back(f, g, group_project(f, g, field))

    def project(f, ref):
        if f in matrix:
            return matrix_project(f, ref[f])
        return [group_project(f, g, ref[f, group(g)]) for g in range(groups)]

    def back(f, seen):
        if f in matrix:
            return matrix_back(f, seen)
        return jnp.concatenate([group_back(f, g, seen[g]) for g in range(groups)], axis=0)

    def apply_beam(fs, ref):
        fs = [f for f in fs if f in matrix] + [f for f in fs if f in vector]
        seen = [project(f, ref) for f in fs]
        return {f: back(f, found) for f, found in zip(fs, seen)}

    def count(f):
        value = float(f > 0) + float(f < last) + float(nf > 1 and f == 0)
        if two_sided and f == last:
            value = value + jnp.where(has_far, 1.0, 0.0)
        return value

    def local_prior(f, ref, rows=slice(None)):
        value = count(f) * ref[f, rows]
        if f > 0:
            value = value - ref[f - 1, rows]
        if f < last:
            value = value - ref[f + 1, rows]
        return power * ref[f, rows] + smooth * value

    for f in edges:
        beam_copies[f].wait()
    rhs_copy.wait()
    for i, f in enumerate(edges):
        for g in range(groups):
            rows = group(g)
            image = group_beam(f, g, x_s[f, rows])
            y_s[i, rows] = rows_of(rhs_s, at(f))[rows] - image - local_prior(f, x_s, rows)
    for g in range(groups):
        send(1, g)

    for f in inner:
        beam_copies[f].wait()
    for i, f in enumerate(matrix):
        for a in range(2):
            rows = slice(a * width, (a + 1) * width)
            high, low = split(beam_s[f, :, a].reshape(width, ell))
            high_s[i, rows] = high
            low_s[i, rows] = low
    for f, image in apply_beam(inner, x_s).items():
        r_s[f] = rows_of(rhs_s, at(f)) - image - local_prior(f, x_s)
    for f, image in apply_beam(inner, r_s).items():
        u_s[f] = image + local_prior(f, r_s) if f in apart else image
    seen = {f: project(f, u_s) for f in apart}
    advance()

    for g in range(groups):
        arrive(0, g)
        rows = group(g)
        for i, f in enumerate(edges):
            halo = jnp.concatenate([first_s[i, 4 * g:4 * g + 4, b, :] for b in range(2)], axis=0)
            r_s[f, rows] = y_s[i, rows] + smooth * halo
        for i, f in enumerate(edges):
            v_s[i, rows] = group_beam(f, g, r_s[f, rows]) + local_prior(f, r_s, rows)
        if paired:
            pl.when(jnp.logical_not(helper))(lambda: cross_copy(g).start())
        else:
            send(2, g)
    if paired:
        for g in range(groups):
            send(2, g)

    for f in beside_edge:
        u_s[f] = u_s[f] + local_prior(f, r_s)
    seen |= {f: project(f, u_s) for f in beside_edge}

    for g in range(groups):
        arrive(1, g)
    for i, f in enumerate(edges):
        u_s[f] = v_s[i] - beside(i, smooth * (halo_s[0, i] + smooth * x_s[f]))
    if paired:
        pull_s[...] = smooth * u_s[0]
        pl.when(jnp.logical_not(helper))(lambda: pull_copy().start())
    seen |= {f: project(f, u_s) for f in edges}
    norm = jnp.zeros((2 * modes, ell), F32)
    curve, square, cube = norm, norm, norm
    beam_part = jnp.zeros((2 * modes, width), F32)
    column_part = jnp.zeros((rank, 128), F32)
    for f in inner + edges:
        if f in matrix:
            beam_part = beam_part + seen[f][0] * seen[f][1]
        else:
            for parts in seen[f]:
                for real, imaginary, real_weighted, imaginary_weighted in parts:
                    column_part = column_part + (real * real_weighted + imaginary * imaginary_weighted)
        w_s[f] = local_prior(f, u_s)
        norm = norm + r_s[f] * r_s[f]
        curve = curve + r_s[f] * u_s[f]
        square = square + u_s[f] * u_s[f]
        cube = cube + u_s[f] * w_s[f]
    lane = lax.broadcasted_iota(jnp.int32, (1, 128), 1)
    message = jnp.zeros((1, 128), F32)
    for i, part in enumerate((norm, curve, square, cube)):
        total = total_of(part)
        if i == 3:
            total = total + total_of(beam_part) + jnp.sum(column_part, axis=0, keepdims=True)
        message = jnp.where(lane == i, total, message)
    if paired:
        message = jnp.where(lane == 4 + my_f, total_of(smooth * r_s[0] * pull_s[...]), message)
    message_s[0] = message
    early_s[me] = message

    while steps:
        advance()

    def share(source, target, slot, turn, device):
        pltpu.make_async_remote_copy(
            src_ref=message_s.at[source], dst_ref=target.at[slot],
            send_sem=sum_send.at[turn], recv_sem=sum_recv.at[turn],
            device_id=device, device_id_type=MESH,
        ).start()

    def share_all(source, target, slot, turn, stride):
        if n > 64:
            def body(i, carry):
                ma, f = my_ma + i * stride // nf, my_f + i * stride % nf
                share(source, target, slot, turn, (lax.rem(ma, nma), lax.rem(f, nf)))
                return carry

            lax.fori_loop(1, n // stride, body, 0)
        else:
            for mask in sorted(range(stride, n, stride), key=lambda m: (-(m // nf // 2), m)):
                device = partner([bit for bit in range(bits) if mask >> bit & 1])
                share(source, target, slot, turn, device)

    def landed(target, sem, rows):
        if rows:
            rows = target.at[pl.ds(0, rows)]
            pltpu.make_async_copy(rows, rows, sem).wait()

    def lanes_of(x):
        x = jnp.sum(x, axis=0, keepdims=True)
        return sum(x[:, i:i + 128] for i in range(0, ell, 128))

    share_all(0, early_s, me, 0, 1)
    for f in matrix + vector:
        w_s[f] = w_s[f] + back(f, seen[f])

    late_rows = late_s.shape[0]
    if paired:
        @pl.when(helper)
        def _():
            cross = jnp.zeros((8, ell), F32)
            for g in range(groups):
                arrive(2, g)
                cross = cross + pull_s[group(g)] * halo_s[1, 0, group(g)]
            pull_copy().wait_recv()
            for g in range(groups):
                cross_copy(g).wait_recv()
                cross = cross + partner_s[group(g)] * cross_s[group(g)]
            message = lanes_of(cross)
            late_s[my_ma // 2] = message
            message_s[1] = message
            share_all(1, late_s, my_ma // 2, 1, nf)

        @pl.when(jnp.logical_not(helper))
        def _():
            for g in range(groups):
                arrive(2, g)
            pull_copy().wait_send()
            for g in range(groups):
                cross_copy(g).wait_send()

        w_s[0] = w_s[0] - smooth * (halo_s[1, 0] - smooth * r_s[0])
    else:
        cross = jnp.zeros((8, ell), F32)
        nexts = []
        for g in range(groups):
            arrive(2, g)
            rows = group(g)
            for i, f in enumerate(edges):
                pull = beside(i, smooth * (halo_s[1, i, rows] - smooth * r_s[f, rows]))
                nexts.append((f, rows, pull))
                cross = cross + pull * u_s[f, rows]
        message = lanes_of(cross)
        late_s[me] = message
        message_s[1] = message
        share_all(1, late_s, me, 1, 1)
        for f, rows, pull in nexts:
            w_s[f, rows] = w_s[f, rows] - pull

    for kind in range(3):
        for g in range(groups):
            sent(kind, g)
    landed(early_s, sum_recv.at[0], n - 1)
    total = jnp.sum(early_s[...], axis=0)
    m0, m1, m2, m3, known = (
        jnp.sum(jnp.where(lane == i, total, 0.0), axis=1, keepdims=True)
        for i in (0, 1, 2, 3, 4 + my_f)
    )
    if paired:
        m3 = m3 + 2.0 * known
    step = m0 / m1
    norm_next = step * (step * m2 - m1)
    growth = norm_next / m0
    curve_part = m1 - 2.0 * step * m2 + step * step * m3 - growth * norm_next / step
    cross_scale = step * step * (2.0 if paired else 1.0)
    for f in range(freqs):
        x, r, u, w = x_s[f], r_s[f], u_s[f], w_s[f]
        for target, value in (
            (sol_s, x + step * r),
            (res_s, r - step * u),
            (sol_move_s, (1.0 + growth) * r - step * u),
            (res_move_s, (1.0 + growth) * u - step * w),
        ):
            for g in range(groups):
                for b in range(2):
                    start = 8 * g + 4 * b
                    target[4 * g:4 * g + 4, at(f), b, :] = value[start:start + 4]
    landed(early_s, sum_send.at[0], n - 1)
    if paired:
        @pl.when(helper)
        def _():
            rows = early_s.at[pl.ds(0, nma - 1)]
            pltpu.make_async_copy(rows, rows, sum_send.at[1]).wait()
            landed(late_s, sum_recv.at[1], late_rows - 1)

        pl.when(jnp.logical_not(helper))(lambda: landed(late_s, sum_recv.at[1], late_rows))
    else:
        landed(late_s, sum_send.at[1], late_rows - 1)
        landed(late_s, sum_recv.at[1], late_rows - 1)
    crossed = jnp.sum(jnp.sum(late_s[...], axis=0), axis=1, keepdims=True)
    step_next = norm_next / (curve_part - cross_scale * crossed)
    sol_s[...] = sol_s[...] + step_next * sol_move_s[...]
    res_s[...] = res_s[...] - step_next * res_move_s[...]


def scoped_kernel(nma, nf, sides, *refs):
    modes, freqs = refs[0].shape[:2]
    dma = pltpu.SemaphoreType.DMA
    pl.run_scoped(
        functools.partial(kernel, nma, nf, *refs),
        dma((7,)), dma((freqs,)), dma((3, modes // 4, sides)), dma((2,)),
    )


def write_out(sol_in, res_in, sol_out, res_out, sem):
    copies = [
        pltpu.make_async_copy(sol_in, sol_out, sem.at[0]),
        pltpu.make_async_copy(res_in, res_out, sem.at[1]),
    ]
    for copy in copies:
        copy.start()
    for copy in copies:
        copy.wait()


def shards(right_side, start_field, beam, noise, inv_power, smooth):
    nma, nf = lax.axis_size("ma"), lax.axis_size("freq")
    modes, freqs, _, ell = right_side.shape
    rank = beam.shape[3]
    width = modes * rank
    sides = 2 if nf > 2 else 1
    vmem_spec = pl.BlockSpec(memory_space=pltpu.VMEM)
    any_spec = pl.BlockSpec(memory_space=pl.ANY)
    field = pltpu.VMEM(right_side.shape, F32)
    edge = pltpu.VMEM((sides, modes, 2, ell), F32)
    slab = pltpu.VMEM((freqs, 2 * modes, ell), F32)
    edge_slab = pltpu.VMEM((sides, 2 * modes, ell), F32)
    vector = max(min(nf - 1, 2), freqs // 2)
    matrix = max(freqs - vector, 1)
    half = pltpu.VMEM((matrix, 2 * width, ell), BF16)
    outs = pl.pallas_call(
        functools.partial(scoped_kernel, nma, nf, sides),
        out_shape=[field] * 2,
        in_specs=[any_spec] * 6,
        out_specs=[vmem_spec] * 2,
        scratch_shapes=[
            field, field, edge,
            pltpu.VMEM((freqs, modes, 2, rank, ell), F32),
            pltpu.VMEM(noise.shape, F32),
            pltpu.VMEM((1, ell), F32), pltpu.VMEM((1, ell), F32),
            half, half,
            slab, edge_slab, slab, edge_slab, slab, slab,
            pltpu.VMEM((matrix, 2 * modes, width), F32),
            pltpu.VMEM((vector, modes, rank, 128), F32),
            edge,
            pltpu.VMEM((2, sides, 2 * modes, ell), F32),
            field, field,
            pltpu.VMEM((2 * modes, ell), F32), pltpu.VMEM((2 * modes, ell), F32),
            pltpu.VMEM((2 * modes, ell), F32),
            pltpu.VMEM((2, 1, 128), F32),
            pltpu.VMEM((nma * nf, 1, 128), F32),
            pltpu.VMEM((nma // 2 if nf == 2 and nma % 2 == 0 else nma * nf, 1, 128), F32),
            pltpu.SemaphoreType.DMA((3, modes // 4, sides)),
            pltpu.SemaphoreType.DMA((2 * (modes // 4) + 2,)),
            pltpu.SemaphoreType.DMA((2,)),
            pltpu.SemaphoreType.REGULAR((max((nma * nf).bit_length() - 4, 1),)),
        ],
        compiler_params=pltpu.CompilerParams(
            collective_id=0, has_side_effects=True, vmem_limit_bytes=67043328 - 2 * right_side.size * 4
        ),
        name="solve",
    )(right_side, start_field, beam, noise, inv_power[None], smooth[None])
    return pl.pallas_call(
        write_out,
        out_shape=[jax.ShapeDtypeStruct(right_side.shape, F32)] * 2,
        in_specs=[vmem_spec] * 2,
        out_specs=[any_spec] * 2,
        scratch_shapes=[pltpu.SemaphoreType.DMA((2,))],
        compiler_params=pltpu.CompilerParams(vmem_limit_bytes=1024 * 1024),
        name="write_out",
    )(*outs)


def solution(mesh):
    in_specs = (
        P("ma", "freq", None, None),
        P("ma", "freq", None, None),
        P("ma", "freq", None, None, None),
        P("ma", "freq", None),
        P(),
        P(),
    )
    out_specs = (P("ma", "freq", None, None), P("ma", "freq", None, None))
    return jax.shard_map(shards, mesh=mesh, in_specs=in_specs, out_specs=out_specs, check_vma=False)
```

```python
import functools

import jax
import jax.numpy as jnp
from jax import lax
from jax.experimental import pallas as pl
from jax.experimental.pallas import tpu as pltpu
from jax.sharding import PartitionSpec as P

MESH = pl.DeviceIdType.MESH
F32, BF16 = jnp.float32, jnp.bfloat16


def split(x):
    high = x.astype(BF16)
    return high, (x - high.astype(F32)).astype(BF16)


def times(x, high, low, transposed):
    dims = (((1,), (1 if transposed else 0,)), ((), ()))
    rows = x.shape[0]
    x_high, x_low = split(x)
    both = jnp.concatenate([x_high, x_low], axis=0)
    main = lax.dot_general(both, high, dims, preferred_element_type=F32)
    rest = lax.dot_general(x_high, low, dims, preferred_element_type=F32)
    return main[:rows] + (main[rows:] + rest)


def folded(parts):
    row = lax.broadcasted_iota(jnp.int32, parts[0].shape, 0)
    upper = row < 4
    fours = [
        jnp.where(upper, parts[s], parts[s + 4])
        + pltpu.roll(jnp.where(upper, parts[s + 4], parts[s]), 4, 0)
        for s in range(4)
    ]
    even = row // 2 % 2 == 0
    twos = [
        jnp.where(
            even, fours[s] + pltpu.roll(fours[s], 6, 0), fours[s + 2] + pltpu.roll(fours[s + 2], 2, 0)
        )
        for s in range(2)
    ]
    return jnp.where(
        row % 2 == 0, twos[0] + pltpu.roll(twos[0], 7, 0), twos[1] + pltpu.roll(twos[1], 1, 0)
    )


def total_of(x):
    return jnp.sum(jnp.sum(x, axis=0, keepdims=True), axis=1, keepdims=True)


def kernel(
    nma, nf, rhs_in, x0_in, beam_in, noise_in, power_in, smooth_in, sol_s, res_s,
    rhs_s, x0_s, edge_s, beam_s, noise_s, power_s, smooth_s,
    high_s, low_s, x_s, y_s, r_s, v_s, u_s, w_s, mask_s, column_s, first_s, halo_s,
    sol_move_s, res_move_s, pull_s, partner_s, cross_s,
    lent_beam_s, lent_column_s, lent_y_s, lent_r_s, lent_first_s, lent_v_s,
    message_s, early_s, late_s,
    halo_recv, pair_recv, sum_recv, word_sem, in_sem, beam_sem, halo_send, pair_send, sum_send,
):
    modes, freqs, _, ell = rhs_in.shape
    rank = beam_in.shape[3]
    width = modes * rank
    n = nma * nf
    my_ma, my_f = lax.axis_index("ma"), lax.axis_index("freq")
    me = my_ma * nf + my_f
    last = freqs - 1
    two_sided = nf > 2
    paired = nf == 2 and nma % 2 == 0 and freqs > 1
    helper = my_ma % 2 == 1
    groups = modes // 4
    edges = [0, last][:min(nf - 1, 2)]
    inner = [f for f in range(freqs) if f not in edges]
    beside_edge = [f for f in inner if f - 1 in edges or f + 1 in edges]
    apart = [f for f in inner if f not in beside_edge]
    vector = edges + inner[:max(freqs // 2 - len(edges), 0)]
    matrix = [f for f in range(freqs) if f not in vector]

    def at(g):
        return jnp.where(my_f == 0, last - g, g)

    edge_copies = [
        pltpu.make_async_copy(x0_in.at[:, at(f)], edge_s.at[i], in_sem.at[i])
        for i, f in enumerate(edges)
    ]
    x0_copy = pltpu.make_async_copy(x0_in, x0_s, in_sem.at[2])
    rhs_copy = pltpu.make_async_copy(rhs_in, rhs_s, in_sem.at[3])
    small = [
        pltpu.make_async_copy(power_in, power_s, in_sem.at[4]),
        pltpu.make_async_copy(smooth_in, smooth_s, in_sem.at[5]),
        pltpu.make_async_copy(noise_in, noise_s, in_sem.at[6]),
    ]
    beam_copies = [
        pltpu.make_async_copy(beam_in.at[:, at(f)], beam_s.at[f], beam_sem.at[f])
        for f in range(freqs)
    ]
    for copy in edge_copies:
        copy.start()

    def flip(bit):
        d = 1 << (bit if bit < freq_bits else bit - freq_bits)
        place = my_f if bit < freq_bits else my_ma
        return d * (1 - 2 * (place // d % 2))

    def partner(bits):
        return (
            my_ma + sum(flip(bit) for bit in bits if bit >= freq_bits),
            my_f + sum(flip(bit) for bit in bits if bit < freq_bits),
        )

    freq_bits = nf.bit_length() - 1
    bits = freq_bits + nma.bit_length() - 1
    close = min(bits, 3)
    greeted = [
        partner([bit for bit in range(close) if mask >> bit & 1]) for mask in range(1, 1 << close)
    ]
    word = [partner([bit]) for bit in range(close, bits)]
    greeted += word
    words = len(word)
    barrier = pltpu.get_barrier_semaphore()
    near = jnp.where(my_f == 0, 1, my_f - 1)
    has_far = (my_f > 0) & (my_f < nf - 1)

    def greet(device):
        pl.semaphore_signal(barrier, inc=1, device_id=device, device_id_type=MESH)

    for i, device in enumerate(greeted):
        greet(device)
        if i == 0:
            others = [beam_copies[f] for f in edges] + [rhs_copy] + [beam_copies[f] for f in inner]
            for copy in [x0_copy] + small + others:
                copy.start()
    expected = len(greeted)
    if nf > 2:
        pl.when(my_f > 0)(lambda: greet((my_ma, my_f - 1)))
        pl.when(my_f < nf - 1)(lambda: greet((my_ma, my_f + 1)))
        expected = expected + jnp.minimum(my_f, 1) + jnp.minimum(nf - 1 - my_f, 1)

    steps = list(range(words + 1))

    def advance():
        if steps:
            step = steps.pop(0)
            if step > 0:
                pl.semaphore_wait(word_sem.at[step - 1], 1)
            if step < words:
                pl.semaphore_signal(
                    word_sem.at[step], inc=1, device_id=word[step], device_id_type=MESH
                )

    def piece(kind, g):
        if kind == 0:
            rows = pl.ds(4 * g, 4)
            return (lambda i: edge_s.at[i, rows]), (lambda i: first_s.at[i, rows])
        source = (y_s, v_s)[kind - 1]
        rows = pl.ds(8 * g, 8)
        return (lambda i: source.at[i, rows]), (lambda i: halo_s.at[kind - 1, i, rows])

    def near_copy(kind, g):
        source, target = piece(kind, g)
        side = jnp.minimum(my_f // 2, 1) if two_sided else 0
        return pltpu.make_async_remote_copy(
            src_ref=source(0), dst_ref=target(side),
            send_sem=halo_send.at[kind, g, 0], recv_sem=halo_recv.at[kind, g, side],
            device_id=(my_ma, near), device_id_type=MESH,
        )

    def far_copy(kind, g):
        source, target = piece(kind, g)
        return pltpu.make_async_remote_copy(
            src_ref=source(1), dst_ref=target(0),
            send_sem=halo_send.at[kind, g, 1], recv_sem=halo_recv.at[kind, g, 0],
            device_id=(my_ma, my_f + 1), device_id_type=MESH,
        )

    def arrival(kind, g, side):
        slot = piece(kind, g)[1](side)
        return pltpu.make_async_copy(slot, slot, halo_recv.at[kind, g, side])

    def send(kind, g):
        if nf > 1:
            near_copy(kind, g).start()
        if two_sided:
            pl.when(has_far)(lambda: far_copy(kind, g).start())

    def arrive(kind, g):
        if nf > 1:
            arrival(kind, g, 0).wait()
        if two_sided:
            pl.when(has_far)(lambda: arrival(kind, g, 1).wait())

    def sent(kind, g):
        if nf > 1:
            near_copy(kind, g).wait_send()
        if two_sided:
            pl.when(has_far)(lambda: far_copy(kind, g).wait_send())

    def pair_copy(k, source, target, ma, f):
        return pltpu.make_async_remote_copy(
            src_ref=source, dst_ref=target, send_sem=pair_send.at[k], recv_sem=pair_recv.at[k],
            device_id=(ma, f), device_id_type=MESH,
        )

    def lend(k):
        source = (lambda: beam_s.at[0], lambda: column_s.at[0], lambda: y_s.at[0], lambda: r_s.at[1])[k]
        target = (lent_beam_s, lent_column_s, lent_y_s, lent_r_s)[k]
        return pair_copy(k, source(), target, my_ma + 1, my_f)

    def pull_copy():
        return pair_copy(4, pull_s, partner_s, my_ma + 1, my_f)

    def first_copy(g):
        rows = pl.ds(4 * g, 4)
        return pair_copy(5 + g, edge_s.at[0, rows], lent_first_s.at[rows], my_ma + 1, 1 - my_f)

    def cross_copy(g):
        rows = pl.ds(8 * g, 8)
        return pair_copy(5 + groups + g, lent_v_s.at[rows], cross_s.at[rows], my_ma, 1 - my_f)

    def even_only(copies):
        @pl.when(jnp.logical_not(helper))
        def _():
            for copy in copies:
                copy.start()

    def beside(i, value):
        return jnp.where(has_far, value, 0.0) if i else value

    if two_sided:
        @pl.when(jnp.logical_not(has_far))
        def _():
            first_s[1] = jnp.zeros_like(first_s[1])
            halo_s[:, 1] = jnp.zeros_like(halo_s[:, 1])

    for copy in edge_copies:
        copy.wait()
    pl.semaphore_wait(barrier, expected)
    for g in range(groups):
        send(0, g)
    if paired:
        even_only([first_copy(g) for g in range(groups)])
    advance()

    x0_copy.wait()
    for copy in small:
        copy.wait()
    def rows_of(ref, *at_f):
        place = (slice(None), *at_f)
        return jnp.concatenate(
            [ref[(slice(4 * g, 4 * g + 4), *place[1:], b)] for g in range(groups) for b in range(2)],
            axis=0,
        )

    def group(g):
        return slice(8 * g, 8 * g + 8)

    for f in range(freqs):
        x_s[f] = rows_of(x0_s, at(f))
    power, smooth = power_s[...], smooth_s[...]
    row = lax.broadcasted_iota(jnp.int32, (2 * modes, width), 0)
    own = lax.broadcasted_iota(jnp.int32, (2 * modes, width), 1) // rank == row // 8 * 4 + row % 4
    sign = jnp.where(row % 8 < 4, 1.0, -1.0)
    for i, f in enumerate(matrix):
        levels = noise_s[:, at(f), :]
        levels = jnp.concatenate(
            [levels[4 * g:4 * g + 4] for g in range(groups) for _ in range(2)], axis=0
        )
        mask_s[i] = jnp.where(own, jnp.concatenate([levels] * modes, axis=1), 0.0)
    unit = (
        lax.broadcasted_iota(jnp.int32, (rank, rank), 0)
        == lax.broadcasted_iota(jnp.int32, (rank, rank), 1)
    )
    for i, f in enumerate(vector):
        levels = noise_s[:, at(f), :]
        for m in range(modes):
            column = jnp.sum(jnp.where(unit, levels[m:m + 1], 0.0), axis=1, keepdims=True)
            column_s[i, m] = jnp.broadcast_to(column, (rank, 128))

    def swapped(x):
        return jnp.concatenate([pltpu.roll(x[group(g)], 4, 0) for g in range(groups)], axis=0)

    def matrix_project(f, field):
        i = matrix.index(f)
        seen = times(field, high_s[i], low_s[i], True)
        parts = seen[:, :width] + sign * swapped(seen[:, width:])
        return parts, mask_s[i] * parts

    def matrix_back(f, seen):
        i = matrix.index(f)
        weighted = jnp.concatenate([seen[1], -sign * swapped(seen[1])], axis=1)
        return times(weighted, high_s[i], low_s[i], False)

    def wide(x):
        return jnp.concatenate([x] * (ell // 128), axis=1)

    def owned(f):
        return (lambda m, a: beam_s[f, m, a]), (lambda m: column_s[vector.index(f), m])

    lent = (lambda m, a: lent_beam_s[m, a]), (lambda m: lent_column_s[m])

    def group_project(source, g, field):
        beam_of, column_of = source
        parts = []
        for j in range(4):
            m = 4 * g + j
            real_beam, imaginary_beam = beam_of(m, 0), beam_of(m, 1)
            real_field, imaginary_field = field[j:j + 1], field[4 + j:5 + j]
            levels = column_of(m)
            real = jnp.sum(
                real_beam * real_field + imaginary_beam * imaginary_field, axis=1, keepdims=True
            )
            imaginary = jnp.sum(
                real_beam * imaginary_field - imaginary_beam * real_field, axis=1, keepdims=True
            )
            parts.append((real, imaginary, levels * real, levels * imaginary))
        return parts

    def group_back(source, g, parts):
        beam_of, _ = source
        reals, imaginaries = [], []
        for j, (_, _, real, imaginary) in enumerate(parts):
            m = 4 * g + j
            real, imaginary = wide(real), wide(imaginary)
            real_beam, imaginary_beam = beam_of(m, 0), beam_of(m, 1)
            for found, value in (
                (reals, real_beam * real - imaginary_beam * imaginary),
                (imaginaries, real_beam * imaginary + imaginary_beam * real),
            ):
                found.append(sum(value[k:k + 8] for k in range(0, rank, 8)))
        return folded(reals + imaginaries)

    def group_beam(source, g, field):
        return group_back(source, g, group_project(source, g, field))

    def project(f, ref):
        if f in matrix:
            return matrix_project(f, ref[f])
        return [group_project(owned(f), g, ref[f, group(g)]) for g in range(groups)]

    def back(f, seen):
        if f in matrix:
            return matrix_back(f, seen)
        return jnp.concatenate([group_back(owned(f), g, seen[g]) for g in range(groups)], axis=0)

    def apply_beam(fs, ref):
        fs = [f for f in fs if f in matrix] + [f for f in fs if f in vector]
        seen = [project(f, ref) for f in fs]
        return {f: back(f, found) for f, found in zip(fs, seen)}

    def count(f):
        value = float(f > 0) + float(f < last) + float(nf > 1 and f == 0)
        if two_sided and f == last:
            value = value + jnp.where(has_far, 1.0, 0.0)
        return value

    def local_prior(f, ref, rows=slice(None)):
        value = count(f) * ref[f, rows]
        if f > 0:
            value = value - ref[f - 1, rows]
        if f < last:
            value = value - ref[f + 1, rows]
        return power * ref[f, rows] + smooth * value

    for f in edges:
        beam_copies[f].wait()
    rhs_copy.wait()
    for i, f in enumerate(edges):
        for g in range(groups):
            rows = group(g)
            image = group_beam(owned(f), g, x_s[f, rows])
            y_s[i, rows] = rows_of(rhs_s, at(f))[rows] - image - local_prior(f, x_s, rows)
    for g in range(groups):
        send(1, g)
    first, rest = [], inner
    if paired:
        even_only([lend(k) for k in range(3)])
        first, rest = inner[:1], inner[1:]

    for f in first:
        beam_copies[f].wait()
        r_s[f] = rows_of(rhs_s, at(f)) - back(f, project(f, x_s)) - local_prior(f, x_s)
    if paired:
        even_only([lend(3)])

    for f in rest:
        beam_copies[f].wait()
    for i, f in enumerate(matrix):
        for a in range(2):
            rows = slice(a * width, (a + 1) * width)
            high, low = split(beam_s[f, :, a].reshape(width, ell))
            high_s[i, rows] = high
            low_s[i, rows] = low
    for f, image in apply_beam(rest, x_s).items():
        r_s[f] = rows_of(rhs_s, at(f)) - image - local_prior(f, x_s)
    for f, image in apply_beam(inner, r_s).items():
        u_s[f] = image + local_prior(f, r_s) if f in apart else image
    seen = {f: project(f, u_s) for f in apart}
    advance()

    for g in range(groups):
        arrive(0, g)
        rows = group(g)
        for i, f in enumerate(edges):
            halo = jnp.concatenate([first_s[i, 4 * g:4 * g + 4, b, :] for b in range(2)], axis=0)
            r_s[f, rows] = y_s[i, rows] + smooth * halo
        for i, f in enumerate(edges):
            v_s[i, rows] = group_beam(owned(f), g, r_s[f, rows]) + local_prior(f, r_s, rows)
        send(2, g)
    if paired:
        @pl.when(helper)
        def _():
            for k in range(4):
                lend(k).wait_recv()
            for g in range(groups):
                first_copy(g).wait_recv()
                rows = group(g)
                halo = jnp.concatenate([lent_first_s[4 * g:4 * g + 4, b, :] for b in range(2)], axis=0)
                r = lent_y_s[rows] + smooth * halo
                local = power * r + smooth * (count(0) * r - lent_r_s[rows])
                lent_v_s[rows] = group_beam(lent, g, r) + local
                cross_copy(g).start()

    for f in beside_edge:
        u_s[f] = u_s[f] + local_prior(f, r_s)
    seen |= {f: project(f, u_s) for f in beside_edge}

    for g in range(groups):
        arrive(1, g)
    for i, f in enumerate(edges):
        u_s[f] = v_s[i] - beside(i, smooth * (halo_s[0, i] + smooth * x_s[f]))
    if paired:
        pull_s[...] = smooth * u_s[0]
        even_only([pull_copy()])
    seen |= {f: project(f, u_s) for f in edges}
    norm = jnp.zeros((2 * modes, ell), F32)
    curve, square, cube = norm, norm, norm
    beam_part = jnp.zeros((2 * modes, width), F32)
    column_part = jnp.zeros((rank, 128), F32)
    for f in inner + edges:
        if f in matrix:
            beam_part = beam_part + seen[f][0] * seen[f][1]
        else:
            for parts in seen[f]:
                for real, imaginary, real_weighted, imaginary_weighted in parts:
                    column_part = column_part + (real * real_weighted + imaginary * imaginary_weighted)
        w_s[f] = local_prior(f, u_s)
        norm = norm + r_s[f] * r_s[f]
        curve = curve + r_s[f] * u_s[f]
        square = square + u_s[f] * u_s[f]
        cube = cube + u_s[f] * w_s[f]
    lane = lax.broadcasted_iota(jnp.int32, (1, 128), 1)
    message = jnp.zeros((1, 128), F32)
    for i, part in enumerate((norm, curve, square, cube)):
        total = total_of(part)
        if i == 3:
            total = total + total_of(beam_part) + jnp.sum(column_part, axis=0, keepdims=True)
        message = jnp.where(lane == i, total, message)
    if paired:
        message = jnp.where(lane == 4 + my_f, total_of(smooth * r_s[0] * pull_s[...]), message)
    message_s[0] = message
    early_s[me] = message

    while steps:
        advance()

    def share(source, target, slot, turn, device):
        pltpu.make_async_remote_copy(
            src_ref=message_s.at[source], dst_ref=target.at[slot],
            send_sem=sum_send.at[turn], recv_sem=sum_recv.at[turn],
            device_id=device, device_id_type=MESH,
        ).start()

    def share_all(source, target, slot, turn, stride):
        if n > 64:
            def body(i, carry):
                ma, f = my_ma + i * stride // nf, my_f + i * stride % nf
                share(source, target, slot, turn, (lax.rem(ma, nma), lax.rem(f, nf)))
                return carry

            lax.fori_loop(1, n // stride, body, 0)
        else:
            for mask in sorted(range(stride, n, stride), key=lambda m: (-(m // nf // 2), m)):
                device = partner([bit for bit in range(bits) if mask >> bit & 1])
                share(source, target, slot, turn, device)

    def landed(target, sem, rows):
        if rows:
            rows = target.at[pl.ds(0, rows)]
            pltpu.make_async_copy(rows, rows, sem).wait()

    def lanes_of(x):
        x = jnp.sum(x, axis=0, keepdims=True)
        return sum(x[:, i:i + 128] for i in range(0, ell, 128))

    share_all(0, early_s, me, 0, 1)
    for f in matrix + vector:
        w_s[f] = w_s[f] + back(f, seen[f])

    late_rows = late_s.shape[0]
    if paired:
        @pl.when(helper)
        def _():
            cross = jnp.zeros((8, ell), F32)
            for g in range(groups):
                arrive(2, g)
                cross = cross + pull_s[group(g)] * halo_s[1, 0, group(g)]
            pull_copy().wait_recv()
            for g in range(groups):
                cross_copy(g).wait_recv()
                cross = cross + partner_s[group(g)] * cross_s[group(g)]
            message = lanes_of(cross)
            late_s[my_ma // 2] = message
            message_s[1] = message
            share_all(1, late_s, my_ma // 2, 1, nf)
            for g in range(groups):
                cross_copy(g).wait_send()

        @pl.when(jnp.logical_not(helper))
        def _():
            for g in range(groups):
                arrive(2, g)
            pull_copy().wait_send()
            for k in range(4):
                lend(k).wait_send()
            for g in range(groups):
                first_copy(g).wait_send()

        w_s[0] = w_s[0] - smooth * (halo_s[1, 0] - smooth * r_s[0])
    else:
        cross = jnp.zeros((8, ell), F32)
        nexts = []
        for g in range(groups):
            arrive(2, g)
            rows = group(g)
            for i, f in enumerate(edges):
                pull = beside(i, smooth * (halo_s[1, i, rows] - smooth * r_s[f, rows]))
                nexts.append((f, rows, pull))
                cross = cross + pull * u_s[f, rows]
        message = lanes_of(cross)
        late_s[me] = message
        message_s[1] = message
        share_all(1, late_s, me, 1, 1)
        for f, rows, pull in nexts:
            w_s[f, rows] = w_s[f, rows] - pull

    for kind in range(3):
        for g in range(groups):
            sent(kind, g)
    landed(early_s, sum_recv.at[0], n - 1)
    total = jnp.sum(early_s[...], axis=0)
    m0, m1, m2, m3, known = (
        jnp.sum(jnp.where(lane == i, total, 0.0), axis=1, keepdims=True)
        for i in (0, 1, 2, 3, 4 + my_f)
    )
    if paired:
        m3 = m3 + 2.0 * known
    step = m0 / m1
    norm_next = step * (step * m2 - m1)
    growth = norm_next / m0
    curve_part = m1 - 2.0 * step * m2 + step * step * m3 - growth * norm_next / step
    cross_scale = step * step * (2.0 if paired else 1.0)
    for f in range(freqs):
        x, r, u, w = x_s[f], r_s[f], u_s[f], w_s[f]
        for target, value in (
            (sol_s, x + step * r),
            (res_s, r - step * u),
            (sol_move_s, (1.0 + growth) * r - step * u),
            (res_move_s, (1.0 + growth) * u - step * w),
        ):
            for g in range(groups):
                for b in range(2):
                    start = 8 * g + 4 * b
                    target[4 * g:4 * g + 4, at(f), b, :] = value[start:start + 4]
    landed(early_s, sum_send.at[0], n - 1)
    if paired:
        @pl.when(helper)
        def _():
            rows = early_s.at[pl.ds(0, nma - 1)]
            pltpu.make_async_copy(rows, rows, sum_send.at[1]).wait()
            landed(late_s, sum_recv.at[1], late_rows - 1)

        pl.when(jnp.logical_not(helper))(lambda: landed(late_s, sum_recv.at[1], late_rows))
    else:
        landed(late_s, sum_send.at[1], late_rows - 1)
        landed(late_s, sum_recv.at[1], late_rows - 1)
    crossed = jnp.sum(jnp.sum(late_s[...], axis=0), axis=1, keepdims=True)
    step_next = norm_next / (curve_part - cross_scale * crossed)
    sol_s[...] = sol_s[...] + step_next * sol_move_s[...]
    res_s[...] = res_s[...] - step_next * res_move_s[...]


def scoped_kernel(nma, nf, sides, *refs):
    modes, freqs = refs[0].shape[:2]
    dma = pltpu.SemaphoreType.DMA
    pl.run_scoped(
        functools.partial(kernel, nma, nf, *refs),
        dma((7,)), dma((freqs,)), dma((3, modes // 4, sides)), dma((2 * (modes // 4) + 5,)), dma((2,)),
    )


def write_out(sol_in, res_in, sol_out, res_out, sem):
    copies = [
        pltpu.make_async_copy(sol_in, sol_out, sem.at[0]),
        pltpu.make_async_copy(res_in, res_out, sem.at[1]),
    ]
    for copy in copies:
        copy.start()
    for copy in copies:
        copy.wait()


def shards(right_side, start_field, beam, noise, inv_power, smooth):
    nma, nf = lax.axis_size("ma"), lax.axis_size("freq")
    modes, freqs, _, ell = right_side.shape
    rank = beam.shape[3]
    width = modes * rank
    sides = 2 if nf > 2 else 1
    vmem_spec = pl.BlockSpec(memory_space=pltpu.VMEM)
    any_spec = pl.BlockSpec(memory_space=pl.ANY)
    field = pltpu.VMEM(right_side.shape, F32)
    edge = pltpu.VMEM((sides, modes, 2, ell), F32)
    slab = pltpu.VMEM((freqs, 2 * modes, ell), F32)
    edge_field = pltpu.VMEM((2 * modes, ell), F32)
    edge_slab = pltpu.VMEM((sides, 2 * modes, ell), F32)
    vector = max(min(nf - 1, 2), freqs // 2)
    matrix = max(freqs - vector, 1)
    half = pltpu.VMEM((matrix, 2 * width, ell), BF16)
    outs = pl.pallas_call(
        functools.partial(scoped_kernel, nma, nf, sides),
        out_shape=[field] * 2,
        in_specs=[any_spec] * 6,
        out_specs=[vmem_spec] * 2,
        scratch_shapes=[
            field, field, edge,
            pltpu.VMEM((freqs, modes, 2, rank, ell), F32),
            pltpu.VMEM(noise.shape, F32),
            pltpu.VMEM((1, ell), F32), pltpu.VMEM((1, ell), F32),
            half, half,
            slab, edge_slab, slab, edge_slab, slab, slab,
            pltpu.VMEM((matrix, 2 * modes, width), F32),
            pltpu.VMEM((vector, modes, rank, 128), F32),
            edge,
            pltpu.VMEM((2, sides, 2 * modes, ell), F32),
            field, field,
            edge_field, edge_field, edge_field,
            pltpu.VMEM((modes, 2, rank, ell), F32), pltpu.VMEM((modes, rank, 128), F32),
            edge_field, edge_field, pltpu.VMEM((modes, 2, ell), F32), edge_field,
            pltpu.VMEM((2, 1, 128), F32),
            pltpu.VMEM((nma * nf, 1, 128), F32),
            pltpu.VMEM((nma // 2 if nf == 2 and nma % 2 == 0 and freqs > 1 else nma * nf, 1, 128), F32),
            pltpu.SemaphoreType.DMA((3, modes // 4, sides)),
            pltpu.SemaphoreType.DMA((2 * (modes // 4) + 5,)),
            pltpu.SemaphoreType.DMA((2,)),
            pltpu.SemaphoreType.REGULAR((max((nma * nf).bit_length() - 4, 1),)),
        ],
        compiler_params=pltpu.CompilerParams(
            collective_id=0, has_side_effects=True, vmem_limit_bytes=67043328 - 2 * right_side.size * 4
        ),
        name="solve",
    )(right_side, start_field, beam, noise, inv_power[None], smooth[None])
    return pl.pallas_call(
        write_out,
        out_shape=[jax.ShapeDtypeStruct(right_side.shape, F32)] * 2,
        in_specs=[vmem_spec] * 2,
        out_specs=[any_spec] * 2,
        scratch_shapes=[pltpu.SemaphoreType.DMA((2,))],
        compiler_params=pltpu.CompilerParams(vmem_limit_bytes=1024 * 1024),
        name="write_out",
    )(*outs)


def solution(mesh):
    in_specs = (
        P("ma", "freq", None, None),
        P("ma", "freq", None, None),
        P("ma", "freq", None, None, None),
        P("ma", "freq", None),
        P(),
        P(),
    )
    out_specs = (P("ma", "freq", None, None), P("ma", "freq", None, None))
    return jax.shard_map(shards, mesh=mesh, in_specs=in_specs, out_specs=out_specs, check_vma=False)
```

```python
import functools

import jax
import jax.numpy as jnp
from jax import lax
from jax.experimental import pallas as pl
from jax.experimental.pallas import tpu as pltpu
from jax.sharding import PartitionSpec as P

MESH = pl.DeviceIdType.MESH
F32, BF16 = jnp.float32, jnp.bfloat16


def split(x):
    high = x.astype(BF16)
    return high, (x - high.astype(F32)).astype(BF16)


def times(x, high, low, transposed):
    dims = (((1,), (1 if transposed else 0,)), ((), ()))
    rows = x.shape[0]
    x_high, x_low = split(x)
    both = jnp.concatenate([x_high, x_low], axis=0)
    main = lax.dot_general(both, high, dims, preferred_element_type=F32)
    rest = lax.dot_general(x_high, low, dims, preferred_element_type=F32)
    return main[:rows] + (main[rows:] + rest)


def folded(parts):
    row = lax.broadcasted_iota(jnp.int32, parts[0].shape, 0)
    upper = row < 4
    fours = [
        jnp.where(upper, parts[s], parts[s + 4])
        + pltpu.roll(jnp.where(upper, parts[s + 4], parts[s]), 4, 0)
        for s in range(4)
    ]
    even = row // 2 % 2 == 0
    twos = [
        jnp.where(
            even, fours[s] + pltpu.roll(fours[s], 6, 0), fours[s + 2] + pltpu.roll(fours[s + 2], 2, 0)
        )
        for s in range(2)
    ]
    return jnp.where(
        row % 2 == 0, twos[0] + pltpu.roll(twos[0], 7, 0), twos[1] + pltpu.roll(twos[1], 1, 0)
    )


def total_of(x):
    return jnp.sum(jnp.sum(x, axis=0, keepdims=True), axis=1, keepdims=True)


def kernel(
    nma, nf, rhs_in, x0_in, beam_in, noise_in, power_in, smooth_in, sol_s, res_s,
    rhs_s, x0_s, edge_s, beam_s, noise_s, power_s, smooth_s,
    high_s, low_s, x_s, y_s, r_s, v_s, u_s, w_s, mask_s, column_s, first_s, halo_s,
    sol_move_s, res_move_s, pull_s, partner_s, cross_s,
    lent_beam_s, lent_column_s, lent_y_s, lent_r_s, lent_first_s, lent_v_s,
    message_s, early_s, late_s,
    halo_recv, pair_recv, sum_recv, word_sem, in_sem, beam_sem, halo_send, pair_send, sum_send,
):
    modes, freqs, _, ell = rhs_in.shape
    rank = beam_in.shape[3]
    width = modes * rank
    n = nma * nf
    my_ma, my_f = lax.axis_index("ma"), lax.axis_index("freq")
    me = my_ma * nf + my_f
    last = freqs - 1
    two_sided = nf > 2
    paired = nf == 2 and nma % 2 == 0 and freqs > 1
    helper = my_ma % 2 == 1
    groups = modes // 4
    edges = [0, last][:min(nf - 1, 2)]
    inner = [f for f in range(freqs) if f not in edges]
    beside_edge = [f for f in inner if f - 1 in edges or f + 1 in edges]
    apart = [f for f in inner if f not in beside_edge]
    vector = edges + inner[:max(freqs // 2 - len(edges), 0)]
    matrix = [f for f in range(freqs) if f not in vector]

    def at(g):
        return jnp.where(my_f == 0, last - g, g)

    edge_copies = [
        pltpu.make_async_copy(x0_in.at[:, at(f)], edge_s.at[i], in_sem.at[i])
        for i, f in enumerate(edges)
    ]
    x0_copy = pltpu.make_async_copy(x0_in, x0_s, in_sem.at[2])
    rhs_copy = pltpu.make_async_copy(rhs_in, rhs_s, in_sem.at[3])
    small = [
        pltpu.make_async_copy(power_in, power_s, in_sem.at[4]),
        pltpu.make_async_copy(smooth_in, smooth_s, in_sem.at[5]),
        pltpu.make_async_copy(noise_in, noise_s, in_sem.at[6]),
    ]
    beam_copies = [
        pltpu.make_async_copy(beam_in.at[:, at(f)], beam_s.at[f], beam_sem.at[f])
        for f in range(freqs)
    ]
    for copy in edge_copies:
        copy.start()

    def flip(bit):
        d = 1 << (bit if bit < freq_bits else bit - freq_bits)
        place = my_f if bit < freq_bits else my_ma
        return d * (1 - 2 * (place // d % 2))

    def partner(bits):
        return (
            my_ma + sum(flip(bit) for bit in bits if bit >= freq_bits),
            my_f + sum(flip(bit) for bit in bits if bit < freq_bits),
        )

    freq_bits = nf.bit_length() - 1
    bits = freq_bits + nma.bit_length() - 1
    close = min(bits, 3)
    greeted = [
        partner([bit for bit in range(close) if mask >> bit & 1]) for mask in range(1, 1 << close)
    ]
    word = [partner([bit]) for bit in range(close, bits)]
    greeted += word
    words = len(word)
    barrier = pltpu.get_barrier_semaphore()
    near = jnp.where(my_f == 0, 1, my_f - 1)
    has_far = (my_f > 0) & (my_f < nf - 1)

    def greet(device):
        pl.semaphore_signal(barrier, inc=1, device_id=device, device_id_type=MESH)

    for i, device in enumerate(greeted):
        greet(device)
        if i == 0:
            for copy in [beam_copies[f] for f in edges] + [x0_copy, rhs_copy] + small:
                copy.start()
    expected = len(greeted)
    if nf > 2:
        pl.when(my_f > 0)(lambda: greet((my_ma, my_f - 1)))
        pl.when(my_f < nf - 1)(lambda: greet((my_ma, my_f + 1)))
        expected = expected + jnp.minimum(my_f, 1) + jnp.minimum(nf - 1 - my_f, 1)

    steps = list(range(words + 1))

    def advance():
        if steps:
            step = steps.pop(0)
            if step > 0:
                pl.semaphore_wait(word_sem.at[step - 1], 1)
            if step < words:
                pl.semaphore_signal(
                    word_sem.at[step], inc=1, device_id=word[step], device_id_type=MESH
                )

    def piece(kind, g):
        if kind == 0:
            rows = pl.ds(4 * g, 4)
            return (lambda i: edge_s.at[i, rows]), (lambda i: first_s.at[i, rows])
        source = (y_s, v_s)[kind - 1]
        rows = pl.ds(8 * g, 8)
        return (lambda i: source.at[i, rows]), (lambda i: halo_s.at[kind - 1, i, rows])

    def near_copy(kind, g):
        source, target = piece(kind, g)
        side = jnp.minimum(my_f // 2, 1) if two_sided else 0
        return pltpu.make_async_remote_copy(
            src_ref=source(0), dst_ref=target(side),
            send_sem=halo_send.at[kind, g, 0], recv_sem=halo_recv.at[kind, g, side],
            device_id=(my_ma, near), device_id_type=MESH,
        )

    def far_copy(kind, g):
        source, target = piece(kind, g)
        return pltpu.make_async_remote_copy(
            src_ref=source(1), dst_ref=target(0),
            send_sem=halo_send.at[kind, g, 1], recv_sem=halo_recv.at[kind, g, 0],
            device_id=(my_ma, my_f + 1), device_id_type=MESH,
        )

    def arrival(kind, g, side):
        slot = piece(kind, g)[1](side)
        return pltpu.make_async_copy(slot, slot, halo_recv.at[kind, g, side])

    def send(kind, g):
        if nf > 1:
            near_copy(kind, g).start()
        if two_sided:
            pl.when(has_far)(lambda: far_copy(kind, g).start())

    def arrive(kind, g):
        if nf > 1:
            arrival(kind, g, 0).wait()
        if two_sided:
            pl.when(has_far)(lambda: arrival(kind, g, 1).wait())

    def sent(kind, g):
        if nf > 1:
            near_copy(kind, g).wait_send()
        if two_sided:
            pl.when(has_far)(lambda: far_copy(kind, g).wait_send())

    def pair_copy(k, source, target, ma, f):
        return pltpu.make_async_remote_copy(
            src_ref=source, dst_ref=target, send_sem=pair_send.at[k], recv_sem=pair_recv.at[k],
            device_id=(ma, f), device_id_type=MESH,
        )

    def lend(k):
        source = (lambda: beam_s.at[0], lambda: column_s.at[0], lambda: y_s.at[0], lambda: r_s.at[1])[k]
        target = (lent_beam_s, lent_column_s, lent_y_s, lent_r_s)[k]
        return pair_copy(k, source(), target, my_ma + 1, my_f)

    def pull_copy():
        return pair_copy(4, pull_s, partner_s, my_ma + 1, my_f)

    def first_copy(g):
        rows = pl.ds(4 * g, 4)
        return pair_copy(5 + g, edge_s.at[0, rows], lent_first_s.at[rows], my_ma + 1, 1 - my_f)

    def cross_copy(g):
        rows = pl.ds(8 * g, 8)
        return pair_copy(5 + groups + g, lent_v_s.at[rows], cross_s.at[rows], my_ma, 1 - my_f)

    def even_only(copies):
        @pl.when(jnp.logical_not(helper))
        def _():
            for copy in copies:
                copy.start()

    def beside(i, value):
        return jnp.where(has_far, value, 0.0) if i else value

    if two_sided:
        @pl.when(jnp.logical_not(has_far))
        def _():
            first_s[1] = jnp.zeros_like(first_s[1])
            halo_s[:, 1] = jnp.zeros_like(halo_s[:, 1])

    for copy in edge_copies:
        copy.wait()
    for f in inner:
        beam_copies[f].start()
    pl.semaphore_wait(barrier, expected)
    if paired:
        even_only([near_copy(0, g) for g in range(groups)] + [first_copy(g) for g in range(groups)])
    else:
        for g in range(groups):
            send(0, g)
    advance()

    x0_copy.wait()
    for copy in small:
        copy.wait()
    def rows_of(ref, *at_f):
        place = (slice(None), *at_f)
        return jnp.concatenate(
            [ref[(slice(4 * g, 4 * g + 4), *place[1:], b)] for g in range(groups) for b in range(2)],
            axis=0,
        )

    def group(g):
        return slice(8 * g, 8 * g + 8)

    for f in range(freqs):
        x_s[f] = rows_of(x0_s, at(f))
    power, smooth = power_s[...], smooth_s[...]
    row = lax.broadcasted_iota(jnp.int32, (2 * modes, width), 0)
    own = lax.broadcasted_iota(jnp.int32, (2 * modes, width), 1) // rank == row // 8 * 4 + row % 4
    sign = jnp.where(row % 8 < 4, 1.0, -1.0)
    for i, f in enumerate(matrix):
        levels = noise_s[:, at(f), :]
        levels = jnp.concatenate(
            [levels[4 * g:4 * g + 4] for g in range(groups) for _ in range(2)], axis=0
        )
        mask_s[i] = jnp.where(own, jnp.concatenate([levels] * modes, axis=1), 0.0)
    unit = (
        lax.broadcasted_iota(jnp.int32, (rank, rank), 0)
        == lax.broadcasted_iota(jnp.int32, (rank, rank), 1)
    )
    for i, f in enumerate(vector):
        levels = noise_s[:, at(f), :]
        for m in range(modes):
            column = jnp.sum(jnp.where(unit, levels[m:m + 1], 0.0), axis=1, keepdims=True)
            column_s[i, m] = jnp.broadcast_to(column, (rank, 128))

    def swapped(x):
        return jnp.concatenate([pltpu.roll(x[group(g)], 4, 0) for g in range(groups)], axis=0)

    def matrix_project(f, field):
        i = matrix.index(f)
        seen = times(field, high_s[i], low_s[i], True)
        parts = seen[:, :width] + sign * swapped(seen[:, width:])
        return parts, mask_s[i] * parts

    def matrix_back(f, seen):
        i = matrix.index(f)
        weighted = jnp.concatenate([seen[1], -sign * swapped(seen[1])], axis=1)
        return times(weighted, high_s[i], low_s[i], False)

    def wide(x):
        return jnp.concatenate([x] * (ell // 128), axis=1)

    def owned(f):
        return (lambda m, a: beam_s[f, m, a]), (lambda m: column_s[vector.index(f), m])

    lent = (lambda m, a: lent_beam_s[m, a]), (lambda m: lent_column_s[m])

    def group_project(source, g, field):
        beam_of, column_of = source
        parts = []
        for j in range(4):
            m = 4 * g + j
            real_beam, imaginary_beam = beam_of(m, 0), beam_of(m, 1)
            real_field, imaginary_field = field[j:j + 1], field[4 + j:5 + j]
            levels = column_of(m)
            real = jnp.sum(
                real_beam * real_field + imaginary_beam * imaginary_field, axis=1, keepdims=True
            )
            imaginary = jnp.sum(
                real_beam * imaginary_field - imaginary_beam * real_field, axis=1, keepdims=True
            )
            parts.append((real, imaginary, levels * real, levels * imaginary))
        return parts

    def group_back(source, g, parts):
        beam_of, _ = source
        reals, imaginaries = [], []
        for j, (_, _, real, imaginary) in enumerate(parts):
            m = 4 * g + j
            real, imaginary = wide(real), wide(imaginary)
            real_beam, imaginary_beam = beam_of(m, 0), beam_of(m, 1)
            for found, value in (
                (reals, real_beam * real - imaginary_beam * imaginary),
                (imaginaries, real_beam * imaginary + imaginary_beam * real),
            ):
                found.append(sum(value[k:k + 8] for k in range(0, rank, 8)))
        return folded(reals + imaginaries)

    def group_beam(source, g, field):
        return group_back(source, g, group_project(source, g, field))

    def project(f, ref):
        if f in matrix:
            return matrix_project(f, ref[f])
        return [group_project(owned(f), g, ref[f, group(g)]) for g in range(groups)]

    def back(f, seen):
        if f in matrix:
            return matrix_back(f, seen)
        return jnp.concatenate([group_back(owned(f), g, seen[g]) for g in range(groups)], axis=0)

    def apply_beam(fs, ref):
        fs = [f for f in fs if f in matrix] + [f for f in fs if f in vector]
        seen = [project(f, ref) for f in fs]
        return {f: back(f, found) for f, found in zip(fs, seen)}

    def count(f):
        value = float(f > 0) + float(f < last) + float(nf > 1 and f == 0)
        if two_sided and f == last:
            value = value + jnp.where(has_far, 1.0, 0.0)
        return value

    def local_prior(f, ref, rows=slice(None)):
        value = count(f) * ref[f, rows]
        if f > 0:
            value = value - ref[f - 1, rows]
        if f < last:
            value = value - ref[f + 1, rows]
        return power * ref[f, rows] + smooth * value

    for f in edges:
        beam_copies[f].wait()
    rhs_copy.wait()
    for i, f in enumerate(edges):
        for g in range(groups):
            rows = group(g)
            image = group_beam(owned(f), g, x_s[f, rows])
            y_s[i, rows] = rows_of(rhs_s, at(f))[rows] - image - local_prior(f, x_s, rows)
    if paired:
        @pl.when(helper)
        def _():
            for g in range(groups):
                near_copy(0, g).start()

    for g in range(groups):
        send(1, g)
    first, rest = [], inner
    if paired:
        even_only([lend(k) for k in range(3)])
        first, rest = inner[:1], inner[1:]

    for f in first:
        beam_copies[f].wait()
        r_s[f] = rows_of(rhs_s, at(f)) - back(f, project(f, x_s)) - local_prior(f, x_s)
    if paired:
        even_only([lend(3)])

    for f in rest:
        beam_copies[f].wait()
    for i, f in enumerate(matrix):
        for a in range(2):
            rows = slice(a * width, (a + 1) * width)
            high, low = split(beam_s[f, :, a].reshape(width, ell))
            high_s[i, rows] = high
            low_s[i, rows] = low
    for f, image in apply_beam(rest, x_s).items():
        r_s[f] = rows_of(rhs_s, at(f)) - image - local_prior(f, x_s)
    for f, image in apply_beam(inner, r_s).items():
        u_s[f] = image + local_prior(f, r_s) if f in apart else image
    seen = {f: project(f, u_s) for f in apart}
    advance()

    if paired:
        @pl.when(helper)
        def _():
            for k in range(4):
                lend(k).wait_recv()
            for g in range(groups):
                first_copy(g).wait_recv()
                rows = group(g)
                halo = jnp.concatenate([lent_first_s[4 * g:4 * g + 4, b, :] for b in range(2)], axis=0)
                r = lent_y_s[rows] + smooth * halo
                local = power * r + smooth * (count(0) * r - lent_r_s[rows])
                lent_v_s[rows] = group_beam(lent, g, r) + local
                cross_copy(g).start()

    for g in range(groups):
        arrive(0, g)
        rows = group(g)
        for i, f in enumerate(edges):
            halo = jnp.concatenate([first_s[i, 4 * g:4 * g + 4, b, :] for b in range(2)], axis=0)
            r_s[f, rows] = y_s[i, rows] + smooth * halo
        for i, f in enumerate(edges):
            v_s[i, rows] = group_beam(owned(f), g, r_s[f, rows]) + local_prior(f, r_s, rows)
        send(2, g)
    for f in beside_edge:
        u_s[f] = u_s[f] + local_prior(f, r_s)
    seen |= {f: project(f, u_s) for f in beside_edge}

    for g in range(groups):
        arrive(1, g)
    for i, f in enumerate(edges):
        u_s[f] = v_s[i] - beside(i, smooth * (halo_s[0, i] + smooth * x_s[f]))
    if paired:
        pull_s[...] = smooth * u_s[0]
        even_only([pull_copy()])
    seen |= {f: project(f, u_s) for f in edges}
    norm = jnp.zeros((2 * modes, ell), F32)
    curve, square, cube = norm, norm, norm
    beam_part = jnp.zeros((2 * modes, width), F32)
    column_part = jnp.zeros((rank, 128), F32)
    for f in inner + edges:
        if f in matrix:
            beam_part = beam_part + seen[f][0] * seen[f][1]
        else:
            for parts in seen[f]:
                for real, imaginary, real_weighted, imaginary_weighted in parts:
                    column_part = column_part + (real * real_weighted + imaginary * imaginary_weighted)
        w_s[f] = local_prior(f, u_s)
        norm = norm + r_s[f] * r_s[f]
        curve = curve + r_s[f] * u_s[f]
        square = square + u_s[f] * u_s[f]
        cube = cube + u_s[f] * w_s[f]
    lane = lax.broadcasted_iota(jnp.int32, (1, 128), 1)
    message = jnp.zeros((1, 128), F32)
    for i, part in enumerate((norm, curve, square, cube)):
        total = total_of(part)
        if i == 3:
            total = total + total_of(beam_part) + jnp.sum(column_part, axis=0, keepdims=True)
        message = jnp.where(lane == i, total, message)
    if paired:
        message = jnp.where(lane == 4 + my_f, total_of(smooth * r_s[0] * pull_s[...]), message)
    message_s[0] = message
    early_s[me] = message

    while steps:
        advance()

    def share(source, target, slot, turn, device):
        pltpu.make_async_remote_copy(
            src_ref=message_s.at[source], dst_ref=target.at[slot],
            send_sem=sum_send.at[turn], recv_sem=sum_recv.at[turn],
            device_id=device, device_id_type=MESH,
        ).start()

    def share_all(source, target, slot, turn, stride):
        if n > 64:
            def body(i, carry):
                ma, f = my_ma + i * stride // nf, my_f + i * stride % nf
                share(source, target, slot, turn, (lax.rem(ma, nma), lax.rem(f, nf)))
                return carry

            lax.fori_loop(1, n // stride, body, 0)
        else:
            for mask in sorted(range(stride, n, stride), key=lambda m: (-(m // nf // 2), m)):
                device = partner([bit for bit in range(bits) if mask >> bit & 1])
                share(source, target, slot, turn, device)

    def landed(target, sem, rows):
        if rows:
            rows = target.at[pl.ds(0, rows)]
            pltpu.make_async_copy(rows, rows, sem).wait()

    def lanes_of(x):
        x = jnp.sum(x, axis=0, keepdims=True)
        return sum(x[:, i:i + 128] for i in range(0, ell, 128))

    share_all(0, early_s, me, 0, 1)
    for f in matrix + vector:
        w_s[f] = w_s[f] + back(f, seen[f])

    late_rows = late_s.shape[0]
    if paired:
        @pl.when(helper)
        def _():
            cross = jnp.zeros((8, ell), F32)
            for g in range(groups):
                arrive(2, g)
                cross = cross + pull_s[group(g)] * halo_s[1, 0, group(g)]
            pull_copy().wait_recv()
            for g in range(groups):
                cross_copy(g).wait_recv()
                cross = cross + partner_s[group(g)] * cross_s[group(g)]
            message = lanes_of(cross)
            late_s[my_ma // 2] = message
            message_s[1] = message
            share_all(1, late_s, my_ma // 2, 1, nf)
            for g in range(groups):
                cross_copy(g).wait_send()

        @pl.when(jnp.logical_not(helper))
        def _():
            for g in range(groups):
                arrive(2, g)
            pull_copy().wait_send()
            for k in range(4):
                lend(k).wait_send()
            for g in range(groups):
                first_copy(g).wait_send()

        w_s[0] = w_s[0] - smooth * (halo_s[1, 0] - smooth * r_s[0])
    else:
        cross = jnp.zeros((8, ell), F32)
        nexts = []
        for g in range(groups):
            arrive(2, g)
            rows = group(g)
            for i, f in enumerate(edges):
                pull = beside(i, smooth * (halo_s[1, i, rows] - smooth * r_s[f, rows]))
                nexts.append((f, rows, pull))
                cross = cross + pull * u_s[f, rows]
        message = lanes_of(cross)
        late_s[me] = message
        message_s[1] = message
        share_all(1, late_s, me, 1, 1)
        for f, rows, pull in nexts:
            w_s[f, rows] = w_s[f, rows] - pull

    for kind in range(3):
        for g in range(groups):
            sent(kind, g)
    landed(early_s, sum_recv.at[0], n - 1)
    total = jnp.sum(early_s[...], axis=0)
    m0, m1, m2, m3, known = (
        jnp.sum(jnp.where(lane == i, total, 0.0), axis=1, keepdims=True)
        for i in (0, 1, 2, 3, 4 + my_f)
    )
    if paired:
        m3 = m3 + 2.0 * known
    step = m0 / m1
    norm_next = step * (step * m2 - m1)
    growth = norm_next / m0
    curve_part = m1 - 2.0 * step * m2 + step * step * m3 - growth * norm_next / step
    cross_scale = step * step * (2.0 if paired else 1.0)
    for f in range(freqs):
        x, r, u, w = x_s[f], r_s[f], u_s[f], w_s[f]
        for target, value in (
            (sol_s, x + step * r),
            (res_s, r - step * u),
            (sol_move_s, (1.0 + growth) * r - step * u),
            (res_move_s, (1.0 + growth) * u - step * w),
        ):
            for g in range(groups):
                for b in range(2):
                    start = 8 * g + 4 * b
                    target[4 * g:4 * g + 4, at(f), b, :] = value[start:start + 4]
    landed(early_s, sum_send.at[0], n - 1)
    if paired:
        @pl.when(helper)
        def _():
            rows = early_s.at[pl.ds(0, nma - 1)]
            pltpu.make_async_copy(rows, rows, sum_send.at[1]).wait()
            landed(late_s, sum_recv.at[1], late_rows - 1)

        pl.when(jnp.logical_not(helper))(lambda: landed(late_s, sum_recv.at[1], late_rows))
    else:
        landed(late_s, sum_send.at[1], late_rows - 1)
        landed(late_s, sum_recv.at[1], late_rows - 1)
    crossed = jnp.sum(jnp.sum(late_s[...], axis=0), axis=1, keepdims=True)
    step_next = norm_next / (curve_part - cross_scale * crossed)
    sol_s[...] = sol_s[...] + step_next * sol_move_s[...]
    res_s[...] = res_s[...] - step_next * res_move_s[...]


def scoped_kernel(nma, nf, sides, *refs):
    modes, freqs = refs[0].shape[:2]
    dma = pltpu.SemaphoreType.DMA
    pl.run_scoped(
        functools.partial(kernel, nma, nf, *refs),
        dma((7,)), dma((freqs,)), dma((3, modes // 4, sides)), dma((2 * (modes // 4) + 5,)), dma((2,)),
    )


def write_out(sol_in, res_in, sol_out, res_out, sem):
    copies = [
        pltpu.make_async_copy(sol_in, sol_out, sem.at[0]),
        pltpu.make_async_copy(res_in, res_out, sem.at[1]),
    ]
    for copy in copies:
        copy.start()
    for copy in copies:
        copy.wait()


def shards(right_side, start_field, beam, noise, inv_power, smooth):
    nma, nf = lax.axis_size("ma"), lax.axis_size("freq")
    modes, freqs, _, ell = right_side.shape
    rank = beam.shape[3]
    width = modes * rank
    sides = 2 if nf > 2 else 1
    vmem_spec = pl.BlockSpec(memory_space=pltpu.VMEM)
    any_spec = pl.BlockSpec(memory_space=pl.ANY)
    field = pltpu.VMEM(right_side.shape, F32)
    edge = pltpu.VMEM((sides, modes, 2, ell), F32)
    slab = pltpu.VMEM((freqs, 2 * modes, ell), F32)
    edge_field = pltpu.VMEM((2 * modes, ell), F32)
    edge_slab = pltpu.VMEM((sides, 2 * modes, ell), F32)
    vector = max(min(nf - 1, 2), freqs // 2)
    matrix = max(freqs - vector, 1)
    half = pltpu.VMEM((matrix, 2 * width, ell), BF16)
    outs = pl.pallas_call(
        functools.partial(scoped_kernel, nma, nf, sides),
        out_shape=[field] * 2,
        in_specs=[any_spec] * 6,
        out_specs=[vmem_spec] * 2,
        scratch_shapes=[
            field, field, edge,
            pltpu.VMEM((freqs, modes, 2, rank, ell), F32),
            pltpu.VMEM(noise.shape, F32),
            pltpu.VMEM((1, ell), F32), pltpu.VMEM((1, ell), F32),
            half, half,
            slab, edge_slab, slab, edge_slab, slab, slab,
            pltpu.VMEM((matrix, 2 * modes, width), F32),
            pltpu.VMEM((vector, modes, rank, 128), F32),
            edge,
            pltpu.VMEM((2, sides, 2 * modes, ell), F32),
            field, field,
            edge_field, edge_field, edge_field,
            pltpu.VMEM((modes, 2, rank, ell), F32), pltpu.VMEM((modes, rank, 128), F32),
            edge_field, edge_field, pltpu.VMEM((modes, 2, ell), F32), edge_field,
            pltpu.VMEM((2, 1, 128), F32),
            pltpu.VMEM((nma * nf, 1, 128), F32),
            pltpu.VMEM((nma // 2 if nf == 2 and nma % 2 == 0 and freqs > 1 else nma * nf, 1, 128), F32),
            pltpu.SemaphoreType.DMA((3, modes // 4, sides)),
            pltpu.SemaphoreType.DMA((2 * (modes // 4) + 5,)),
            pltpu.SemaphoreType.DMA((2,)),
            pltpu.SemaphoreType.REGULAR((max((nma * nf).bit_length() - 4, 1),)),
        ],
        compiler_params=pltpu.CompilerParams(
            collective_id=0, has_side_effects=True, vmem_limit_bytes=67043328 - 2 * right_side.size * 4
        ),
        name="solve",
    )(right_side, start_field, beam, noise, inv_power[None], smooth[None])
    return pl.pallas_call(
        write_out,
        out_shape=[jax.ShapeDtypeStruct(right_side.shape, F32)] * 2,
        in_specs=[vmem_spec] * 2,
        out_specs=[any_spec] * 2,
        scratch_shapes=[pltpu.SemaphoreType.DMA((2,))],
        compiler_params=pltpu.CompilerParams(vmem_limit_bytes=1024 * 1024),
        name="write_out",
    )(*outs)


def solution(mesh):
    in_specs = (
        P("ma", "freq", None, None),
        P("ma", "freq", None, None),
        P("ma", "freq", None, None, None),
        P("ma", "freq", None),
        P(),
        P(),
    )
    out_specs = (P("ma", "freq", None, None), P("ma", "freq", None, None))
    return jax.shard_map(shards, mesh=mesh, in_specs=in_specs, out_specs=out_specs, check_vma=False)
```

```python
import functools

import jax
import jax.numpy as jnp
from jax import lax
from jax.experimental import pallas as pl
from jax.experimental.pallas import tpu as pltpu
from jax.sharding import PartitionSpec as P

MESH = pl.DeviceIdType.MESH
F32, BF16 = jnp.float32, jnp.bfloat16


def split(x):
    high = x.astype(BF16)
    return high, (x - high.astype(F32)).astype(BF16)


def times(x, high, low, transposed):
    dims = (((1,), (1 if transposed else 0,)), ((), ()))
    rows = x.shape[0]
    x_high, x_low = split(x)
    both = jnp.concatenate([x_high, x_low], axis=0)
    main = lax.dot_general(both, high, dims, preferred_element_type=F32)
    rest = lax.dot_general(x_high, low, dims, preferred_element_type=F32)
    return main[:rows] + (main[rows:] + rest)


def folded(parts):
    row = lax.broadcasted_iota(jnp.int32, parts[0].shape, 0)
    upper = row < 4
    fours = [
        jnp.where(upper, parts[s], parts[s + 4])
        + pltpu.roll(jnp.where(upper, parts[s + 4], parts[s]), 4, 0)
        for s in range(4)
    ]
    even = row // 2 % 2 == 0
    twos = [
        jnp.where(
            even, fours[s] + pltpu.roll(fours[s], 6, 0), fours[s + 2] + pltpu.roll(fours[s + 2], 2, 0)
        )
        for s in range(2)
    ]
    return jnp.where(
        row % 2 == 0, twos[0] + pltpu.roll(twos[0], 7, 0), twos[1] + pltpu.roll(twos[1], 1, 0)
    )


def total_of(x):
    return jnp.sum(jnp.sum(x, axis=0, keepdims=True), axis=1, keepdims=True)


def kernel(
    nma, nf, rhs_in, x0_in, beam_in, noise_in, power_in, smooth_in, sol_s, res_s,
    rhs_s, x0_s, edge_s, beam_s, noise_s, power_s, smooth_s,
    high_s, low_s, x_s, y_s, r_s, v_s, u_s, w_s, mask_s, column_s, first_s, halo_s,
    sol_move_s, res_move_s, pull_s, partner_s, cross_s,
    lent_beam_s, lent_column_s, lent_y_s, lent_r_s, lent_first_s, lent_v_s,
    message_s, early_s, late_s,
    halo_recv, pair_recv, sum_recv, word_sem, in_sem, beam_sem, halo_send, pair_send, sum_send,
):
    modes, freqs, _, ell = rhs_in.shape
    rank = beam_in.shape[3]
    width = modes * rank
    n = nma * nf
    my_ma, my_f = lax.axis_index("ma"), lax.axis_index("freq")
    me = my_ma * nf + my_f
    last = freqs - 1
    two_sided = nf > 2
    paired = nf == 2 and nma % 2 == 0 and freqs > 1
    helper = my_ma % 2 == 1
    groups = modes // 4
    edges = [0, last][:min(nf - 1, 2)]
    inner = [f for f in range(freqs) if f not in edges]
    beside_edge = [f for f in inner if f - 1 in edges or f + 1 in edges]
    apart = [f for f in inner if f not in beside_edge]
    vector = edges + inner[:max(freqs // 2 - len(edges), 0)]
    matrix = [f for f in range(freqs) if f not in vector]

    def at(g):
        return jnp.where(my_f == 0, last - g, g)

    edge_copies = [
        pltpu.make_async_copy(x0_in.at[:, at(f)], edge_s.at[i], in_sem.at[i])
        for i, f in enumerate(edges)
    ]
    x0_copy = pltpu.make_async_copy(x0_in, x0_s, in_sem.at[2])
    rhs_copy = pltpu.make_async_copy(rhs_in, rhs_s, in_sem.at[3])
    small = [
        pltpu.make_async_copy(power_in, power_s, in_sem.at[4]),
        pltpu.make_async_copy(smooth_in, smooth_s, in_sem.at[5]),
        pltpu.make_async_copy(noise_in, noise_s, in_sem.at[6]),
    ]
    beam_copies = [
        pltpu.make_async_copy(beam_in.at[:, at(f)], beam_s.at[f], beam_sem.at[f])
        for f in range(freqs)
    ]
    for copy in edge_copies:
        copy.start()

    def flip(bit):
        d = 1 << (bit if bit < freq_bits else bit - freq_bits)
        place = my_f if bit < freq_bits else my_ma
        return d * (1 - 2 * (place // d % 2))

    def partner(bits):
        return (
            my_ma + sum(flip(bit) for bit in bits if bit >= freq_bits),
            my_f + sum(flip(bit) for bit in bits if bit < freq_bits),
        )

    freq_bits = nf.bit_length() - 1
    bits = freq_bits + nma.bit_length() - 1
    close = min(bits, 3)
    greeted = [
        partner([bit for bit in range(close) if mask >> bit & 1]) for mask in range(1, 1 << close)
    ]
    word = [partner([bit]) for bit in range(close, bits)]
    greeted += word
    words = len(word)
    barrier = pltpu.get_barrier_semaphore()
    near = jnp.where(my_f == 0, 1, my_f - 1)
    has_far = (my_f > 0) & (my_f < nf - 1)

    def greet(device):
        pl.semaphore_signal(barrier, inc=1, device_id=device, device_id_type=MESH)

    for i, device in enumerate(greeted):
        greet(device)
        if i == 0:
            for copy in [beam_copies[f] for f in edges] + [x0_copy, rhs_copy] + small:
                copy.start()
    expected = len(greeted)
    if nf > 2:
        pl.when(my_f > 0)(lambda: greet((my_ma, my_f - 1)))
        pl.when(my_f < nf - 1)(lambda: greet((my_ma, my_f + 1)))
        expected = expected + jnp.minimum(my_f, 1) + jnp.minimum(nf - 1 - my_f, 1)

    steps = list(range(words + 1))

    def advance():
        if steps:
            step = steps.pop(0)
            if step > 0:
                pl.semaphore_wait(word_sem.at[step - 1], 1)
            if step < words:
                pl.semaphore_signal(
                    word_sem.at[step], inc=1, device_id=word[step], device_id_type=MESH
                )

    def piece(kind, g):
        if kind == 0:
            rows = pl.ds(4 * g, 4)
            return (lambda i: edge_s.at[i, rows]), (lambda i: first_s.at[i, rows])
        source = (y_s, v_s)[kind - 1]
        rows = pl.ds(8 * g, 8)
        return (lambda i: source.at[i, rows]), (lambda i: halo_s.at[kind - 1, i, rows])

    def near_copy(kind, g):
        source, target = piece(kind, g)
        side = jnp.minimum(my_f // 2, 1) if two_sided else 0
        return pltpu.make_async_remote_copy(
            src_ref=source(0), dst_ref=target(side),
            send_sem=halo_send.at[kind, g, 0], recv_sem=halo_recv.at[kind, g, side],
            device_id=(my_ma, near), device_id_type=MESH,
        )

    def far_copy(kind, g):
        source, target = piece(kind, g)
        return pltpu.make_async_remote_copy(
            src_ref=source(1), dst_ref=target(0),
            send_sem=halo_send.at[kind, g, 1], recv_sem=halo_recv.at[kind, g, 0],
            device_id=(my_ma, my_f + 1), device_id_type=MESH,
        )

    def arrival(kind, g, side):
        slot = piece(kind, g)[1](side)
        return pltpu.make_async_copy(slot, slot, halo_recv.at[kind, g, side])

    def send(kind, g):
        if nf > 1:
            near_copy(kind, g).start()
        if two_sided:
            pl.when(has_far)(lambda: far_copy(kind, g).start())

    def arrive(kind, g):
        if nf > 1:
            arrival(kind, g, 0).wait()
        if two_sided:
            pl.when(has_far)(lambda: arrival(kind, g, 1).wait())

    def sent(kind, g):
        if nf > 1:
            near_copy(kind, g).wait_send()
        if two_sided:
            pl.when(has_far)(lambda: far_copy(kind, g).wait_send())

    def pair_copy(k, source, target, ma, f):
        return pltpu.make_async_remote_copy(
            src_ref=source, dst_ref=target, send_sem=pair_send.at[k], recv_sem=pair_recv.at[k],
            device_id=(ma, f), device_id_type=MESH,
        )

    def lend(k):
        source = (lambda: beam_s.at[0], lambda: column_s.at[0], lambda: y_s.at[0], lambda: r_s.at[1])[k]
        target = (lent_beam_s, lent_column_s, lent_y_s, lent_r_s)[k]
        return pair_copy(k, source(), target, my_ma + 1, my_f)

    def pull_copy():
        return pair_copy(4, pull_s, partner_s, my_ma + 1, my_f)

    def first_copy(g):
        rows = pl.ds(4 * g, 4)
        return pair_copy(5 + g, edge_s.at[0, rows], lent_first_s.at[rows], my_ma + 1, 1 - my_f)

    def cross_copy(g):
        rows = pl.ds(8 * g, 8)
        return pair_copy(5 + groups + g, lent_v_s.at[rows], cross_s.at[rows], my_ma, 1 - my_f)

    def even_only(copies):
        @pl.when(jnp.logical_not(helper))
        def _():
            for copy in copies:
                copy.start()

    def beside(i, value):
        return jnp.where(has_far, value, 0.0) if i else value

    if two_sided:
        @pl.when(jnp.logical_not(has_far))
        def _():
            first_s[1] = jnp.zeros_like(first_s[1])
            halo_s[:, 1] = jnp.zeros_like(halo_s[:, 1])

    for copy in edge_copies:
        copy.wait()
    for f in inner:
        beam_copies[f].start()
    pl.semaphore_wait(barrier, expected)
    if paired:
        even_only([first_copy(g) for g in range(groups)] + [near_copy(0, g) for g in range(groups)])
    else:
        for g in range(groups):
            send(0, g)
    advance()

    x0_copy.wait()
    for copy in small:
        copy.wait()
    def rows_of(ref, *at_f):
        place = (slice(None), *at_f)
        return jnp.concatenate(
            [ref[(slice(4 * g, 4 * g + 4), *place[1:], b)] for g in range(groups) for b in range(2)],
            axis=0,
        )

    def group(g):
        return slice(8 * g, 8 * g + 8)

    for f in range(freqs):
        x_s[f] = rows_of(x0_s, at(f))
    power, smooth = power_s[...], smooth_s[...]
    row = lax.broadcasted_iota(jnp.int32, (2 * modes, width), 0)
    own = lax.broadcasted_iota(jnp.int32, (2 * modes, width), 1) // rank == row // 8 * 4 + row % 4
    sign = jnp.where(row % 8 < 4, 1.0, -1.0)
    for i, f in enumerate(matrix):
        levels = noise_s[:, at(f), :]
        levels = jnp.concatenate(
            [levels[4 * g:4 * g + 4] for g in range(groups) for _ in range(2)], axis=0
        )
        mask_s[i] = jnp.where(own, jnp.concatenate([levels] * modes, axis=1), 0.0)
    unit = (
        lax.broadcasted_iota(jnp.int32, (rank, rank), 0)
        == lax.broadcasted_iota(jnp.int32, (rank, rank), 1)
    )
    for i, f in enumerate(vector):
        levels = noise_s[:, at(f), :]
        for m in range(modes):
            column = jnp.sum(jnp.where(unit, levels[m:m + 1], 0.0), axis=1, keepdims=True)
            column_s[i, m] = jnp.broadcast_to(column, (rank, 128))

    def swapped(x):
        return jnp.concatenate([pltpu.roll(x[group(g)], 4, 0) for g in range(groups)], axis=0)

    def matrix_project(f, field):
        i = matrix.index(f)
        seen = times(field, high_s[i], low_s[i], True)
        parts = seen[:, :width] + sign * swapped(seen[:, width:])
        return parts, mask_s[i] * parts

    def matrix_back(f, seen):
        i = matrix.index(f)
        weighted = jnp.concatenate([seen[1], -sign * swapped(seen[1])], axis=1)
        return times(weighted, high_s[i], low_s[i], False)

    def wide(x):
        return jnp.concatenate([x] * (ell // 128), axis=1)

    def owned(f):
        return (lambda m, a: beam_s[f, m, a]), (lambda m: column_s[vector.index(f), m])

    lent = (lambda m, a: lent_beam_s[m, a]), (lambda m: lent_column_s[m])

    def group_project(source, g, field):
        beam_of, column_of = source
        parts = []
        for j in range(4):
            m = 4 * g + j
            real_beam, imaginary_beam = beam_of(m, 0), beam_of(m, 1)
            real_field, imaginary_field = field[j:j + 1], field[4 + j:5 + j]
            levels = column_of(m)
            real = jnp.sum(
                real_beam * real_field + imaginary_beam * imaginary_field, axis=1, keepdims=True
            )
            imaginary = jnp.sum(
                real_beam * imaginary_field - imaginary_beam * real_field, axis=1, keepdims=True
            )
            parts.append((real, imaginary, levels * real, levels * imaginary))
        return parts

    def group_back(source, g, parts):
        beam_of, _ = source
        reals, imaginaries = [], []
        for j, (_, _, real, imaginary) in enumerate(parts):
            m = 4 * g + j
            real, imaginary = wide(real), wide(imaginary)
            real_beam, imaginary_beam = beam_of(m, 0), beam_of(m, 1)
            for found, value in (
                (reals, real_beam * real - imaginary_beam * imaginary),
                (imaginaries, real_beam * imaginary + imaginary_beam * real),
            ):
                found.append(sum(value[k:k + 8] for k in range(0, rank, 8)))
        return folded(reals + imaginaries)

    def group_beam(source, g, field):
        return group_back(source, g, group_project(source, g, field))

    def project(f, ref):
        if f in matrix:
            return matrix_project(f, ref[f])
        return [group_project(owned(f), g, ref[f, group(g)]) for g in range(groups)]

    def back(f, seen):
        if f in matrix:
            return matrix_back(f, seen)
        return jnp.concatenate([group_back(owned(f), g, seen[g]) for g in range(groups)], axis=0)

    def apply_beam(fs, ref):
        fs = [f for f in fs if f in matrix] + [f for f in fs if f in vector]
        seen = [project(f, ref) for f in fs]
        return {f: back(f, found) for f, found in zip(fs, seen)}

    def count(f):
        value = float(f > 0) + float(f < last) + float(nf > 1 and f == 0)
        if two_sided and f == last:
            value = value + jnp.where(has_far, 1.0, 0.0)
        return value

    def local_prior(f, ref, rows=slice(None)):
        value = count(f) * ref[f, rows]
        if f > 0:
            value = value - ref[f - 1, rows]
        if f < last:
            value = value - ref[f + 1, rows]
        return power * ref[f, rows] + smooth * value

    for f in edges:
        beam_copies[f].wait()
    rhs_copy.wait()
    for i, f in enumerate(edges):
        for g in range(groups):
            rows = group(g)
            image = group_beam(owned(f), g, x_s[f, rows])
            y_s[i, rows] = rows_of(rhs_s, at(f))[rows] - image - local_prior(f, x_s, rows)
    first, rest = [], inner
    if paired:
        even_only([near_copy(1, g) for g in range(groups)] + [lend(k) for k in range(3)])
        first, rest = inner[:1], inner[1:]
    else:
        for g in range(groups):
            send(1, g)

    for f in first:
        beam_copies[f].wait()
        r_s[f] = rows_of(rhs_s, at(f)) - back(f, project(f, x_s)) - local_prior(f, x_s)
    if paired:
        even_only([lend(3)])

        @pl.when(helper)
        def _():
            for kind in range(2):
                for g in range(groups):
                    near_copy(kind, g).start()

    for f in rest:
        beam_copies[f].wait()
    for i, f in enumerate(matrix):
        for a in range(2):
            rows = slice(a * width, (a + 1) * width)
            high, low = split(beam_s[f, :, a].reshape(width, ell))
            high_s[i, rows] = high
            low_s[i, rows] = low
    for f, image in apply_beam(rest, x_s).items():
        r_s[f] = rows_of(rhs_s, at(f)) - image - local_prior(f, x_s)
    for f, image in apply_beam(inner, r_s).items():
        u_s[f] = image + local_prior(f, r_s) if f in apart else image
    seen = {f: project(f, u_s) for f in apart}
    advance()

    if paired:
        @pl.when(helper)
        def _():
            for k in range(4):
                lend(k).wait_recv()
            for g in range(groups):
                first_copy(g).wait_recv()
                rows = group(g)
                halo = jnp.concatenate([lent_first_s[4 * g:4 * g + 4, b, :] for b in range(2)], axis=0)
                r = lent_y_s[rows] + smooth * halo
                local = power * r + smooth * (count(0) * r - lent_r_s[rows])
                lent_v_s[rows] = group_beam(lent, g, r) + local
                cross_copy(g).start()

    for g in range(groups):
        arrive(0, g)
        rows = group(g)
        for i, f in enumerate(edges):
            halo = jnp.concatenate([first_s[i, 4 * g:4 * g + 4, b, :] for b in range(2)], axis=0)
            r_s[f, rows] = y_s[i, rows] + smooth * halo
        for i, f in enumerate(edges):
            v_s[i, rows] = group_beam(owned(f), g, r_s[f, rows]) + local_prior(f, r_s, rows)
        if paired:
            pl.when(helper)(lambda: near_copy(2, g).start())
        else:
            send(2, g)
    for f in beside_edge:
        u_s[f] = u_s[f] + local_prior(f, r_s)
    seen |= {f: project(f, u_s) for f in beside_edge}

    for g in range(groups):
        arrive(1, g)
    for i, f in enumerate(edges):
        u_s[f] = v_s[i] - beside(i, smooth * (halo_s[0, i] + smooth * x_s[f]))
    if paired:
        pull_s[...] = smooth * u_s[0]
        even_only([pull_copy()])
    seen |= {f: project(f, u_s) for f in edges}
    norm = jnp.zeros((2 * modes, ell), F32)
    curve, square, cube = norm, norm, norm
    beam_part = jnp.zeros((2 * modes, width), F32)
    column_part = jnp.zeros((rank, 128), F32)
    for f in inner + edges:
        if f in matrix:
            beam_part = beam_part + seen[f][0] * seen[f][1]
        else:
            for parts in seen[f]:
                for real, imaginary, real_weighted, imaginary_weighted in parts:
                    column_part = column_part + (real * real_weighted + imaginary * imaginary_weighted)
        w_s[f] = local_prior(f, u_s)
        norm = norm + r_s[f] * r_s[f]
        curve = curve + r_s[f] * u_s[f]
        square = square + u_s[f] * u_s[f]
        cube = cube + u_s[f] * w_s[f]
    lane = lax.broadcasted_iota(jnp.int32, (1, 128), 1)
    message = jnp.zeros((1, 128), F32)
    for i, part in enumerate((norm, curve, square, cube)):
        total = total_of(part)
        if i == 3:
            total = total + total_of(beam_part) + jnp.sum(column_part, axis=0, keepdims=True)
        message = jnp.where(lane == i, total, message)
    if paired:
        message = jnp.where(lane == 4 + my_f, total_of(smooth * r_s[0] * pull_s[...]), message)
    message_s[0] = message
    early_s[me] = message

    while steps:
        advance()

    def share(source, target, slot, turn, device):
        pltpu.make_async_remote_copy(
            src_ref=message_s.at[source], dst_ref=target.at[slot],
            send_sem=sum_send.at[turn], recv_sem=sum_recv.at[turn],
            device_id=device, device_id_type=MESH,
        ).start()

    def share_all(source, target, slot, turn, stride):
        if n > 64:
            def body(i, carry):
                ma, f = my_ma + i * stride // nf, my_f + i * stride % nf
                share(source, target, slot, turn, (lax.rem(ma, nma), lax.rem(f, nf)))
                return carry

            lax.fori_loop(1, n // stride, body, 0)
        else:
            for mask in sorted(range(stride, n, stride), key=lambda m: (-(m // nf // 2), m)):
                device = partner([bit for bit in range(bits) if mask >> bit & 1])
                share(source, target, slot, turn, device)

    def landed(target, sem, rows):
        if rows:
            rows = target.at[pl.ds(0, rows)]
            pltpu.make_async_copy(rows, rows, sem).wait()

    def lanes_of(x):
        x = jnp.sum(x, axis=0, keepdims=True)
        return sum(x[:, i:i + 128] for i in range(0, ell, 128))

    share_all(0, early_s, me, 0, 1)
    if paired:
        even_only([near_copy(2, g) for g in range(groups)])
    for f in matrix + vector:
        w_s[f] = w_s[f] + back(f, seen[f])

    late_rows = late_s.shape[0]
    if paired:
        @pl.when(helper)
        def _():
            cross = jnp.zeros((8, ell), F32)
            for g in range(groups):
                arrive(2, g)
                cross = cross + pull_s[group(g)] * halo_s[1, 0, group(g)]
            pull_copy().wait_recv()
            for g in range(groups):
                cross_copy(g).wait_recv()
                cross = cross + partner_s[group(g)] * cross_s[group(g)]
            message = lanes_of(cross)
            late_s[my_ma // 2] = message
            message_s[1] = message
            share_all(1, late_s, my_ma // 2, 1, nf)
            for g in range(groups):
                cross_copy(g).wait_send()

        @pl.when(jnp.logical_not(helper))
        def _():
            for g in range(groups):
                arrive(2, g)
            pull_copy().wait_send()
            for k in range(4):
                lend(k).wait_send()
            for g in range(groups):
                first_copy(g).wait_send()

        w_s[0] = w_s[0] - smooth * (halo_s[1, 0] - smooth * r_s[0])
    else:
        cross = jnp.zeros((8, ell), F32)
        nexts = []
        for g in range(groups):
            arrive(2, g)
            rows = group(g)
            for i, f in enumerate(edges):
                pull = beside(i, smooth * (halo_s[1, i, rows] - smooth * r_s[f, rows]))
                nexts.append((f, rows, pull))
                cross = cross + pull * u_s[f, rows]
        message = lanes_of(cross)
        late_s[me] = message
        message_s[1] = message
        share_all(1, late_s, me, 1, 1)
        for f, rows, pull in nexts:
            w_s[f, rows] = w_s[f, rows] - pull

    for kind in range(3):
        for g in range(groups):
            sent(kind, g)
    landed(early_s, sum_recv.at[0], n - 1)
    total = jnp.sum(early_s[...], axis=0)
    m0, m1, m2, m3, known = (
        jnp.sum(jnp.where(lane == i, total, 0.0), axis=1, keepdims=True)
        for i in (0, 1, 2, 3, 4 + my_f)
    )
    if paired:
        m3 = m3 + 2.0 * known
    step = m0 / m1
    norm_next = step * (step * m2 - m1)
    growth = norm_next / m0
    curve_part = m1 - 2.0 * step * m2 + step * step * m3 - growth * norm_next / step
    cross_scale = step * step * (2.0 if paired else 1.0)
    for f in range(freqs):
        x, r, u, w = x_s[f], r_s[f], u_s[f], w_s[f]
        for target, value in (
            (sol_s, x + step * r),
            (res_s, r - step * u),
            (sol_move_s, (1.0 + growth) * r - step * u),
            (res_move_s, (1.0 + growth) * u - step * w),
        ):
            for g in range(groups):
                for b in range(2):
                    start = 8 * g + 4 * b
                    target[4 * g:4 * g + 4, at(f), b, :] = value[start:start + 4]
    landed(early_s, sum_send.at[0], n - 1)
    if paired:
        @pl.when(helper)
        def _():
            rows = early_s.at[pl.ds(0, nma - 1)]
            pltpu.make_async_copy(rows, rows, sum_send.at[1]).wait()
            landed(late_s, sum_recv.at[1], late_rows - 1)

        pl.when(jnp.logical_not(helper))(lambda: landed(late_s, sum_recv.at[1], late_rows))
    else:
        landed(late_s, sum_send.at[1], late_rows - 1)
        landed(late_s, sum_recv.at[1], late_rows - 1)
    crossed = jnp.sum(jnp.sum(late_s[...], axis=0), axis=1, keepdims=True)
    step_next = norm_next / (curve_part - cross_scale * crossed)
    sol_s[...] = sol_s[...] + step_next * sol_move_s[...]
    res_s[...] = res_s[...] - step_next * res_move_s[...]


def scoped_kernel(nma, nf, sides, *refs):
    modes, freqs = refs[0].shape[:2]
    dma = pltpu.SemaphoreType.DMA
    pl.run_scoped(
        functools.partial(kernel, nma, nf, *refs),
        dma((7,)), dma((freqs,)), dma((3, modes // 4, sides)), dma((2 * (modes // 4) + 5,)), dma((2,)),
    )


def write_out(sol_in, res_in, sol_out, res_out, sem):
    copies = [
        pltpu.make_async_copy(sol_in, sol_out, sem.at[0]),
        pltpu.make_async_copy(res_in, res_out, sem.at[1]),
    ]
    for copy in copies:
        copy.start()
    for copy in copies:
        copy.wait()


def shards(right_side, start_field, beam, noise, inv_power, smooth):
    nma, nf = lax.axis_size("ma"), lax.axis_size("freq")
    modes, freqs, _, ell = right_side.shape
    rank = beam.shape[3]
    width = modes * rank
    sides = 2 if nf > 2 else 1
    vmem_spec = pl.BlockSpec(memory_space=pltpu.VMEM)
    any_spec = pl.BlockSpec(memory_space=pl.ANY)
    field = pltpu.VMEM(right_side.shape, F32)
    edge = pltpu.VMEM((sides, modes, 2, ell), F32)
    slab = pltpu.VMEM((freqs, 2 * modes, ell), F32)
    edge_field = pltpu.VMEM((2 * modes, ell), F32)
    edge_slab = pltpu.VMEM((sides, 2 * modes, ell), F32)
    vector = max(min(nf - 1, 2), freqs // 2)
    matrix = max(freqs - vector, 1)
    half = pltpu.VMEM((matrix, 2 * width, ell), BF16)
    outs = pl.pallas_call(
        functools.partial(scoped_kernel, nma, nf, sides),
        out_shape=[field] * 2,
        in_specs=[any_spec] * 6,
        out_specs=[vmem_spec] * 2,
        scratch_shapes=[
            field, field, edge,
            pltpu.VMEM((freqs, modes, 2, rank, ell), F32),
            pltpu.VMEM(noise.shape, F32),
            pltpu.VMEM((1, ell), F32), pltpu.VMEM((1, ell), F32),
            half, half,
            slab, edge_slab, slab, edge_slab, slab, slab,
            pltpu.VMEM((matrix, 2 * modes, width), F32),
            pltpu.VMEM((vector, modes, rank, 128), F32),
            edge,
            pltpu.VMEM((2, sides, 2 * modes, ell), F32),
            field, field,
            edge_field, edge_field, edge_field,
            pltpu.VMEM((modes, 2, rank, ell), F32), pltpu.VMEM((modes, rank, 128), F32),
            edge_field, edge_field, pltpu.VMEM((modes, 2, ell), F32), edge_field,
            pltpu.VMEM((2, 1, 128), F32),
            pltpu.VMEM((nma * nf, 1, 128), F32),
            pltpu.VMEM((nma // 2 if nf == 2 and nma % 2 == 0 and freqs > 1 else nma * nf, 1, 128), F32),
            pltpu.SemaphoreType.DMA((3, modes // 4, sides)),
            pltpu.SemaphoreType.DMA((2 * (modes // 4) + 5,)),
            pltpu.SemaphoreType.DMA((2,)),
            pltpu.SemaphoreType.REGULAR((max((nma * nf).bit_length() - 4, 1),)),
        ],
        compiler_params=pltpu.CompilerParams(
            collective_id=0, has_side_effects=True, vmem_limit_bytes=67043328 - 2 * right_side.size * 4
        ),
        name="solve",
    )(right_side, start_field, beam, noise, inv_power[None], smooth[None])
    return pl.pallas_call(
        write_out,
        out_shape=[jax.ShapeDtypeStruct(right_side.shape, F32)] * 2,
        in_specs=[vmem_spec] * 2,
        out_specs=[any_spec] * 2,
        scratch_shapes=[pltpu.SemaphoreType.DMA((2,))],
        compiler_params=pltpu.CompilerParams(vmem_limit_bytes=1024 * 1024),
        name="write_out",
    )(*outs)


def solution(mesh):
    in_specs = (
        P("ma", "freq", None, None),
        P("ma", "freq", None, None),
        P("ma", "freq", None, None, None),
        P("ma", "freq", None),
        P(),
        P(),
    )
    out_specs = (P("ma", "freq", None, None), P("ma", "freq", None, None))
    return jax.shard_map(shards, mesh=mesh, in_specs=in_specs, out_specs=out_specs, check_vma=False)
```

```python
import functools

import jax
import jax.numpy as jnp
from jax import lax
from jax.experimental import pallas as pl
from jax.experimental.pallas import tpu as pltpu
from jax.sharding import PartitionSpec as P

MESH = pl.DeviceIdType.MESH
F32, BF16 = jnp.float32, jnp.bfloat16


def split(x):
    high = x.astype(BF16)
    return high, (x - high.astype(F32)).astype(BF16)


def times(x, high, low, transposed):
    dims = (((1,), (1 if transposed else 0,)), ((), ()))
    rows = x.shape[0]
    x_high, x_low = split(x)
    both = jnp.concatenate([x_high, x_low], axis=0)
    main = lax.dot_general(both, high, dims, preferred_element_type=F32)
    rest = lax.dot_general(x_high, low, dims, preferred_element_type=F32)
    return main[:rows] + (main[rows:] + rest)


def folded(parts):
    row = lax.broadcasted_iota(jnp.int32, parts[0].shape, 0)
    upper = row < 4
    fours = [
        jnp.where(upper, parts[s], parts[s + 4])
        + pltpu.roll(jnp.where(upper, parts[s + 4], parts[s]), 4, 0)
        for s in range(4)
    ]
    even = row // 2 % 2 == 0
    twos = [
        jnp.where(
            even, fours[s] + pltpu.roll(fours[s], 6, 0), fours[s + 2] + pltpu.roll(fours[s + 2], 2, 0)
        )
        for s in range(2)
    ]
    return jnp.where(
        row % 2 == 0, twos[0] + pltpu.roll(twos[0], 7, 0), twos[1] + pltpu.roll(twos[1], 1, 0)
    )


def total_of(x):
    return jnp.sum(jnp.sum(x, axis=0, keepdims=True), axis=1, keepdims=True)


def kernel(
    nma, nf, rhs_in, x0_in, beam_in, noise_in, power_in, smooth_in, sol_s, res_s,
    rhs_s, x0_s, edge_s, beam_s, noise_s, power_s, smooth_s,
    high_s, low_s, x_s, y_s, r_s, v_s, u_s, w_s, mask_s, column_s, first_s, halo_s,
    r_out_s, u_out_s, w_out_s, pull_s, partner_s, cross_s,
    lent_beam_s, lent_column_s, lent_y_s, lent_r_s, lent_first_s, lent_v_s,
    message_s, early_s, late_s,
    halo_recv, pair_recv, sum_recv, word_sem, in_sem, beam_sem, halo_send, pair_send, sum_send,
):
    modes, freqs, _, ell = rhs_in.shape
    rank = beam_in.shape[3]
    width = modes * rank
    n = nma * nf
    my_ma, my_f = lax.axis_index("ma"), lax.axis_index("freq")
    me = my_ma * nf + my_f
    last = freqs - 1
    two_sided = nf > 2
    paired = nf == 2 and nma % 2 == 0 and freqs > 1
    helper = my_ma % 2 == 1
    groups = modes // 4
    edges = [0, last][:min(nf - 1, 2)]
    inner = [f for f in range(freqs) if f not in edges]
    beside_edge = [f for f in inner if f - 1 in edges or f + 1 in edges]
    apart = [f for f in inner if f not in beside_edge]
    vector = edges + inner[:max(freqs // 2 - len(edges), 0)]
    matrix = [f for f in range(freqs) if f not in vector]

    def at(g):
        return jnp.where(my_f == 0, last - g, g)

    edge_copies = [
        pltpu.make_async_copy(x0_in.at[:, at(f)], edge_s.at[i], in_sem.at[i])
        for i, f in enumerate(edges)
    ]
    x0_copy = pltpu.make_async_copy(x0_in, x0_s, in_sem.at[2])
    rhs_copy = pltpu.make_async_copy(rhs_in, rhs_s, in_sem.at[3])
    small = [
        pltpu.make_async_copy(power_in, power_s, in_sem.at[4]),
        pltpu.make_async_copy(smooth_in, smooth_s, in_sem.at[5]),
        pltpu.make_async_copy(noise_in, noise_s, in_sem.at[6]),
    ]
    beam_copies = [
        pltpu.make_async_copy(beam_in.at[:, at(f)], beam_s.at[f], beam_sem.at[f])
        for f in range(freqs)
    ]
    for copy in edge_copies:
        copy.start()

    def flip(bit):
        d = 1 << (bit if bit < freq_bits else bit - freq_bits)
        place = my_f if bit < freq_bits else my_ma
        return d * (1 - 2 * (place // d % 2))

    def partner(bits):
        return (
            my_ma + sum(flip(bit) for bit in bits if bit >= freq_bits),
            my_f + sum(flip(bit) for bit in bits if bit < freq_bits),
        )

    freq_bits = nf.bit_length() - 1
    bits = freq_bits + nma.bit_length() - 1
    close = min(bits, 3)
    greeted = [
        partner([bit for bit in range(close) if mask >> bit & 1]) for mask in range(1, 1 << close)
    ]
    word = [partner([bit]) for bit in range(close, bits)]
    greeted += word
    words = len(word)
    barrier = pltpu.get_barrier_semaphore()
    near = jnp.where(my_f == 0, 1, my_f - 1)
    has_far = (my_f > 0) & (my_f < nf - 1)

    def greet(device):
        pl.semaphore_signal(barrier, inc=1, device_id=device, device_id_type=MESH)

    for i, device in enumerate(greeted):
        greet(device)
        if i == 0:
            for copy in [beam_copies[f] for f in edges] + [x0_copy, rhs_copy] + small:
                copy.start()
    expected = len(greeted)
    if nf > 2:
        pl.when(my_f > 0)(lambda: greet((my_ma, my_f - 1)))
        pl.when(my_f < nf - 1)(lambda: greet((my_ma, my_f + 1)))
        expected = expected + jnp.minimum(my_f, 1) + jnp.minimum(nf - 1 - my_f, 1)

    steps = list(range(words + 1))

    def advance():
        if steps:
            step = steps.pop(0)
            if step > 0:
                pl.semaphore_wait(word_sem.at[step - 1], 1)
            if step < words:
                pl.semaphore_signal(
                    word_sem.at[step], inc=1, device_id=word[step], device_id_type=MESH
                )

    def piece(kind, g):
        if kind == 0:
            rows = pl.ds(4 * g, 4)
            return (lambda i: edge_s.at[i, rows]), (lambda i: first_s.at[i, rows])
        source = (y_s, v_s)[kind - 1]
        rows = pl.ds(8 * g, 8)
        return (lambda i: source.at[i, rows]), (lambda i: halo_s.at[kind - 1, i, rows])

    def near_copy(kind, g):
        source, target = piece(kind, g)
        side = jnp.minimum(my_f // 2, 1) if two_sided else 0
        return pltpu.make_async_remote_copy(
            src_ref=source(0), dst_ref=target(side),
            send_sem=halo_send.at[kind, g, 0], recv_sem=halo_recv.at[kind, g, side],
            device_id=(my_ma, near), device_id_type=MESH,
        )

    def far_copy(kind, g):
        source, target = piece(kind, g)
        return pltpu.make_async_remote_copy(
            src_ref=source(1), dst_ref=target(0),
            send_sem=halo_send.at[kind, g, 1], recv_sem=halo_recv.at[kind, g, 0],
            device_id=(my_ma, my_f + 1), device_id_type=MESH,
        )

    def arrival(kind, g, side):
        slot = piece(kind, g)[1](side)
        return pltpu.make_async_copy(slot, slot, halo_recv.at[kind, g, side])

    def send(kind, g):
        if nf > 1:
            near_copy(kind, g).start()
        if two_sided:
            pl.when(has_far)(lambda: far_copy(kind, g).start())

    def arrive(kind, g):
        if nf > 1:
            arrival(kind, g, 0).wait()
        if two_sided:
            pl.when(has_far)(lambda: arrival(kind, g, 1).wait())

    def sent(kind, g):
        if nf > 1:
            near_copy(kind, g).wait_send()
        if two_sided:
            pl.when(has_far)(lambda: far_copy(kind, g).wait_send())

    def pair_copy(k, source, target, ma, f):
        return pltpu.make_async_remote_copy(
            src_ref=source, dst_ref=target, send_sem=pair_send.at[k], recv_sem=pair_recv.at[k],
            device_id=(ma, f), device_id_type=MESH,
        )

    def lend(k):
        source = (lambda: beam_s.at[0], lambda: column_s.at[0], lambda: y_s.at[0], lambda: r_s.at[1])[k]
        target = (lent_beam_s, lent_column_s, lent_y_s, lent_r_s)[k]
        return pair_copy(k, source(), target, my_ma + 1, my_f)

    def pull_copy():
        return pair_copy(4, pull_s, partner_s, my_ma + 1, my_f)

    def first_copy(g):
        rows = pl.ds(4 * g, 4)
        return pair_copy(5 + g, edge_s.at[0, rows], lent_first_s.at[rows], my_ma + 1, 1 - my_f)

    def cross_copy(g):
        rows = pl.ds(8 * g, 8)
        return pair_copy(5 + groups + g, lent_v_s.at[rows], cross_s.at[rows], my_ma, 1 - my_f)

    def even_only(copies):
        @pl.when(jnp.logical_not(helper))
        def _():
            for copy in copies:
                copy.start()

    def beside(i, value):
        return jnp.where(has_far, value, 0.0) if i else value

    if two_sided:
        @pl.when(jnp.logical_not(has_far))
        def _():
            first_s[1] = jnp.zeros_like(first_s[1])
            halo_s[:, 1] = jnp.zeros_like(halo_s[:, 1])

    for copy in edge_copies:
        copy.wait()
    for f in inner:
        beam_copies[f].start()
    pl.semaphore_wait(barrier, expected)
    for g in range(groups):
        send(0, g)
    if paired:
        even_only([first_copy(g) for g in range(groups)])
    advance()

    x0_copy.wait()
    for copy in small:
        copy.wait()
    def rows_of(ref, *at_f):
        place = (slice(None), *at_f)
        return jnp.concatenate(
            [ref[(slice(4 * g, 4 * g + 4), *place[1:], b)] for g in range(groups) for b in range(2)],
            axis=0,
        )

    def group(g):
        return slice(8 * g, 8 * g + 8)

    for f in range(freqs):
        x_s[f] = rows_of(x0_s, at(f))
    power, smooth = power_s[...], smooth_s[...]
    row = lax.broadcasted_iota(jnp.int32, (2 * modes, width), 0)
    own = lax.broadcasted_iota(jnp.int32, (2 * modes, width), 1) // rank == row // 8 * 4 + row % 4
    sign = jnp.where(row % 8 < 4, 1.0, -1.0)
    for i, f in enumerate(matrix):
        levels = noise_s[:, at(f), :]
        levels = jnp.concatenate(
            [levels[4 * g:4 * g + 4] for g in range(groups) for _ in range(2)], axis=0
        )
        mask_s[i] = jnp.where(own, jnp.concatenate([levels] * modes, axis=1), 0.0)
    unit = (
        lax.broadcasted_iota(jnp.int32, (rank, rank), 0)
        == lax.broadcasted_iota(jnp.int32, (rank, rank), 1)
    )
    for i, f in enumerate(vector):
        levels = noise_s[:, at(f), :]
        for m in range(modes):
            column = jnp.sum(jnp.where(unit, levels[m:m + 1], 0.0), axis=1, keepdims=True)
            column_s[i, m] = jnp.broadcast_to(column, (rank, 128))

    def swapped(x):
        return jnp.concatenate([pltpu.roll(x[group(g)], 4, 0) for g in range(groups)], axis=0)

    def matrix_project(f, field):
        i = matrix.index(f)
        seen = times(field, high_s[i], low_s[i], True)
        parts = seen[:, :width] + sign * swapped(seen[:, width:])
        return parts, mask_s[i] * parts

    def matrix_back(f, seen):
        i = matrix.index(f)
        weighted = jnp.concatenate([seen[1], -sign * swapped(seen[1])], axis=1)
        return times(weighted, high_s[i], low_s[i], False)

    def wide(x):
        return jnp.concatenate([x] * (ell // 128), axis=1)

    def owned(f):
        return (lambda m, a: beam_s[f, m, a]), (lambda m: column_s[vector.index(f), m])

    lent = (lambda m, a: lent_beam_s[m, a]), (lambda m: lent_column_s[m])

    def group_project(source, g, field):
        beam_of, column_of = source
        parts = []
        for j in range(4):
            m = 4 * g + j
            real_beam, imaginary_beam = beam_of(m, 0), beam_of(m, 1)
            real_field, imaginary_field = field[j:j + 1], field[4 + j:5 + j]
            levels = column_of(m)
            real = jnp.sum(
                real_beam * real_field + imaginary_beam * imaginary_field, axis=1, keepdims=True
            )
            imaginary = jnp.sum(
                real_beam * imaginary_field - imaginary_beam * real_field, axis=1, keepdims=True
            )
            parts.append((real, imaginary, levels * real, levels * imaginary))
        return parts

    def group_back(source, g, parts):
        beam_of, _ = source
        reals, imaginaries = [], []
        for j, (_, _, real, imaginary) in enumerate(parts):
            m = 4 * g + j
            real, imaginary = wide(real), wide(imaginary)
            real_beam, imaginary_beam = beam_of(m, 0), beam_of(m, 1)
            for found, value in (
                (reals, real_beam * real - imaginary_beam * imaginary),
                (imaginaries, real_beam * imaginary + imaginary_beam * real),
            ):
                found.append(sum(value[k:k + 8] for k in range(0, rank, 8)))
        return folded(reals + imaginaries)

    def group_beam(source, g, field):
        return group_back(source, g, group_project(source, g, field))

    def project(f, ref):
        if f in matrix:
            return matrix_project(f, ref[f])
        return [group_project(owned(f), g, ref[f, group(g)]) for g in range(groups)]

    def back(f, seen):
        if f in matrix:
            return matrix_back(f, seen)
        return jnp.concatenate([group_back(owned(f), g, seen[g]) for g in range(groups)], axis=0)

    def apply_beam(fs, ref):
        fs = [f for f in fs if f in matrix] + [f for f in fs if f in vector]
        seen = [project(f, ref) for f in fs]
        return {f: back(f, found) for f, found in zip(fs, seen)}

    def count(f):
        value = float(f > 0) + float(f < last) + float(nf > 1 and f == 0)
        if two_sided and f == last:
            value = value + jnp.where(has_far, 1.0, 0.0)
        return value

    def local_prior(f, ref, rows=slice(None)):
        value = count(f) * ref[f, rows]
        if f > 0:
            value = value - ref[f - 1, rows]
        if f < last:
            value = value - ref[f + 1, rows]
        return power * ref[f, rows] + smooth * value

    for f in edges:
        beam_copies[f].wait()
    rhs_copy.wait()
    for i, f in enumerate(edges):
        for g in range(groups):
            rows = group(g)
            image = group_beam(owned(f), g, x_s[f, rows])
            y_s[i, rows] = rows_of(rhs_s, at(f))[rows] - image - local_prior(f, x_s, rows)
    first, rest = [], inner
    if paired:
        even_only([near_copy(1, g) for g in range(groups)] + [lend(k) for k in range(3)])
        first, rest = inner[:1], inner[1:]
    else:
        for g in range(groups):
            send(1, g)

    for f in first:
        beam_copies[f].wait()
        r_s[f] = rows_of(rhs_s, at(f)) - back(f, project(f, x_s)) - local_prior(f, x_s)
    if paired:
        even_only([lend(3)])

        @pl.when(helper)
        def _():
            for g in range(groups):
                near_copy(1, g).start()

    for f in rest:
        beam_copies[f].wait()
    for i, f in enumerate(matrix):
        for a in range(2):
            rows = slice(a * width, (a + 1) * width)
            high, low = split(beam_s[f, :, a].reshape(width, ell))
            high_s[i, rows] = high
            low_s[i, rows] = low
    for f, image in apply_beam(rest, x_s).items():
        r_s[f] = rows_of(rhs_s, at(f)) - image - local_prior(f, x_s)
    for f, image in apply_beam(inner, r_s).items():
        u_s[f] = image + local_prior(f, r_s) if f in apart else image
    seen = {f: project(f, u_s) for f in apart}
    advance()

    for g in range(groups):
        arrive(0, g)
        rows = group(g)
        for i, f in enumerate(edges):
            halo = jnp.concatenate([first_s[i, 4 * g:4 * g + 4, b, :] for b in range(2)], axis=0)
            r_s[f, rows] = y_s[i, rows] + smooth * halo
        for i, f in enumerate(edges):
            v_s[i, rows] = group_beam(owned(f), g, r_s[f, rows]) + local_prior(f, r_s, rows)
        if paired:
            pl.when(helper)(lambda: near_copy(2, g).start())
        else:
            send(2, g)
    if paired:
        @pl.when(helper)
        def _():
            for k in range(4):
                lend(k).wait_recv()
            for g in range(groups):
                first_copy(g).wait_recv()
                rows = group(g)
                halo = jnp.concatenate([lent_first_s[4 * g:4 * g + 4, b, :] for b in range(2)], axis=0)
                r = lent_y_s[rows] + smooth * halo
                local = power * r + smooth * (count(0) * r - lent_r_s[rows])
                lent_v_s[rows] = group_beam(lent, g, r) + local
                cross_copy(g).start()

    for f in beside_edge:
        u_s[f] = u_s[f] + local_prior(f, r_s)
    seen |= {f: project(f, u_s) for f in beside_edge}

    for g in range(groups):
        arrive(1, g)
    for i, f in enumerate(edges):
        u_s[f] = v_s[i] - beside(i, smooth * (halo_s[0, i] + smooth * x_s[f]))
    if paired:
        pull_s[...] = smooth * u_s[0]
        even_only([pull_copy()])
    seen |= {f: project(f, u_s) for f in edges}
    norm = jnp.zeros((2 * modes, ell), F32)
    curve, square, cube = norm, norm, norm
    beam_part = jnp.zeros((2 * modes, width), F32)
    column_part = jnp.zeros((rank, 128), F32)
    for f in inner + edges:
        if f in matrix:
            beam_part = beam_part + seen[f][0] * seen[f][1]
        else:
            for parts in seen[f]:
                for real, imaginary, real_weighted, imaginary_weighted in parts:
                    column_part = column_part + (real * real_weighted + imaginary * imaginary_weighted)
        w_s[f] = local_prior(f, u_s)
        norm = norm + r_s[f] * r_s[f]
        curve = curve + r_s[f] * u_s[f]
        square = square + u_s[f] * u_s[f]
        cube = cube + u_s[f] * w_s[f]
    lane = lax.broadcasted_iota(jnp.int32, (1, 128), 1)
    message = jnp.zeros((1, 128), F32)
    for i, part in enumerate((norm, curve, square, cube)):
        total = total_of(part)
        if i == 3:
            total = total + total_of(beam_part) + jnp.sum(column_part, axis=0, keepdims=True)
        message = jnp.where(lane == i, total, message)
    if paired:
        message = jnp.where(lane == 4 + my_f, total_of(smooth * r_s[0] * pull_s[...]), message)
    message_s[0] = message
    early_s[me] = message

    while steps:
        advance()

    def share(source, target, slot, turn, device):
        pltpu.make_async_remote_copy(
            src_ref=message_s.at[source], dst_ref=target.at[slot],
            send_sem=sum_send.at[turn], recv_sem=sum_recv.at[turn],
            device_id=device, device_id_type=MESH,
        ).start()

    def share_all(source, target, slot, turn, stride):
        if n > 64:
            def body(i, carry):
                ma, f = my_ma + i * stride // nf, my_f + i * stride % nf
                share(source, target, slot, turn, (lax.rem(ma, nma), lax.rem(f, nf)))
                return carry

            lax.fori_loop(1, n // stride, body, 0)
        else:
            for mask in sorted(range(stride, n, stride), key=lambda m: (-(m // nf // 2), m)):
                device = partner([bit for bit in range(bits) if mask >> bit & 1])
                share(source, target, slot, turn, device)

    def landed(target, sem, rows):
        if rows:
            rows = target.at[pl.ds(0, rows)]
            pltpu.make_async_copy(rows, rows, sem).wait()

    def lanes_of(x):
        x = jnp.sum(x, axis=0, keepdims=True)
        return sum(x[:, i:i + 128] for i in range(0, ell, 128))

    share_all(0, early_s, me, 0, 1)
    if paired:
        even_only([near_copy(2, g) for g in range(groups)])
    for f in matrix + vector:
        w_s[f] = w_s[f] + back(f, seen[f])

    late_rows = late_s.shape[0]
    if paired:
        @pl.when(helper)
        def _():
            cross = jnp.zeros((8, ell), F32)
            for g in range(groups):
                arrive(2, g)
                cross = cross + pull_s[group(g)] * halo_s[1, 0, group(g)]
            pull_copy().wait_recv()
            for g in range(groups):
                cross_copy(g).wait_recv()
                cross = cross + partner_s[group(g)] * cross_s[group(g)]
            message = lanes_of(cross)
            late_s[my_ma // 2] = message
            message_s[1] = message
            share_all(1, late_s, my_ma // 2, 1, nf)
            for g in range(groups):
                cross_copy(g).wait_send()

        @pl.when(jnp.logical_not(helper))
        def _():
            for g in range(groups):
                arrive(2, g)
            pull_copy().wait_send()
            for k in range(4):
                lend(k).wait_send()
            for g in range(groups):
                first_copy(g).wait_send()

        w_s[0] = w_s[0] - smooth * (halo_s[1, 0] - smooth * r_s[0])
    else:
        cross = jnp.zeros((8, ell), F32)
        nexts = []
        for g in range(groups):
            arrive(2, g)
            rows = group(g)
            for i, f in enumerate(edges):
                pull = beside(i, smooth * (halo_s[1, i, rows] - smooth * r_s[f, rows]))
                nexts.append((f, rows, pull))
                cross = cross + pull * u_s[f, rows]
        message = lanes_of(cross)
        late_s[me] = message
        message_s[1] = message
        share_all(1, late_s, me, 1, 1)
        for f, rows, pull in nexts:
            w_s[f, rows] = w_s[f, rows] - pull

    for kind in range(3):
        for g in range(groups):
            sent(kind, g)
    for source, target in ((r_s, r_out_s), (u_s, u_out_s), (w_s, w_out_s)):
        for f in range(freqs):
            value = source[f]
            for g in range(groups):
                for b in range(2):
                    start = 8 * g + 4 * b
                    target[4 * g:4 * g + 4, at(f), b, :] = value[start:start + 4]

    landed(early_s, sum_send.at[0], n - 1)
    landed(early_s, sum_recv.at[0], n - 1)
    if paired:
        @pl.when(helper)
        def _():
            rows = early_s.at[pl.ds(0, nma - 1)]
            pltpu.make_async_copy(rows, rows, sum_send.at[1]).wait()
            landed(late_s, sum_recv.at[1], late_rows - 1)

        pl.when(jnp.logical_not(helper))(lambda: landed(late_s, sum_recv.at[1], late_rows))
    else:
        landed(late_s, sum_send.at[1], late_rows - 1)
        landed(late_s, sum_recv.at[1], late_rows - 1)
    total = jnp.sum(early_s[...], axis=0)
    m0, m1, m2, m3, known = (
        jnp.sum(jnp.where(lane == i, total, 0.0), axis=1, keepdims=True)
        for i in (0, 1, 2, 3, 4 + my_f)
    )
    crossed = jnp.sum(jnp.sum(late_s[...], axis=0), axis=1, keepdims=True)
    m3 = m3 - 2.0 * (crossed - known) if paired else m3 - crossed
    inverse = 1.0 / m1
    step = m0 * inverse
    drop = step * m2 - m1
    growth = drop * inverse
    curve_next = m1 - 2.0 * step * m2 + step * step * m3
    step_next = step * drop / (curve_next - growth * drop)
    c = step + step_next * (1.0 + growth)
    e = step * step_next
    r, u = r_out_s[...], u_out_s[...]
    sol_s[...] = x0_s[...] + c * r - e * u
    res_s[...] = r - c * u + e * w_out_s[...]


def scoped_kernel(nma, nf, sides, *refs):
    modes, freqs = refs[0].shape[:2]
    dma = pltpu.SemaphoreType.DMA
    pl.run_scoped(
        functools.partial(kernel, nma, nf, *refs),
        dma((7,)), dma((freqs,)), dma((3, modes // 4, sides)), dma((2 * (modes // 4) + 5,)), dma((2,)),
    )


def write_out(sol_in, res_in, sol_out, res_out, sem):
    copies = [
        pltpu.make_async_copy(sol_in, sol_out, sem.at[0]),
        pltpu.make_async_copy(res_in, res_out, sem.at[1]),
    ]
    for copy in copies:
        copy.start()
    for copy in copies:
        copy.wait()


def shards(right_side, start_field, beam, noise, inv_power, smooth):
    nma, nf = lax.axis_size("ma"), lax.axis_size("freq")
    modes, freqs, _, ell = right_side.shape
    rank = beam.shape[3]
    width = modes * rank
    sides = 2 if nf > 2 else 1
    vmem_spec = pl.BlockSpec(memory_space=pltpu.VMEM)
    any_spec = pl.BlockSpec(memory_space=pl.ANY)
    field = pltpu.VMEM(right_side.shape, F32)
    edge = pltpu.VMEM((sides, modes, 2, ell), F32)
    slab = pltpu.VMEM((freqs, 2 * modes, ell), F32)
    edge_field = pltpu.VMEM((2 * modes, ell), F32)
    edge_slab = pltpu.VMEM((sides, 2 * modes, ell), F32)
    vector = max(min(nf - 1, 2), freqs // 2)
    matrix = max(freqs - vector, 1)
    half = pltpu.VMEM((matrix, 2 * width, ell), BF16)
    outs = pl.pallas_call(
        functools.partial(scoped_kernel, nma, nf, sides),
        out_shape=[field] * 2,
        in_specs=[any_spec] * 6,
        out_specs=[vmem_spec] * 2,
        scratch_shapes=[
            field, field, edge,
            pltpu.VMEM((freqs, modes, 2, rank, ell), F32),
            pltpu.VMEM(noise.shape, F32),
            pltpu.VMEM((1, ell), F32), pltpu.VMEM((1, ell), F32),
            half, half,
            slab, edge_slab, slab, edge_slab, slab, slab,
            pltpu.VMEM((matrix, 2 * modes, width), F32),
            pltpu.VMEM((vector, modes, rank, 128), F32),
            edge,
            pltpu.VMEM((2, sides, 2 * modes, ell), F32),
            field, field, field,
            edge_field, edge_field, edge_field,
            pltpu.VMEM((modes, 2, rank, ell), F32), pltpu.VMEM((modes, rank, 128), F32),
            edge_field, edge_field, pltpu.VMEM((modes, 2, ell), F32), edge_field,
            pltpu.VMEM((2, 1, 128), F32),
            pltpu.VMEM((nma * nf, 1, 128), F32),
            pltpu.VMEM((nma // 2 if nf == 2 and nma % 2 == 0 and freqs > 1 else nma * nf, 1, 128), F32),
            pltpu.SemaphoreType.DMA((3, modes // 4, sides)),
            pltpu.SemaphoreType.DMA((2 * (modes // 4) + 5,)),
            pltpu.SemaphoreType.DMA((2,)),
            pltpu.SemaphoreType.REGULAR((max((nma * nf).bit_length() - 4, 1),)),
        ],
        compiler_params=pltpu.CompilerParams(
            collective_id=0, has_side_effects=True, vmem_limit_bytes=67043328 - 2 * right_side.size * 4
        ),
        name="solve",
    )(right_side, start_field, beam, noise, inv_power[None], smooth[None])
    return pl.pallas_call(
        write_out,
        out_shape=[jax.ShapeDtypeStruct(right_side.shape, F32)] * 2,
        in_specs=[vmem_spec] * 2,
        out_specs=[any_spec] * 2,
        scratch_shapes=[pltpu.SemaphoreType.DMA((2,))],
        compiler_params=pltpu.CompilerParams(vmem_limit_bytes=1024 * 1024),
        name="write_out",
    )(*outs)


def solution(mesh):
    in_specs = (
        P("ma", "freq", None, None),
        P("ma", "freq", None, None),
        P("ma", "freq", None, None, None),
        P("ma", "freq", None),
        P(),
        P(),
    )
    out_specs = (P("ma", "freq", None, None), P("ma", "freq", None, None))
    return jax.shard_map(shards, mesh=mesh, in_specs=in_specs, out_specs=out_specs, check_vma=False)
```

```python
import functools

import jax
import jax.numpy as jnp
from jax import lax
from jax.experimental import pallas as pl
from jax.experimental.pallas import tpu as pltpu
from jax.sharding import PartitionSpec as P

MESH = pl.DeviceIdType.MESH
F32, BF16 = jnp.float32, jnp.bfloat16


def split(x):
    high = x.astype(BF16)
    return high, (x - high.astype(F32)).astype(BF16)


def times(x, high, low, transposed):
    dims = (((1,), (1 if transposed else 0,)), ((), ()))
    rows = x.shape[0]
    x_high, x_low = split(x)
    both = jnp.concatenate([x_high, x_low], axis=0)
    main = lax.dot_general(both, high, dims, preferred_element_type=F32)
    rest = lax.dot_general(x_high, low, dims, preferred_element_type=F32)
    return main[:rows] + (main[rows:] + rest)


def folded(parts):
    row = lax.broadcasted_iota(jnp.int32, parts[0].shape, 0)
    upper = row < 4
    fours = [
        jnp.where(upper, parts[s], parts[s + 4])
        + pltpu.roll(jnp.where(upper, parts[s + 4], parts[s]), 4, 0)
        for s in range(4)
    ]
    even = row // 2 % 2 == 0
    twos = [
        jnp.where(
            even, fours[s] + pltpu.roll(fours[s], 6, 0), fours[s + 2] + pltpu.roll(fours[s + 2], 2, 0)
        )
        for s in range(2)
    ]
    return jnp.where(
        row % 2 == 0, twos[0] + pltpu.roll(twos[0], 7, 0), twos[1] + pltpu.roll(twos[1], 1, 0)
    )


def total_of(x):
    return jnp.sum(jnp.sum(x, axis=0, keepdims=True), axis=1, keepdims=True)


def kernel(
    nma, nf, rhs_in, x0_in, beam_in, noise_in, power_in, smooth_in, sol_s, res_s,
    rhs_s, x0_s, edge_s, beam_s, noise_s, power_s, smooth_s,
    high_s, low_s, x_s, y_s, r_s, v_s, u_s, w_s, mask_s, column_s, first_s, halo_s,
    r_out_s, u_out_s, w_out_s, pull_s, partner_s, cross_s,
    lent_beam_s, lent_column_s, lent_y_s, lent_r_s, lent_first_s, lent_v_s,
    message_s, early_s, late_s,
    halo_recv, pair_recv, sum_recv, word_sem, in_sem, beam_sem, halo_send, pair_send, hand_send, sum_send,
):
    modes, freqs, _, ell = rhs_in.shape
    rank = beam_in.shape[3]
    width = modes * rank
    n = nma * nf
    my_ma, my_f = lax.axis_index("ma"), lax.axis_index("freq")
    me = my_ma * nf + my_f
    last = freqs - 1
    two_sided = nf > 2
    paired = nf == 2 and nma % 2 == 0 and freqs > 1
    helper = my_ma % 2 == 1
    groups = modes // 4
    edges = [0, last][:min(nf - 1, 2)]
    inner = [f for f in range(freqs) if f not in edges]
    beside_edge = [f for f in inner if f - 1 in edges or f + 1 in edges]
    apart = [f for f in inner if f not in beside_edge]
    vector = edges + inner[:max(freqs // 2 - len(edges), 0)]
    matrix = [f for f in range(freqs) if f not in vector]

    def at(g):
        return jnp.where(my_f == 0, last - g, g)

    edge_copies = [
        pltpu.make_async_copy(x0_in.at[:, at(f)], edge_s.at[i], in_sem.at[i])
        for i, f in enumerate(edges)
    ]
    x0_copy = pltpu.make_async_copy(x0_in, x0_s, in_sem.at[2])
    rhs_copy = pltpu.make_async_copy(rhs_in, rhs_s, in_sem.at[3])
    small = [
        pltpu.make_async_copy(power_in, power_s, in_sem.at[4]),
        pltpu.make_async_copy(smooth_in, smooth_s, in_sem.at[5]),
        pltpu.make_async_copy(noise_in, noise_s, in_sem.at[6]),
    ]
    beam_copies = [
        pltpu.make_async_copy(beam_in.at[:, at(f)], beam_s.at[f], beam_sem.at[f])
        for f in range(freqs)
    ]
    for copy in edge_copies:
        copy.start()

    def flip(bit):
        d = 1 << (bit if bit < freq_bits else bit - freq_bits)
        place = my_f if bit < freq_bits else my_ma
        return d * (1 - 2 * (place // d % 2))

    def partner(bits):
        return (
            my_ma + sum(flip(bit) for bit in bits if bit >= freq_bits),
            my_f + sum(flip(bit) for bit in bits if bit < freq_bits),
        )

    freq_bits = nf.bit_length() - 1
    bits = freq_bits + nma.bit_length() - 1
    close = min(bits, 3)
    greeted = [
        partner([bit for bit in range(close) if mask >> bit & 1]) for mask in range(1, 1 << close)
    ]
    word = [partner([bit]) for bit in range(close, bits)]
    greeted += word
    words = len(word)
    barrier = pltpu.get_barrier_semaphore()
    near = jnp.where(my_f == 0, 1, my_f - 1)
    has_far = (my_f > 0) & (my_f < nf - 1)

    def greet(device):
        pl.semaphore_signal(barrier, inc=1, device_id=device, device_id_type=MESH)

    for i, device in enumerate(greeted):
        greet(device)
        if i == 0:
            for copy in [beam_copies[f] for f in edges] + [x0_copy, rhs_copy] + small:
                copy.start()
    expected = len(greeted)
    if nf > 2:
        pl.when(my_f > 0)(lambda: greet((my_ma, my_f - 1)))
        pl.when(my_f < nf - 1)(lambda: greet((my_ma, my_f + 1)))
        expected = expected + jnp.minimum(my_f, 1) + jnp.minimum(nf - 1 - my_f, 1)

    steps = list(range(words + 1))

    def advance():
        if steps:
            step = steps.pop(0)
            if step > 0:
                pl.semaphore_wait(word_sem.at[step - 1], 1)
            if step < words:
                pl.semaphore_signal(
                    word_sem.at[step], inc=1, device_id=word[step], device_id_type=MESH
                )

    def piece(kind, g):
        if kind == 0:
            rows = pl.ds(4 * g, 4)
            return (lambda i: edge_s.at[i, rows]), (lambda i: first_s.at[i, rows])
        source = (y_s, v_s)[kind - 1]
        rows = pl.ds(8 * g, 8)
        return (lambda i: source.at[i, rows]), (lambda i: halo_s.at[kind - 1, i, rows])

    def near_copy(kind, g):
        source, target = piece(kind, g)
        side = jnp.minimum(my_f // 2, 1) if two_sided else 0
        return pltpu.make_async_remote_copy(
            src_ref=source(0), dst_ref=target(side),
            send_sem=halo_send.at[kind, g, 0], recv_sem=halo_recv.at[kind, g, side],
            device_id=(my_ma, near), device_id_type=MESH,
        )

    def far_copy(kind, g):
        source, target = piece(kind, g)
        return pltpu.make_async_remote_copy(
            src_ref=source(1), dst_ref=target(0),
            send_sem=halo_send.at[kind, g, 1], recv_sem=halo_recv.at[kind, g, 0],
            device_id=(my_ma, my_f + 1), device_id_type=MESH,
        )

    def arrival(kind, g, side):
        slot = piece(kind, g)[1](side)
        return pltpu.make_async_copy(slot, slot, halo_recv.at[kind, g, side])

    def send(kind, g):
        if nf > 1:
            near_copy(kind, g).start()
        if two_sided:
            pl.when(has_far)(lambda: far_copy(kind, g).start())

    def arrive(kind, g):
        if nf > 1:
            arrival(kind, g, 0).wait()
        if two_sided:
            pl.when(has_far)(lambda: arrival(kind, g, 1).wait())

    def sent(kind, g):
        if nf > 1:
            near_copy(kind, g).wait_send()
        if two_sided:
            pl.when(has_far)(lambda: far_copy(kind, g).wait_send())

    def pair_copy(k, source, target, ma, f):
        return pltpu.make_async_remote_copy(
            src_ref=source, dst_ref=target, send_sem=pair_send.at[k], recv_sem=pair_recv.at[k],
            device_id=(ma, f), device_id_type=MESH,
        )

    def lend(k):
        source = (lambda: beam_s.at[0], lambda: column_s.at[0], lambda: y_s.at[0], lambda: r_s.at[1])[k]
        target = (lent_beam_s, lent_column_s, lent_y_s, lent_r_s)[k]
        return pair_copy(k, source(), target, my_ma + 1, my_f)

    def pull_copy():
        return pair_copy(4, pull_s, partner_s, my_ma + 1, my_f)

    def first_copy(g):
        rows = pl.ds(4 * g, 4)
        return pair_copy(5 + g, edge_s.at[0, rows], lent_first_s.at[rows], my_ma + 1, 1 - my_f)

    def cross_copy(g):
        rows = pl.ds(8 * g, 8)
        return pair_copy(5 + groups + g, lent_v_s.at[rows], cross_s.at[rows], my_ma, 1 - my_f)

    def hand_copy(g):
        rows = pl.ds(4 * g, 4)
        return pltpu.make_async_remote_copy(
            src_ref=lent_first_s.at[rows], dst_ref=first_s.at[0, rows],
            send_sem=hand_send.at[g], recv_sem=halo_recv.at[0, g, 0],
            device_id=(my_ma - 1, my_f), device_id_type=MESH,
        )

    def even_only(copies):
        @pl.when(jnp.logical_not(helper))
        def _():
            for copy in copies:
                copy.start()

    def beside(i, value):
        return jnp.where(has_far, value, 0.0) if i else value

    if two_sided:
        @pl.when(jnp.logical_not(has_far))
        def _():
            first_s[1] = jnp.zeros_like(first_s[1])
            halo_s[:, 1] = jnp.zeros_like(halo_s[:, 1])

    for copy in edge_copies:
        copy.wait()
    for f in inner:
        beam_copies[f].start()
    pl.semaphore_wait(barrier, expected)
    if paired:
        even_only([first_copy(g) for g in range(groups)])

        @pl.when(helper)
        def _():
            for g in range(groups):
                near_copy(0, g).start()
    else:
        for g in range(groups):
            send(0, g)
    advance()

    x0_copy.wait()
    for copy in small:
        copy.wait()
    def rows_of(ref, *at_f):
        place = (slice(None), *at_f)
        return jnp.concatenate(
            [ref[(slice(4 * g, 4 * g + 4), *place[1:], b)] for g in range(groups) for b in range(2)],
            axis=0,
        )

    def group(g):
        return slice(8 * g, 8 * g + 8)

    for f in range(freqs):
        x_s[f] = rows_of(x0_s, at(f))
    power, smooth = power_s[...], smooth_s[...]
    row = lax.broadcasted_iota(jnp.int32, (2 * modes, width), 0)
    own = lax.broadcasted_iota(jnp.int32, (2 * modes, width), 1) // rank == row // 8 * 4 + row % 4
    sign = jnp.where(row % 8 < 4, 1.0, -1.0)
    for i, f in enumerate(matrix):
        levels = noise_s[:, at(f), :]
        levels = jnp.concatenate(
            [levels[4 * g:4 * g + 4] for g in range(groups) for _ in range(2)], axis=0
        )
        mask_s[i] = jnp.where(own, jnp.concatenate([levels] * modes, axis=1), 0.0)
    unit = (
        lax.broadcasted_iota(jnp.int32, (rank, rank), 0)
        == lax.broadcasted_iota(jnp.int32, (rank, rank), 1)
    )
    for i, f in enumerate(vector):
        levels = noise_s[:, at(f), :]
        for m in range(modes):
            column = jnp.sum(jnp.where(unit, levels[m:m + 1], 0.0), axis=1, keepdims=True)
            column_s[i, m] = jnp.broadcast_to(column, (rank, 128))

    def swapped(x):
        return jnp.concatenate([pltpu.roll(x[group(g)], 4, 0) for g in range(groups)], axis=0)

    def matrix_project(f, field):
        i = matrix.index(f)
        seen = times(field, high_s[i], low_s[i], True)
        parts = seen[:, :width] + sign * swapped(seen[:, width:])
        return parts, mask_s[i] * parts

    def matrix_back(f, seen):
        i = matrix.index(f)
        weighted = jnp.concatenate([seen[1], -sign * swapped(seen[1])], axis=1)
        return times(weighted, high_s[i], low_s[i], False)

    def wide(x):
        return jnp.concatenate([x] * (ell // 128), axis=1)

    def owned(f):
        return (lambda m, a: beam_s[f, m, a]), (lambda m: column_s[vector.index(f), m])

    lent = (lambda m, a: lent_beam_s[m, a]), (lambda m: lent_column_s[m])

    def group_project(source, g, field):
        beam_of, column_of = source
        parts = []
        for j in range(4):
            m = 4 * g + j
            real_beam, imaginary_beam = beam_of(m, 0), beam_of(m, 1)
            real_field, imaginary_field = field[j:j + 1], field[4 + j:5 + j]
            levels = column_of(m)
            real = jnp.sum(
                real_beam * real_field + imaginary_beam * imaginary_field, axis=1, keepdims=True
            )
            imaginary = jnp.sum(
                real_beam * imaginary_field - imaginary_beam * real_field, axis=1, keepdims=True
            )
            parts.append((real, imaginary, levels * real, levels * imaginary))
        return parts

    def group_back(source, g, parts):
        beam_of, _ = source
        reals, imaginaries = [], []
        for j, (_, _, real, imaginary) in enumerate(parts):
            m = 4 * g + j
            real, imaginary = wide(real), wide(imaginary)
            real_beam, imaginary_beam = beam_of(m, 0), beam_of(m, 1)
            for found, value in (
                (reals, real_beam * real - imaginary_beam * imaginary),
                (imaginaries, real_beam * imaginary + imaginary_beam * real),
            ):
                found.append(sum(value[k:k + 8] for k in range(0, rank, 8)))
        return folded(reals + imaginaries)

    def group_beam(source, g, field):
        return group_back(source, g, group_project(source, g, field))

    def project(f, ref):
        if f in matrix:
            return matrix_project(f, ref[f])
        return [group_project(owned(f), g, ref[f, group(g)]) for g in range(groups)]

    def back(f, seen):
        if f in matrix:
            return matrix_back(f, seen)
        return jnp.concatenate([group_back(owned(f), g, seen[g]) for g in range(groups)], axis=0)

    def apply_beam(fs, ref):
        fs = [f for f in fs if f in matrix] + [f for f in fs if f in vector]
        seen = [project(f, ref) for f in fs]
        return {f: back(f, found) for f, found in zip(fs, seen)}

    def count(f):
        value = float(f > 0) + float(f < last) + float(nf > 1 and f == 0)
        if two_sided and f == last:
            value = value + jnp.where(has_far, 1.0, 0.0)
        return value

    def local_prior(f, ref, rows=slice(None)):
        value = count(f) * ref[f, rows]
        if f > 0:
            value = value - ref[f - 1, rows]
        if f < last:
            value = value - ref[f + 1, rows]
        return power * ref[f, rows] + smooth * value

    for f in edges:
        beam_copies[f].wait()
    rhs_copy.wait()
    for i, f in enumerate(edges):
        for g in range(groups):
            rows = group(g)
            image = group_beam(owned(f), g, x_s[f, rows])
            y_s[i, rows] = rows_of(rhs_s, at(f))[rows] - image - local_prior(f, x_s, rows)
    first, rest = [], inner
    if paired:
        even_only([near_copy(1, g) for g in range(groups)] + [lend(k) for k in range(3)])
        first, rest = inner[:1], inner[1:]
    else:
        for g in range(groups):
            send(1, g)

    for f in first:
        beam_copies[f].wait()
        r_s[f] = rows_of(rhs_s, at(f)) - back(f, project(f, x_s)) - local_prior(f, x_s)
    if paired:
        even_only([lend(3)])

        @pl.when(helper)
        def _():
            for g in range(groups):
                near_copy(1, g).start()

    for f in rest:
        beam_copies[f].wait()
    for i, f in enumerate(matrix):
        for a in range(2):
            rows = slice(a * width, (a + 1) * width)
            high, low = split(beam_s[f, :, a].reshape(width, ell))
            high_s[i, rows] = high
            low_s[i, rows] = low
    for f, image in apply_beam(rest, x_s).items():
        r_s[f] = rows_of(rhs_s, at(f)) - image - local_prior(f, x_s)
    for f, image in apply_beam(inner, r_s).items():
        u_s[f] = image + local_prior(f, r_s) if f in apart else image
    seen = {f: project(f, u_s) for f in apart}
    advance()

    for g in range(groups):
        arrive(0, g)
        rows = group(g)
        for i, f in enumerate(edges):
            halo = jnp.concatenate([first_s[i, 4 * g:4 * g + 4, b, :] for b in range(2)], axis=0)
            r_s[f, rows] = y_s[i, rows] + smooth * halo
        for i, f in enumerate(edges):
            v_s[i, rows] = group_beam(owned(f), g, r_s[f, rows]) + local_prior(f, r_s, rows)
        if paired:
            pl.when(helper)(lambda: near_copy(2, g).start())
        else:
            send(2, g)
    if paired:
        @pl.when(helper)
        def _():
            for g in range(groups):
                first_copy(g).wait_recv()
                hand_copy(g).start()
            for k in range(4):
                lend(k).wait_recv()
            for g in range(groups):
                rows = group(g)
                halo = jnp.concatenate([lent_first_s[4 * g:4 * g + 4, b, :] for b in range(2)], axis=0)
                r = lent_y_s[rows] + smooth * halo
                local = power * r + smooth * (count(0) * r - lent_r_s[rows])
                lent_v_s[rows] = group_beam(lent, g, r) + local
                cross_copy(g).start()

    for f in beside_edge:
        u_s[f] = u_s[f] + local_prior(f, r_s)
    seen |= {f: project(f, u_s) for f in beside_edge}

    for g in range(groups):
        arrive(1, g)
    for i, f in enumerate(edges):
        u_s[f] = v_s[i] - beside(i, smooth * (halo_s[0, i] + smooth * x_s[f]))
    if paired:
        pull_s[...] = smooth * u_s[0]
        even_only([pull_copy()])
    seen |= {f: project(f, u_s) for f in edges}
    norm = jnp.zeros((2 * modes, ell), F32)
    curve, square, cube = norm, norm, norm
    beam_part = jnp.zeros((2 * modes, width), F32)
    column_part = jnp.zeros((rank, 128), F32)
    for f in inner + edges:
        if f in matrix:
            beam_part = beam_part + seen[f][0] * seen[f][1]
        else:
            for parts in seen[f]:
                for real, imaginary, real_weighted, imaginary_weighted in parts:
                    column_part = column_part + (real * real_weighted + imaginary * imaginary_weighted)
        w_s[f] = local_prior(f, u_s)
        norm = norm + r_s[f] * r_s[f]
        curve = curve + r_s[f] * u_s[f]
        square = square + u_s[f] * u_s[f]
        cube = cube + u_s[f] * w_s[f]
    lane = lax.broadcasted_iota(jnp.int32, (1, 128), 1)
    message = jnp.zeros((1, 128), F32)
    for i, part in enumerate((norm, curve, square, cube)):
        total = total_of(part)
        if i == 3:
            total = total + total_of(beam_part) + jnp.sum(column_part, axis=0, keepdims=True)
        message = jnp.where(lane == i, total, message)
    if paired:
        message = jnp.where(lane == 4 + my_f, total_of(smooth * r_s[0] * pull_s[...]), message)
    message_s[0] = message
    early_s[me] = message

    while steps:
        advance()

    def share(source, target, slot, turn, device):
        pltpu.make_async_remote_copy(
            src_ref=message_s.at[source], dst_ref=target.at[slot],
            send_sem=sum_send.at[turn], recv_sem=sum_recv.at[turn],
            device_id=device, device_id_type=MESH,
        ).start()

    def share_all(source, target, slot, turn, stride):
        if n > 64:
            def body(i, carry):
                ma, f = my_ma + i * stride // nf, my_f + i * stride % nf
                share(source, target, slot, turn, (lax.rem(ma, nma), lax.rem(f, nf)))
                return carry

            lax.fori_loop(1, n // stride, body, 0)
        else:
            for mask in sorted(range(stride, n, stride), key=lambda m: (-(m // nf // 2), m)):
                device = partner([bit for bit in range(bits) if mask >> bit & 1])
                share(source, target, slot, turn, device)

    def landed(target, sem, rows):
        if rows:
            rows = target.at[pl.ds(0, rows)]
            pltpu.make_async_copy(rows, rows, sem).wait()

    def lanes_of(x):
        x = jnp.sum(x, axis=0, keepdims=True)
        return sum(x[:, i:i + 128] for i in range(0, ell, 128))

    share_all(0, early_s, me, 0, 1)
    if paired:
        even_only([near_copy(2, g) for g in range(groups)])
    for f in matrix + vector:
        w_s[f] = w_s[f] + back(f, seen[f])

    late_rows = late_s.shape[0]
    if paired:
        @pl.when(helper)
        def _():
            cross = jnp.zeros((8, ell), F32)
            for g in range(groups):
                arrive(2, g)
                cross = cross + pull_s[group(g)] * halo_s[1, 0, group(g)]
            pull_copy().wait_recv()
            for g in range(groups):
                cross_copy(g).wait_recv()
                cross = cross + partner_s[group(g)] * cross_s[group(g)]
            message = lanes_of(cross)
            late_s[my_ma // 2] = message
            message_s[1] = message
            share_all(1, late_s, my_ma // 2, 1, nf)
            for g in range(groups):
                cross_copy(g).wait_send()

        @pl.when(jnp.logical_not(helper))
        def _():
            for g in range(groups):
                arrive(2, g)
            pull_copy().wait_send()
            for k in range(4):
                lend(k).wait_send()
            for g in range(groups):
                first_copy(g).wait_send()

        w_s[0] = w_s[0] - smooth * (halo_s[1, 0] - smooth * r_s[0])
    else:
        cross = jnp.zeros((8, ell), F32)
        nexts = []
        for g in range(groups):
            arrive(2, g)
            rows = group(g)
            for i, f in enumerate(edges):
                pull = beside(i, smooth * (halo_s[1, i, rows] - smooth * r_s[f, rows]))
                nexts.append((f, rows, pull))
                cross = cross + pull * u_s[f, rows]
        message = lanes_of(cross)
        late_s[me] = message
        message_s[1] = message
        share_all(1, late_s, me, 1, 1)
        for f, rows, pull in nexts:
            w_s[f, rows] = w_s[f, rows] - pull

    if paired:
        for g in range(groups):
            for kind in (1, 2):
                sent(kind, g)

        @pl.when(helper)
        def _():
            for g in range(groups):
                sent(0, g)
                hand_copy(g).wait_send()
    else:
        for kind in range(3):
            for g in range(groups):
                sent(kind, g)
    for source, target in ((r_s, r_out_s), (u_s, u_out_s), (w_s, w_out_s)):
        for f in range(freqs):
            value = source[f]
            for g in range(groups):
                for b in range(2):
                    start = 8 * g + 4 * b
                    target[4 * g:4 * g + 4, at(f), b, :] = value[start:start + 4]

    landed(early_s, sum_send.at[0], n - 1)
    landed(early_s, sum_recv.at[0], n - 1)
    if paired:
        @pl.when(helper)
        def _():
            rows = early_s.at[pl.ds(0, nma - 1)]
            pltpu.make_async_copy(rows, rows, sum_send.at[1]).wait()
            landed(late_s, sum_recv.at[1], late_rows - 1)

        pl.when(jnp.logical_not(helper))(lambda: landed(late_s, sum_recv.at[1], late_rows))
    else:
        landed(late_s, sum_send.at[1], late_rows - 1)
        landed(late_s, sum_recv.at[1], late_rows - 1)
    total = jnp.sum(early_s[...], axis=0)
    m0, m1, m2, m3, known = (
        jnp.sum(jnp.where(lane == i, total, 0.0), axis=1, keepdims=True)
        for i in (0, 1, 2, 3, 4 + my_f)
    )
    crossed = jnp.sum(jnp.sum(late_s[...], axis=0), axis=1, keepdims=True)
    m3 = m3 - 2.0 * (crossed - known) if paired else m3 - crossed
    inverse = 1.0 / m1
    step = m0 * inverse
    drop = step * m2 - m1
    growth = drop * inverse
    curve_next = m1 - 2.0 * step * m2 + step * step * m3
    step_next = step * drop / (curve_next - growth * drop)
    c = step + step_next * (1.0 + growth)
    e = step * step_next
    r, u = r_out_s[...], u_out_s[...]
    sol_s[...] = x0_s[...] + c * r - e * u
    res_s[...] = r - c * u + e * w_out_s[...]


def scoped_kernel(nma, nf, sides, *refs):
    modes, freqs = refs[0].shape[:2]
    dma = pltpu.SemaphoreType.DMA
    pl.run_scoped(
        functools.partial(kernel, nma, nf, *refs),
        dma((7,)), dma((freqs,)), dma((3, modes // 4, sides)), dma((2 * (modes // 4) + 5,)),
        dma((modes // 4,)), dma((2,)),
    )


def write_out(sol_in, res_in, sol_out, res_out, sem):
    copies = [
        pltpu.make_async_copy(sol_in, sol_out, sem.at[0]),
        pltpu.make_async_copy(res_in, res_out, sem.at[1]),
    ]
    for copy in copies:
        copy.start()
    for copy in copies:
        copy.wait()


def shards(right_side, start_field, beam, noise, inv_power, smooth):
    nma, nf = lax.axis_size("ma"), lax.axis_size("freq")
    modes, freqs, _, ell = right_side.shape
    rank = beam.shape[3]
    width = modes * rank
    sides = 2 if nf > 2 else 1
    vmem_spec = pl.BlockSpec(memory_space=pltpu.VMEM)
    any_spec = pl.BlockSpec(memory_space=pl.ANY)
    field = pltpu.VMEM(right_side.shape, F32)
    edge = pltpu.VMEM((sides, modes, 2, ell), F32)
    slab = pltpu.VMEM((freqs, 2 * modes, ell), F32)
    edge_field = pltpu.VMEM((2 * modes, ell), F32)
    edge_slab = pltpu.VMEM((sides, 2 * modes, ell), F32)
    vector = max(min(nf - 1, 2), freqs // 2)
    matrix = max(freqs - vector, 1)
    half = pltpu.VMEM((matrix, 2 * width, ell), BF16)
    outs = pl.pallas_call(
        functools.partial(scoped_kernel, nma, nf, sides),
        out_shape=[field] * 2,
        in_specs=[any_spec] * 6,
        out_specs=[vmem_spec] * 2,
        scratch_shapes=[
            field, field, edge,
            pltpu.VMEM((freqs, modes, 2, rank, ell), F32),
            pltpu.VMEM(noise.shape, F32),
            pltpu.VMEM((1, ell), F32), pltpu.VMEM((1, ell), F32),
            half, half,
            slab, edge_slab, slab, edge_slab, slab, slab,
            pltpu.VMEM((matrix, 2 * modes, width), F32),
            pltpu.VMEM((vector, modes, rank, 128), F32),
            edge,
            pltpu.VMEM((2, sides, 2 * modes, ell), F32),
            field, field, field,
            edge_field, edge_field, edge_field,
            pltpu.VMEM((modes, 2, rank, ell), F32), pltpu.VMEM((modes, rank, 128), F32),
            edge_field, edge_field, pltpu.VMEM((modes, 2, ell), F32), edge_field,
            pltpu.VMEM((2, 1, 128), F32),
            pltpu.VMEM((nma * nf, 1, 128), F32),
            pltpu.VMEM((nma // 2 if nf == 2 and nma % 2 == 0 and freqs > 1 else nma * nf, 1, 128), F32),
            pltpu.SemaphoreType.DMA((3, modes // 4, sides)),
            pltpu.SemaphoreType.DMA((2 * (modes // 4) + 5,)),
            pltpu.SemaphoreType.DMA((2,)),
            pltpu.SemaphoreType.REGULAR((max((nma * nf).bit_length() - 4, 1),)),
        ],
        compiler_params=pltpu.CompilerParams(
            collective_id=0, has_side_effects=True, vmem_limit_bytes=67043328 - 2 * right_side.size * 4
        ),
        name="solve",
    )(right_side, start_field, beam, noise, inv_power[None], smooth[None])
    return pl.pallas_call(
        write_out,
        out_shape=[jax.ShapeDtypeStruct(right_side.shape, F32)] * 2,
        in_specs=[vmem_spec] * 2,
        out_specs=[any_spec] * 2,
        scratch_shapes=[pltpu.SemaphoreType.DMA((2,))],
        compiler_params=pltpu.CompilerParams(vmem_limit_bytes=1024 * 1024),
        name="write_out",
    )(*outs)


def solution(mesh):
    in_specs = (
        P("ma", "freq", None, None),
        P("ma", "freq", None, None),
        P("ma", "freq", None, None, None),
        P("ma", "freq", None),
        P(),
        P(),
    )
    out_specs = (P("ma", "freq", None, None), P("ma", "freq", None, None))
    return jax.shard_map(shards, mesh=mesh, in_specs=in_specs, out_specs=out_specs, check_vma=False)
```

```python
import functools

import jax
import jax.numpy as jnp
from jax import lax
from jax.experimental import pallas as pl
from jax.experimental.pallas import tpu as pltpu
from jax.sharding import PartitionSpec as P

MESH = pl.DeviceIdType.MESH
F32, BF16 = jnp.float32, jnp.bfloat16


def split(x):
    high = x.astype(BF16)
    return high, (x - high.astype(F32)).astype(BF16)


def times(x, high, low, transposed):
    dims = (((1,), (1 if transposed else 0,)), ((), ()))
    rows = x.shape[0]
    x_high, x_low = split(x)
    both = jnp.concatenate([x_high, x_low], axis=0)
    main = lax.dot_general(both, high, dims, preferred_element_type=F32)
    rest = lax.dot_general(x_high, low, dims, preferred_element_type=F32)
    return main[:rows] + (main[rows:] + rest)


def folded(parts):
    row = lax.broadcasted_iota(jnp.int32, parts[0].shape, 0)
    upper = row < 4
    fours = [
        jnp.where(upper, parts[s], parts[s + 4])
        + pltpu.roll(jnp.where(upper, parts[s + 4], parts[s]), 4, 0)
        for s in range(4)
    ]
    even = row // 2 % 2 == 0
    twos = [
        jnp.where(
            even, fours[s] + pltpu.roll(fours[s], 6, 0), fours[s + 2] + pltpu.roll(fours[s + 2], 2, 0)
        )
        for s in range(2)
    ]
    return jnp.where(
        row % 2 == 0, twos[0] + pltpu.roll(twos[0], 7, 0), twos[1] + pltpu.roll(twos[1], 1, 0)
    )


def total_of(x):
    return jnp.sum(jnp.sum(x, axis=0, keepdims=True), axis=1, keepdims=True)


def kernel(
    nma, nf, rhs_in, x0_in, beam_in, noise_in, power_in, smooth_in, sol_s, res_s,
    rhs_s, x0_s, edge_s, beam_s, noise_s, power_s, smooth_s,
    high_s, low_s, x_s, y_s, r_s, v_s, u_s, w_s, mask_s, column_s, first_s, halo_s,
    r_out_s, u_out_s, w_out_s, pull_s, partner_s, cross_s,
    lent_beam_s, lent_column_s, lent_y_s, lent_r_s, lent_first_s, lent_v_s, ahead_s,
    message_s, early_s, late_s,
    halo_recv, pair_recv, sum_recv, word_sem, in_sem, beam_sem, halo_send, pair_send, hand_send, sum_send,
):
    modes, freqs, _, ell = rhs_in.shape
    rank = beam_in.shape[3]
    width = modes * rank
    n = nma * nf
    my_ma, my_f = lax.axis_index("ma"), lax.axis_index("freq")
    me = my_ma * nf + my_f
    last = freqs - 1
    two_sided = nf > 2
    paired = nf == 2 and nma % 2 == 0 and freqs > 1
    helper = my_ma % 2 == 1
    groups = modes // 4
    edges = [0, last][:min(nf - 1, 2)]
    inner = [f for f in range(freqs) if f not in edges]
    beside_edge = [f for f in inner if f - 1 in edges or f + 1 in edges]
    apart = [f for f in inner if f not in beside_edge]
    vector = edges + inner[:max(freqs // 2 - len(edges), 0)]
    matrix = [f for f in range(freqs) if f not in vector]

    def at(g):
        return jnp.where(my_f == 0, last - g, g)

    edge_copies = [
        pltpu.make_async_copy(x0_in.at[:, at(f)], edge_s.at[i], in_sem.at[i])
        for i, f in enumerate(edges)
    ]
    x0_copy = pltpu.make_async_copy(x0_in, x0_s, in_sem.at[2])
    rhs_copy = pltpu.make_async_copy(rhs_in, rhs_s, in_sem.at[3])
    small = [
        pltpu.make_async_copy(power_in, power_s, in_sem.at[4]),
        pltpu.make_async_copy(smooth_in, smooth_s, in_sem.at[5]),
        pltpu.make_async_copy(noise_in, noise_s, in_sem.at[6]),
    ]
    beam_copies = [
        pltpu.make_async_copy(beam_in.at[:, at(f)], beam_s.at[f], beam_sem.at[f])
        for f in range(freqs)
    ]
    for copy in edge_copies:
        copy.start()

    def flip(bit):
        d = 1 << (bit if bit < freq_bits else bit - freq_bits)
        place = my_f if bit < freq_bits else my_ma
        return d * (1 - 2 * (place // d % 2))

    def partner(bits):
        return (
            my_ma + sum(flip(bit) for bit in bits if bit >= freq_bits),
            my_f + sum(flip(bit) for bit in bits if bit < freq_bits),
        )

    freq_bits = nf.bit_length() - 1
    bits = freq_bits + nma.bit_length() - 1
    close = min(bits, 3)
    greeted = [
        partner([bit for bit in range(close) if mask >> bit & 1]) for mask in range(1, 1 << close)
    ]
    word = [partner([bit]) for bit in range(close, bits)]
    greeted += word
    words = len(word)
    barrier = pltpu.get_barrier_semaphore()
    near = jnp.where(my_f == 0, 1, my_f - 1)
    has_far = (my_f > 0) & (my_f < nf - 1)

    def greet(device):
        pl.semaphore_signal(barrier, inc=1, device_id=device, device_id_type=MESH)

    for i, device in enumerate(greeted):
        greet(device)
        if i == 0:
            for copy in [beam_copies[f] for f in edges] + [x0_copy, rhs_copy] + small:
                copy.start()
    expected = len(greeted)
    if nf > 2:
        pl.when(my_f > 0)(lambda: greet((my_ma, my_f - 1)))
        pl.when(my_f < nf - 1)(lambda: greet((my_ma, my_f + 1)))
        expected = expected + jnp.minimum(my_f, 1) + jnp.minimum(nf - 1 - my_f, 1)

    steps = list(range(words + 1))

    def advance():
        if steps:
            step = steps.pop(0)
            if step > 0:
                pl.semaphore_wait(word_sem.at[step - 1], 1)
            if step < words:
                pl.semaphore_signal(
                    word_sem.at[step], inc=1, device_id=word[step], device_id_type=MESH
                )

    def piece(kind, g):
        if kind == 0:
            rows = pl.ds(4 * g, 4)
            return (lambda i: edge_s.at[i, rows]), (lambda i: first_s.at[i, rows])
        source = (y_s, v_s)[kind - 1]
        rows = pl.ds(8 * g, 8)
        return (lambda i: source.at[i, rows]), (lambda i: halo_s.at[kind - 1, i, rows])

    def near_copy(kind, g):
        source, target = piece(kind, g)
        side = jnp.minimum(my_f // 2, 1) if two_sided else 0
        return pltpu.make_async_remote_copy(
            src_ref=source(0), dst_ref=target(side),
            send_sem=halo_send.at[kind, g, 0], recv_sem=halo_recv.at[kind, g, side],
            device_id=(my_ma, near), device_id_type=MESH,
        )

    def far_copy(kind, g):
        source, target = piece(kind, g)
        return pltpu.make_async_remote_copy(
            src_ref=source(1), dst_ref=target(0),
            send_sem=halo_send.at[kind, g, 1], recv_sem=halo_recv.at[kind, g, 0],
            device_id=(my_ma, my_f + 1), device_id_type=MESH,
        )

    def arrival(kind, g, side):
        slot = piece(kind, g)[1](side)
        return pltpu.make_async_copy(slot, slot, halo_recv.at[kind, g, side])

    def send(kind, g):
        if nf > 1:
            near_copy(kind, g).start()
        if two_sided:
            pl.when(has_far)(lambda: far_copy(kind, g).start())

    def arrive(kind, g):
        if nf > 1:
            arrival(kind, g, 0).wait()
        if two_sided:
            pl.when(has_far)(lambda: arrival(kind, g, 1).wait())

    def sent(kind, g):
        if nf > 1:
            near_copy(kind, g).wait_send()
        if two_sided:
            pl.when(has_far)(lambda: far_copy(kind, g).wait_send())

    def pair_copy(k, source, target, ma, f):
        return pltpu.make_async_remote_copy(
            src_ref=source, dst_ref=target, send_sem=pair_send.at[k], recv_sem=pair_recv.at[k],
            device_id=(ma, f), device_id_type=MESH,
        )

    def lend(k):
        source = (lambda: beam_s.at[0], lambda: column_s.at[0], lambda: y_s.at[0], lambda: r_s.at[1])[k]
        target = (lent_beam_s, lent_column_s, lent_y_s, lent_r_s)[k]
        return pair_copy(k, source(), target, my_ma + 1, my_f)

    def pull_copy():
        return pair_copy(4, pull_s, partner_s, my_ma + 1, my_f)

    def first_copy(g):
        rows = pl.ds(4 * g, 4)
        return pair_copy(5 + g, edge_s.at[0, rows], lent_first_s.at[rows], my_ma + 1, 1 - my_f)

    def cross_copy(g):
        rows = pl.ds(8 * g, 8)
        return pair_copy(5 + groups + g, lent_v_s.at[rows], cross_s.at[rows], my_ma, 1 - my_f)

    def ahead_copy(g):
        rows = pl.ds(8 * g, 8)
        return pltpu.make_async_remote_copy(
            src_ref=ahead_s.at[rows], dst_ref=halo_s.at[1, 0, rows],
            send_sem=halo_send.at[2, g, 0], recv_sem=halo_recv.at[2, g, 0],
            device_id=(my_ma, 1 - my_f), device_id_type=MESH,
        )

    def hand_copy(g):
        rows = pl.ds(4 * g, 4)
        return pltpu.make_async_remote_copy(
            src_ref=lent_first_s.at[rows], dst_ref=first_s.at[0, rows],
            send_sem=hand_send.at[g], recv_sem=halo_recv.at[0, g, 0],
            device_id=(my_ma - 1, my_f), device_id_type=MESH,
        )

    def even_only(copies):
        @pl.when(jnp.logical_not(helper))
        def _():
            for copy in copies:
                copy.start()

    def beside(i, value):
        return jnp.where(has_far, value, 0.0) if i else value

    if two_sided:
        @pl.when(jnp.logical_not(has_far))
        def _():
            first_s[1] = jnp.zeros_like(first_s[1])
            halo_s[:, 1] = jnp.zeros_like(halo_s[:, 1])

    for copy in edge_copies:
        copy.wait()
    for f in inner:
        beam_copies[f].start()
    pl.semaphore_wait(barrier, expected)
    if paired:
        even_only([first_copy(g) for g in range(groups)])

        @pl.when(helper)
        def _():
            for g in range(groups):
                near_copy(0, g).start()
    else:
        for g in range(groups):
            send(0, g)
    advance()

    x0_copy.wait()
    for copy in small:
        copy.wait()
    def rows_of(ref, *at_f):
        place = (slice(None), *at_f)
        return jnp.concatenate(
            [ref[(slice(4 * g, 4 * g + 4), *place[1:], b)] for g in range(groups) for b in range(2)],
            axis=0,
        )

    def group(g):
        return slice(8 * g, 8 * g + 8)

    for f in range(freqs):
        x_s[f] = rows_of(x0_s, at(f))
    power, smooth = power_s[...], smooth_s[...]
    row = lax.broadcasted_iota(jnp.int32, (2 * modes, width), 0)
    own = lax.broadcasted_iota(jnp.int32, (2 * modes, width), 1) // rank == row // 8 * 4 + row % 4
    sign = jnp.where(row % 8 < 4, 1.0, -1.0)
    for i, f in enumerate(matrix):
        levels = noise_s[:, at(f), :]
        levels = jnp.concatenate(
            [levels[4 * g:4 * g + 4] for g in range(groups) for _ in range(2)], axis=0
        )
        mask_s[i] = jnp.where(own, jnp.concatenate([levels] * modes, axis=1), 0.0)
    unit = (
        lax.broadcasted_iota(jnp.int32, (rank, rank), 0)
        == lax.broadcasted_iota(jnp.int32, (rank, rank), 1)
    )
    for i, f in enumerate(vector):
        levels = noise_s[:, at(f), :]
        for m in range(modes):
            column = jnp.sum(jnp.where(unit, levels[m:m + 1], 0.0), axis=1, keepdims=True)
            column_s[i, m] = jnp.broadcast_to(column, (rank, 128))

    def swapped(x):
        return jnp.concatenate([pltpu.roll(x[group(g)], 4, 0) for g in range(groups)], axis=0)

    def matrix_project(f, field):
        i = matrix.index(f)
        seen = times(field, high_s[i], low_s[i], True)
        parts = seen[:, :width] + sign * swapped(seen[:, width:])
        return parts, mask_s[i] * parts

    def matrix_back(f, seen):
        i = matrix.index(f)
        weighted = jnp.concatenate([seen[1], -sign * swapped(seen[1])], axis=1)
        return times(weighted, high_s[i], low_s[i], False)

    def wide(x):
        return jnp.concatenate([x] * (ell // 128), axis=1)

    def owned(f):
        return (lambda m, a: beam_s[f, m, a]), (lambda m: column_s[vector.index(f), m])

    lent = (lambda m, a: lent_beam_s[m, a]), (lambda m: lent_column_s[m])

    def group_project(source, g, field):
        beam_of, column_of = source
        parts = []
        for j in range(4):
            m = 4 * g + j
            real_beam, imaginary_beam = beam_of(m, 0), beam_of(m, 1)
            real_field, imaginary_field = field[j:j + 1], field[4 + j:5 + j]
            levels = column_of(m)
            real = jnp.sum(
                real_beam * real_field + imaginary_beam * imaginary_field, axis=1, keepdims=True
            )
            imaginary = jnp.sum(
                real_beam * imaginary_field - imaginary_beam * real_field, axis=1, keepdims=True
            )
            parts.append((real, imaginary, levels * real, levels * imaginary))
        return parts

    def group_back(source, g, parts):
        beam_of, _ = source
        reals, imaginaries = [], []
        for j, (_, _, real, imaginary) in enumerate(parts):
            m = 4 * g + j
            real, imaginary = wide(real), wide(imaginary)
            real_beam, imaginary_beam = beam_of(m, 0), beam_of(m, 1)
            for found, value in (
                (reals, real_beam * real - imaginary_beam * imaginary),
                (imaginaries, real_beam * imaginary + imaginary_beam * real),
            ):
                found.append(sum(value[k:k + 8] for k in range(0, rank, 8)))
        return folded(reals + imaginaries)

    def group_beam(source, g, field):
        return group_back(source, g, group_project(source, g, field))

    def project(f, ref):
        if f in matrix:
            return matrix_project(f, ref[f])
        return [group_project(owned(f), g, ref[f, group(g)]) for g in range(groups)]

    def back(f, seen):
        if f in matrix:
            return matrix_back(f, seen)
        return jnp.concatenate([group_back(owned(f), g, seen[g]) for g in range(groups)], axis=0)

    def apply_beam(fs, ref):
        fs = [f for f in fs if f in matrix] + [f for f in fs if f in vector]
        seen = [project(f, ref) for f in fs]
        return {f: back(f, found) for f, found in zip(fs, seen)}

    def count(f):
        value = float(f > 0) + float(f < last) + float(nf > 1 and f == 0)
        if two_sided and f == last:
            value = value + jnp.where(has_far, 1.0, 0.0)
        return value

    def local_prior(f, ref, rows=slice(None)):
        value = count(f) * ref[f, rows]
        if f > 0:
            value = value - ref[f - 1, rows]
        if f < last:
            value = value - ref[f + 1, rows]
        return power * ref[f, rows] + smooth * value

    for f in edges:
        beam_copies[f].wait()
    rhs_copy.wait()
    for i, f in enumerate(edges):
        for g in range(groups):
            rows = group(g)
            image = group_beam(owned(f), g, x_s[f, rows])
            y_s[i, rows] = rows_of(rhs_s, at(f))[rows] - image - local_prior(f, x_s, rows)
    first, rest = [], inner
    if paired:
        even_only([near_copy(1, g) for g in range(groups)] + [lend(k) for k in range(3)])
        first, rest = inner[:1], inner[1:]
    else:
        for g in range(groups):
            send(1, g)

    for f in first:
        beam_copies[f].wait()
        r_s[f] = rows_of(rhs_s, at(f)) - back(f, project(f, x_s)) - local_prior(f, x_s)
    if paired:
        even_only([lend(3)])

        @pl.when(helper)
        def _():
            for g in range(groups):
                near_copy(1, g).start()

    for f in rest:
        beam_copies[f].wait()
    for i, f in enumerate(matrix):
        for a in range(2):
            rows = slice(a * width, (a + 1) * width)
            high, low = split(beam_s[f, :, a].reshape(width, ell))
            high_s[i, rows] = high
            low_s[i, rows] = low
    for f, image in apply_beam(rest, x_s).items():
        r_s[f] = rows_of(rhs_s, at(f)) - image - local_prior(f, x_s)
    for f, image in apply_beam(inner, r_s).items():
        u_s[f] = image + local_prior(f, r_s) if f in apart else image
    advance()

    def complete(i, f, g):
        rows = group(g)
        halo = jnp.concatenate([first_s[i, 4 * g:4 * g + 4, b, :] for b in range(2)], axis=0)
        r_s[f, rows] = y_s[i, rows] + smooth * halo

    def edge_image(f, g):
        rows = group(g)
        return group_beam(owned(f), g, r_s[f, rows]) + local_prior(f, r_s, rows)

    if paired:
        @pl.when(helper)
        def _():
            for g in range(groups):
                arrive(0, g)
                complete(0, 0, g)
                ahead_s[group(g)] = edge_image(0, g)
                ahead_copy(g).start()
            for g in range(groups):
                first_copy(g).wait_recv()
                hand_copy(g).start()
                if g == 0:
                    for k in range(4):
                        lend(k).wait_recv()
                rows = group(g)
                halo = jnp.concatenate([lent_first_s[4 * g:4 * g + 4, b, :] for b in range(2)], axis=0)
                r = lent_y_s[rows] + smooth * halo
                local = power * r + smooth * (count(0) * r - lent_r_s[rows])
                lent_v_s[rows] = group_beam(lent, g, r) + local
                cross_copy(g).start()

    seen = {f: project(f, u_s) for f in apart}
    if paired:
        @pl.when(jnp.logical_not(helper))
        def _():
            for g in range(groups):
                arrive(0, g)

        for g in range(groups):
            arrive(1, g)
    for g in range(groups):
        if not paired:
            arrive(0, g)
        for i, f in enumerate(edges):
            complete(i, f, g)
        for i, f in enumerate(edges):
            v_s[i, group(g)] = edge_image(f, g)
        if not paired:
            send(2, g)
    for f in beside_edge:
        u_s[f] = u_s[f] + local_prior(f, r_s)
    seen |= {f: project(f, u_s) for f in beside_edge}

    if not paired:
        for g in range(groups):
            arrive(1, g)
    for i, f in enumerate(edges):
        u_s[f] = v_s[i] - beside(i, smooth * (halo_s[0, i] + smooth * x_s[f]))
    if paired:
        pull_s[...] = smooth * u_s[0]
        even_only([pull_copy()])
    seen |= {f: project(f, u_s) for f in edges}
    norm = jnp.zeros((2 * modes, ell), F32)
    curve, square, cube = norm, norm, norm
    beam_part = jnp.zeros((2 * modes, width), F32)
    column_part = jnp.zeros((rank, 128), F32)
    for f in inner + edges:
        if f in matrix:
            beam_part = beam_part + seen[f][0] * seen[f][1]
        else:
            for parts in seen[f]:
                for real, imaginary, real_weighted, imaginary_weighted in parts:
                    column_part = column_part + (real * real_weighted + imaginary * imaginary_weighted)
        w_s[f] = local_prior(f, u_s)
        norm = norm + r_s[f] * r_s[f]
        curve = curve + r_s[f] * u_s[f]
        square = square + u_s[f] * u_s[f]
        cube = cube + u_s[f] * w_s[f]
    lane = lax.broadcasted_iota(jnp.int32, (1, 128), 1)
    message = jnp.zeros((1, 128), F32)
    for i, part in enumerate((norm, curve, square, cube)):
        total = total_of(part)
        if i == 3:
            total = total + total_of(beam_part) + jnp.sum(column_part, axis=0, keepdims=True)
        message = jnp.where(lane == i, total, message)
    if paired:
        message = jnp.where(lane == 4 + my_f, total_of(smooth * r_s[0] * pull_s[...]), message)
    message_s[0] = message
    early_s[me] = message

    while steps:
        advance()

    def share(source, target, slot, turn, device):
        pltpu.make_async_remote_copy(
            src_ref=message_s.at[source], dst_ref=target.at[slot],
            send_sem=sum_send.at[turn], recv_sem=sum_recv.at[turn],
            device_id=device, device_id_type=MESH,
        ).start()

    def share_all(source, target, slot, turn, stride):
        if n > 64:
            def body(i, carry):
                ma, f = my_ma + i * stride // nf, my_f + i * stride % nf
                share(source, target, slot, turn, (lax.rem(ma, nma), lax.rem(f, nf)))
                return carry

            lax.fori_loop(1, n // stride, body, 0)
        else:
            for mask in sorted(range(stride, n, stride), key=lambda m: (-(m // nf // 2), m)):
                device = partner([bit for bit in range(bits) if mask >> bit & 1])
                share(source, target, slot, turn, device)

    def landed(target, sem, rows):
        if rows:
            rows = target.at[pl.ds(0, rows)]
            pltpu.make_async_copy(rows, rows, sem).wait()

    def lanes_of(x):
        x = jnp.sum(x, axis=0, keepdims=True)
        return sum(x[:, i:i + 128] for i in range(0, ell, 128))

    share_all(0, early_s, me, 0, 1)
    if paired:
        even_only([near_copy(2, g) for g in range(groups)])
    for f in matrix + vector:
        w_s[f] = w_s[f] + back(f, seen[f])

    late_rows = late_s.shape[0]
    if paired:
        @pl.when(helper)
        def _():
            cross = jnp.zeros((8, ell), F32)
            for g in range(groups):
                arrive(2, g)
                cross = cross + pull_s[group(g)] * halo_s[1, 0, group(g)]
            pull_copy().wait_recv()
            for g in range(groups):
                cross_copy(g).wait_recv()
                cross = cross + partner_s[group(g)] * cross_s[group(g)]
            message = lanes_of(cross)
            late_s[my_ma // 2] = message
            message_s[1] = message
            share_all(1, late_s, my_ma // 2, 1, nf)
            for g in range(groups):
                cross_copy(g).wait_send()

        @pl.when(jnp.logical_not(helper))
        def _():
            for g in range(groups):
                arrive(2, g)
            pull_copy().wait_send()
            for k in range(4):
                lend(k).wait_send()
            for g in range(groups):
                first_copy(g).wait_send()

        w_s[0] = w_s[0] - smooth * (halo_s[1, 0] - smooth * r_s[0])
    else:
        cross = jnp.zeros((8, ell), F32)
        nexts = []
        for g in range(groups):
            arrive(2, g)
            rows = group(g)
            for i, f in enumerate(edges):
                pull = beside(i, smooth * (halo_s[1, i, rows] - smooth * r_s[f, rows]))
                nexts.append((f, rows, pull))
                cross = cross + pull * u_s[f, rows]
        message = lanes_of(cross)
        late_s[me] = message
        message_s[1] = message
        share_all(1, late_s, me, 1, 1)
        for f, rows, pull in nexts:
            w_s[f, rows] = w_s[f, rows] - pull

    if paired:
        for g in range(groups):
            for kind in (1, 2):
                sent(kind, g)

        @pl.when(helper)
        def _():
            for g in range(groups):
                sent(0, g)
                hand_copy(g).wait_send()
    else:
        for kind in range(3):
            for g in range(groups):
                sent(kind, g)
    for source, target in ((r_s, r_out_s), (u_s, u_out_s), (w_s, w_out_s)):
        for f in range(freqs):
            value = source[f]
            for g in range(groups):
                for b in range(2):
                    start = 8 * g + 4 * b
                    target[4 * g:4 * g + 4, at(f), b, :] = value[start:start + 4]

    landed(early_s, sum_send.at[0], n - 1)
    landed(early_s, sum_recv.at[0], n - 1)
    if paired:
        @pl.when(helper)
        def _():
            rows = early_s.at[pl.ds(0, nma - 1)]
            pltpu.make_async_copy(rows, rows, sum_send.at[1]).wait()
            landed(late_s, sum_recv.at[1], late_rows - 1)

        pl.when(jnp.logical_not(helper))(lambda: landed(late_s, sum_recv.at[1], late_rows))
    else:
        landed(late_s, sum_send.at[1], late_rows - 1)
        landed(late_s, sum_recv.at[1], late_rows - 1)
    total = jnp.sum(early_s[...], axis=0)
    m0, m1, m2, m3, known = (
        jnp.sum(jnp.where(lane == i, total, 0.0), axis=1, keepdims=True)
        for i in (0, 1, 2, 3, 4 + my_f)
    )
    crossed = jnp.sum(jnp.sum(late_s[...], axis=0), axis=1, keepdims=True)
    m3 = m3 - 2.0 * (crossed - known) if paired else m3 - crossed
    inverse = 1.0 / m1
    step = m0 * inverse
    drop = step * m2 - m1
    growth = drop * inverse
    curve_next = m1 - 2.0 * step * m2 + step * step * m3
    step_next = step * drop / (curve_next - growth * drop)
    c = step + step_next * (1.0 + growth)
    e = step * step_next
    r, u = r_out_s[...], u_out_s[...]
    sol_s[...] = x0_s[...] + c * r - e * u
    res_s[...] = r - c * u + e * w_out_s[...]


def scoped_kernel(nma, nf, sides, *refs):
    modes, freqs = refs[0].shape[:2]
    dma = pltpu.SemaphoreType.DMA
    pl.run_scoped(
        functools.partial(kernel, nma, nf, *refs),
        dma((7,)), dma((freqs,)), dma((3, modes // 4, sides)), dma((2 * (modes // 4) + 5,)),
        dma((modes // 4,)), dma((2,)),
    )


def write_out(sol_in, res_in, sol_out, res_out, sem):
    copies = [
        pltpu.make_async_copy(sol_in, sol_out, sem.at[0]),
        pltpu.make_async_copy(res_in, res_out, sem.at[1]),
    ]
    for copy in copies:
        copy.start()
    for copy in copies:
        copy.wait()


def shards(right_side, start_field, beam, noise, inv_power, smooth):
    nma, nf = lax.axis_size("ma"), lax.axis_size("freq")
    modes, freqs, _, ell = right_side.shape
    rank = beam.shape[3]
    width = modes * rank
    sides = 2 if nf > 2 else 1
    vmem_spec = pl.BlockSpec(memory_space=pltpu.VMEM)
    any_spec = pl.BlockSpec(memory_space=pl.ANY)
    field = pltpu.VMEM(right_side.shape, F32)
    edge = pltpu.VMEM((sides, modes, 2, ell), F32)
    slab = pltpu.VMEM((freqs, 2 * modes, ell), F32)
    edge_field = pltpu.VMEM((2 * modes, ell), F32)
    edge_slab = pltpu.VMEM((sides, 2 * modes, ell), F32)
    vector = max(min(nf - 1, 2), freqs // 2)
    matrix = max(freqs - vector, 1)
    half = pltpu.VMEM((matrix, 2 * width, ell), BF16)
    outs = pl.pallas_call(
        functools.partial(scoped_kernel, nma, nf, sides),
        out_shape=[field] * 2,
        in_specs=[any_spec] * 6,
        out_specs=[vmem_spec] * 2,
        scratch_shapes=[
            field, field, edge,
            pltpu.VMEM((freqs, modes, 2, rank, ell), F32),
            pltpu.VMEM(noise.shape, F32),
            pltpu.VMEM((1, ell), F32), pltpu.VMEM((1, ell), F32),
            half, half,
            slab, edge_slab, slab, edge_slab, slab, slab,
            pltpu.VMEM((matrix, 2 * modes, width), F32),
            pltpu.VMEM((vector, modes, rank, 128), F32),
            edge,
            pltpu.VMEM((2, sides, 2 * modes, ell), F32),
            field, field, field,
            edge_field, edge_field, edge_field,
            pltpu.VMEM((modes, 2, rank, ell), F32), pltpu.VMEM((modes, rank, 128), F32),
            edge_field, edge_field, pltpu.VMEM((modes, 2, ell), F32), edge_field, edge_field,
            pltpu.VMEM((2, 1, 128), F32),
            pltpu.VMEM((nma * nf, 1, 128), F32),
            pltpu.VMEM((nma // 2 if nf == 2 and nma % 2 == 0 and freqs > 1 else nma * nf, 1, 128), F32),
            pltpu.SemaphoreType.DMA((3, modes // 4, sides)),
            pltpu.SemaphoreType.DMA((2 * (modes // 4) + 5,)),
            pltpu.SemaphoreType.DMA((2,)),
            pltpu.SemaphoreType.REGULAR((max((nma * nf).bit_length() - 4, 1),)),
        ],
        compiler_params=pltpu.CompilerParams(
            collective_id=0, has_side_effects=True, vmem_limit_bytes=67043328 - 2 * right_side.size * 4
        ),
        name="solve",
    )(right_side, start_field, beam, noise, inv_power[None], smooth[None])
    return pl.pallas_call(
        write_out,
        out_shape=[jax.ShapeDtypeStruct(right_side.shape, F32)] * 2,
        in_specs=[vmem_spec] * 2,
        out_specs=[any_spec] * 2,
        scratch_shapes=[pltpu.SemaphoreType.DMA((2,))],
        compiler_params=pltpu.CompilerParams(vmem_limit_bytes=1024 * 1024),
        name="write_out",
    )(*outs)


def solution(mesh):
    in_specs = (
        P("ma", "freq", None, None),
        P("ma", "freq", None, None),
        P("ma", "freq", None, None, None),
        P("ma", "freq", None),
        P(),
        P(),
    )
    out_specs = (P("ma", "freq", None, None), P("ma", "freq", None, None))
    return jax.shard_map(shards, mesh=mesh, in_specs=in_specs, out_specs=out_specs, check_vma=False)
```

```python
import functools

import jax
import jax.numpy as jnp
from jax import lax
from jax.experimental import pallas as pl
from jax.experimental.pallas import tpu as pltpu
from jax.sharding import PartitionSpec as P

MESH = pl.DeviceIdType.MESH
F32, BF16 = jnp.float32, jnp.bfloat16


def split(x):
    high = x.astype(BF16)
    return high, (x - high.astype(F32)).astype(BF16)


def times(x, high, low, transposed):
    dims = (((1,), (1 if transposed else 0,)), ((), ()))
    rows = x.shape[0]
    x_high, x_low = split(x)
    both = jnp.concatenate([x_high, x_low], axis=0)
    main = lax.dot_general(both, high, dims, preferred_element_type=F32)
    rest = lax.dot_general(x_high, low, dims, preferred_element_type=F32)
    return main[:rows] + (main[rows:] + rest)


def folded(parts):
    row = lax.broadcasted_iota(jnp.int32, parts[0].shape, 0)
    upper = row < 4
    fours = [
        jnp.where(upper, parts[s], parts[s + 4])
        + pltpu.roll(jnp.where(upper, parts[s + 4], parts[s]), 4, 0)
        for s in range(4)
    ]
    even = row // 2 % 2 == 0
    twos = [
        jnp.where(
            even, fours[s] + pltpu.roll(fours[s], 6, 0), fours[s + 2] + pltpu.roll(fours[s + 2], 2, 0)
        )
        for s in range(2)
    ]
    return jnp.where(
        row % 2 == 0, twos[0] + pltpu.roll(twos[0], 7, 0), twos[1] + pltpu.roll(twos[1], 1, 0)
    )


def total_of(x):
    return jnp.sum(jnp.sum(x, axis=0, keepdims=True), axis=1, keepdims=True)


def kernel(
    nma, nf, rhs_in, x0_in, beam_in, noise_in, power_in, smooth_in, sol_s, res_s,
    rhs_s, x0_s, edge_s, beam_s, noise_s, power_s, smooth_s,
    high_s, low_s, x_s, y_s, r_s, v_s, u_s, w_s, mask_s, column_s, first_s, halo_s,
    r_out_s, u_out_s, w_out_s, pull_s, partner_s, cross_s,
    lent_beam_s, lent_column_s, lent_y_s, lent_r_s, lent_first_s, lent_v_s, ahead_s,
    message_s, early_s, late_s,
    halo_recv, pair_recv, sum_recv, word_sem, in_sem, beam_sem, halo_send, pair_send, hand_send, sum_send,
):
    modes, freqs, _, ell = rhs_in.shape
    rank = beam_in.shape[3]
    width = modes * rank
    n = nma * nf
    my_ma, my_f = lax.axis_index("ma"), lax.axis_index("freq")
    me = my_ma * nf + my_f
    last = freqs - 1
    two_sided = nf > 2
    paired = nf == 2 and nma % 2 == 0 and freqs > 1
    helper = my_ma % 2 == 1
    groups = modes // 4
    edges = [0, last][:min(nf - 1, 2)]
    inner = [f for f in range(freqs) if f not in edges]
    beside_edge = [f for f in inner if f - 1 in edges or f + 1 in edges]
    apart = [f for f in inner if f not in beside_edge]
    vector = edges + inner[:max(freqs // 2 - len(edges), 0)]
    matrix = [f for f in range(freqs) if f not in vector]

    def at(g):
        return jnp.where(my_f == 0, last - g, g)

    edge_copies = [
        pltpu.make_async_copy(x0_in.at[:, at(f)], edge_s.at[i], in_sem.at[i])
        for i, f in enumerate(edges)
    ]
    x0_copy = pltpu.make_async_copy(x0_in, x0_s, in_sem.at[2])
    rhs_copy = pltpu.make_async_copy(rhs_in, rhs_s, in_sem.at[3])
    small = [
        pltpu.make_async_copy(power_in, power_s, in_sem.at[4]),
        pltpu.make_async_copy(smooth_in, smooth_s, in_sem.at[5]),
        pltpu.make_async_copy(noise_in, noise_s, in_sem.at[6]),
    ]
    beam_copies = [
        pltpu.make_async_copy(beam_in.at[:, at(f)], beam_s.at[f], beam_sem.at[f])
        for f in range(freqs)
    ]
    for copy in edge_copies:
        copy.start()

    def flip(bit):
        d = 1 << (bit if bit < freq_bits else bit - freq_bits)
        place = my_f if bit < freq_bits else my_ma
        return d * (1 - 2 * (place // d % 2))

    def partner(bits):
        return (
            my_ma + sum(flip(bit) for bit in bits if bit >= freq_bits),
            my_f + sum(flip(bit) for bit in bits if bit < freq_bits),
        )

    freq_bits = nf.bit_length() - 1
    bits = freq_bits + nma.bit_length() - 1
    close = min(bits, 3)
    greeted = [
        partner([bit for bit in range(close) if mask >> bit & 1]) for mask in range(1, 1 << close)
    ]
    word = [partner([bit]) for bit in range(close, bits)]
    greeted += word
    words = len(word)
    barrier = pltpu.get_barrier_semaphore()
    near = jnp.where(my_f == 0, 1, my_f - 1)
    has_far = (my_f > 0) & (my_f < nf - 1)

    def greet(device):
        pl.semaphore_signal(barrier, inc=1, device_id=device, device_id_type=MESH)

    for i, device in enumerate(greeted):
        greet(device)
        if i == 0:
            for copy in [beam_copies[f] for f in edges] + [x0_copy, rhs_copy] + small:
                copy.start()
    expected = len(greeted)
    if nf > 2:
        pl.when(my_f > 0)(lambda: greet((my_ma, my_f - 1)))
        pl.when(my_f < nf - 1)(lambda: greet((my_ma, my_f + 1)))
        expected = expected + jnp.minimum(my_f, 1) + jnp.minimum(nf - 1 - my_f, 1)

    steps = list(range(words + 1))

    def advance():
        if steps:
            step = steps.pop(0)
            if step > 0:
                pl.semaphore_wait(word_sem.at[step - 1], 1)
            if step < words:
                pl.semaphore_signal(
                    word_sem.at[step], inc=1, device_id=word[step], device_id_type=MESH
                )

    def piece(kind, g):
        if kind == 0:
            rows = pl.ds(4 * g, 4)
            return (lambda i: edge_s.at[i, rows]), (lambda i: first_s.at[i, rows])
        source = (y_s, v_s)[kind - 1]
        rows = pl.ds(8 * g, 8)
        return (lambda i: source.at[i, rows]), (lambda i: halo_s.at[kind - 1, i, rows])

    def near_copy(kind, g):
        source, target = piece(kind, g)
        side = jnp.minimum(my_f // 2, 1) if two_sided else 0
        return pltpu.make_async_remote_copy(
            src_ref=source(0), dst_ref=target(side),
            send_sem=halo_send.at[kind, g, 0], recv_sem=halo_recv.at[kind, g, side],
            device_id=(my_ma, near), device_id_type=MESH,
        )

    def far_copy(kind, g):
        source, target = piece(kind, g)
        return pltpu.make_async_remote_copy(
            src_ref=source(1), dst_ref=target(0),
            send_sem=halo_send.at[kind, g, 1], recv_sem=halo_recv.at[kind, g, 0],
            device_id=(my_ma, my_f + 1), device_id_type=MESH,
        )

    def arrival(kind, g, side):
        slot = piece(kind, g)[1](side)
        return pltpu.make_async_copy(slot, slot, halo_recv.at[kind, g, side])

    def send(kind, g):
        if nf > 1:
            near_copy(kind, g).start()
        if two_sided:
            pl.when(has_far)(lambda: far_copy(kind, g).start())

    def arrive(kind, g):
        if nf > 1:
            arrival(kind, g, 0).wait()
        if two_sided:
            pl.when(has_far)(lambda: arrival(kind, g, 1).wait())

    def sent(kind, g):
        if nf > 1:
            near_copy(kind, g).wait_send()
        if two_sided:
            pl.when(has_far)(lambda: far_copy(kind, g).wait_send())

    def pair_copy(k, source, target, ma, f):
        return pltpu.make_async_remote_copy(
            src_ref=source, dst_ref=target, send_sem=pair_send.at[k], recv_sem=pair_recv.at[k],
            device_id=(ma, f), device_id_type=MESH,
        )

    def lend(k):
        source = (lambda: beam_s.at[0], lambda: column_s.at[0], lambda: y_s.at[0], lambda: r_s.at[1])[k]
        target = (lent_beam_s, lent_column_s, lent_y_s, lent_r_s)[k]
        return pair_copy(k, source(), target, my_ma + 1, my_f)

    def pull_copy():
        return pair_copy(4, pull_s, partner_s, my_ma + 1, my_f)

    def first_copy(g):
        rows = pl.ds(4 * g, 4)
        return pair_copy(5 + g, edge_s.at[0, rows], lent_first_s.at[rows], my_ma + 1, 1 - my_f)

    def cross_copy(g):
        rows = pl.ds(8 * g, 8)
        return pair_copy(5 + groups + g, lent_v_s.at[rows], cross_s.at[rows], my_ma, 1 - my_f)

    def ahead_copy(g):
        rows = pl.ds(8 * g, 8)
        return pltpu.make_async_remote_copy(
            src_ref=ahead_s.at[rows], dst_ref=halo_s.at[1, 0, rows],
            send_sem=halo_send.at[2, g, 0], recv_sem=halo_recv.at[2, g, 0],
            device_id=(my_ma, 1 - my_f), device_id_type=MESH,
        )

    def hand_copy(g):
        rows = pl.ds(4 * g, 4)
        return pltpu.make_async_remote_copy(
            src_ref=lent_first_s.at[rows], dst_ref=first_s.at[0, rows],
            send_sem=hand_send.at[g], recv_sem=halo_recv.at[0, g, 0],
            device_id=(my_ma - 1, my_f), device_id_type=MESH,
        )

    def even_only(copies):
        @pl.when(jnp.logical_not(helper))
        def _():
            for copy in copies:
                copy.start()

    def beside(i, value):
        return jnp.where(has_far, value, 0.0) if i else value

    if two_sided:
        @pl.when(jnp.logical_not(has_far))
        def _():
            first_s[1] = jnp.zeros_like(first_s[1])
            halo_s[:, 1] = jnp.zeros_like(halo_s[:, 1])

    for copy in edge_copies:
        copy.wait()
    for f in inner:
        beam_copies[f].start()
    pl.semaphore_wait(barrier, expected)
    if paired:
        even_only([first_copy(g) for g in range(groups)])

        @pl.when(helper)
        def _():
            for g in range(groups):
                near_copy(0, g).start()
    else:
        for g in range(groups):
            send(0, g)
    advance()

    x0_copy.wait()
    for copy in small:
        copy.wait()
    def rows_of(ref, *at_f):
        place = (slice(None), *at_f)
        return jnp.concatenate(
            [ref[(slice(4 * g, 4 * g + 4), *place[1:], b)] for g in range(groups) for b in range(2)],
            axis=0,
        )

    def group(g):
        return slice(8 * g, 8 * g + 8)

    for f in range(freqs):
        x_s[f] = rows_of(x0_s, at(f))
    power, smooth = power_s[...], smooth_s[...]
    row = lax.broadcasted_iota(jnp.int32, (2 * modes, width), 0)
    own = lax.broadcasted_iota(jnp.int32, (2 * modes, width), 1) // rank == row // 8 * 4 + row % 4
    sign = jnp.where(row % 8 < 4, 1.0, -1.0)
    for i, f in enumerate(matrix):
        levels = noise_s[:, at(f), :]
        levels = jnp.concatenate(
            [levels[4 * g:4 * g + 4] for g in range(groups) for _ in range(2)], axis=0
        )
        mask_s[i] = jnp.where(own, jnp.concatenate([levels] * modes, axis=1), 0.0)
    unit = (
        lax.broadcasted_iota(jnp.int32, (rank, rank), 0)
        == lax.broadcasted_iota(jnp.int32, (rank, rank), 1)
    )
    for i, f in enumerate(vector):
        levels = noise_s[:, at(f), :]
        for m in range(modes):
            column = jnp.sum(jnp.where(unit, levels[m:m + 1], 0.0), axis=1, keepdims=True)
            column_s[i, m] = jnp.broadcast_to(column, (rank, 128))

    def swapped(x):
        return jnp.concatenate([pltpu.roll(x[group(g)], 4, 0) for g in range(groups)], axis=0)

    def matrix_project(f, field):
        i = matrix.index(f)
        seen = times(field, high_s[i], low_s[i], True)
        parts = seen[:, :width] + sign * swapped(seen[:, width:])
        return parts, mask_s[i] * parts

    def matrix_back(f, seen):
        i = matrix.index(f)
        weighted = jnp.concatenate([seen[1], -sign * swapped(seen[1])], axis=1)
        return times(weighted, high_s[i], low_s[i], False)

    def wide(x):
        return jnp.concatenate([x] * (ell // 128), axis=1)

    def owned(f):
        return (lambda m, a: beam_s[f, m, a]), (lambda m: column_s[vector.index(f), m])

    lent = (lambda m, a: lent_beam_s[m, a]), (lambda m: lent_column_s[m])

    def group_project(source, g, field):
        beam_of, column_of = source
        parts = []
        for j in range(4):
            m = 4 * g + j
            real_beam, imaginary_beam = beam_of(m, 0), beam_of(m, 1)
            real_field, imaginary_field = field[j:j + 1], field[4 + j:5 + j]
            levels = column_of(m)
            real = jnp.sum(
                real_beam * real_field + imaginary_beam * imaginary_field, axis=1, keepdims=True
            )
            imaginary = jnp.sum(
                real_beam * imaginary_field - imaginary_beam * real_field, axis=1, keepdims=True
            )
            parts.append((real, imaginary, levels * real, levels * imaginary))
        return parts

    def group_back(source, g, parts):
        beam_of, _ = source
        reals, imaginaries = [], []
        for j, (_, _, real, imaginary) in enumerate(parts):
            m = 4 * g + j
            real, imaginary = wide(real), wide(imaginary)
            real_beam, imaginary_beam = beam_of(m, 0), beam_of(m, 1)
            for found, value in (
                (reals, real_beam * real - imaginary_beam * imaginary),
                (imaginaries, real_beam * imaginary + imaginary_beam * real),
            ):
                found.append(sum(value[k:k + 8] for k in range(0, rank, 8)))
        return folded(reals + imaginaries)

    def group_beam(source, g, field):
        return group_back(source, g, group_project(source, g, field))

    def project(f, ref):
        if f in matrix:
            return matrix_project(f, ref[f])
        return [group_project(owned(f), g, ref[f, group(g)]) for g in range(groups)]

    def back(f, seen):
        if f in matrix:
            return matrix_back(f, seen)
        return jnp.concatenate([group_back(owned(f), g, seen[g]) for g in range(groups)], axis=0)

    def apply_beam(fs, ref):
        fs = [f for f in fs if f in matrix] + [f for f in fs if f in vector]
        seen = [project(f, ref) for f in fs]
        return {f: back(f, found) for f, found in zip(fs, seen)}

    def count(f):
        value = float(f > 0) + float(f < last) + float(nf > 1 and f == 0)
        if two_sided and f == last:
            value = value + jnp.where(has_far, 1.0, 0.0)
        return value

    def local_prior(f, ref, rows=slice(None)):
        value = count(f) * ref[f, rows]
        if f > 0:
            value = value - ref[f - 1, rows]
        if f < last:
            value = value - ref[f + 1, rows]
        return power * ref[f, rows] + smooth * value

    for f in edges:
        beam_copies[f].wait()
    rhs_copy.wait()
    for i, f in enumerate(edges):
        for g in range(groups):
            rows = group(g)
            image = group_beam(owned(f), g, x_s[f, rows])
            y_s[i, rows] = rows_of(rhs_s, at(f))[rows] - image - local_prior(f, x_s, rows)
    first, rest = [], inner
    if paired:
        even_only([near_copy(1, g) for g in range(groups)] + [lend(k) for k in range(3)])
        first, rest = inner[:1], inner[1:]
    else:
        for g in range(groups):
            send(1, g)

    for f in first:
        beam_copies[f].wait()
        r_s[f] = rows_of(rhs_s, at(f)) - back(f, project(f, x_s)) - local_prior(f, x_s)
    if paired:
        even_only([lend(3)])

        @pl.when(helper)
        def _():
            for g in range(groups):
                near_copy(1, g).start()

    for f in rest:
        beam_copies[f].wait()
    for i, f in enumerate(matrix):
        for a in range(2):
            rows = slice(a * width, (a + 1) * width)
            high, low = split(beam_s[f, :, a].reshape(width, ell))
            high_s[i, rows] = high
            low_s[i, rows] = low
    for f, image in apply_beam(rest, x_s).items():
        r_s[f] = rows_of(rhs_s, at(f)) - image - local_prior(f, x_s)
    for f, image in apply_beam(inner, r_s).items():
        u_s[f] = image + local_prior(f, r_s) if f in apart else image
    advance()

    def complete(i, f, g):
        rows = group(g)
        halo = jnp.concatenate([first_s[i, 4 * g:4 * g + 4, b, :] for b in range(2)], axis=0)
        r_s[f, rows] = y_s[i, rows] + smooth * halo

    def edge_image(f, g):
        rows = group(g)
        return group_beam(owned(f), g, r_s[f, rows]) + local_prior(f, r_s, rows)

    if paired:
        @pl.when(helper)
        def _():
            for g in range(groups):
                arrive(0, g)
                complete(0, 0, g)
                ahead_s[group(g)] = edge_image(0, g)
                ahead_copy(g).start()
            for g in range(groups):
                first_copy(g).wait_recv()
                hand_copy(g).start()
                if g == 0:
                    for k in range(4):
                        lend(k).wait_recv()
                rows = group(g)
                halo = jnp.concatenate([lent_first_s[4 * g:4 * g + 4, b, :] for b in range(2)], axis=0)
                r = lent_y_s[rows] + smooth * halo
                local = power * r + smooth * (count(0) * r - lent_r_s[rows])
                lent_v_s[rows] = group_beam(lent, g, r) + local
                cross_copy(g).start()

    seen = {f: project(f, u_s) for f in apart}
    grouped = [f for f in beside_edge if f in vector]
    whole = [f for f in beside_edge if f in matrix]
    seen |= {f: [] for f in grouped + edges}
    zero = jnp.zeros((8, ell), F32)
    sums = [zero, zero, zero, zero]
    column_part = jnp.zeros((rank, 128), F32)

    def add_up(g, sums, column_part):
        rows = group(g)
        norm, curve, square, cube = sums
        for f in inner + edges:
            if f in vector:
                for real, imaginary, real_weighted, imaginary_weighted in seen[f][g]:
                    column_part = column_part + (real * real_weighted + imaginary * imaginary_weighted)
            r, u = r_s[f, rows], u_s[f, rows]
            w = local_prior(f, u_s, rows)
            w_s[f, rows] = w
            norm = norm + r * r
            curve = curve + r * u
            square = square + u * u
            cube = cube + u * w
        return [norm, curve, square, cube], column_part

    def finish_edges(g):
        rows = group(g)
        for i, f in enumerate(edges):
            u_s[f, rows] = v_s[i, rows] - beside(
                i, smooth * (halo_s[0, i, rows] + smooth * x_s[f, rows])
            )
            seen[f].append(group_project(owned(f), g, u_s[f, rows]))

    for g in range(groups):
        rows = group(g)
        if paired:
            pl.when(jnp.logical_not(helper))(lambda: arrive(0, g))
            arrive(1, g)
        else:
            arrive(0, g)
        for i, f in enumerate(edges):
            complete(i, f, g)
        for i, f in enumerate(edges):
            v_s[i, rows] = edge_image(f, g)
        if not paired:
            send(2, g)
        for f in grouped:
            u_s[f, rows] = u_s[f, rows] + local_prior(f, r_s, rows)
            seen[f].append(group_project(owned(f), g, u_s[f, rows]))
        if paired:
            finish_edges(g)
            pull_s[rows] = smooth * u_s[0, rows]
            if not whole:
                sums, column_part = add_up(g, sums, column_part)
    for f in whole:
        u_s[f] = u_s[f] + local_prior(f, r_s)
        seen[f] = project(f, u_s)
    if paired:
        even_only([pull_copy()])
    else:
        for g in range(groups):
            arrive(1, g)
            finish_edges(g)
    if whole or not paired:
        for g in range(groups):
            sums, column_part = add_up(g, sums, column_part)
    beam_part = jnp.zeros((2 * modes, width), F32)
    for f in matrix:
        beam_part = beam_part + seen[f][0] * seen[f][1]
    lane = lax.broadcasted_iota(jnp.int32, (1, 128), 1)
    message = jnp.zeros((1, 128), F32)
    for i, part in enumerate(sums):
        total = total_of(part)
        if i == 3:
            total = total + total_of(beam_part) + jnp.sum(column_part, axis=0, keepdims=True)
        message = jnp.where(lane == i, total, message)
    if paired:
        message = jnp.where(lane == 4 + my_f, total_of(smooth * r_s[0] * pull_s[...]), message)
    message_s[0] = message
    early_s[me] = message

    while steps:
        advance()

    def share(source, target, slot, turn, device):
        pltpu.make_async_remote_copy(
            src_ref=message_s.at[source], dst_ref=target.at[slot],
            send_sem=sum_send.at[turn], recv_sem=sum_recv.at[turn],
            device_id=device, device_id_type=MESH,
        ).start()

    def share_all(source, target, slot, turn, stride):
        if n > 64:
            def body(i, carry):
                ma, f = my_ma + i * stride // nf, my_f + i * stride % nf
                share(source, target, slot, turn, (lax.rem(ma, nma), lax.rem(f, nf)))
                return carry

            lax.fori_loop(1, n // stride, body, 0)
        else:
            for mask in sorted(range(stride, n, stride), key=lambda m: (-(m // nf // 2), m)):
                device = partner([bit for bit in range(bits) if mask >> bit & 1])
                share(source, target, slot, turn, device)

    def landed(target, sem, rows):
        if rows:
            rows = target.at[pl.ds(0, rows)]
            pltpu.make_async_copy(rows, rows, sem).wait()

    def lanes_of(x):
        x = jnp.sum(x, axis=0, keepdims=True)
        return sum(x[:, i:i + 128] for i in range(0, ell, 128))

    share_all(0, early_s, me, 0, 1)
    if paired:
        even_only([near_copy(2, g) for g in range(groups)])
    for f in matrix + vector:
        w_s[f] = w_s[f] + back(f, seen[f])

    late_rows = late_s.shape[0]
    if paired:
        @pl.when(helper)
        def _():
            cross = jnp.zeros((8, ell), F32)
            for g in range(groups):
                arrive(2, g)
                cross = cross + pull_s[group(g)] * halo_s[1, 0, group(g)]
            pull_copy().wait_recv()
            for g in range(groups):
                cross_copy(g).wait_recv()
                cross = cross + partner_s[group(g)] * cross_s[group(g)]
            message = lanes_of(cross)
            late_s[my_ma // 2] = message
            message_s[1] = message
            share_all(1, late_s, my_ma // 2, 1, nf)
            for g in range(groups):
                cross_copy(g).wait_send()

        @pl.when(jnp.logical_not(helper))
        def _():
            for g in range(groups):
                arrive(2, g)
            pull_copy().wait_send()
            for k in range(4):
                lend(k).wait_send()
            for g in range(groups):
                first_copy(g).wait_send()

        w_s[0] = w_s[0] - smooth * (halo_s[1, 0] - smooth * r_s[0])
    else:
        cross = jnp.zeros((8, ell), F32)
        nexts = []
        for g in range(groups):
            arrive(2, g)
            rows = group(g)
            for i, f in enumerate(edges):
                pull = beside(i, smooth * (halo_s[1, i, rows] - smooth * r_s[f, rows]))
                nexts.append((f, rows, pull))
                cross = cross + pull * u_s[f, rows]
        message = lanes_of(cross)
        late_s[me] = message
        message_s[1] = message
        share_all(1, late_s, me, 1, 1)
        for f, rows, pull in nexts:
            w_s[f, rows] = w_s[f, rows] - pull

    if paired:
        for g in range(groups):
            for kind in (1, 2):
                sent(kind, g)

        @pl.when(helper)
        def _():
            for g in range(groups):
                sent(0, g)
                hand_copy(g).wait_send()
    else:
        for kind in range(3):
            for g in range(groups):
                sent(kind, g)
    for source, target in ((r_s, r_out_s), (u_s, u_out_s), (w_s, w_out_s)):
        for f in range(freqs):
            value = source[f]
            for g in range(groups):
                for b in range(2):
                    start = 8 * g + 4 * b
                    target[4 * g:4 * g + 4, at(f), b, :] = value[start:start + 4]

    landed(early_s, sum_send.at[0], n - 1)
    landed(early_s, sum_recv.at[0], n - 1)
    if paired:
        @pl.when(helper)
        def _():
            rows = early_s.at[pl.ds(0, nma - 1)]
            pltpu.make_async_copy(rows, rows, sum_send.at[1]).wait()
            landed(late_s, sum_recv.at[1], late_rows - 1)

        pl.when(jnp.logical_not(helper))(lambda: landed(late_s, sum_recv.at[1], late_rows))
    else:
        landed(late_s, sum_send.at[1], late_rows - 1)
        landed(late_s, sum_recv.at[1], late_rows - 1)
    total = jnp.sum(early_s[...], axis=0)
    m0, m1, m2, m3, known = (
        jnp.sum(jnp.where(lane == i, total, 0.0), axis=1, keepdims=True)
        for i in (0, 1, 2, 3, 4 + my_f)
    )
    crossed = jnp.sum(jnp.sum(late_s[...], axis=0), axis=1, keepdims=True)
    m3 = m3 - 2.0 * (crossed - known) if paired else m3 - crossed
    inverse = 1.0 / m1
    step = m0 * inverse
    drop = step * m2 - m1
    growth = drop * inverse
    curve_next = m1 - 2.0 * step * m2 + step * step * m3
    step_next = step * drop / (curve_next - growth * drop)
    c = step + step_next * (1.0 + growth)
    e = step * step_next
    r, u = r_out_s[...], u_out_s[...]
    sol_s[...] = x0_s[...] + c * r - e * u
    res_s[...] = r - c * u + e * w_out_s[...]


def scoped_kernel(nma, nf, sides, *refs):
    modes, freqs = refs[0].shape[:2]
    dma = pltpu.SemaphoreType.DMA
    pl.run_scoped(
        functools.partial(kernel, nma, nf, *refs),
        dma((7,)), dma((freqs,)), dma((3, modes // 4, sides)), dma((2 * (modes // 4) + 5,)),
        dma((modes // 4,)), dma((2,)),
    )


def write_out(sol_in, res_in, sol_out, res_out, sem):
    copies = [
        pltpu.make_async_copy(sol_in, sol_out, sem.at[0]),
        pltpu.make_async_copy(res_in, res_out, sem.at[1]),
    ]
    for copy in copies:
        copy.start()
    for copy in copies:
        copy.wait()


def shards(right_side, start_field, beam, noise, inv_power, smooth):
    nma, nf = lax.axis_size("ma"), lax.axis_size("freq")
    modes, freqs, _, ell = right_side.shape
    rank = beam.shape[3]
    width = modes * rank
    sides = 2 if nf > 2 else 1
    vmem_spec = pl.BlockSpec(memory_space=pltpu.VMEM)
    any_spec = pl.BlockSpec(memory_space=pl.ANY)
    field = pltpu.VMEM(right_side.shape, F32)
    edge = pltpu.VMEM((sides, modes, 2, ell), F32)
    slab = pltpu.VMEM((freqs, 2 * modes, ell), F32)
    edge_field = pltpu.VMEM((2 * modes, ell), F32)
    edge_slab = pltpu.VMEM((sides, 2 * modes, ell), F32)
    vector = max(min(nf - 1, 2), freqs // 2)
    matrix = max(freqs - vector, 1)
    half = pltpu.VMEM((matrix, 2 * width, ell), BF16)
    outs = pl.pallas_call(
        functools.partial(scoped_kernel, nma, nf, sides),
        out_shape=[field] * 2,
        in_specs=[any_spec] * 6,
        out_specs=[vmem_spec] * 2,
        scratch_shapes=[
            field, field, edge,
            pltpu.VMEM((freqs, modes, 2, rank, ell), F32),
            pltpu.VMEM(noise.shape, F32),
            pltpu.VMEM((1, ell), F32), pltpu.VMEM((1, ell), F32),
            half, half,
            slab, edge_slab, slab, edge_slab, slab, slab,
            pltpu.VMEM((matrix, 2 * modes, width), F32),
            pltpu.VMEM((vector, modes, rank, 128), F32),
            edge,
            pltpu.VMEM((2, sides, 2 * modes, ell), F32),
            field, field, field,
            edge_field, edge_field, edge_field,
            pltpu.VMEM((modes, 2, rank, ell), F32), pltpu.VMEM((modes, rank, 128), F32),
            edge_field, edge_field, pltpu.VMEM((modes, 2, ell), F32), edge_field, edge_field,
            pltpu.VMEM((2, 1, 128), F32),
            pltpu.VMEM((nma * nf, 1, 128), F32),
            pltpu.VMEM((nma // 2 if nf == 2 and nma % 2 == 0 and freqs > 1 else nma * nf, 1, 128), F32),
            pltpu.SemaphoreType.DMA((3, modes // 4, sides)),
            pltpu.SemaphoreType.DMA((2 * (modes // 4) + 5,)),
            pltpu.SemaphoreType.DMA((2,)),
            pltpu.SemaphoreType.REGULAR((max((nma * nf).bit_length() - 4, 1),)),
        ],
        compiler_params=pltpu.CompilerParams(
            collective_id=0, has_side_effects=True, vmem_limit_bytes=67043328 - 2 * right_side.size * 4
        ),
        name="solve",
    )(right_side, start_field, beam, noise, inv_power[None], smooth[None])
    return pl.pallas_call(
        write_out,
        out_shape=[jax.ShapeDtypeStruct(right_side.shape, F32)] * 2,
        in_specs=[vmem_spec] * 2,
        out_specs=[any_spec] * 2,
        scratch_shapes=[pltpu.SemaphoreType.DMA((2,))],
        compiler_params=pltpu.CompilerParams(vmem_limit_bytes=1024 * 1024),
        name="write_out",
    )(*outs)


def solution(mesh):
    in_specs = (
        P("ma", "freq", None, None),
        P("ma", "freq", None, None),
        P("ma", "freq", None, None, None),
        P("ma", "freq", None),
        P(),
        P(),
    )
    out_specs = (P("ma", "freq", None, None), P("ma", "freq", None, None))
    return jax.shard_map(shards, mesh=mesh, in_specs=in_specs, out_specs=out_specs, check_vma=False)
```

```python
import functools

import jax
import jax.numpy as jnp
from jax import lax
from jax.experimental import pallas as pl
from jax.experimental.pallas import tpu as pltpu
from jax.sharding import PartitionSpec as P

MESH = pl.DeviceIdType.MESH
F32, BF16 = jnp.float32, jnp.bfloat16


def split(x):
    high = x.astype(BF16)
    return high, (x - high.astype(F32)).astype(BF16)


def times(x, high, low, transposed):
    dims = (((1,), (1 if transposed else 0,)), ((), ()))
    rows = x.shape[0]
    x_high, x_low = split(x)
    both = jnp.concatenate([x_high, x_low], axis=0)
    main = lax.dot_general(both, high, dims, preferred_element_type=F32)
    rest = lax.dot_general(x_high, low, dims, preferred_element_type=F32)
    return main[:rows] + (main[rows:] + rest)


def folded(parts):
    row = lax.broadcasted_iota(jnp.int32, parts[0].shape, 0)
    upper = row < 4
    fours = [
        jnp.where(upper, parts[s], parts[s + 4])
        + pltpu.roll(jnp.where(upper, parts[s + 4], parts[s]), 4, 0)
        for s in range(4)
    ]
    even = row // 2 % 2 == 0
    twos = [
        jnp.where(
            even, fours[s] + pltpu.roll(fours[s], 6, 0), fours[s + 2] + pltpu.roll(fours[s + 2], 2, 0)
        )
        for s in range(2)
    ]
    return jnp.where(
        row % 2 == 0, twos[0] + pltpu.roll(twos[0], 7, 0), twos[1] + pltpu.roll(twos[1], 1, 0)
    )


def tree(parts):
    while len(parts) > 1:
        half = len(parts) // 2
        parts = [parts[k] + parts[half + k] for k in range(half)] + parts[2 * half:]
    return parts[0]


def total_of(x):
    return jnp.sum(jnp.sum(x, axis=0, keepdims=True), axis=1, keepdims=True)


def kernel(
    nma, nf, rhs_in, x0_in, beam_in, noise_in, power_in, smooth_in, sol_s, res_s,
    rhs_s, x0_s, edge_s, beam_s, noise_s, power_s, smooth_s,
    high_s, low_s, x_s, y_s, r_s, v_s, u_s, w_s, mask_s, column_s, first_s, halo_s,
    r_out_s, u_out_s, w_out_s, pull_s, partner_s, cross_s,
    lent_beam_s, lent_column_s, lent_y_s, lent_r_s, lent_first_s, lent_v_s, ahead_s,
    message_s, early_s, late_s,
    halo_recv, pair_recv, sum_recv, word_sem, in_sem, beam_sem, halo_send, pair_send, hand_send, sum_send,
):
    modes, freqs, _, ell = rhs_in.shape
    rank = beam_in.shape[3]
    width = modes * rank
    n = nma * nf
    my_ma, my_f = lax.axis_index("ma"), lax.axis_index("freq")
    me = my_ma * nf + my_f
    last = freqs - 1
    two_sided = nf > 2
    paired = nf == 2 and nma % 2 == 0 and freqs > 1
    helper = my_ma % 2 == 1
    groups = modes // 4
    edges = [0, last][:min(nf - 1, 2)]
    inner = [f for f in range(freqs) if f not in edges]
    beside_edge = [f for f in inner if f - 1 in edges or f + 1 in edges]
    apart = [f for f in inner if f not in beside_edge]
    vector = edges + inner[:max(freqs // 2 - len(edges), 0)]
    matrix = [f for f in range(freqs) if f not in vector]

    def at(g):
        return jnp.where(my_f == 0, last - g, g)

    edge_copies = [
        pltpu.make_async_copy(x0_in.at[:, at(f)], edge_s.at[i], in_sem.at[i])
        for i, f in enumerate(edges)
    ]
    x0_copy = pltpu.make_async_copy(x0_in, x0_s, in_sem.at[2])
    rhs_copy = pltpu.make_async_copy(rhs_in, rhs_s, in_sem.at[3])
    small = [
        pltpu.make_async_copy(power_in, power_s, in_sem.at[4]),
        pltpu.make_async_copy(smooth_in, smooth_s, in_sem.at[5]),
        pltpu.make_async_copy(noise_in, noise_s, in_sem.at[6]),
    ]
    beam_copies = [
        pltpu.make_async_copy(beam_in.at[:, at(f)], beam_s.at[f], beam_sem.at[f])
        for f in range(freqs)
    ]
    for copy in edge_copies:
        copy.start()

    def flip(bit):
        if bit == 0 and nf == 2:
            return 1 - 2 * my_f
        d = 1 << (bit if bit < freq_bits else bit - freq_bits)
        place = my_f if bit < freq_bits else my_ma
        return d * (1 - 2 * (place // d % 2))

    def partner(bits):
        return (
            my_ma + sum(flip(bit) for bit in bits if bit >= freq_bits),
            my_f + sum(flip(bit) for bit in bits if bit < freq_bits),
        )

    freq_bits = nf.bit_length() - 1
    bits = freq_bits + nma.bit_length() - 1
    close = min(bits, 3)
    greeted = [
        partner([bit for bit in range(close) if mask >> bit & 1]) for mask in range(1, 1 << close)
    ]
    word = [partner([bit]) for bit in range(close, bits)]
    greeted += word
    words = len(word)
    barrier = pltpu.get_barrier_semaphore()
    near = jnp.where(my_f == 0, 1, my_f - 1)
    has_far = (my_f > 0) & (my_f < nf - 1)

    def greet(device):
        pl.semaphore_signal(barrier, inc=1, device_id=device, device_id_type=MESH)

    for i, device in enumerate(greeted):
        greet(device)
        if i == 0:
            for copy in [beam_copies[f] for f in edges] + [x0_copy, rhs_copy] + small:
                copy.start()
    expected = len(greeted)
    if nf > 2:
        pl.when(my_f > 0)(lambda: greet((my_ma, my_f - 1)))
        pl.when(my_f < nf - 1)(lambda: greet((my_ma, my_f + 1)))
        expected = expected + jnp.minimum(my_f, 1) + jnp.minimum(nf - 1 - my_f, 1)

    steps = list(range(words + 1))

    def advance():
        if steps:
            step = steps.pop(0)
            if step > 0:
                pl.semaphore_wait(word_sem.at[step - 1], 1)
            if step < words:
                pl.semaphore_signal(
                    word_sem.at[step], inc=1, device_id=word[step], device_id_type=MESH
                )

    def piece(kind, g):
        if kind == 0:
            rows = pl.ds(4 * g, 4)
            return (lambda i: edge_s.at[i, rows]), (lambda i: first_s.at[i, rows])
        source = (y_s, v_s)[kind - 1]
        rows = pl.ds(8 * g, 8)
        return (lambda i: source.at[i, rows]), (lambda i: halo_s.at[kind - 1, i, rows])

    def near_copy(kind, g):
        source, target = piece(kind, g)
        side = jnp.minimum(my_f // 2, 1) if two_sided else 0
        return pltpu.make_async_remote_copy(
            src_ref=source(0), dst_ref=target(side),
            send_sem=halo_send.at[kind, g, 0], recv_sem=halo_recv.at[kind, g, side],
            device_id=(my_ma, near), device_id_type=MESH,
        )

    def far_copy(kind, g):
        source, target = piece(kind, g)
        return pltpu.make_async_remote_copy(
            src_ref=source(1), dst_ref=target(0),
            send_sem=halo_send.at[kind, g, 1], recv_sem=halo_recv.at[kind, g, 0],
            device_id=(my_ma, my_f + 1), device_id_type=MESH,
        )

    def arrival(kind, g, side):
        slot = piece(kind, g)[1](side)
        return pltpu.make_async_copy(slot, slot, halo_recv.at[kind, g, side])

    def send(kind, g):
        if nf > 1:
            near_copy(kind, g).start()
        if two_sided:
            pl.when(has_far)(lambda: far_copy(kind, g).start())

    def arrive(kind, g):
        if nf > 1:
            arrival(kind, g, 0).wait()
        if two_sided:
            pl.when(has_far)(lambda: arrival(kind, g, 1).wait())

    def sent(kind, g):
        if nf > 1:
            near_copy(kind, g).wait_send()
        if two_sided:
            pl.when(has_far)(lambda: far_copy(kind, g).wait_send())

    def pair_copy(k, source, target, ma, f):
        return pltpu.make_async_remote_copy(
            src_ref=source, dst_ref=target, send_sem=pair_send.at[k], recv_sem=pair_recv.at[k],
            device_id=(ma, f), device_id_type=MESH,
        )

    def lend(k):
        source = (lambda: beam_s.at[0], lambda: column_s.at[0], lambda: y_s.at[0], lambda: r_s.at[1])[k]
        target = (lent_beam_s, lent_column_s, lent_y_s, lent_r_s)[k]
        return pair_copy(k, source(), target, my_ma + 1, my_f)

    def pull_copy():
        return pair_copy(4, pull_s, partner_s, my_ma + 1, my_f)

    def first_copy(g):
        rows = pl.ds(4 * g, 4)
        return pair_copy(5 + g, edge_s.at[0, rows], lent_first_s.at[rows], my_ma + 1, 1 - my_f)

    def cross_copy(g):
        rows = pl.ds(8 * g, 8)
        return pair_copy(5 + groups + g, lent_v_s.at[rows], cross_s.at[rows], my_ma, 1 - my_f)

    def ahead_copy(g):
        rows = pl.ds(8 * g, 8)
        return pltpu.make_async_remote_copy(
            src_ref=ahead_s.at[rows], dst_ref=halo_s.at[1, 0, rows],
            send_sem=halo_send.at[2, g, 0], recv_sem=halo_recv.at[2, g, 0],
            device_id=(my_ma, 1 - my_f), device_id_type=MESH,
        )

    def hand_copy(g):
        rows = pl.ds(4 * g, 4)
        return pltpu.make_async_remote_copy(
            src_ref=lent_first_s.at[rows], dst_ref=first_s.at[0, rows],
            send_sem=hand_send.at[g], recv_sem=halo_recv.at[0, g, 0],
            device_id=(my_ma - 1, my_f), device_id_type=MESH,
        )

    def even_only(copies):
        @pl.when(jnp.logical_not(helper))
        def _():
            for copy in copies:
                copy.start()

    def beside(i, value):
        return jnp.where(has_far, value, 0.0) if i else value

    if two_sided:
        @pl.when(jnp.logical_not(has_far))
        def _():
            first_s[1] = jnp.zeros_like(first_s[1])
            halo_s[:, 1] = jnp.zeros_like(halo_s[:, 1])

    for copy in edge_copies:
        copy.wait()
    for f in inner:
        beam_copies[f].start()
    pl.semaphore_wait(barrier, expected)
    if paired:
        even_only([first_copy(g) for g in range(groups)])

        @pl.when(helper)
        def _():
            for g in range(groups):
                near_copy(0, g).start()
    else:
        for g in range(groups):
            send(0, g)
    advance()

    x0_copy.wait()
    for copy in small:
        copy.wait()
    def rows_of(ref, *at_f):
        place = (slice(None), *at_f)
        return jnp.concatenate(
            [ref[(slice(4 * g, 4 * g + 4), *place[1:], b)] for g in range(groups) for b in range(2)],
            axis=0,
        )

    def group(g):
        return slice(8 * g, 8 * g + 8)

    for f in range(freqs):
        x_s[f] = rows_of(x0_s, at(f))
    power, smooth = power_s[...], smooth_s[...]
    row = lax.broadcasted_iota(jnp.int32, (2 * modes, width), 0)
    own = lax.broadcasted_iota(jnp.int32, (2 * modes, width), 1) // rank == row // 8 * 4 + row % 4
    sign = jnp.where(row % 8 < 4, 1.0, -1.0)
    for i, f in enumerate(matrix):
        levels = noise_s[:, at(f), :]
        levels = jnp.concatenate(
            [levels[4 * g:4 * g + 4] for g in range(groups) for _ in range(2)], axis=0
        )
        mask_s[i] = jnp.where(own, jnp.concatenate([levels] * modes, axis=1), 0.0)
    unit = (
        lax.broadcasted_iota(jnp.int32, (rank, rank), 0)
        == lax.broadcasted_iota(jnp.int32, (rank, rank), 1)
    )
    for i, f in enumerate(vector):
        levels = noise_s[:, at(f), :]
        for m in range(modes):
            column = jnp.sum(jnp.where(unit, levels[m:m + 1], 0.0), axis=1, keepdims=True)
            column_s[i, m] = jnp.broadcast_to(column, (rank, 128))

    def swapped(x):
        return jnp.concatenate([pltpu.roll(x[group(g)], 4, 0) for g in range(groups)], axis=0)

    def matrix_project(f, field):
        i = matrix.index(f)
        seen = times(field, high_s[i], low_s[i], True)
        parts = seen[:, :width] + sign * swapped(seen[:, width:])
        return parts, mask_s[i] * parts

    def matrix_back(f, seen):
        i = matrix.index(f)
        weighted = jnp.concatenate([seen[1], -sign * swapped(seen[1])], axis=1)
        return times(weighted, high_s[i], low_s[i], False)

    def wide(x):
        return jnp.concatenate([x] * (ell // 128), axis=1)

    def owned(f):
        return (lambda m, a: beam_s[f, m, a]), (lambda m: column_s[vector.index(f), m])

    lent = (lambda m, a: lent_beam_s[m, a]), (lambda m: lent_column_s[m])

    def group_project(source, g, field):
        beam_of, column_of = source
        parts = []
        for j in range(4):
            m = 4 * g + j
            real_beam, imaginary_beam = beam_of(m, 0), beam_of(m, 1)
            real_field, imaginary_field = field[j:j + 1], field[4 + j:5 + j]
            levels = column_of(m)
            real = jnp.sum(
                real_beam * real_field + imaginary_beam * imaginary_field, axis=1, keepdims=True
            )
            imaginary = jnp.sum(
                real_beam * imaginary_field - imaginary_beam * real_field, axis=1, keepdims=True
            )
            parts.append((real, imaginary, levels * real, levels * imaginary))
        return parts

    def group_back(source, g, parts):
        beam_of, _ = source
        reals, imaginaries = [], []
        for j, (_, _, real, imaginary) in enumerate(parts):
            m = 4 * g + j
            real, imaginary = wide(real), wide(imaginary)
            real_beam, imaginary_beam = beam_of(m, 0), beam_of(m, 1)
            for found, value in (
                (reals, real_beam * real - imaginary_beam * imaginary),
                (imaginaries, real_beam * imaginary + imaginary_beam * real),
            ):
                found.append(sum(value[k:k + 8] for k in range(0, rank, 8)))
        return folded(reals + imaginaries)

    def group_beam(source, g, field):
        return group_back(source, g, group_project(source, g, field))

    def project(f, ref):
        if f in matrix:
            return matrix_project(f, ref[f])
        return [group_project(owned(f), g, ref[f, group(g)]) for g in range(groups)]

    def back(f, seen):
        if f in matrix:
            return matrix_back(f, seen)
        return jnp.concatenate([group_back(owned(f), g, seen[g]) for g in range(groups)], axis=0)

    def apply_beam(fs, ref):
        fs = [f for f in fs if f in matrix] + [f for f in fs if f in vector]
        seen = [project(f, ref) for f in fs]
        return {f: back(f, found) for f, found in zip(fs, seen)}

    def count(f):
        value = float(f > 0) + float(f < last) + float(nf > 1 and f == 0)
        if two_sided and f == last:
            value = value + jnp.where(has_far, 1.0, 0.0)
        return value

    def local_prior(f, ref, rows=slice(None)):
        value = count(f) * ref[f, rows]
        if f > 0:
            value = value - ref[f - 1, rows]
        if f < last:
            value = value - ref[f + 1, rows]
        return power * ref[f, rows] + smooth * value

    for f in edges:
        beam_copies[f].wait()
    rhs_copy.wait()
    for i, f in enumerate(edges):
        for g in range(groups):
            rows = group(g)
            image = group_beam(owned(f), g, x_s[f, rows])
            y_s[i, rows] = rows_of(rhs_s, at(f))[rows] - image - local_prior(f, x_s, rows)
    first, rest = [], inner
    if paired:
        even_only([near_copy(1, g) for g in range(groups)] + [lend(k) for k in range(3)])
        first, rest = inner[:1], inner[1:]
    else:
        for g in range(groups):
            send(1, g)

    for f in first:
        beam_copies[f].wait()
        r_s[f] = rows_of(rhs_s, at(f)) - back(f, project(f, x_s)) - local_prior(f, x_s)
    if paired:
        even_only([lend(3)])

        @pl.when(helper)
        def _():
            for g in range(groups):
                near_copy(1, g).start()

    for f in rest:
        beam_copies[f].wait()
    for i, f in enumerate(matrix):
        for a in range(2):
            rows = slice(a * width, (a + 1) * width)
            high, low = split(beam_s[f, :, a].reshape(width, ell))
            high_s[i, rows] = high
            low_s[i, rows] = low
    for f, image in apply_beam(rest, x_s).items():
        r_s[f] = rows_of(rhs_s, at(f)) - image - local_prior(f, x_s)
    for f, image in apply_beam(inner, r_s).items():
        u_s[f] = image + local_prior(f, r_s) if f in apart else image
    advance()

    def complete(i, f, g):
        rows = group(g)
        halo = jnp.concatenate([first_s[i, 4 * g:4 * g + 4, b, :] for b in range(2)], axis=0)
        r_s[f, rows] = y_s[i, rows] + smooth * halo

    def edge_image(f, g):
        rows = group(g)
        return group_beam(owned(f), g, r_s[f, rows]) + local_prior(f, r_s, rows)

    if paired:
        @pl.when(helper)
        def _():
            for g in range(groups):
                arrive(0, g)
                complete(0, 0, g)
                ahead_s[group(g)] = edge_image(0, g)
                ahead_copy(g).start()
            for g in range(groups):
                first_copy(g).wait_recv()
                hand_copy(g).start()
                if g == 0:
                    for k in range(4):
                        lend(k).wait_recv()
                rows = group(g)
                halo = jnp.concatenate([lent_first_s[4 * g:4 * g + 4, b, :] for b in range(2)], axis=0)
                r = lent_y_s[rows] + smooth * halo
                local = power * r + smooth * (count(0) * r - lent_r_s[rows])
                lent_v_s[rows] = group_beam(lent, g, r) + local
                cross_copy(g).start()

    seen = {f: project(f, u_s) for f in apart}
    grouped = [f for f in beside_edge if f in vector]
    whole = [f for f in beside_edge if f in matrix]
    seen |= {f: [] for f in grouped + edges}
    zero = jnp.zeros((8, ell), F32)
    sums = [zero, zero, zero, zero]
    column_part = jnp.zeros((rank, 128), F32)

    def add_up(g, sums, column_part):
        rows = group(g)
        norm, curve, square, cube = sums
        for f in inner + edges:
            if f in vector:
                for real, imaginary, real_weighted, imaginary_weighted in seen[f][g]:
                    column_part = column_part + (real * real_weighted + imaginary * imaginary_weighted)
            r, u = r_s[f, rows], u_s[f, rows]
            w = local_prior(f, u_s, rows)
            w_s[f, rows] = w
            norm = norm + r * r
            curve = curve + r * u
            square = square + u * u
            cube = cube + u * w
        return [norm, curve, square, cube], column_part

    def finish_edges(g):
        rows = group(g)
        for i, f in enumerate(edges):
            u_s[f, rows] = v_s[i, rows] - beside(
                i, smooth * (halo_s[0, i, rows] + smooth * x_s[f, rows])
            )
            seen[f].append(group_project(owned(f), g, u_s[f, rows]))

    for g in range(groups):
        rows = group(g)
        if paired:
            pl.when(jnp.logical_not(helper))(lambda: arrive(0, g))
            arrive(1, g)
        else:
            arrive(0, g)
        for i, f in enumerate(edges):
            complete(i, f, g)
        for i, f in enumerate(edges):
            v_s[i, rows] = edge_image(f, g)
        if not paired:
            send(2, g)
        for f in grouped:
            u_s[f, rows] = u_s[f, rows] + local_prior(f, r_s, rows)
            seen[f].append(group_project(owned(f), g, u_s[f, rows]))
        if paired:
            finish_edges(g)
            pull_s[rows] = smooth * u_s[0, rows]
            if not whole:
                sums, column_part = add_up(g, sums, column_part)
    for f in whole:
        u_s[f] = u_s[f] + local_prior(f, r_s)
        seen[f] = project(f, u_s)
    if paired:
        even_only([pull_copy()])
    else:
        for g in range(groups):
            arrive(1, g)
            finish_edges(g)
    if whole or not paired:
        for g in range(groups):
            sums, column_part = add_up(g, sums, column_part)
    beam_part = jnp.zeros((2 * modes, width), F32)
    for f in matrix:
        beam_part = beam_part + seen[f][0] * seen[f][1]
    lane = lax.broadcasted_iota(jnp.int32, (1, 128), 1)
    message = jnp.zeros((1, 128), F32)
    for i, part in enumerate(sums):
        total = total_of(part)
        if i == 3:
            total = total + total_of(beam_part) + jnp.sum(column_part, axis=0, keepdims=True)
        message = jnp.where(lane == i, total, message)
    if paired:
        message = jnp.where(lane == 4 + my_f, total_of(smooth * r_s[0] * pull_s[...]), message)
    message_s[0] = message
    early_s[me] = message

    while steps:
        advance()

    def share(source, target, slot, turn, device):
        pltpu.make_async_remote_copy(
            src_ref=message_s.at[source], dst_ref=target.at[slot],
            send_sem=sum_send.at[turn], recv_sem=sum_recv.at[turn],
            device_id=device, device_id_type=MESH,
        ).start()

    def share_all(source, target, slot, turn, stride):
        if n > 64:
            def body(i, carry):
                ma, f = my_ma + i * stride // nf, my_f + i * stride % nf
                share(source, target, slot, turn, (lax.rem(ma, nma), lax.rem(f, nf)))
                return carry

            lax.fori_loop(1, n // stride, body, 0)
        else:
            for mask in sorted(range(stride, n, stride), key=lambda m: (-(m // nf // 2), m)):
                device = partner([bit for bit in range(bits) if mask >> bit & 1])
                share(source, target, slot, turn, device)

    def landed(target, sem, rows):
        if rows:
            rows = target.at[pl.ds(0, rows)]
            pltpu.make_async_copy(rows, rows, sem).wait()

    def lanes_of(x):
        x = jnp.sum(x, axis=0, keepdims=True)
        return sum(x[:, i:i + 128] for i in range(0, ell, 128))

    share_all(0, early_s, me, 0, 1)
    if paired:
        even_only([near_copy(2, g) for g in range(groups)])
    for f in matrix + vector:
        w_s[f] = w_s[f] + back(f, seen[f])

    late_rows = late_s.shape[0]
    if paired:
        @pl.when(helper)
        def _():
            cross = jnp.zeros((8, ell), F32)
            for g in range(groups):
                arrive(2, g)
                cross = cross + pull_s[group(g)] * halo_s[1, 0, group(g)]
            pull_copy().wait_recv()
            for g in range(groups):
                cross_copy(g).wait_recv()
                cross = cross + partner_s[group(g)] * cross_s[group(g)]
            message = lanes_of(cross)
            late_s[my_ma // 2] = message
            message_s[1] = message
            share_all(1, late_s, my_ma // 2, 1, nf)
            for g in range(groups):
                cross_copy(g).wait_send()

        @pl.when(jnp.logical_not(helper))
        def _():
            for g in range(groups):
                arrive(2, g)
            pull_copy().wait_send()
            for k in range(4):
                lend(k).wait_send()
            for g in range(groups):
                first_copy(g).wait_send()

        w_s[0] = w_s[0] - smooth * (halo_s[1, 0] - smooth * r_s[0])
    else:
        cross = jnp.zeros((8, ell), F32)
        nexts = []
        for g in range(groups):
            arrive(2, g)
            rows = group(g)
            for i, f in enumerate(edges):
                pull = beside(i, smooth * (halo_s[1, i, rows] - smooth * r_s[f, rows]))
                nexts.append((f, rows, pull))
                cross = cross + pull * u_s[f, rows]
        message = lanes_of(cross)
        late_s[me] = message
        message_s[1] = message
        share_all(1, late_s, me, 1, 1)
        for f, rows, pull in nexts:
            w_s[f, rows] = w_s[f, rows] - pull

    if paired:
        for g in range(groups):
            for kind in (1, 2):
                sent(kind, g)

        @pl.when(helper)
        def _():
            for g in range(groups):
                sent(0, g)
                hand_copy(g).wait_send()
    else:
        for kind in range(3):
            for g in range(groups):
                sent(kind, g)
    for source, target in ((r_s, r_out_s), (u_s, u_out_s), (w_s, w_out_s)):
        for f in range(freqs):
            value = source[f]
            for g in range(groups):
                for b in range(2):
                    start = 8 * g + 4 * b
                    target[4 * g:4 * g + 4, at(f), b, :] = value[start:start + 4]

    landed(early_s, sum_send.at[0], n - 1)
    landed(early_s, sum_recv.at[0], n - 1)
    if paired:
        @pl.when(helper)
        def _():
            rows = early_s.at[pl.ds(0, nma - 1)]
            pltpu.make_async_copy(rows, rows, sum_send.at[1]).wait()
            landed(late_s, sum_recv.at[1], late_rows - 1)

        pl.when(jnp.logical_not(helper))(lambda: landed(late_s, sum_recv.at[1], late_rows))
    else:
        landed(late_s, sum_send.at[1], late_rows - 1)
        landed(late_s, sum_recv.at[1], late_rows - 1)
    def rows_total(ref):
        if ref.shape[0] > 64:
            return jnp.sum(ref[...], axis=0)
        return tree([ref[k] for k in range(ref.shape[0])])

    total = rows_total(early_s)
    m0, m1, m2, m3, known = (
        jnp.sum(jnp.where(lane == i, total, 0.0), axis=1, keepdims=True)
        for i in (0, 1, 2, 3, 4 + my_f)
    )
    crossed = jnp.sum(rows_total(late_s), axis=1, keepdims=True)
    m3 = m3 - 2.0 * (crossed - known) if paired else m3 - crossed
    inverse = 1.0 / m1
    step = m0 * inverse
    drop = step * m2 - m1
    growth = drop * inverse
    curve_next = m1 - 2.0 * step * m2 + step * step * m3
    step_next = step * drop / (curve_next - growth * drop)
    c = step + step_next * (1.0 + growth)
    e = step * step_next
    for m in range(modes):
        r, u = r_out_s[m], u_out_s[m]
        sol_s[m] = x0_s[m] + c * r - e * u
        res_s[m] = r - c * u + e * w_out_s[m]


def scoped_kernel(nma, nf, sides, *refs):
    modes, freqs = refs[0].shape[:2]
    dma = pltpu.SemaphoreType.DMA
    pl.run_scoped(
        functools.partial(kernel, nma, nf, *refs),
        dma((7,)), dma((freqs,)), dma((3, modes // 4, sides)), dma((2 * (modes // 4) + 5,)),
        dma((modes // 4,)), dma((2,)),
    )


def write_out(sol_in, res_in, sol_out, res_out, sem):
    copies = [
        pltpu.make_async_copy(sol_in, sol_out, sem.at[0]),
        pltpu.make_async_copy(res_in, res_out, sem.at[1]),
    ]
    for copy in copies:
        copy.start()
    for copy in copies:
        copy.wait()


def shards(right_side, start_field, beam, noise, inv_power, smooth):
    nma, nf = lax.axis_size("ma"), lax.axis_size("freq")
    modes, freqs, _, ell = right_side.shape
    rank = beam.shape[3]
    width = modes * rank
    sides = 2 if nf > 2 else 1
    vmem_spec = pl.BlockSpec(memory_space=pltpu.VMEM)
    any_spec = pl.BlockSpec(memory_space=pl.ANY)
    field = pltpu.VMEM(right_side.shape, F32)
    edge = pltpu.VMEM((sides, modes, 2, ell), F32)
    slab = pltpu.VMEM((freqs, 2 * modes, ell), F32)
    edge_field = pltpu.VMEM((2 * modes, ell), F32)
    edge_slab = pltpu.VMEM((sides, 2 * modes, ell), F32)
    vector = max(min(nf - 1, 2), freqs // 2)
    matrix = max(freqs - vector, 1)
    half = pltpu.VMEM((matrix, 2 * width, ell), BF16)
    outs = pl.pallas_call(
        functools.partial(scoped_kernel, nma, nf, sides),
        out_shape=[field] * 2,
        in_specs=[any_spec] * 6,
        out_specs=[vmem_spec] * 2,
        scratch_shapes=[
            field, field, edge,
            pltpu.VMEM((freqs, modes, 2, rank, ell), F32),
            pltpu.VMEM(noise.shape, F32),
            pltpu.VMEM((1, ell), F32), pltpu.VMEM((1, ell), F32),
            half, half,
            slab, edge_slab, slab, edge_slab, slab, slab,
            pltpu.VMEM((matrix, 2 * modes, width), F32),
            pltpu.VMEM((vector, modes, rank, 128), F32),
            edge,
            pltpu.VMEM((2, sides, 2 * modes, ell), F32),
            field, field, field,
            edge_field, edge_field, edge_field,
            pltpu.VMEM((modes, 2, rank, ell), F32), pltpu.VMEM((modes, rank, 128), F32),
            edge_field, edge_field, pltpu.VMEM((modes, 2, ell), F32), edge_field, edge_field,
            pltpu.VMEM((2, 1, 128), F32),
            pltpu.VMEM((nma * nf, 1, 128), F32),
            pltpu.VMEM((nma // 2 if nf == 2 and nma % 2 == 0 and freqs > 1 else nma * nf, 1, 128), F32),
            pltpu.SemaphoreType.DMA((3, modes // 4, sides)),
            pltpu.SemaphoreType.DMA((2 * (modes // 4) + 5,)),
            pltpu.SemaphoreType.DMA((2,)),
            pltpu.SemaphoreType.REGULAR((max((nma * nf).bit_length() - 4, 1),)),
        ],
        compiler_params=pltpu.CompilerParams(
            collective_id=0, has_side_effects=True, vmem_limit_bytes=67043328 - 2 * right_side.size * 4
        ),
        name="solve",
    )(right_side, start_field, beam, noise, inv_power[None], smooth[None])
    return pl.pallas_call(
        write_out,
        out_shape=[jax.ShapeDtypeStruct(right_side.shape, F32)] * 2,
        in_specs=[vmem_spec] * 2,
        out_specs=[any_spec] * 2,
        scratch_shapes=[pltpu.SemaphoreType.DMA((2,))],
        compiler_params=pltpu.CompilerParams(vmem_limit_bytes=1024 * 1024),
        name="write_out",
    )(*outs)


def solution(mesh):
    in_specs = (
        P("ma", "freq", None, None),
        P("ma", "freq", None, None),
        P("ma", "freq", None, None, None),
        P("ma", "freq", None),
        P(),
        P(),
    )
    out_specs = (P("ma", "freq", None, None), P("ma", "freq", None, None))
    return jax.shard_map(shards, mesh=mesh, in_specs=in_specs, out_specs=out_specs, check_vma=False)
```

```python
import functools

import jax
import jax.numpy as jnp
from jax import lax
from jax.experimental import pallas as pl
from jax.experimental.pallas import tpu as pltpu
from jax.sharding import PartitionSpec as P

MESH = pl.DeviceIdType.MESH
F32, BF16 = jnp.float32, jnp.bfloat16


def split(x):
    high = x.astype(BF16)
    return high, (x - high.astype(F32)).astype(BF16)


def times(x, high, low, transposed):
    dims = (((1,), (1 if transposed else 0,)), ((), ()))
    rows = x.shape[0]
    x_high, x_low = split(x)
    both = jnp.concatenate([x_high, x_low], axis=0)
    main = lax.dot_general(both, high, dims, preferred_element_type=F32)
    rest = lax.dot_general(x_high, low, dims, preferred_element_type=F32)
    return main[:rows] + (main[rows:] + rest)


def folded(parts):
    row = lax.broadcasted_iota(jnp.int32, parts[0].shape, 0)
    upper = row < 4
    fours = [
        jnp.where(upper, parts[s], parts[s + 4])
        + pltpu.roll(jnp.where(upper, parts[s + 4], parts[s]), 4, 0)
        for s in range(4)
    ]
    even = row // 2 % 2 == 0
    twos = [
        jnp.where(
            even, fours[s] + pltpu.roll(fours[s], 6, 0), fours[s + 2] + pltpu.roll(fours[s + 2], 2, 0)
        )
        for s in range(2)
    ]
    return jnp.where(
        row % 2 == 0, twos[0] + pltpu.roll(twos[0], 7, 0), twos[1] + pltpu.roll(twos[1], 1, 0)
    )


def tree(parts):
    while len(parts) > 1:
        half = len(parts) // 2
        parts = [parts[k] + parts[half + k] for k in range(half)] + parts[2 * half:]
    return parts[0]


def total_of(x):
    return jnp.sum(jnp.sum(x, axis=0, keepdims=True), axis=1, keepdims=True)


def kernel(
    nma, nf, rhs_in, x0_in, beam_in, noise_in, power_in, smooth_in, sol_s, res_s,
    rhs_s, x0_s, edge_s, beam_s, noise_s, power_s, smooth_s,
    high_s, low_s, x_s, y_s, r_s, v_s, u_s, w_s, mask_s, column_s, first_s, halo_s,
    r_out_s, u_out_s, w_out_s, pull_s, partner_s, cross_s,
    lent_beam_s, lent_column_s, lent_y_s, lent_r_s, lent_first_s, lent_v_s, ahead_s,
    message_s, early_s, late_s,
    halo_recv, pair_recv, sum_recv, word_sem, in_sem, beam_sem, halo_send, pair_send, hand_send, sum_send,
):
    modes, freqs, _, ell = rhs_in.shape
    rank = beam_in.shape[3]
    width = modes * rank
    n = nma * nf
    my_ma, my_f = lax.axis_index("ma"), lax.axis_index("freq")
    me = my_ma * nf + my_f
    last = freqs - 1
    two_sided = nf > 2
    paired = nf == 2 and nma % 2 == 0 and freqs > 1
    helper = my_ma % 2 == 1
    groups = modes // 4
    edges = [0, last][:min(nf - 1, 2)]
    inner = [f for f in range(freqs) if f not in edges]
    beside_edge = [f for f in inner if f - 1 in edges or f + 1 in edges]
    apart = [f for f in inner if f not in beside_edge]
    vector = edges + inner[:max(freqs // 2 - len(edges), 0)]
    matrix = [f for f in range(freqs) if f not in vector]

    def at(g):
        return jnp.where(my_f == 0, last - g, g)

    edge_copies = [
        pltpu.make_async_copy(x0_in.at[:, at(f)], edge_s.at[i], in_sem.at[i])
        for i, f in enumerate(edges)
    ]
    x0_copy = pltpu.make_async_copy(x0_in, x0_s, in_sem.at[2])
    rhs_copy = pltpu.make_async_copy(rhs_in, rhs_s, in_sem.at[3])
    small = [
        pltpu.make_async_copy(power_in, power_s, in_sem.at[4]),
        pltpu.make_async_copy(smooth_in, smooth_s, in_sem.at[5]),
        pltpu.make_async_copy(noise_in, noise_s, in_sem.at[6]),
    ]
    beam_copies = [
        pltpu.make_async_copy(beam_in.at[:, at(f)], beam_s.at[f], beam_sem.at[f])
        for f in range(freqs)
    ]
    for copy in edge_copies:
        copy.start()

    def flip(bit):
        if bit == 0 and nf == 2:
            return 1 - 2 * my_f
        d = 1 << (bit if bit < freq_bits else bit - freq_bits)
        place = my_f if bit < freq_bits else my_ma
        return d * (1 - 2 * (place // d % 2))

    def partner(bits):
        return (
            my_ma + sum(flip(bit) for bit in bits if bit >= freq_bits),
            my_f + sum(flip(bit) for bit in bits if bit < freq_bits),
        )

    freq_bits = nf.bit_length() - 1
    bits = freq_bits + nma.bit_length() - 1
    close = min(bits, 3)
    greeted = [
        partner([bit for bit in range(close) if mask >> bit & 1]) for mask in range(1, 1 << close)
    ]
    word = [partner([bit]) for bit in range(close, bits)]
    greeted += word
    words = len(word)
    barrier = pltpu.get_barrier_semaphore()
    near = jnp.where(my_f == 0, 1, my_f - 1)
    has_far = (my_f > 0) & (my_f < nf - 1)

    def greet(device):
        pl.semaphore_signal(barrier, inc=1, device_id=device, device_id_type=MESH)

    for i, device in enumerate(greeted):
        greet(device)
        if i == 0:
            for copy in [beam_copies[f] for f in edges] + [x0_copy, rhs_copy] + small:
                copy.start()
    expected = len(greeted)
    if nf > 2:
        pl.when(my_f > 0)(lambda: greet((my_ma, my_f - 1)))
        pl.when(my_f < nf - 1)(lambda: greet((my_ma, my_f + 1)))
        expected = expected + jnp.minimum(my_f, 1) + jnp.minimum(nf - 1 - my_f, 1)

    steps = list(range(words + 1))

    def advance():
        if steps:
            step = steps.pop(0)
            if step > 0:
                pl.semaphore_wait(word_sem.at[step - 1], 1)
            if step < words:
                pl.semaphore_signal(
                    word_sem.at[step], inc=1, device_id=word[step], device_id_type=MESH
                )

    def piece(kind, g):
        if kind == 0:
            rows = pl.ds(4 * g, 4)
            return (lambda i: edge_s.at[i, rows]), (lambda i: first_s.at[i, rows])
        source = (y_s, v_s)[kind - 1]
        rows = pl.ds(8 * g, 8)
        return (lambda i: source.at[i, rows]), (lambda i: halo_s.at[kind - 1, i, rows])

    def near_copy(kind, g):
        source, target = piece(kind, g)
        side = jnp.minimum(my_f // 2, 1) if two_sided else 0
        return pltpu.make_async_remote_copy(
            src_ref=source(0), dst_ref=target(side),
            send_sem=halo_send.at[kind, g, 0], recv_sem=halo_recv.at[kind, g, side],
            device_id=(my_ma, near), device_id_type=MESH,
        )

    def far_copy(kind, g):
        source, target = piece(kind, g)
        return pltpu.make_async_remote_copy(
            src_ref=source(1), dst_ref=target(0),
            send_sem=halo_send.at[kind, g, 1], recv_sem=halo_recv.at[kind, g, 0],
            device_id=(my_ma, my_f + 1), device_id_type=MESH,
        )

    def arrival(kind, g, side):
        slot = piece(kind, g)[1](side)
        return pltpu.make_async_copy(slot, slot, halo_recv.at[kind, g, side])

    def send(kind, g):
        if nf > 1:
            near_copy(kind, g).start()
        if two_sided:
            pl.when(has_far)(lambda: far_copy(kind, g).start())

    def arrive(kind, g):
        if nf > 1:
            arrival(kind, g, 0).wait()
        if two_sided:
            pl.when(has_far)(lambda: arrival(kind, g, 1).wait())

    def sent(kind, g):
        if nf > 1:
            near_copy(kind, g).wait_send()
        if two_sided:
            pl.when(has_far)(lambda: far_copy(kind, g).wait_send())

    def pair_copy(k, source, target, ma, f):
        return pltpu.make_async_remote_copy(
            src_ref=source, dst_ref=target, send_sem=pair_send.at[k], recv_sem=pair_recv.at[k],
            device_id=(ma, f), device_id_type=MESH,
        )

    def lend(k):
        source = (lambda: beam_s.at[0], lambda: column_s.at[0], lambda: y_s.at[0], lambda: r_s.at[1])[k]
        target = (lent_beam_s, lent_column_s, lent_y_s, lent_r_s)[k]
        return pair_copy(k, source(), target, my_ma + 1, my_f)

    def pull_copy():
        return pair_copy(4, pull_s, partner_s, my_ma + 1, my_f)

    def first_copy(g):
        rows = pl.ds(4 * g, 4)
        return pair_copy(5 + g, edge_s.at[0, rows], lent_first_s.at[rows], my_ma + 1, 1 - my_f)

    def cross_copy(g):
        rows = pl.ds(8 * g, 8)
        return pair_copy(5 + groups + g, lent_v_s.at[rows], cross_s.at[rows], my_ma, 1 - my_f)

    def ahead_copy(g):
        rows = pl.ds(8 * g, 8)
        return pltpu.make_async_remote_copy(
            src_ref=ahead_s.at[rows], dst_ref=halo_s.at[1, 0, rows],
            send_sem=halo_send.at[2, g, 0], recv_sem=halo_recv.at[2, g, 0],
            device_id=(my_ma, 1 - my_f), device_id_type=MESH,
        )

    def hand_copy(g):
        rows = pl.ds(4 * g, 4)
        return pltpu.make_async_remote_copy(
            src_ref=lent_first_s.at[rows], dst_ref=first_s.at[0, rows],
            send_sem=hand_send.at[g], recv_sem=halo_recv.at[0, g, 0],
            device_id=(my_ma - 1, my_f), device_id_type=MESH,
        )

    def even_only(copies):
        @pl.when(jnp.logical_not(helper))
        def _():
            for copy in copies:
                copy.start()

    def beside(i, value):
        return jnp.where(has_far, value, 0.0) if i else value

    if two_sided:
        @pl.when(jnp.logical_not(has_far))
        def _():
            first_s[1] = jnp.zeros_like(first_s[1])
            halo_s[:, 1] = jnp.zeros_like(halo_s[:, 1])

    for copy in edge_copies:
        copy.wait()
    for f in inner:
        beam_copies[f].start()
    pl.semaphore_wait(barrier, expected)
    if paired:
        even_only([first_copy(g) for g in range(groups)])

        pl.when(helper)(lambda: near_copy(0, 0).start())
    else:
        for g in range(groups):
            send(0, g)
    advance()

    x0_copy.wait()
    for copy in small:
        copy.wait()
    def rows_of(ref, *at_f):
        place = (slice(None), *at_f)
        return jnp.concatenate(
            [ref[(slice(4 * g, 4 * g + 4), *place[1:], b)] for g in range(groups) for b in range(2)],
            axis=0,
        )

    def group(g):
        return slice(8 * g, 8 * g + 8)

    for f in range(freqs):
        x_s[f] = rows_of(x0_s, at(f))
    power, smooth = power_s[...], smooth_s[...]
    row = lax.broadcasted_iota(jnp.int32, (2 * modes, width), 0)
    own = lax.broadcasted_iota(jnp.int32, (2 * modes, width), 1) // rank == row // 8 * 4 + row % 4
    sign = jnp.where(row % 8 < 4, 1.0, -1.0)
    for i, f in enumerate(matrix):
        levels = noise_s[:, at(f), :]
        levels = jnp.concatenate(
            [levels[4 * g:4 * g + 4] for g in range(groups) for _ in range(2)], axis=0
        )
        mask_s[i] = jnp.where(own, jnp.concatenate([levels] * modes, axis=1), 0.0)
    unit = (
        lax.broadcasted_iota(jnp.int32, (rank, rank), 0)
        == lax.broadcasted_iota(jnp.int32, (rank, rank), 1)
    )
    for i, f in enumerate(vector):
        levels = noise_s[:, at(f), :]
        for m in range(modes):
            column = jnp.sum(jnp.where(unit, levels[m:m + 1], 0.0), axis=1, keepdims=True)
            column_s[i, m] = jnp.broadcast_to(column, (rank, 128))

    def swapped(x):
        return jnp.concatenate([pltpu.roll(x[group(g)], 4, 0) for g in range(groups)], axis=0)

    def matrix_project(f, field):
        i = matrix.index(f)
        seen = times(field, high_s[i], low_s[i], True)
        parts = seen[:, :width] + sign * swapped(seen[:, width:])
        return parts, mask_s[i] * parts

    def matrix_back(f, seen):
        i = matrix.index(f)
        weighted = jnp.concatenate([seen[1], -sign * swapped(seen[1])], axis=1)
        return times(weighted, high_s[i], low_s[i], False)

    def wide(x):
        return jnp.concatenate([x] * (ell // 128), axis=1)

    def owned(f):
        return (lambda m, a: beam_s[f, m, a]), (lambda m: column_s[vector.index(f), m])

    lent = (lambda m, a: lent_beam_s[m, a]), (lambda m: lent_column_s[m])

    def group_project(source, g, field):
        beam_of, column_of = source
        parts = []
        for j in range(4):
            m = 4 * g + j
            real_beam, imaginary_beam = beam_of(m, 0), beam_of(m, 1)
            real_field, imaginary_field = field[j:j + 1], field[4 + j:5 + j]
            levels = column_of(m)
            real = jnp.sum(
                real_beam * real_field + imaginary_beam * imaginary_field, axis=1, keepdims=True
            )
            imaginary = jnp.sum(
                real_beam * imaginary_field - imaginary_beam * real_field, axis=1, keepdims=True
            )
            parts.append((real, imaginary, levels * real, levels * imaginary))
        return parts

    def group_back(source, g, parts):
        beam_of, _ = source
        reals, imaginaries = [], []
        for j, (_, _, real, imaginary) in enumerate(parts):
            m = 4 * g + j
            real, imaginary = wide(real), wide(imaginary)
            real_beam, imaginary_beam = beam_of(m, 0), beam_of(m, 1)
            for found, value in (
                (reals, real_beam * real - imaginary_beam * imaginary),
                (imaginaries, real_beam * imaginary + imaginary_beam * real),
            ):
                found.append(sum(value[k:k + 8] for k in range(0, rank, 8)))
        return folded(reals + imaginaries)

    def group_beam(source, g, field):
        return group_back(source, g, group_project(source, g, field))

    def project(f, ref):
        if f in matrix:
            return matrix_project(f, ref[f])
        return [group_project(owned(f), g, ref[f, group(g)]) for g in range(groups)]

    def back(f, seen):
        if f in matrix:
            return matrix_back(f, seen)
        return jnp.concatenate([group_back(owned(f), g, seen[g]) for g in range(groups)], axis=0)

    def apply_beam(fs, ref):
        fs = [f for f in fs if f in matrix] + [f for f in fs if f in vector]
        seen = [project(f, ref) for f in fs]
        return {f: back(f, found) for f, found in zip(fs, seen)}

    def count(f):
        value = float(f > 0) + float(f < last) + float(nf > 1 and f == 0)
        if two_sided and f == last:
            value = value + jnp.where(has_far, 1.0, 0.0)
        return value

    def local_prior(f, ref, rows=slice(None)):
        value = count(f) * ref[f, rows]
        if f > 0:
            value = value - ref[f - 1, rows]
        if f < last:
            value = value - ref[f + 1, rows]
        return power * ref[f, rows] + smooth * value

    for f in edges:
        beam_copies[f].wait()
    rhs_copy.wait()
    for i, f in enumerate(edges):
        for g in range(groups):
            rows = group(g)
            image = group_beam(owned(f), g, x_s[f, rows])
            y_s[i, rows] = rows_of(rhs_s, at(f))[rows] - image - local_prior(f, x_s, rows)
    first, rest = [], inner
    if paired:
        even_only([near_copy(1, g) for g in range(groups)] + [lend(k) for k in range(3)])

        @pl.when(helper)
        def _():
            for g in range(1, groups):
                near_copy(0, g).start()

        first, rest = inner[:1], inner[1:]
    else:
        for g in range(groups):
            send(1, g)

    for f in first:
        beam_copies[f].wait()
        r_s[f] = rows_of(rhs_s, at(f)) - back(f, project(f, x_s)) - local_prior(f, x_s)
    if paired:
        even_only([lend(3)])

        @pl.when(helper)
        def _():
            for g in range(groups):
                near_copy(1, g).start()

    for f in rest:
        beam_copies[f].wait()
    for i, f in enumerate(matrix):
        for a in range(2):
            rows = slice(a * width, (a + 1) * width)
            high, low = split(beam_s[f, :, a].reshape(width, ell))
            high_s[i, rows] = high
            low_s[i, rows] = low
    for f, image in apply_beam(rest, x_s).items():
        r_s[f] = rows_of(rhs_s, at(f)) - image - local_prior(f, x_s)
    for f, image in apply_beam(inner, r_s).items():
        u_s[f] = image + local_prior(f, r_s) if f in apart else image
    advance()

    def complete(i, f, g):
        rows = group(g)
        halo = jnp.concatenate([first_s[i, 4 * g:4 * g + 4, b, :] for b in range(2)], axis=0)
        r_s[f, rows] = y_s[i, rows] + smooth * halo

    def edge_image(f, g):
        rows = group(g)
        return group_beam(owned(f), g, r_s[f, rows]) + local_prior(f, r_s, rows)

    if paired:
        @pl.when(helper)
        def _():
            for g in range(groups):
                arrive(0, g)
                complete(0, 0, g)
                ahead_s[group(g)] = edge_image(0, g)
                ahead_copy(g).start()
            for g in range(groups):
                first_copy(g).wait_recv()
                hand_copy(g).start()
                if g == 0:
                    for k in range(4):
                        lend(k).wait_recv()
                rows = group(g)
                halo = jnp.concatenate([lent_first_s[4 * g:4 * g + 4, b, :] for b in range(2)], axis=0)
                r = lent_y_s[rows] + smooth * halo
                local = power * r + smooth * (count(0) * r - lent_r_s[rows])
                lent_v_s[rows] = group_beam(lent, g, r) + local
                cross_copy(g).start()

    seen = {f: project(f, u_s) for f in apart}
    grouped = [f for f in beside_edge if f in vector]
    whole = [f for f in beside_edge if f in matrix]
    seen |= {f: [] for f in grouped + edges}
    zero = jnp.zeros((8, ell), F32)
    sums = [zero, zero, zero, zero]
    column_part = jnp.zeros((rank, 128), F32)

    def add_up(g, sums, column_part):
        rows = group(g)
        norm, curve, square, cube = sums
        for f in inner + edges:
            if f in vector:
                for real, imaginary, real_weighted, imaginary_weighted in seen[f][g]:
                    column_part = column_part + (real * real_weighted + imaginary * imaginary_weighted)
            r, u = r_s[f, rows], u_s[f, rows]
            w = local_prior(f, u_s, rows)
            w_s[f, rows] = w
            norm = norm + r * r
            curve = curve + r * u
            square = square + u * u
            cube = cube + u * w
        return [norm, curve, square, cube], column_part

    def finish_edges(g):
        rows = group(g)
        for i, f in enumerate(edges):
            u_s[f, rows] = v_s[i, rows] - beside(
                i, smooth * (halo_s[0, i, rows] + smooth * x_s[f, rows])
            )
            seen[f].append(group_project(owned(f), g, u_s[f, rows]))

    for g in range(groups):
        rows = group(g)
        if paired:
            pl.when(jnp.logical_not(helper))(lambda: arrive(0, g))
            arrive(1, g)
        else:
            arrive(0, g)
        for i, f in enumerate(edges):
            complete(i, f, g)
        for i, f in enumerate(edges):
            v_s[i, rows] = edge_image(f, g)
        if not paired:
            send(2, g)
        for f in grouped:
            u_s[f, rows] = u_s[f, rows] + local_prior(f, r_s, rows)
            seen[f].append(group_project(owned(f), g, u_s[f, rows]))
        if paired:
            finish_edges(g)
            pull_s[rows] = smooth * u_s[0, rows]
            if not whole:
                sums, column_part = add_up(g, sums, column_part)
    for f in whole:
        u_s[f] = u_s[f] + local_prior(f, r_s)
        seen[f] = project(f, u_s)
    if paired:
        even_only([pull_copy()])
    else:
        for g in range(groups):
            arrive(1, g)
            finish_edges(g)
    if whole or not paired:
        for g in range(groups):
            sums, column_part = add_up(g, sums, column_part)
    beam_part = jnp.zeros((2 * modes, width), F32)
    for f in matrix:
        beam_part = beam_part + seen[f][0] * seen[f][1]
    lane = lax.broadcasted_iota(jnp.int32, (1, 128), 1)
    message = jnp.zeros((1, 128), F32)
    for i, part in enumerate(sums):
        total = total_of(part)
        if i == 3:
            total = total + total_of(beam_part) + jnp.sum(column_part, axis=0, keepdims=True)
        message = jnp.where(lane == i, total, message)
    if paired:
        message = jnp.where(lane == 4 + my_f, total_of(smooth * r_s[0] * pull_s[...]), message)
    message_s[0] = message
    early_s[me] = message

    while steps:
        advance()

    def share(source, target, slot, turn, device):
        pltpu.make_async_remote_copy(
            src_ref=message_s.at[source], dst_ref=target.at[slot],
            send_sem=sum_send.at[turn], recv_sem=sum_recv.at[turn],
            device_id=device, device_id_type=MESH,
        ).start()

    def share_all(source, target, slot, turn, stride):
        if n > 64:
            def body(i, carry):
                ma, f = my_ma + i * stride // nf, my_f + i * stride % nf
                share(source, target, slot, turn, (lax.rem(ma, nma), lax.rem(f, nf)))
                return carry

            lax.fori_loop(1, n // stride, body, 0)
        else:
            for mask in sorted(range(stride, n, stride), key=lambda m: (-(m // nf // 2), m)):
                device = partner([bit for bit in range(bits) if mask >> bit & 1])
                share(source, target, slot, turn, device)

    def landed(target, sem, rows):
        if rows:
            rows = target.at[pl.ds(0, rows)]
            pltpu.make_async_copy(rows, rows, sem).wait()

    def lanes_of(x):
        x = jnp.sum(x, axis=0, keepdims=True)
        return sum(x[:, i:i + 128] for i in range(0, ell, 128))

    share_all(0, early_s, me, 0, 1)
    if paired:
        even_only([near_copy(2, g) for g in range(groups)])
    for f in matrix + vector:
        w_s[f] = w_s[f] + back(f, seen[f])

    late_rows = late_s.shape[0]
    if paired:
        @pl.when(helper)
        def _():
            cross = jnp.zeros((8, ell), F32)
            for g in range(groups):
                arrive(2, g)
                cross = cross + pull_s[group(g)] * halo_s[1, 0, group(g)]
            pull_copy().wait_recv()
            for g in range(groups):
                cross_copy(g).wait_recv()
                cross = cross + partner_s[group(g)] * cross_s[group(g)]
            message = lanes_of(cross)
            late_s[my_ma // 2] = message
            message_s[1] = message
            share_all(1, late_s, my_ma // 2, 1, nf)
            for g in range(groups):
                cross_copy(g).wait_send()

        @pl.when(jnp.logical_not(helper))
        def _():
            for g in range(groups):
                arrive(2, g)
            pull_copy().wait_send()
            for k in range(4):
                lend(k).wait_send()
            for g in range(groups):
                first_copy(g).wait_send()

        w_s[0] = w_s[0] - smooth * (halo_s[1, 0] - smooth * r_s[0])
    else:
        cross = jnp.zeros((8, ell), F32)
        nexts = []
        for g in range(groups):
            arrive(2, g)
            rows = group(g)
            for i, f in enumerate(edges):
                pull = beside(i, smooth * (halo_s[1, i, rows] - smooth * r_s[f, rows]))
                nexts.append((f, rows, pull))
                cross = cross + pull * u_s[f, rows]
        message = lanes_of(cross)
        late_s[me] = message
        message_s[1] = message
        share_all(1, late_s, me, 1, 1)
        for f, rows, pull in nexts:
            w_s[f, rows] = w_s[f, rows] - pull

    if paired:
        for g in range(groups):
            for kind in (1, 2):
                sent(kind, g)

        @pl.when(helper)
        def _():
            for g in range(groups):
                sent(0, g)
                hand_copy(g).wait_send()
    else:
        for kind in range(3):
            for g in range(groups):
                sent(kind, g)
    for source, target in ((r_s, r_out_s), (u_s, u_out_s), (w_s, w_out_s)):
        for f in range(freqs):
            value = source[f]
            for g in range(groups):
                for b in range(2):
                    start = 8 * g + 4 * b
                    target[4 * g:4 * g + 4, at(f), b, :] = value[start:start + 4]

    landed(early_s, sum_send.at[0], n - 1)
    landed(early_s, sum_recv.at[0], n - 1)
    if paired:
        @pl.when(helper)
        def _():
            rows = early_s.at[pl.ds(0, nma - 1)]
            pltpu.make_async_copy(rows, rows, sum_send.at[1]).wait()
            landed(late_s, sum_recv.at[1], late_rows - 1)

        pl.when(jnp.logical_not(helper))(lambda: landed(late_s, sum_recv.at[1], late_rows))
    else:
        landed(late_s, sum_send.at[1], late_rows - 1)
        landed(late_s, sum_recv.at[1], late_rows - 1)
    def rows_total(ref):
        if ref.shape[0] > 64:
            return jnp.sum(ref[...], axis=0)
        return tree([ref[k] for k in range(ref.shape[0])])

    total = rows_total(early_s)
    m0, m1, m2, m3, known = (
        jnp.sum(jnp.where(lane == i, total, 0.0), axis=1, keepdims=True)
        for i in (0, 1, 2, 3, 4 + my_f)
    )
    crossed = jnp.sum(rows_total(late_s), axis=1, keepdims=True)
    m3 = m3 - 2.0 * (crossed - known) if paired else m3 - crossed
    inverse = 1.0 / m1
    step = m0 * inverse
    drop = step * m2 - m1
    growth = drop * inverse
    curve_next = m1 - 2.0 * step * m2 + step * step * m3
    step_next = step * drop / (curve_next - growth * drop)
    c = step + step_next * (1.0 + growth)
    e = step * step_next
    for m in range(modes):
        r, u = r_out_s[m], u_out_s[m]
        sol_s[m] = x0_s[m] + c * r - e * u
        res_s[m] = r - c * u + e * w_out_s[m]


def scoped_kernel(nma, nf, sides, *refs):
    modes, freqs = refs[0].shape[:2]
    dma = pltpu.SemaphoreType.DMA
    pl.run_scoped(
        functools.partial(kernel, nma, nf, *refs),
        dma((7,)), dma((freqs,)), dma((3, modes // 4, sides)), dma((2 * (modes // 4) + 5,)),
        dma((modes // 4,)), dma((2,)),
    )


def write_out(sol_in, res_in, sol_out, res_out):
    def body(sem):
        copies = [
            pltpu.make_async_copy(sol_in, sol_out, sem.at[0]),
            pltpu.make_async_copy(res_in, res_out, sem.at[1]),
        ]
        for copy in copies:
            copy.start()
        for copy in copies:
            copy.wait()

    pl.run_scoped(body, pltpu.SemaphoreType.DMA((2,)))


def shards(right_side, start_field, beam, noise, inv_power, smooth):
    nma, nf = lax.axis_size("ma"), lax.axis_size("freq")
    modes, freqs, _, ell = right_side.shape
    rank = beam.shape[3]
    width = modes * rank
    sides = 2 if nf > 2 else 1
    vmem_spec = pl.BlockSpec(memory_space=pltpu.VMEM)
    any_spec = pl.BlockSpec(memory_space=pl.ANY)
    field = pltpu.VMEM(right_side.shape, F32)
    edge = pltpu.VMEM((sides, modes, 2, ell), F32)
    slab = pltpu.VMEM((freqs, 2 * modes, ell), F32)
    edge_field = pltpu.VMEM((2 * modes, ell), F32)
    edge_slab = pltpu.VMEM((sides, 2 * modes, ell), F32)
    vector = max(min(nf - 1, 2), freqs // 2)
    matrix = max(freqs - vector, 1)
    half = pltpu.VMEM((matrix, 2 * width, ell), BF16)
    outs = pl.pallas_call(
        functools.partial(scoped_kernel, nma, nf, sides),
        out_shape=[field] * 2,
        in_specs=[any_spec] * 6,
        out_specs=[vmem_spec] * 2,
        scratch_shapes=[
            field, field, edge,
            pltpu.VMEM((freqs, modes, 2, rank, ell), F32),
            pltpu.VMEM(noise.shape, F32),
            pltpu.VMEM((1, ell), F32), pltpu.VMEM((1, ell), F32),
            half, half,
            slab, edge_slab, slab, edge_slab, slab, slab,
            pltpu.VMEM((matrix, 2 * modes, width), F32),
            pltpu.VMEM((vector, modes, rank, 128), F32),
            edge,
            pltpu.VMEM((2, sides, 2 * modes, ell), F32),
            field, field, field,
            edge_field, edge_field, edge_field,
            pltpu.VMEM((modes, 2, rank, ell), F32), pltpu.VMEM((modes, rank, 128), F32),
            edge_field, edge_field, pltpu.VMEM((modes, 2, ell), F32), edge_field, edge_field,
            pltpu.VMEM((2, 1, 128), F32),
            pltpu.VMEM((nma * nf, 1, 128), F32),
            pltpu.VMEM((nma // 2 if nf == 2 and nma % 2 == 0 and freqs > 1 else nma * nf, 1, 128), F32),
            pltpu.SemaphoreType.DMA((3, modes // 4, sides)),
            pltpu.SemaphoreType.DMA((2 * (modes // 4) + 5,)),
            pltpu.SemaphoreType.DMA((2,)),
            pltpu.SemaphoreType.REGULAR((max((nma * nf).bit_length() - 4, 1),)),
        ],
        compiler_params=pltpu.CompilerParams(
            collective_id=0, has_side_effects=True, vmem_limit_bytes=67043328 - 2 * right_side.size * 4
        ),
        name="solve",
    )(right_side, start_field, beam, noise, inv_power[None], smooth[None])
    return pl.pallas_call(
        write_out,
        out_shape=[jax.ShapeDtypeStruct(right_side.shape, F32)] * 2,
        in_specs=[vmem_spec] * 2,
        out_specs=[any_spec] * 2,
        compiler_params=pltpu.CompilerParams(vmem_limit_bytes=1024 * 1024),
        name="write_out",
    )(*outs)


def solution(mesh):
    in_specs = (
        P("ma", "freq", None, None),
        P("ma", "freq", None, None),
        P("ma", "freq", None, None, None),
        P("ma", "freq", None),
        P(),
        P(),
    )
    out_specs = (P("ma", "freq", None, None), P("ma", "freq", None, None))
    return jax.shard_map(shards, mesh=mesh, in_specs=in_specs, out_specs=out_specs, check_vma=False)
```

```python
import functools

import jax
import jax.numpy as jnp
from jax import lax
from jax.experimental import pallas as pl
from jax.experimental.pallas import tpu as pltpu
from jax.sharding import PartitionSpec as P

MESH = pl.DeviceIdType.MESH
F32, BF16 = jnp.float32, jnp.bfloat16


def split(x):
    high = x.astype(BF16)
    return high, (x - high.astype(F32)).astype(BF16)


def times(x, high, low, transposed):
    dims = (((1,), (1 if transposed else 0,)), ((), ()))
    rows = x.shape[0]
    x_high, x_low = split(x)
    both = jnp.concatenate([x_high, x_low], axis=0)
    main = lax.dot_general(both, high, dims, preferred_element_type=F32)
    rest = lax.dot_general(x_high, low, dims, preferred_element_type=F32)
    return main[:rows] + (main[rows:] + rest)


def folded(parts):
    row = lax.broadcasted_iota(jnp.int32, parts[0].shape, 0)
    upper = row < 4
    fours = [
        jnp.where(upper, parts[s], parts[s + 4])
        + pltpu.roll(jnp.where(upper, parts[s + 4], parts[s]), 4, 0)
        for s in range(4)
    ]
    even = row // 2 % 2 == 0
    twos = [
        jnp.where(
            even, fours[s] + pltpu.roll(fours[s], 6, 0), fours[s + 2] + pltpu.roll(fours[s + 2], 2, 0)
        )
        for s in range(2)
    ]
    return jnp.where(
        row % 2 == 0, twos[0] + pltpu.roll(twos[0], 7, 0), twos[1] + pltpu.roll(twos[1], 1, 0)
    )


def tree(parts):
    while len(parts) > 1:
        half = len(parts) // 2
        parts = [parts[k] + parts[half + k] for k in range(half)] + parts[2 * half:]
    return parts[0]


def total_of(x):
    return jnp.sum(jnp.sum(x, axis=0, keepdims=True), axis=1, keepdims=True)


def kernel(
    nma, nf, rhs_in, x0_in, beam_in, noise_in, power_in, smooth_in, sol_s, res_s,
    rhs_s, x0_s, edge_s, beam_s, noise_s, power_s, smooth_s,
    high_s, low_s, x_s, y_s, r_s, v_s, u_s, w_s, mask_s, column_s, first_s, halo_s,
    r_out_s, u_out_s, w_out_s, pull_s, partner_s, cross_s,
    lent_beam_s, lent_column_s, lent_y_s, lent_r_s, lent_first_s, lent_v_s, ahead_s,
    message_s, early_s, late_s,
    halo_recv, pair_recv, sum_recv, word_sem, in_sem, beam_sem, halo_send, pair_send, hand_send, sum_send,
):
    modes, freqs, _, ell = rhs_in.shape
    rank = beam_in.shape[3]
    width = modes * rank
    n = nma * nf
    my_ma, my_f = lax.axis_index("ma"), lax.axis_index("freq")
    me = my_ma * nf + my_f
    last = freqs - 1
    two_sided = nf > 2
    paired = nf == 2 and nma % 2 == 0 and freqs > 1
    helper = my_ma % 2 == 1
    groups = modes // 4
    edges = [0, last][:min(nf - 1, 2)]
    inner = [f for f in range(freqs) if f not in edges]
    beside_edge = [f for f in inner if f - 1 in edges or f + 1 in edges]
    apart = [f for f in inner if f not in beside_edge]
    vector = edges + inner[:max(freqs // 2 - len(edges), 0)]
    matrix = [f for f in range(freqs) if f not in vector]

    def at(g):
        return jnp.where(my_f == 0, last - g, g)

    edge_copies = [
        pltpu.make_async_copy(x0_in.at[:, at(f)], edge_s.at[i], in_sem.at[i])
        for i, f in enumerate(edges)
    ]
    x0_copy = pltpu.make_async_copy(x0_in, x0_s, in_sem.at[2])
    rhs_copy = pltpu.make_async_copy(rhs_in, rhs_s, in_sem.at[3])
    small = [
        pltpu.make_async_copy(power_in, power_s, in_sem.at[4]),
        pltpu.make_async_copy(smooth_in, smooth_s, in_sem.at[5]),
        pltpu.make_async_copy(noise_in, noise_s, in_sem.at[6]),
    ]
    beam_copies = [
        pltpu.make_async_copy(beam_in.at[:, at(f)], beam_s.at[f], beam_sem.at[f])
        for f in range(freqs)
    ]
    for copy in edge_copies:
        copy.start()

    def flip(bit):
        if bit == 0 and nf == 2:
            return 1 - 2 * my_f
        d = 1 << (bit if bit < freq_bits else bit - freq_bits)
        place = my_f if bit < freq_bits else my_ma
        return d * (1 - 2 * (place // d % 2))

    def partner(bits):
        return (
            my_ma + sum(flip(bit) for bit in bits if bit >= freq_bits),
            my_f + sum(flip(bit) for bit in bits if bit < freq_bits),
        )

    freq_bits = nf.bit_length() - 1
    bits = freq_bits + nma.bit_length() - 1
    close = min(bits, 3)
    barrier = pltpu.get_barrier_semaphore()

    def greet(device):
        pl.semaphore_signal(barrier, inc=1, device_id=device, device_id_type=MESH)

    greeted = []
    for mask in range(1, 1 << close):
        greeted.append(partner([bit for bit in range(close) if mask >> bit & 1]))
        greet(greeted[-1])
        if mask == 1:
            for copy in [beam_copies[f] for f in edges] + [x0_copy, rhs_copy] + small:
                copy.start()
    word = [partner([bit]) for bit in range(close, bits)]
    for device in word:
        greet(device)
    greeted += word
    words = len(word)
    near = jnp.where(my_f == 0, 1, my_f - 1)
    has_far = (my_f > 0) & (my_f < nf - 1)
    expected = len(greeted)
    if nf > 2:
        pl.when(my_f > 0)(lambda: greet((my_ma, my_f - 1)))
        pl.when(my_f < nf - 1)(lambda: greet((my_ma, my_f + 1)))
        expected = expected + jnp.minimum(my_f, 1) + jnp.minimum(nf - 1 - my_f, 1)

    steps = list(range(words + 1))

    def advance():
        if steps:
            step = steps.pop(0)
            if step > 0:
                pl.semaphore_wait(word_sem.at[step - 1], 1)
            if step < words:
                pl.semaphore_signal(
                    word_sem.at[step], inc=1, device_id=word[step], device_id_type=MESH
                )

    def piece(kind, g):
        if kind == 0:
            rows = pl.ds(4 * g, 4)
            return (lambda i: edge_s.at[i, rows]), (lambda i: first_s.at[i, rows])
        source = (y_s, v_s)[kind - 1]
        rows = pl.ds(8 * g, 8)
        return (lambda i: source.at[i, rows]), (lambda i: halo_s.at[kind - 1, i, rows])

    def near_copy(kind, g):
        source, target = piece(kind, g)
        side = jnp.minimum(my_f // 2, 1) if two_sided else 0
        return pltpu.make_async_remote_copy(
            src_ref=source(0), dst_ref=target(side),
            send_sem=halo_send.at[kind, g, 0], recv_sem=halo_recv.at[kind, g, side],
            device_id=(my_ma, near), device_id_type=MESH,
        )

    def far_copy(kind, g):
        source, target = piece(kind, g)
        return pltpu.make_async_remote_copy(
            src_ref=source(1), dst_ref=target(0),
            send_sem=halo_send.at[kind, g, 1], recv_sem=halo_recv.at[kind, g, 0],
            device_id=(my_ma, my_f + 1), device_id_type=MESH,
        )

    def arrival(kind, g, side):
        slot = piece(kind, g)[1](side)
        return pltpu.make_async_copy(slot, slot, halo_recv.at[kind, g, side])

    def send(kind, g):
        if nf > 1:
            near_copy(kind, g).start()
        if two_sided:
            pl.when(has_far)(lambda: far_copy(kind, g).start())

    def arrive(kind, g):
        if nf > 1:
            arrival(kind, g, 0).wait()
        if two_sided:
            pl.when(has_far)(lambda: arrival(kind, g, 1).wait())

    def sent(kind, g):
        if nf > 1:
            near_copy(kind, g).wait_send()
        if two_sided:
            pl.when(has_far)(lambda: far_copy(kind, g).wait_send())

    def pair_copy(k, source, target, ma, f):
        return pltpu.make_async_remote_copy(
            src_ref=source, dst_ref=target, send_sem=pair_send.at[k], recv_sem=pair_recv.at[k],
            device_id=(ma, f), device_id_type=MESH,
        )

    def lend(k):
        source = (lambda: beam_s.at[0], lambda: column_s.at[0], lambda: y_s.at[0], lambda: r_s.at[1])[k]
        target = (lent_beam_s, lent_column_s, lent_y_s, lent_r_s)[k]
        return pair_copy(k, source(), target, my_ma + 1, my_f)

    def pull_copy():
        return pair_copy(4, pull_s, partner_s, my_ma + 1, my_f)

    def first_copy(g):
        rows = pl.ds(4 * g, 4)
        return pair_copy(5 + g, edge_s.at[0, rows], lent_first_s.at[rows], my_ma + 1, 1 - my_f)

    def cross_copy(g):
        rows = pl.ds(8 * g, 8)
        return pair_copy(5 + groups + g, lent_v_s.at[rows], cross_s.at[rows], my_ma, 1 - my_f)

    def ahead_copy(g):
        rows = pl.ds(8 * g, 8)
        return pltpu.make_async_remote_copy(
            src_ref=ahead_s.at[rows], dst_ref=halo_s.at[1, 0, rows],
            send_sem=halo_send.at[2, g, 0], recv_sem=halo_recv.at[2, g, 0],
            device_id=(my_ma, 1 - my_f), device_id_type=MESH,
        )

    def hand_copy(g):
        rows = pl.ds(4 * g, 4)
        return pltpu.make_async_remote_copy(
            src_ref=lent_first_s.at[rows], dst_ref=first_s.at[0, rows],
            send_sem=hand_send.at[g], recv_sem=halo_recv.at[0, g, 0],
            device_id=(my_ma - 1, my_f), device_id_type=MESH,
        )

    def even_only(copies):
        @pl.when(jnp.logical_not(helper))
        def _():
            for copy in copies:
                copy.start()

    def beside(i, value):
        return jnp.where(has_far, value, 0.0) if i else value

    if two_sided:
        @pl.when(jnp.logical_not(has_far))
        def _():
            first_s[1] = jnp.zeros_like(first_s[1])
            halo_s[:, 1] = jnp.zeros_like(halo_s[:, 1])

    for copy in edge_copies:
        copy.wait()
    for f in inner:
        beam_copies[f].start()
    pl.semaphore_wait(barrier, expected)
    if paired:
        even_only([first_copy(g) for g in range(groups)])

        pl.when(helper)(lambda: near_copy(0, 0).start())
    else:
        for g in range(groups):
            send(0, g)
    advance()

    x0_copy.wait()
    for copy in small:
        copy.wait()
    def rows_of(ref, *at_f):
        place = (slice(None), *at_f)
        return jnp.concatenate(
            [ref[(slice(4 * g, 4 * g + 4), *place[1:], b)] for g in range(groups) for b in range(2)],
            axis=0,
        )

    def group(g):
        return slice(8 * g, 8 * g + 8)

    for f in range(freqs):
        x_s[f] = rows_of(x0_s, at(f))
    power, smooth = power_s[...], smooth_s[...]
    row = lax.broadcasted_iota(jnp.int32, (2 * modes, width), 0)
    own = lax.broadcasted_iota(jnp.int32, (2 * modes, width), 1) // rank == row // 8 * 4 + row % 4
    sign = jnp.where(row % 8 < 4, 1.0, -1.0)
    for i, f in enumerate(matrix):
        levels = noise_s[:, at(f), :]
        levels = jnp.concatenate(
            [levels[4 * g:4 * g + 4] for g in range(groups) for _ in range(2)], axis=0
        )
        mask_s[i] = jnp.where(own, jnp.concatenate([levels] * modes, axis=1), 0.0)
    unit = (
        lax.broadcasted_iota(jnp.int32, (rank, rank), 0)
        == lax.broadcasted_iota(jnp.int32, (rank, rank), 1)
    )
    for i, f in enumerate(vector):
        levels = noise_s[:, at(f), :]
        for m in range(modes):
            column = jnp.sum(jnp.where(unit, levels[m:m + 1], 0.0), axis=1, keepdims=True)
            column_s[i, m] = jnp.broadcast_to(column, (rank, 128))

    def swapped(x):
        return jnp.concatenate([pltpu.roll(x[group(g)], 4, 0) for g in range(groups)], axis=0)

    def matrix_project(f, field):
        i = matrix.index(f)
        seen = times(field, high_s[i], low_s[i], True)
        parts = seen[:, :width] + sign * swapped(seen[:, width:])
        return parts, mask_s[i] * parts

    def matrix_back(f, seen):
        i = matrix.index(f)
        weighted = jnp.concatenate([seen[1], -sign * swapped(seen[1])], axis=1)
        return times(weighted, high_s[i], low_s[i], False)

    def wide(x):
        return jnp.concatenate([x] * (ell // 128), axis=1)

    def owned(f):
        return (lambda m, a: beam_s[f, m, a]), (lambda m: column_s[vector.index(f), m])

    lent = (lambda m, a: lent_beam_s[m, a]), (lambda m: lent_column_s[m])

    def group_project(source, g, field):
        beam_of, column_of = source
        parts = []
        for j in range(4):
            m = 4 * g + j
            real_beam, imaginary_beam = beam_of(m, 0), beam_of(m, 1)
            real_field, imaginary_field = field[j:j + 1], field[4 + j:5 + j]
            levels = column_of(m)
            real = jnp.sum(
                real_beam * real_field + imaginary_beam * imaginary_field, axis=1, keepdims=True
            )
            imaginary = jnp.sum(
                real_beam * imaginary_field - imaginary_beam * real_field, axis=1, keepdims=True
            )
            parts.append((real, imaginary, levels * real, levels * imaginary))
        return parts

    def group_back(source, g, parts):
        beam_of, _ = source
        reals, imaginaries = [], []
        for j, (_, _, real, imaginary) in enumerate(parts):
            m = 4 * g + j
            real, imaginary = wide(real), wide(imaginary)
            real_beam, imaginary_beam = beam_of(m, 0), beam_of(m, 1)
            for found, value in (
                (reals, real_beam * real - imaginary_beam * imaginary),
                (imaginaries, real_beam * imaginary + imaginary_beam * real),
            ):
                found.append(sum(value[k:k + 8] for k in range(0, rank, 8)))
        return folded(reals + imaginaries)

    def group_beam(source, g, field):
        return group_back(source, g, group_project(source, g, field))

    def project(f, ref):
        if f in matrix:
            return matrix_project(f, ref[f])
        return [group_project(owned(f), g, ref[f, group(g)]) for g in range(groups)]

    def back(f, seen):
        if f in matrix:
            return matrix_back(f, seen)
        return jnp.concatenate([group_back(owned(f), g, seen[g]) for g in range(groups)], axis=0)

    def apply_beam(fs, ref):
        fs = [f for f in fs if f in matrix] + [f for f in fs if f in vector]
        seen = [project(f, ref) for f in fs]
        return {f: back(f, found) for f, found in zip(fs, seen)}

    def count(f):
        value = float(f > 0) + float(f < last) + float(nf > 1 and f == 0)
        if two_sided and f == last:
            value = value + jnp.where(has_far, 1.0, 0.0)
        return value

    def local_prior(f, ref, rows=slice(None)):
        value = count(f) * ref[f, rows]
        if f > 0:
            value = value - ref[f - 1, rows]
        if f < last:
            value = value - ref[f + 1, rows]
        return power * ref[f, rows] + smooth * value

    for f in edges:
        beam_copies[f].wait()
    rhs_copy.wait()
    for i, f in enumerate(edges):
        for g in range(groups):
            rows = group(g)
            image = group_beam(owned(f), g, x_s[f, rows])
            y_s[i, rows] = rows_of(rhs_s, at(f))[rows] - image - local_prior(f, x_s, rows)
    first, rest = [], inner
    if paired:
        even_only([near_copy(1, g) for g in range(groups)] + [lend(k) for k in range(3)])

        @pl.when(helper)
        def _():
            for g in range(1, groups):
                near_copy(0, g).start()

        first, rest = inner[:1], inner[1:]
    else:
        for g in range(groups):
            send(1, g)

    for f in first:
        beam_copies[f].wait()
        r_s[f] = rows_of(rhs_s, at(f)) - back(f, project(f, x_s)) - local_prior(f, x_s)
    if paired:
        even_only([lend(3)])

        @pl.when(helper)
        def _():
            for g in range(groups):
                near_copy(1, g).start()

    for f in rest:
        beam_copies[f].wait()
    for i, f in enumerate(matrix):
        for a in range(2):
            rows = slice(a * width, (a + 1) * width)
            high, low = split(beam_s[f, :, a].reshape(width, ell))
            high_s[i, rows] = high
            low_s[i, rows] = low
    for f, image in apply_beam(rest, x_s).items():
        r_s[f] = rows_of(rhs_s, at(f)) - image - local_prior(f, x_s)
    for f, image in apply_beam(inner, r_s).items():
        u_s[f] = image + local_prior(f, r_s) if f in apart else image
    advance()

    def complete(i, f, g):
        rows = group(g)
        halo = jnp.concatenate([first_s[i, 4 * g:4 * g + 4, b, :] for b in range(2)], axis=0)
        r_s[f, rows] = y_s[i, rows] + smooth * halo

    def edge_image(f, g):
        rows = group(g)
        return group_beam(owned(f), g, r_s[f, rows]) + local_prior(f, r_s, rows)

    if paired:
        @pl.when(helper)
        def _():
            for g in range(groups):
                arrive(0, g)
                complete(0, 0, g)
                ahead_s[group(g)] = edge_image(0, g)
                ahead_copy(g).start()
            for g in range(groups):
                first_copy(g).wait_recv()
                hand_copy(g).start()
                if g == 0:
                    for k in range(4):
                        lend(k).wait_recv()
                rows = group(g)
                halo = jnp.concatenate([lent_first_s[4 * g:4 * g + 4, b, :] for b in range(2)], axis=0)
                r = lent_y_s[rows] + smooth * halo
                local = power * r + smooth * (count(0) * r - lent_r_s[rows])
                lent_v_s[rows] = group_beam(lent, g, r) + local
                cross_copy(g).start()

    seen = {f: project(f, u_s) for f in apart}
    grouped = [f for f in beside_edge if f in vector]
    whole = [f for f in beside_edge if f in matrix]
    seen |= {f: [] for f in grouped + edges}
    zero = jnp.zeros((8, ell), F32)
    sums = [zero, zero, zero, zero]
    column_part = jnp.zeros((rank, 128), F32)

    def add_up(g, sums, column_part):
        rows = group(g)
        norm, curve, square, cube = sums
        for f in inner + edges:
            if f in vector:
                for real, imaginary, real_weighted, imaginary_weighted in seen[f][g]:
                    column_part = column_part + (real * real_weighted + imaginary * imaginary_weighted)
            r, u = r_s[f, rows], u_s[f, rows]
            w = local_prior(f, u_s, rows)
            w_s[f, rows] = w
            norm = norm + r * r
            curve = curve + r * u
            square = square + u * u
            cube = cube + u * w
        return [norm, curve, square, cube], column_part

    def finish_edges(g):
        rows = group(g)
        for i, f in enumerate(edges):
            u_s[f, rows] = v_s[i, rows] - beside(
                i, smooth * (halo_s[0, i, rows] + smooth * x_s[f, rows])
            )
            seen[f].append(group_project(owned(f), g, u_s[f, rows]))

    for g in range(groups):
        rows = group(g)
        if paired:
            pl.when(jnp.logical_not(helper))(lambda: arrive(0, g))
            arrive(1, g)
        else:
            arrive(0, g)
        for i, f in enumerate(edges):
            complete(i, f, g)
        for i, f in enumerate(edges):
            v_s[i, rows] = edge_image(f, g)
        if not paired:
            send(2, g)
        for f in grouped:
            u_s[f, rows] = u_s[f, rows] + local_prior(f, r_s, rows)
            seen[f].append(group_project(owned(f), g, u_s[f, rows]))
        if paired:
            finish_edges(g)
            pull_s[rows] = smooth * u_s[0, rows]
            if not whole:
                sums, column_part = add_up(g, sums, column_part)
    for f in whole:
        u_s[f] = u_s[f] + local_prior(f, r_s)
        seen[f] = project(f, u_s)
    if paired:
        even_only([pull_copy()])
    else:
        for g in range(groups):
            arrive(1, g)
            finish_edges(g)
    if whole or not paired:
        for g in range(groups):
            sums, column_part = add_up(g, sums, column_part)
    beam_part = jnp.zeros((2 * modes, width), F32)
    for f in matrix:
        beam_part = beam_part + seen[f][0] * seen[f][1]
    lane = lax.broadcasted_iota(jnp.int32, (1, 128), 1)
    message = jnp.zeros((1, 128), F32)
    for i, part in enumerate(sums):
        total = total_of(part)
        if i == 3:
            total = total + total_of(beam_part) + jnp.sum(column_part, axis=0, keepdims=True)
        message = jnp.where(lane == i, total, message)
    if paired:
        message = jnp.where(lane == 4 + my_f, total_of(smooth * r_s[0] * pull_s[...]), message)
    message_s[0] = message
    early_s[me] = message

    while steps:
        advance()

    def share(source, target, slot, turn, device):
        pltpu.make_async_remote_copy(
            src_ref=message_s.at[source], dst_ref=target.at[slot],
            send_sem=sum_send.at[turn], recv_sem=sum_recv.at[turn],
            device_id=device, device_id_type=MESH,
        ).start()

    def share_all(source, target, slot, turn, stride):
        if n > 64:
            def body(i, carry):
                ma, f = my_ma + i * stride // nf, my_f + i * stride % nf
                share(source, target, slot, turn, (lax.rem(ma, nma), lax.rem(f, nf)))
                return carry

            lax.fori_loop(1, n // stride, body, 0)
        else:
            for mask in sorted(range(stride, n, stride), key=lambda m: (-(m // nf // 2), m)):
                device = partner([bit for bit in range(bits) if mask >> bit & 1])
                share(source, target, slot, turn, device)

    def landed(target, sem, rows):
        if rows:
            rows = target.at[pl.ds(0, rows)]
            pltpu.make_async_copy(rows, rows, sem).wait()

    def lanes_of(x):
        x = jnp.sum(x, axis=0, keepdims=True)
        return sum(x[:, i:i + 128] for i in range(0, ell, 128))

    share_all(0, early_s, me, 0, 1)
    if paired:
        even_only([near_copy(2, g) for g in range(groups)])
    for f in matrix + vector:
        w_s[f] = w_s[f] + back(f, seen[f])

    late_rows = late_s.shape[0]
    if paired:
        @pl.when(helper)
        def _():
            cross = jnp.zeros((8, ell), F32)
            for g in range(groups):
                arrive(2, g)
                cross = cross + pull_s[group(g)] * halo_s[1, 0, group(g)]
            pull_copy().wait_recv()
            for g in range(groups):
                cross_copy(g).wait_recv()
                cross = cross + partner_s[group(g)] * cross_s[group(g)]
            message = lanes_of(cross)
            late_s[my_ma // 2] = message
            message_s[1] = message
            share_all(1, late_s, my_ma // 2, 1, nf)
            for g in range(groups):
                cross_copy(g).wait_send()

        @pl.when(jnp.logical_not(helper))
        def _():
            for g in range(groups):
                arrive(2, g)
            pull_copy().wait_send()
            for k in range(4):
                lend(k).wait_send()
            for g in range(groups):
                first_copy(g).wait_send()

        w_s[0] = w_s[0] - smooth * (halo_s[1, 0] - smooth * r_s[0])
    else:
        cross = jnp.zeros((8, ell), F32)
        nexts = []
        for g in range(groups):
            arrive(2, g)
            rows = group(g)
            for i, f in enumerate(edges):
                pull = beside(i, smooth * (halo_s[1, i, rows] - smooth * r_s[f, rows]))
                nexts.append((f, rows, pull))
                cross = cross + pull * u_s[f, rows]
        message = lanes_of(cross)
        late_s[me] = message
        message_s[1] = message
        share_all(1, late_s, me, 1, 1)
        for f, rows, pull in nexts:
            w_s[f, rows] = w_s[f, rows] - pull

    if paired:
        for g in range(groups):
            for kind in (1, 2):
                sent(kind, g)

        @pl.when(helper)
        def _():
            for g in range(groups):
                sent(0, g)
                hand_copy(g).wait_send()
    else:
        for kind in range(3):
            for g in range(groups):
                sent(kind, g)
    for source, target in ((r_s, r_out_s), (u_s, u_out_s), (w_s, w_out_s)):
        for f in range(freqs):
            value = source[f]
            for g in range(groups):
                for b in range(2):
                    start = 8 * g + 4 * b
                    target[4 * g:4 * g + 4, at(f), b, :] = value[start:start + 4]

    landed(early_s, sum_send.at[0], n - 1)
    landed(early_s, sum_recv.at[0], n - 1)
    if paired:
        @pl.when(helper)
        def _():
            rows = early_s.at[pl.ds(0, nma - 1)]
            pltpu.make_async_copy(rows, rows, sum_send.at[1]).wait()
            landed(late_s, sum_recv.at[1], late_rows - 1)

        pl.when(jnp.logical_not(helper))(lambda: landed(late_s, sum_recv.at[1], late_rows))
    else:
        landed(late_s, sum_send.at[1], late_rows - 1)
        landed(late_s, sum_recv.at[1], late_rows - 1)
    def rows_total(ref):
        if ref.shape[0] > 64:
            return jnp.sum(ref[...], axis=0)
        return tree([ref[k] for k in range(ref.shape[0])])

    total = rows_total(early_s)
    m0, m1, m2, m3, known = (
        jnp.sum(jnp.where(lane == i, total, 0.0), axis=1, keepdims=True)
        for i in (0, 1, 2, 3, 4 + my_f)
    )
    crossed = jnp.sum(rows_total(late_s), axis=1, keepdims=True)
    m3 = m3 - 2.0 * (crossed - known) if paired else m3 - crossed
    inverse = 1.0 / m1
    step = m0 * inverse
    drop = step * m2 - m1
    growth = drop * inverse
    curve_next = m1 - 2.0 * step * m2 + step * step * m3
    step_next = step * drop / (curve_next - growth * drop)
    c = step + step_next * (1.0 + growth)
    e = step * step_next
    for m in range(modes):
        r, u = r_out_s[m], u_out_s[m]
        sol_s[m] = x0_s[m] + c * r - e * u
        res_s[m] = r - c * u + e * w_out_s[m]


def scoped_kernel(nma, nf, sides, *refs):
    modes, freqs = refs[0].shape[:2]
    dma = pltpu.SemaphoreType.DMA
    pl.run_scoped(
        functools.partial(kernel, nma, nf, *refs),
        dma((7,)), dma((freqs,)), dma((3, modes // 4, sides)), dma((2 * (modes // 4) + 5,)),
        dma((modes // 4,)), dma((2,)),
    )


def write_out(sol_in, res_in, sol_out, res_out):
    def body(sem):
        copies = [
            pltpu.make_async_copy(sol_in, sol_out, sem.at[0]),
            pltpu.make_async_copy(res_in, res_out, sem.at[1]),
        ]
        for copy in copies:
            copy.start()
        for copy in copies:
            copy.wait()

    pl.run_scoped(body, pltpu.SemaphoreType.DMA((2,)))


def shards(right_side, start_field, beam, noise, inv_power, smooth):
    nma, nf = lax.axis_size("ma"), lax.axis_size("freq")
    modes, freqs, _, ell = right_side.shape
    rank = beam.shape[3]
    width = modes * rank
    sides = 2 if nf > 2 else 1
    vmem_spec = pl.BlockSpec(memory_space=pltpu.VMEM)
    any_spec = pl.BlockSpec(memory_space=pl.ANY)
    field = pltpu.VMEM(right_side.shape, F32)
    edge = pltpu.VMEM((sides, modes, 2, ell), F32)
    slab = pltpu.VMEM((freqs, 2 * modes, ell), F32)
    edge_field = pltpu.VMEM((2 * modes, ell), F32)
    edge_slab = pltpu.VMEM((sides, 2 * modes, ell), F32)
    vector = max(min(nf - 1, 2), freqs // 2)
    matrix = max(freqs - vector, 1)
    half = pltpu.VMEM((matrix, 2 * width, ell), BF16)
    outs = pl.pallas_call(
        functools.partial(scoped_kernel, nma, nf, sides),
        out_shape=[field] * 2,
        in_specs=[any_spec] * 6,
        out_specs=[vmem_spec] * 2,
        scratch_shapes=[
            field, field, edge,
            pltpu.VMEM((freqs, modes, 2, rank, ell), F32),
            pltpu.VMEM(noise.shape, F32),
            pltpu.VMEM((1, ell), F32), pltpu.VMEM((1, ell), F32),
            half, half,
            slab, edge_slab, slab, edge_slab, slab, slab,
            pltpu.VMEM((matrix, 2 * modes, width), F32),
            pltpu.VMEM((vector, modes, rank, 128), F32),
            edge,
            pltpu.VMEM((2, sides, 2 * modes, ell), F32),
            field, field, field,
            edge_field, edge_field, edge_field,
            pltpu.VMEM((modes, 2, rank, ell), F32), pltpu.VMEM((modes, rank, 128), F32),
            edge_field, edge_field, pltpu.VMEM((modes, 2, ell), F32), edge_field, edge_field,
            pltpu.VMEM((2, 1, 128), F32),
            pltpu.VMEM((nma * nf, 1, 128), F32),
            pltpu.VMEM((nma // 2 if nf == 2 and nma % 2 == 0 and freqs > 1 else nma * nf, 1, 128), F32),
            pltpu.SemaphoreType.DMA((3, modes // 4, sides)),
            pltpu.SemaphoreType.DMA((2 * (modes // 4) + 5,)),
            pltpu.SemaphoreType.DMA((2,)),
            pltpu.SemaphoreType.REGULAR((max((nma * nf).bit_length() - 4, 1),)),
        ],
        compiler_params=pltpu.CompilerParams(
            collective_id=0, has_side_effects=True, vmem_limit_bytes=67043328 - 2 * right_side.size * 4
        ),
        name="solve",
    )(right_side, start_field, beam, noise, inv_power[None], smooth[None])
    return pl.pallas_call(
        write_out,
        out_shape=[jax.ShapeDtypeStruct(right_side.shape, F32)] * 2,
        in_specs=[vmem_spec] * 2,
        out_specs=[any_spec] * 2,
        compiler_params=pltpu.CompilerParams(vmem_limit_bytes=1024 * 1024),
        name="write_out",
    )(*outs)


def solution(mesh):
    in_specs = (
        P("ma", "freq", None, None),
        P("ma", "freq", None, None),
        P("ma", "freq", None, None, None),
        P("ma", "freq", None),
        P(),
        P(),
    )
    out_specs = (P("ma", "freq", None, None), P("ma", "freq", None, None))
    return jax.shard_map(shards, mesh=mesh, in_specs=in_specs, out_specs=out_specs, check_vma=False)
```

```python
import functools

import jax
import jax.numpy as jnp
from jax import lax
from jax.experimental import pallas as pl
from jax.experimental.pallas import tpu as pltpu
from jax.sharding import PartitionSpec as P

MESH = pl.DeviceIdType.MESH
F32, BF16 = jnp.float32, jnp.bfloat16


def split(x):
    high = x.astype(BF16)
    return high, (x - high.astype(F32)).astype(BF16)


def times(x, high, low, transposed):
    dims = (((1,), (1 if transposed else 0,)), ((), ()))
    rows = x.shape[0]
    x_high, x_low = split(x)
    both = jnp.concatenate([x_high, x_low], axis=0)
    main = lax.dot_general(both, high, dims, preferred_element_type=F32)
    rest = lax.dot_general(x_high, low, dims, preferred_element_type=F32)
    return main[:rows] + (main[rows:] + rest)


def folded(parts):
    row = lax.broadcasted_iota(jnp.int32, parts[0].shape, 0)
    upper = row < 4
    fours = [
        jnp.where(upper, parts[s], parts[s + 4])
        + pltpu.roll(jnp.where(upper, parts[s + 4], parts[s]), 4, 0)
        for s in range(4)
    ]
    even = row // 2 % 2 == 0
    twos = [
        jnp.where(
            even, fours[s] + pltpu.roll(fours[s], 6, 0), fours[s + 2] + pltpu.roll(fours[s + 2], 2, 0)
        )
        for s in range(2)
    ]
    return jnp.where(
        row % 2 == 0, twos[0] + pltpu.roll(twos[0], 7, 0), twos[1] + pltpu.roll(twos[1], 1, 0)
    )


def tree(parts):
    while len(parts) > 1:
        half = len(parts) // 2
        parts = [parts[k] + parts[half + k] for k in range(half)] + parts[2 * half:]
    return parts[0]


def total_of(x):
    return jnp.sum(jnp.sum(x, axis=0, keepdims=True), axis=1, keepdims=True)


def kernel(
    nma, nf, rhs_in, x0_in, beam_in, noise_in, power_in, smooth_in, sol_s, res_s,
    rhs_s, x0_s, edge_s, beam_s, noise_s, power_s, smooth_s,
    high_s, low_s, x_s, y_s, r_s, v_s, u_s, w_s, mask_s, column_s, first_s, halo_s,
    r_out_s, u_out_s, w_out_s, pull_s, partner_s, cross_s,
    lent_beam_s, lent_column_s, lent_y_s, lent_r_s, lent_first_s, lent_v_s, ahead_s,
    message_s, early_s, late_s,
    halo_recv, pair_recv, sum_recv, word_sem, in_sem, beam_sem, halo_send, pair_send, hand_send, sum_send,
):
    modes, freqs, _, ell = rhs_in.shape
    rank = beam_in.shape[3]
    width = modes * rank
    n = nma * nf
    my_ma, my_f = lax.axis_index("ma"), lax.axis_index("freq")
    me = my_ma * nf + my_f
    last = freqs - 1
    two_sided = nf > 2
    paired = nf == 2 and nma % 2 == 0 and freqs > 3
    helper = my_ma % 2 == 1
    groups = modes // 4
    edges = [0, last][:min(nf - 1, 2)]
    inner = [f for f in range(freqs) if f not in edges]
    beside_edge = [f for f in inner if f - 1 in edges or f + 1 in edges]
    apart = [f for f in inner if f not in beside_edge]
    vector = edges + inner[:max(freqs // 2 - len(edges), 0)]
    matrix = [f for f in range(freqs) if f not in vector]

    def at(g):
        return jnp.where(my_f == 0, last - g, g)

    edge_copies = [
        pltpu.make_async_copy(x0_in.at[:, at(f)], edge_s.at[i], in_sem.at[i])
        for i, f in enumerate(edges)
    ]
    x0_copy = pltpu.make_async_copy(x0_in, x0_s, in_sem.at[2])
    rhs_copy = pltpu.make_async_copy(rhs_in, rhs_s, in_sem.at[3])
    small = [
        pltpu.make_async_copy(power_in, power_s, in_sem.at[4]),
        pltpu.make_async_copy(smooth_in, smooth_s, in_sem.at[5]),
        pltpu.make_async_copy(noise_in, noise_s, in_sem.at[6]),
    ]
    beam_copies = [
        pltpu.make_async_copy(beam_in.at[:, at(f)], beam_s.at[f], beam_sem.at[f])
        for f in range(freqs)
    ]
    for copy in edge_copies:
        copy.start()

    def flip(bit):
        if bit == 0 and nf == 2:
            return 1 - 2 * my_f
        d = 1 << (bit if bit < freq_bits else bit - freq_bits)
        place = my_f if bit < freq_bits else my_ma
        return d * (1 - 2 * (place // d % 2))

    def partner(bits):
        return (
            my_ma + sum(flip(bit) for bit in bits if bit >= freq_bits),
            my_f + sum(flip(bit) for bit in bits if bit < freq_bits),
        )

    freq_bits = nf.bit_length() - 1
    bits = freq_bits + nma.bit_length() - 1
    close = min(bits, 3)
    barrier = pltpu.get_barrier_semaphore()

    def greet(device):
        pl.semaphore_signal(barrier, inc=1, device_id=device, device_id_type=MESH)

    greeted = []
    for mask in range(1, 1 << close):
        greeted.append(partner([bit for bit in range(close) if mask >> bit & 1]))
        greet(greeted[-1])
        if mask == 1:
            for copy in [beam_copies[f] for f in edges] + [x0_copy, rhs_copy] + small:
                copy.start()
    word = [partner([bit]) for bit in range(close, bits)]
    for device in word:
        greet(device)
    greeted += word
    words = len(word)
    near = jnp.where(my_f == 0, 1, my_f - 1)
    has_far = (my_f > 0) & (my_f < nf - 1)
    expected = len(greeted)
    if nf > 2:
        pl.when(my_f > 0)(lambda: greet((my_ma, my_f - 1)))
        pl.when(my_f < nf - 1)(lambda: greet((my_ma, my_f + 1)))
        expected = expected + jnp.minimum(my_f, 1) + jnp.minimum(nf - 1 - my_f, 1)

    steps = list(range(words + 1))

    def advance():
        if steps:
            step = steps.pop(0)
            if step > 0:
                pl.semaphore_wait(word_sem.at[step - 1], 1)
            if step < words:
                pl.semaphore_signal(
                    word_sem.at[step], inc=1, device_id=word[step], device_id_type=MESH
                )

    def piece(kind, g):
        if kind == 0:
            rows = pl.ds(4 * g, 4)
            return (lambda i: edge_s.at[i, rows]), (lambda i: first_s.at[i, rows])
        source = (y_s, v_s)[kind - 1]
        rows = pl.ds(8 * g, 8)
        return (lambda i: source.at[i, rows]), (lambda i: halo_s.at[kind - 1, i, rows])

    def near_copy(kind, g):
        source, target = piece(kind, g)
        side = jnp.minimum(my_f // 2, 1) if two_sided else 0
        return pltpu.make_async_remote_copy(
            src_ref=source(0), dst_ref=target(side),
            send_sem=halo_send.at[kind, g, 0], recv_sem=halo_recv.at[kind, g, side],
            device_id=(my_ma, near), device_id_type=MESH,
        )

    def far_copy(kind, g):
        source, target = piece(kind, g)
        return pltpu.make_async_remote_copy(
            src_ref=source(1), dst_ref=target(0),
            send_sem=halo_send.at[kind, g, 1], recv_sem=halo_recv.at[kind, g, 0],
            device_id=(my_ma, my_f + 1), device_id_type=MESH,
        )

    def arrival(kind, g, side):
        slot = piece(kind, g)[1](side)
        return pltpu.make_async_copy(slot, slot, halo_recv.at[kind, g, side])

    def send(kind, g):
        if nf > 1:
            near_copy(kind, g).start()
        if two_sided:
            pl.when(has_far)(lambda: far_copy(kind, g).start())

    def arrive(kind, g):
        if nf > 1:
            arrival(kind, g, 0).wait()
        if two_sided:
            pl.when(has_far)(lambda: arrival(kind, g, 1).wait())

    def sent(kind, g):
        if nf > 1:
            near_copy(kind, g).wait_send()
        if two_sided:
            pl.when(has_far)(lambda: far_copy(kind, g).wait_send())

    def pair_copy(k, source, target, ma, f):
        return pltpu.make_async_remote_copy(
            src_ref=source, dst_ref=target, send_sem=pair_send.at[k], recv_sem=pair_recv.at[k],
            device_id=(ma, f), device_id_type=MESH,
        )

    def lend(k):
        source = (lambda: beam_s.at[0], lambda: column_s.at[0], lambda: y_s.at[0], lambda: r_s.at[1])[k]
        target = (lent_beam_s, lent_column_s, lent_y_s, lent_r_s)[k]
        return pair_copy(k, source(), target, my_ma + 1, my_f)

    def pull_copy():
        return pair_copy(4, pull_s, partner_s, my_ma + 1, my_f)

    def first_copy(g):
        rows = pl.ds(4 * g, 4)
        return pair_copy(5 + g, edge_s.at[0, rows], lent_first_s.at[rows], my_ma + 1, 1 - my_f)

    def cross_copy(g):
        rows = pl.ds(8 * g, 8)
        return pair_copy(5 + groups + g, lent_v_s.at[rows], cross_s.at[rows], my_ma, 1 - my_f)

    def ahead_copy(g):
        rows = pl.ds(8 * g, 8)
        return pltpu.make_async_remote_copy(
            src_ref=ahead_s.at[rows], dst_ref=halo_s.at[1, 0, rows],
            send_sem=halo_send.at[2, g, 0], recv_sem=halo_recv.at[2, g, 0],
            device_id=(my_ma, 1 - my_f), device_id_type=MESH,
        )

    def hand_copy(g):
        rows = pl.ds(4 * g, 4)
        return pltpu.make_async_remote_copy(
            src_ref=lent_first_s.at[rows], dst_ref=first_s.at[0, rows],
            send_sem=hand_send.at[g], recv_sem=halo_recv.at[0, g, 0],
            device_id=(my_ma - 1, my_f), device_id_type=MESH,
        )

    def even_only(copies):
        @pl.when(jnp.logical_not(helper))
        def _():
            for copy in copies:
                copy.start()

    def beside(i, value):
        return jnp.where(has_far, value, 0.0) if i else value

    if two_sided:
        @pl.when(jnp.logical_not(has_far))
        def _():
            first_s[1] = jnp.zeros_like(first_s[1])
            halo_s[:, 1] = jnp.zeros_like(halo_s[:, 1])

    for copy in edge_copies:
        copy.wait()
    for f in inner:
        beam_copies[f].start()
    pl.semaphore_wait(barrier, expected)
    if paired:
        even_only([first_copy(g) for g in range(groups)])

        pl.when(helper)(lambda: near_copy(0, 0).start())
    else:
        for g in range(groups):
            send(0, g)
    advance()

    x0_copy.wait()
    for copy in small:
        copy.wait()
    def rows_of(ref, *at_f):
        place = (slice(None), *at_f)
        return jnp.concatenate(
            [ref[(slice(4 * g, 4 * g + 4), *place[1:], b)] for g in range(groups) for b in range(2)],
            axis=0,
        )

    def group(g):
        return slice(8 * g, 8 * g + 8)

    for f in range(freqs):
        x_s[f] = rows_of(x0_s, at(f))
    power, smooth = power_s[...], smooth_s[...]
    row = lax.broadcasted_iota(jnp.int32, (2 * modes, width), 0)
    own = lax.broadcasted_iota(jnp.int32, (2 * modes, width), 1) // rank == row // 8 * 4 + row % 4
    sign = jnp.where(row % 8 < 4, 1.0, -1.0)
    for i, f in enumerate(matrix):
        levels = noise_s[:, at(f), :]
        levels = jnp.concatenate(
            [levels[4 * g:4 * g + 4] for g in range(groups) for _ in range(2)], axis=0
        )
        mask_s[i] = jnp.where(own, jnp.concatenate([levels] * modes, axis=1), 0.0)
    unit = (
        lax.broadcasted_iota(jnp.int32, (rank, rank), 0)
        == lax.broadcasted_iota(jnp.int32, (rank, rank), 1)
    )
    for i, f in enumerate(vector):
        levels = noise_s[:, at(f), :]
        for m in range(modes):
            column = jnp.sum(jnp.where(unit, levels[m:m + 1], 0.0), axis=1, keepdims=True)
            column_s[i, m] = jnp.broadcast_to(column, (rank, 128))

    def swapped(x):
        return jnp.concatenate([pltpu.roll(x[group(g)], 4, 0) for g in range(groups)], axis=0)

    def matrix_project(f, field):
        i = matrix.index(f)
        seen = times(field, high_s[i], low_s[i], True)
        parts = seen[:, :width] + sign * swapped(seen[:, width:])
        return parts, mask_s[i] * parts

    def matrix_back(f, seen):
        i = matrix.index(f)
        weighted = jnp.concatenate([seen[1], -sign * swapped(seen[1])], axis=1)
        return times(weighted, high_s[i], low_s[i], False)

    def wide(x):
        return jnp.concatenate([x] * (ell // 128), axis=1)

    def owned(f):
        return (lambda m, a: beam_s[f, m, a]), (lambda m: column_s[vector.index(f), m])

    lent = (lambda m, a: lent_beam_s[m, a]), (lambda m: lent_column_s[m])

    def group_project(source, g, field):
        beam_of, column_of = source
        parts = []
        for j in range(4):
            m = 4 * g + j
            real_beam, imaginary_beam = beam_of(m, 0), beam_of(m, 1)
            real_field, imaginary_field = field[j:j + 1], field[4 + j:5 + j]
            levels = column_of(m)
            real = jnp.sum(
                real_beam * real_field + imaginary_beam * imaginary_field, axis=1, keepdims=True
            )
            imaginary = jnp.sum(
                real_beam * imaginary_field - imaginary_beam * real_field, axis=1, keepdims=True
            )
            parts.append((real, imaginary, levels * real, levels * imaginary))
        return parts

    def group_back(source, g, parts):
        beam_of, _ = source
        reals, imaginaries = [], []
        for j, (_, _, real, imaginary) in enumerate(parts):
            m = 4 * g + j
            real, imaginary = wide(real), wide(imaginary)
            real_beam, imaginary_beam = beam_of(m, 0), beam_of(m, 1)
            for found, value in (
                (reals, real_beam * real - imaginary_beam * imaginary),
                (imaginaries, real_beam * imaginary + imaginary_beam * real),
            ):
                found.append(sum(value[k:k + 8] for k in range(0, rank, 8)))
        return folded(reals + imaginaries)

    def group_beam(source, g, field):
        return group_back(source, g, group_project(source, g, field))

    def project(f, ref):
        if f in matrix:
            return matrix_project(f, ref[f])
        return [group_project(owned(f), g, ref[f, group(g)]) for g in range(groups)]

    def back(f, seen):
        if f in matrix:
            return matrix_back(f, seen)
        return jnp.concatenate([group_back(owned(f), g, seen[g]) for g in range(groups)], axis=0)

    def apply_beam(fs, ref):
        fs = [f for f in fs if f in matrix] + [f for f in fs if f in vector]
        seen = [project(f, ref) for f in fs]
        return {f: back(f, found) for f, found in zip(fs, seen)}

    def count(f):
        value = float(f > 0) + float(f < last) + float(nf > 1 and f == 0)
        if two_sided and f == last:
            value = value + jnp.where(has_far, 1.0, 0.0)
        return value

    def local_prior(f, ref, rows=slice(None)):
        value = count(f) * ref[f, rows]
        if f > 0:
            value = value - ref[f - 1, rows]
        if f < last:
            value = value - ref[f + 1, rows]
        return power * ref[f, rows] + smooth * value

    for f in edges:
        beam_copies[f].wait()
    rhs_copy.wait()
    for i, f in enumerate(edges):
        for g in range(groups):
            rows = group(g)
            image = group_beam(owned(f), g, x_s[f, rows])
            y_s[i, rows] = rows_of(rhs_s, at(f))[rows] - image - local_prior(f, x_s, rows)
    first, rest = [], inner
    if paired:
        even_only([near_copy(1, g) for g in range(groups)] + [lend(k) for k in range(3)])

        @pl.when(helper)
        def _():
            for g in range(1, groups):
                near_copy(0, g).start()

        first, rest = inner[:1], inner[1:]
    else:
        for g in range(groups):
            send(1, g)

    for f in first:
        beam_copies[f].wait()
        r_s[f] = rows_of(rhs_s, at(f)) - back(f, project(f, x_s)) - local_prior(f, x_s)
    if paired:
        even_only([lend(3)])

        @pl.when(helper)
        def _():
            for g in range(groups):
                near_copy(1, g).start()

    for f in rest:
        beam_copies[f].wait()
    for i, f in enumerate(matrix):
        for a in range(2):
            rows = slice(a * width, (a + 1) * width)
            high, low = split(beam_s[f, :, a].reshape(width, ell))
            high_s[i, rows] = high
            low_s[i, rows] = low
    for f, image in apply_beam(rest, x_s).items():
        r_s[f] = rows_of(rhs_s, at(f)) - image - local_prior(f, x_s)
    for f, image in apply_beam(inner, r_s).items():
        u_s[f] = image + local_prior(f, r_s) if f in apart else image
    advance()

    def complete(i, f, g):
        rows = group(g)
        halo = jnp.concatenate([first_s[i, 4 * g:4 * g + 4, b, :] for b in range(2)], axis=0)
        r_s[f, rows] = y_s[i, rows] + smooth * halo

    def edge_image(f, g):
        rows = group(g)
        return group_beam(owned(f), g, r_s[f, rows]) + local_prior(f, r_s, rows)

    if paired:
        @pl.when(helper)
        def _():
            for g in range(groups):
                arrive(0, g)
                complete(0, 0, g)
                ahead_s[group(g)] = edge_image(0, g)
                ahead_copy(g).start()
            for g in range(groups):
                first_copy(g).wait_recv()
                hand_copy(g).start()
                if g == 0:
                    for k in range(4):
                        lend(k).wait_recv()
                rows = group(g)
                halo = jnp.concatenate([lent_first_s[4 * g:4 * g + 4, b, :] for b in range(2)], axis=0)
                r = lent_y_s[rows] + smooth * halo
                local = power * r + smooth * (count(0) * r - lent_r_s[rows])
                lent_v_s[rows] = group_beam(lent, g, r) + local
                cross_copy(g).start()

    seen = {f: project(f, u_s) for f in apart}
    grouped = [f for f in beside_edge if f in vector]
    whole = [f for f in beside_edge if f in matrix]
    seen |= {f: [] for f in grouped + edges}
    zero = jnp.zeros((8, ell), F32)
    sums = [zero, zero, zero, zero]
    column_part = jnp.zeros((rank, 128), F32)

    def add_up(g, sums, column_part):
        rows = group(g)
        norm, curve, square, cube = sums
        for f in inner + edges:
            if f in vector:
                for real, imaginary, real_weighted, imaginary_weighted in seen[f][g]:
                    column_part = column_part + (real * real_weighted + imaginary * imaginary_weighted)
            r, u = r_s[f, rows], u_s[f, rows]
            w = local_prior(f, u_s, rows)
            w_s[f, rows] = w
            norm = norm + r * r
            curve = curve + r * u
            square = square + u * u
            cube = cube + u * w
        return [norm, curve, square, cube], column_part

    def finish_edges(g):
        rows = group(g)
        for i, f in enumerate(edges):
            u_s[f, rows] = v_s[i, rows] - beside(
                i, smooth * (halo_s[0, i, rows] + smooth * x_s[f, rows])
            )
            seen[f].append(group_project(owned(f), g, u_s[f, rows]))

    for g in range(groups):
        rows = group(g)
        if paired:
            pl.when(jnp.logical_not(helper))(lambda: arrive(0, g))
            arrive(1, g)
        else:
            arrive(0, g)
        for i, f in enumerate(edges):
            complete(i, f, g)
        for i, f in enumerate(edges):
            v_s[i, rows] = edge_image(f, g)
        if not paired:
            send(2, g)
        for f in grouped:
            u_s[f, rows] = u_s[f, rows] + local_prior(f, r_s, rows)
            seen[f].append(group_project(owned(f), g, u_s[f, rows]))
        if paired:
            finish_edges(g)
            pull_s[rows] = smooth * u_s[0, rows]
            if not whole:
                sums, column_part = add_up(g, sums, column_part)
    for f in whole:
        u_s[f] = u_s[f] + local_prior(f, r_s)
        seen[f] = project(f, u_s)
    if paired:
        even_only([pull_copy()])
    else:
        for g in range(groups):
            arrive(1, g)
            finish_edges(g)
    if whole or not paired:
        for g in range(groups):
            sums, column_part = add_up(g, sums, column_part)
    beam_part = jnp.zeros((2 * modes, width), F32)
    for f in matrix:
        beam_part = beam_part + seen[f][0] * seen[f][1]
    lane = lax.broadcasted_iota(jnp.int32, (1, 128), 1)
    message = jnp.zeros((1, 128), F32)
    for i, part in enumerate(sums):
        total = total_of(part)
        if i == 3:
            total = total + total_of(beam_part) + jnp.sum(column_part, axis=0, keepdims=True)
        message = jnp.where(lane == i, total, message)
    if paired:
        message = jnp.where(lane == 4 + my_f, total_of(smooth * r_s[0] * pull_s[...]), message)
    message_s[0] = message
    early_s[me] = message

    while steps:
        advance()

    def share(source, target, slot, turn, device):
        pltpu.make_async_remote_copy(
            src_ref=message_s.at[source], dst_ref=target.at[slot],
            send_sem=sum_send.at[turn], recv_sem=sum_recv.at[turn],
            device_id=device, device_id_type=MESH,
        ).start()

    def share_all(source, target, slot, turn, stride):
        if n > 64:
            def body(i, carry):
                ma, f = my_ma + i * stride // nf, my_f + i * stride % nf
                share(source, target, slot, turn, (lax.rem(ma, nma), lax.rem(f, nf)))
                return carry

            lax.fori_loop(1, n // stride, body, 0)
        else:
            for mask in sorted(range(stride, n, stride), key=lambda m: (-(m // nf // 2), m)):
                device = partner([bit for bit in range(bits) if mask >> bit & 1])
                share(source, target, slot, turn, device)

    def landed(target, sem, rows):
        if rows:
            rows = target.at[pl.ds(0, rows)]
            pltpu.make_async_copy(rows, rows, sem).wait()

    def lanes_of(x):
        x = jnp.sum(x, axis=0, keepdims=True)
        return sum(x[:, i:i + 128] for i in range(0, ell, 128))

    share_all(0, early_s, me, 0, 1)
    if paired:
        even_only([near_copy(2, g) for g in range(groups)])
    for f in matrix + vector:
        w_s[f] = w_s[f] + back(f, seen[f])

    late_rows = late_s.shape[0]
    if paired:
        @pl.when(helper)
        def _():
            cross = jnp.zeros((8, ell), F32)
            for g in range(groups):
                arrive(2, g)
                cross = cross + pull_s[group(g)] * halo_s[1, 0, group(g)]
            pull_copy().wait_recv()
            for g in range(groups):
                cross_copy(g).wait_recv()
                cross = cross + partner_s[group(g)] * cross_s[group(g)]
            message = lanes_of(cross)
            late_s[my_ma // 2] = message
            message_s[1] = message
            share_all(1, late_s, my_ma // 2, 1, nf)
            for g in range(groups):
                cross_copy(g).wait_send()

        @pl.when(jnp.logical_not(helper))
        def _():
            for g in range(groups):
                arrive(2, g)
            pull_copy().wait_send()
            for k in range(4):
                lend(k).wait_send()
            for g in range(groups):
                first_copy(g).wait_send()

        w_s[0] = w_s[0] - smooth * (halo_s[1, 0] - smooth * r_s[0])
    else:
        cross = jnp.zeros((8, ell), F32)
        nexts = []
        for g in range(groups):
            arrive(2, g)
            rows = group(g)
            for i, f in enumerate(edges):
                pull = beside(i, smooth * (halo_s[1, i, rows] - smooth * r_s[f, rows]))
                nexts.append((f, rows, pull))
                cross = cross + pull * u_s[f, rows]
        message = lanes_of(cross)
        late_s[me] = message
        message_s[1] = message
        share_all(1, late_s, me, 1, 1)
        for f, rows, pull in nexts:
            w_s[f, rows] = w_s[f, rows] - pull

    if paired:
        for g in range(groups):
            for kind in (1, 2):
                sent(kind, g)

        @pl.when(helper)
        def _():
            for g in range(groups):
                sent(0, g)
                hand_copy(g).wait_send()
    else:
        for kind in range(3):
            for g in range(groups):
                sent(kind, g)
    for source, target in ((r_s, r_out_s), (u_s, u_out_s), (w_s, w_out_s)):
        for f in range(freqs):
            value = source[f]
            for g in range(groups):
                for b in range(2):
                    start = 8 * g + 4 * b
                    target[4 * g:4 * g + 4, at(f), b, :] = value[start:start + 4]

    landed(early_s, sum_send.at[0], n - 1)
    landed(early_s, sum_recv.at[0], n - 1)
    if paired:
        @pl.when(helper)
        def _():
            rows = early_s.at[pl.ds(0, nma - 1)]
            pltpu.make_async_copy(rows, rows, sum_send.at[1]).wait()
            landed(late_s, sum_recv.at[1], late_rows - 1)

        pl.when(jnp.logical_not(helper))(lambda: landed(late_s, sum_recv.at[1], late_rows))
    else:
        landed(late_s, sum_send.at[1], late_rows - 1)
        landed(late_s, sum_recv.at[1], late_rows - 1)
    def rows_total(ref):
        if ref.shape[0] > 64:
            return jnp.sum(ref[...], axis=0)
        return tree([ref[k] for k in range(ref.shape[0])])

    total = rows_total(early_s)
    m0, m1, m2, m3, known = (
        jnp.sum(jnp.where(lane == i, total, 0.0), axis=1, keepdims=True)
        for i in (0, 1, 2, 3, 4 + my_f)
    )
    crossed = jnp.sum(rows_total(late_s), axis=1, keepdims=True)
    m3 = m3 - 2.0 * (crossed - known) if paired else m3 - crossed
    inverse = 1.0 / m1
    step = m0 * inverse
    drop = step * m2 - m1
    growth = drop * inverse
    curve_next = m1 - 2.0 * step * m2 + step * step * m3
    step_next = step * drop / (curve_next - growth * drop)
    c = step + step_next * (1.0 + growth)
    e = step * step_next
    for m in range(modes):
        r, u = r_out_s[m], u_out_s[m]
        sol_s[m] = x0_s[m] + c * r - e * u
        res_s[m] = r - c * u + e * w_out_s[m]


def scoped_kernel(nma, nf, sides, *refs):
    modes, freqs = refs[0].shape[:2]
    dma = pltpu.SemaphoreType.DMA
    pl.run_scoped(
        functools.partial(kernel, nma, nf, *refs),
        dma((7,)), dma((freqs,)), dma((3, modes // 4, sides)), dma((2 * (modes // 4) + 5,)),
        dma((modes // 4,)), dma((2,)),
    )


def write_out(sol_in, res_in, sol_out, res_out):
    def body(sem):
        copies = [
            pltpu.make_async_copy(sol_in, sol_out, sem.at[0]),
            pltpu.make_async_copy(res_in, res_out, sem.at[1]),
        ]
        for copy in copies:
            copy.start()
        for copy in copies:
            copy.wait()

    pl.run_scoped(body, pltpu.SemaphoreType.DMA((2,)))


def shards(right_side, start_field, beam, noise, inv_power, smooth):
    nma, nf = lax.axis_size("ma"), lax.axis_size("freq")
    modes, freqs, _, ell = right_side.shape
    rank = beam.shape[3]
    width = modes * rank
    sides = 2 if nf > 2 else 1
    vmem_spec = pl.BlockSpec(memory_space=pltpu.VMEM)
    any_spec = pl.BlockSpec(memory_space=pl.ANY)
    field = pltpu.VMEM(right_side.shape, F32)
    edge = pltpu.VMEM((sides, modes, 2, ell), F32)
    slab = pltpu.VMEM((freqs, 2 * modes, ell), F32)
    edge_field = pltpu.VMEM((2 * modes, ell), F32)
    edge_slab = pltpu.VMEM((sides, 2 * modes, ell), F32)
    vector = max(min(nf - 1, 2), freqs // 2)
    matrix = max(freqs - vector, 1)
    half = pltpu.VMEM((matrix, 2 * width, ell), BF16)
    outs = pl.pallas_call(
        functools.partial(scoped_kernel, nma, nf, sides),
        out_shape=[field] * 2,
        in_specs=[any_spec] * 6,
        out_specs=[vmem_spec] * 2,
        scratch_shapes=[
            field, field, edge,
            pltpu.VMEM((freqs, modes, 2, rank, ell), F32),
            pltpu.VMEM(noise.shape, F32),
            pltpu.VMEM((1, ell), F32), pltpu.VMEM((1, ell), F32),
            half, half,
            slab, edge_slab, slab, edge_slab, slab, slab,
            pltpu.VMEM((matrix, 2 * modes, width), F32),
            pltpu.VMEM((vector, modes, rank, 128), F32),
            edge,
            pltpu.VMEM((2, sides, 2 * modes, ell), F32),
            field, field, field,
            edge_field, edge_field, edge_field,
            pltpu.VMEM((modes, 2, rank, ell), F32), pltpu.VMEM((modes, rank, 128), F32),
            edge_field, edge_field, pltpu.VMEM((modes, 2, ell), F32), edge_field, edge_field,
            pltpu.VMEM((2, 1, 128), F32),
            pltpu.VMEM((nma * nf, 1, 128), F32),
            pltpu.VMEM((nma // 2 if nf == 2 and nma % 2 == 0 and freqs > 3 else nma * nf, 1, 128), F32),
            pltpu.SemaphoreType.DMA((3, modes // 4, sides)),
            pltpu.SemaphoreType.DMA((2 * (modes // 4) + 5,)),
            pltpu.SemaphoreType.DMA((2,)),
            pltpu.SemaphoreType.REGULAR((max((nma * nf).bit_length() - 4, 1),)),
        ],
        compiler_params=pltpu.CompilerParams(
            collective_id=0, has_side_effects=True, vmem_limit_bytes=67043328 - 2 * right_side.size * 4
        ),
        name="solve",
    )(right_side, start_field, beam, noise, inv_power[None], smooth[None])
    return pl.pallas_call(
        write_out,
        out_shape=[jax.ShapeDtypeStruct(right_side.shape, F32)] * 2,
        in_specs=[vmem_spec] * 2,
        out_specs=[any_spec] * 2,
        compiler_params=pltpu.CompilerParams(vmem_limit_bytes=1024 * 1024),
        name="write_out",
    )(*outs)


def solution(mesh):
    in_specs = (
        P("ma", "freq", None, None),
        P("ma", "freq", None, None),
        P("ma", "freq", None, None, None),
        P("ma", "freq", None),
        P(),
        P(),
    )
    out_specs = (P("ma", "freq", None, None), P("ma", "freq", None, None))
    return jax.shard_map(shards, mesh=mesh, in_specs=in_specs, out_specs=out_specs, check_vma=False)
```

```python
import functools

import jax
import jax.numpy as jnp
from jax import lax
from jax.experimental import pallas as pl
from jax.experimental.pallas import tpu as pltpu
from jax.sharding import PartitionSpec as P

MESH = pl.DeviceIdType.MESH
F32, BF16 = jnp.float32, jnp.bfloat16


def split(x):
    high = x.astype(BF16)
    return high, (x - high.astype(F32)).astype(BF16)


def times(x, high, low, transposed):
    dims = (((1,), (1 if transposed else 0,)), ((), ()))
    rows = x.shape[0]
    x_high, x_low = split(x)
    both = jnp.concatenate([x_high, x_low], axis=0)
    main = lax.dot_general(both, high, dims, preferred_element_type=F32)
    rest = lax.dot_general(x_high, low, dims, preferred_element_type=F32)
    return main[:rows] + (main[rows:] + rest)


def folded(parts):
    row = lax.broadcasted_iota(jnp.int32, parts[0].shape, 0)
    upper = row < 4
    fours = [
        jnp.where(upper, parts[s], parts[s + 4])
        + pltpu.roll(jnp.where(upper, parts[s + 4], parts[s]), 4, 0)
        for s in range(4)
    ]
    even = row // 2 % 2 == 0
    twos = [
        jnp.where(
            even, fours[s] + pltpu.roll(fours[s], 6, 0), fours[s + 2] + pltpu.roll(fours[s + 2], 2, 0)
        )
        for s in range(2)
    ]
    return jnp.where(
        row % 2 == 0, twos[0] + pltpu.roll(twos[0], 7, 0), twos[1] + pltpu.roll(twos[1], 1, 0)
    )


def tree(parts):
    while len(parts) > 1:
        half = len(parts) // 2
        parts = [parts[k] + parts[half + k] for k in range(half)] + parts[2 * half:]
    return parts[0]


def total_of(x):
    return jnp.sum(jnp.sum(x, axis=0, keepdims=True), axis=1, keepdims=True)


def kernel(
    nma, nf, rhs_in, x0_in, beam_in, noise_in, power_in, smooth_in, sol_s, res_s,
    rhs_s, x0_s, edge_s, beam_s, noise_s, power_s, smooth_s,
    high_s, low_s, x_s, y_s, r_s, v_s, u_s, w_s, mask_s, column_s, first_s, halo_s,
    r_out_s, u_out_s, w_out_s, pull_s, partner_s, cross_s,
    lent_beam_s, lent_column_s, lent_y_s, lent_r_s, lent_first_s, lent_v_s, ahead_s,
    message_s, early_s, late_s,
    halo_recv, pair_recv, sum_recv, word_sem, in_sem, beam_sem, halo_send, pair_send, hand_send, sum_send,
):
    modes, freqs, _, ell = rhs_in.shape
    rank = beam_in.shape[3]
    width = modes * rank
    n = nma * nf
    my_ma, my_f = lax.axis_index("ma"), lax.axis_index("freq")
    me = my_ma * nf + my_f
    last = freqs - 1
    two_sided = nf > 2
    paired = nf == 2 and nma % 2 == 0 and freqs > 3
    helper = my_ma % 2 == 1
    groups = modes // 4
    edges = [0, last][:min(nf - 1, 2)]
    inner = [f for f in range(freqs) if f not in edges]
    beside_edge = [f for f in inner if f - 1 in edges or f + 1 in edges]
    apart = [f for f in inner if f not in beside_edge]
    vector = edges + inner[:max(freqs // 2 - len(edges), 0)]
    matrix = [f for f in range(freqs) if f not in vector]

    def at(g):
        return jnp.where(my_f == 0, last - g, g)

    edge_copies = [
        pltpu.make_async_copy(x0_in.at[:, at(f)], edge_s.at[i], in_sem.at[i])
        for i, f in enumerate(edges)
    ]
    x0_copy = pltpu.make_async_copy(x0_in, x0_s, in_sem.at[2])
    rhs_copy = pltpu.make_async_copy(rhs_in, rhs_s, in_sem.at[3])
    small = [
        pltpu.make_async_copy(power_in, power_s, in_sem.at[4]),
        pltpu.make_async_copy(smooth_in, smooth_s, in_sem.at[5]),
        pltpu.make_async_copy(noise_in, noise_s, in_sem.at[6]),
    ]
    beam_copies = [
        pltpu.make_async_copy(beam_in.at[:, at(f)], beam_s.at[f], beam_sem.at[f])
        for f in range(freqs)
    ]
    for copy in edge_copies:
        copy.start()

    def flip(bit):
        if bit == 0 and nf == 2:
            return 1 - 2 * my_f
        d = 1 << (bit if bit < freq_bits else bit - freq_bits)
        place = my_f if bit < freq_bits else my_ma
        return d * (1 - 2 * (place // d % 2))

    def partner(bits):
        return (
            my_ma + sum(flip(bit) for bit in bits if bit >= freq_bits),
            my_f + sum(flip(bit) for bit in bits if bit < freq_bits),
        )

    freq_bits = nf.bit_length() - 1
    bits = freq_bits + nma.bit_length() - 1
    close = min(bits, 3)
    barrier = pltpu.get_barrier_semaphore()

    def greet(device):
        pl.semaphore_signal(barrier, inc=1, device_id=device, device_id_type=MESH)

    greeted = []
    for mask in range(1, 1 << close):
        greeted.append(partner([bit for bit in range(close) if mask >> bit & 1]))
        greet(greeted[-1])
        if mask == 1:
            for copy in [beam_copies[f] for f in edges] + [x0_copy, rhs_copy] + small:
                copy.start()
    word = [partner([bit]) for bit in range(close, bits)]
    for device in word:
        greet(device)
    greeted += word
    words = len(word)
    near = jnp.where(my_f == 0, 1, my_f - 1)
    has_far = (my_f > 0) & (my_f < nf - 1)
    expected = len(greeted)
    if nf > 2:
        pl.when(my_f > 0)(lambda: greet((my_ma, my_f - 1)))
        pl.when(my_f < nf - 1)(lambda: greet((my_ma, my_f + 1)))
        expected = expected + jnp.minimum(my_f, 1) + jnp.minimum(nf - 1 - my_f, 1)

    steps = list(range(words + 1))

    def advance():
        if steps:
            step = steps.pop(0)
            if step > 0:
                pl.semaphore_wait(word_sem.at[step - 1], 1)
            if step < words:
                pl.semaphore_signal(
                    word_sem.at[step], inc=1, device_id=word[step], device_id_type=MESH
                )

    def piece(kind, g):
        if kind == 0:
            rows = pl.ds(4 * g, 4)
            return (lambda i: edge_s.at[i, rows]), (lambda i: first_s.at[i, rows])
        source = (y_s, v_s)[kind - 1]
        rows = pl.ds(8 * g, 8)
        return (lambda i: source.at[i, rows]), (lambda i: halo_s.at[kind - 1, i, rows])

    def near_copy(kind, g):
        source, target = piece(kind, g)
        side = jnp.minimum(my_f // 2, 1) if two_sided else 0
        return pltpu.make_async_remote_copy(
            src_ref=source(0), dst_ref=target(side),
            send_sem=halo_send.at[kind, g, 0], recv_sem=halo_recv.at[kind, g, side],
            device_id=(my_ma, near), device_id_type=MESH,
        )

    def far_copy(kind, g):
        source, target = piece(kind, g)
        return pltpu.make_async_remote_copy(
            src_ref=source(1), dst_ref=target(0),
            send_sem=halo_send.at[kind, g, 1], recv_sem=halo_recv.at[kind, g, 0],
            device_id=(my_ma, my_f + 1), device_id_type=MESH,
        )

    def arrival(kind, g, side):
        slot = piece(kind, g)[1](side)
        return pltpu.make_async_copy(slot, slot, halo_recv.at[kind, g, side])

    def send(kind, g):
        if nf > 1:
            near_copy(kind, g).start()
        if two_sided:
            pl.when(has_far)(lambda: far_copy(kind, g).start())

    def arrive(kind, g):
        if nf > 1:
            arrival(kind, g, 0).wait()
        if two_sided:
            pl.when(has_far)(lambda: arrival(kind, g, 1).wait())

    def sent(kind, g):
        if nf > 1:
            near_copy(kind, g).wait_send()
        if two_sided:
            pl.when(has_far)(lambda: far_copy(kind, g).wait_send())

    def pair_copy(k, source, target, ma, f):
        return pltpu.make_async_remote_copy(
            src_ref=source, dst_ref=target, send_sem=pair_send.at[k], recv_sem=pair_recv.at[k],
            device_id=(ma, f), device_id_type=MESH,
        )

    def lend(k):
        source = (lambda: beam_s.at[0], lambda: column_s.at[0], lambda: y_s.at[0], lambda: r_s.at[1])[k]
        target = (lent_beam_s, lent_column_s, lent_y_s, lent_r_s)[k]
        return pair_copy(k, source(), target, my_ma + 1, my_f)

    def pull_copy():
        return pair_copy(4, pull_s, partner_s, my_ma + 1, my_f)

    def first_copy(g):
        rows = pl.ds(4 * g, 4)
        return pair_copy(5 + g, edge_s.at[0, rows], lent_first_s.at[rows], my_ma + 1, 1 - my_f)

    def cross_copy(g):
        rows = pl.ds(8 * g, 8)
        return pair_copy(5 + groups + g, lent_v_s.at[rows], cross_s.at[rows], my_ma, 1 - my_f)

    def ahead_copy(g):
        rows = pl.ds(8 * g, 8)
        return pltpu.make_async_remote_copy(
            src_ref=ahead_s.at[rows], dst_ref=halo_s.at[1, 0, rows],
            send_sem=halo_send.at[2, g, 0], recv_sem=halo_recv.at[2, g, 0],
            device_id=(my_ma, 1 - my_f), device_id_type=MESH,
        )

    def hand_copy(g):
        rows = pl.ds(4 * g, 4)
        return pltpu.make_async_remote_copy(
            src_ref=lent_first_s.at[rows], dst_ref=first_s.at[0, rows],
            send_sem=hand_send.at[g], recv_sem=halo_recv.at[0, g, 0],
            device_id=(my_ma - 1, my_f), device_id_type=MESH,
        )

    def even_only(copies):
        @pl.when(jnp.logical_not(helper))
        def _():
            for copy in copies:
                copy.start()

    def beside(i, value):
        return jnp.where(has_far, value, 0.0) if i else value

    if two_sided:
        @pl.when(jnp.logical_not(has_far))
        def _():
            first_s[1] = jnp.zeros_like(first_s[1])
            halo_s[:, 1] = jnp.zeros_like(halo_s[:, 1])

    for copy in edge_copies:
        copy.wait()
    for f in inner:
        beam_copies[f].start()
    pl.semaphore_wait(barrier, expected)
    if paired:
        even_only([first_copy(g) for g in range(groups)])

        pl.when(helper)(lambda: near_copy(0, 0).start())
    else:
        for g in range(groups):
            send(0, g)
    advance()

    x0_copy.wait()
    for copy in small:
        copy.wait()
    def rows_of(ref, *at_f):
        place = (slice(None), *at_f)
        return jnp.concatenate(
            [ref[(slice(4 * g, 4 * g + 4), *place[1:], b)] for g in range(groups) for b in range(2)],
            axis=0,
        )

    def group(g):
        return slice(8 * g, 8 * g + 8)

    for f in range(freqs):
        x_s[f] = rows_of(x0_s, at(f))
    power, smooth = power_s[...], smooth_s[...]
    row = lax.broadcasted_iota(jnp.int32, (2 * modes, width), 0)
    own = lax.broadcasted_iota(jnp.int32, (2 * modes, width), 1) // rank == row // 8 * 4 + row % 4
    sign = jnp.where(row % 8 < 4, 1.0, -1.0)
    for i, f in enumerate(matrix):
        levels = noise_s[:, at(f), :]
        levels = jnp.concatenate(
            [levels[4 * g:4 * g + 4] for g in range(groups) for _ in range(2)], axis=0
        )
        mask_s[i] = jnp.where(own, jnp.concatenate([levels] * modes, axis=1), 0.0)
    unit = (
        lax.broadcasted_iota(jnp.int32, (rank, rank), 0)
        == lax.broadcasted_iota(jnp.int32, (rank, rank), 1)
    )
    for i, f in enumerate(vector):
        levels = noise_s[:, at(f), :]
        for m in range(modes):
            column = jnp.sum(jnp.where(unit, levels[m:m + 1], 0.0), axis=1, keepdims=True)
            column_s[i, m] = jnp.broadcast_to(column, (rank, 128))

    def swapped(x):
        return jnp.concatenate([pltpu.roll(x[group(g)], 4, 0) for g in range(groups)], axis=0)

    def matrix_project(f, field):
        i = matrix.index(f)
        seen = times(field, high_s[i], low_s[i], True)
        parts = seen[:, :width] + sign * swapped(seen[:, width:])
        return parts, mask_s[i] * parts

    def matrix_back(f, seen):
        i = matrix.index(f)
        weighted = jnp.concatenate([seen[1], -sign * swapped(seen[1])], axis=1)
        return times(weighted, high_s[i], low_s[i], False)

    def wide(x):
        return jnp.concatenate([x] * (ell // 128), axis=1)

    def owned(f):
        return (lambda m, a: beam_s[f, m, a]), (lambda m: column_s[vector.index(f), m])

    lent = (lambda m, a: lent_beam_s[m, a]), (lambda m: lent_column_s[m])

    def group_project(source, g, field):
        beam_of, column_of = source
        parts = []
        for j in range(4):
            m = 4 * g + j
            real_beam, imaginary_beam = beam_of(m, 0), beam_of(m, 1)
            real_field, imaginary_field = field[j:j + 1], field[4 + j:5 + j]
            levels = column_of(m)
            real = jnp.sum(
                real_beam * real_field + imaginary_beam * imaginary_field, axis=1, keepdims=True
            )
            imaginary = jnp.sum(
                real_beam * imaginary_field - imaginary_beam * real_field, axis=1, keepdims=True
            )
            parts.append((real, imaginary, levels * real, levels * imaginary))
        return parts

    def group_back(source, g, parts):
        beam_of, _ = source
        reals, imaginaries = [], []
        for j, (_, _, real, imaginary) in enumerate(parts):
            m = 4 * g + j
            real, imaginary = wide(real), wide(imaginary)
            real_beam, imaginary_beam = beam_of(m, 0), beam_of(m, 1)
            for found, value in (
                (reals, real_beam * real - imaginary_beam * imaginary),
                (imaginaries, real_beam * imaginary + imaginary_beam * real),
            ):
                found.append(sum(value[k:k + 8] for k in range(0, rank, 8)))
        return folded(reals + imaginaries)

    def group_beam(source, g, field):
        return group_back(source, g, group_project(source, g, field))

    def project(f, ref):
        if f in matrix:
            return matrix_project(f, ref[f])
        return [group_project(owned(f), g, ref[f, group(g)]) for g in range(groups)]

    def back(f, seen):
        if f in matrix:
            return matrix_back(f, seen)
        return jnp.concatenate([group_back(owned(f), g, seen[g]) for g in range(groups)], axis=0)

    def apply_beam(fs, ref):
        fs = [f for f in fs if f in matrix] + [f for f in fs if f in vector]
        seen = [project(f, ref) for f in fs]
        return {f: back(f, found) for f, found in zip(fs, seen)}

    def count(f):
        value = float(f > 0) + float(f < last) + float(nf > 1 and f == 0)
        if two_sided and f == last:
            value = value + jnp.where(has_far, 1.0, 0.0)
        return value

    def local_prior(f, ref, rows=slice(None)):
        value = count(f) * ref[f, rows]
        if f > 0:
            value = value - ref[f - 1, rows]
        if f < last:
            value = value - ref[f + 1, rows]
        return power * ref[f, rows] + smooth * value

    for f in edges:
        beam_copies[f].wait()
    rhs_copy.wait()
    for i, f in enumerate(edges):
        for g in range(groups):
            rows = group(g)
            image = group_beam(owned(f), g, x_s[f, rows])
            y_s[i, rows] = rows_of(rhs_s, at(f))[rows] - image - local_prior(f, x_s, rows)
    first, rest = [], inner
    if paired:
        even_only([near_copy(1, g) for g in range(groups)] + [lend(k) for k in range(3)])

        @pl.when(helper)
        def _():
            for g in range(1, groups):
                near_copy(0, g).start()

        first, rest = inner[:1], inner[1:]
    else:
        for g in range(groups):
            send(1, g)

    for f in first:
        beam_copies[f].wait()
        r_s[f] = rows_of(rhs_s, at(f)) - back(f, project(f, x_s)) - local_prior(f, x_s)
    if paired:
        even_only([lend(3)])

        @pl.when(helper)
        def _():
            for g in range(groups):
                near_copy(1, g).start()

    for f in rest:
        beam_copies[f].wait()
    for i, f in enumerate(matrix):
        for a in range(2):
            rows = slice(a * width, (a + 1) * width)
            high, low = split(beam_s[f, :, a].reshape(width, ell))
            high_s[i, rows] = high
            low_s[i, rows] = low
    for f, image in apply_beam(rest, x_s).items():
        r_s[f] = rows_of(rhs_s, at(f)) - image - local_prior(f, x_s)
    for f, image in apply_beam(inner, r_s).items():
        u_s[f] = image + local_prior(f, r_s) if f in apart else image
    advance()

    def complete(i, f, g):
        rows = group(g)
        halo = jnp.concatenate([first_s[i, 4 * g:4 * g + 4, b, :] for b in range(2)], axis=0)
        r_s[f, rows] = y_s[i, rows] + smooth * halo

    def edge_image(f, g):
        rows = group(g)
        return group_beam(owned(f), g, r_s[f, rows]) + local_prior(f, r_s, rows)

    if paired:
        @pl.when(helper)
        def _():
            for g in range(groups):
                arrive(0, g)
                complete(0, 0, g)
                ahead_s[group(g)] = edge_image(0, g)
                ahead_copy(g).start()
            for g in range(groups):
                first_copy(g).wait_recv()
                hand_copy(g).start()
                if g == 0:
                    for k in range(4):
                        lend(k).wait_recv()
                rows = group(g)
                halo = jnp.concatenate([lent_first_s[4 * g:4 * g + 4, b, :] for b in range(2)], axis=0)
                r = lent_y_s[rows] + smooth * halo
                local = power * r + smooth * (count(0) * r - lent_r_s[rows])
                lent_v_s[rows] = group_beam(lent, g, r) + local
                cross_copy(g).start()

    seen = {f: project(f, u_s) for f in apart}
    grouped = [f for f in beside_edge if f in vector]
    whole = [f for f in beside_edge if f in matrix]
    seen |= {f: [] for f in grouped + edges}
    zero = jnp.zeros((8, ell), F32)
    sums = [zero, zero, zero, zero]
    column_part = jnp.zeros((rank, 128), F32)

    def add_up(g, sums, column_part):
        rows = group(g)
        norm, curve, square, cube = sums
        for f in inner + edges:
            if f in vector:
                for real, imaginary, real_weighted, imaginary_weighted in seen[f][g]:
                    column_part = column_part + (real * real_weighted + imaginary * imaginary_weighted)
            r, u = r_s[f, rows], u_s[f, rows]
            w = local_prior(f, u_s, rows)
            w_s[f, rows] = w
            norm = norm + r * r
            curve = curve + r * u
            square = square + u * u
            cube = cube + u * w
        return [norm, curve, square, cube], column_part

    def finish_edges(g):
        rows = group(g)
        for i, f in enumerate(edges):
            u_s[f, rows] = v_s[i, rows] - beside(
                i, smooth * (halo_s[0, i, rows] + smooth * x_s[f, rows])
            )
            seen[f].append(group_project(owned(f), g, u_s[f, rows]))

    for g in range(groups):
        rows = group(g)
        if paired:
            pl.when(jnp.logical_not(helper))(lambda: arrive(0, g))
            arrive(1, g)
        else:
            arrive(0, g)
        for i, f in enumerate(edges):
            complete(i, f, g)
        for i, f in enumerate(edges):
            v_s[i, rows] = edge_image(f, g)
        if not paired:
            send(2, g)
        for f in grouped:
            u_s[f, rows] = u_s[f, rows] + local_prior(f, r_s, rows)
            seen[f].append(group_project(owned(f), g, u_s[f, rows]))
        if paired:
            finish_edges(g)
            pull_s[rows] = smooth * u_s[0, rows]
            if not whole:
                sums, column_part = add_up(g, sums, column_part)
    for f in whole:
        u_s[f] = u_s[f] + local_prior(f, r_s)
        seen[f] = project(f, u_s)
    if paired:
        even_only([pull_copy()])
    else:
        for g in range(groups):
            arrive(1, g)
            finish_edges(g)
    if whole or not paired:
        for g in range(groups):
            sums, column_part = add_up(g, sums, column_part)
    beam_part = jnp.zeros((2 * modes, width), F32)
    for f in matrix:
        beam_part = beam_part + seen[f][0] * seen[f][1]
    lane = lax.broadcasted_iota(jnp.int32, (1, 128), 1)
    message = jnp.zeros((1, 128), F32)
    for i, part in enumerate(sums):
        total = total_of(part)
        if i == 3:
            total = total + total_of(beam_part) + jnp.sum(column_part, axis=0, keepdims=True)
        message = jnp.where(lane == i, total, message)
    if paired:
        message = jnp.where(lane == 4 + my_f, total_of(smooth * r_s[0] * pull_s[...]), message)
    message_s[0] = message
    early_s[me] = message

    while steps:
        advance()

    def share(source, target, slot, turn, device):
        pltpu.make_async_remote_copy(
            src_ref=message_s.at[source], dst_ref=target.at[slot],
            send_sem=sum_send.at[turn], recv_sem=sum_recv.at[turn],
            device_id=device, device_id_type=MESH,
        ).start()

    def share_all(source, target, slot, turn, stride):
        if n > 64:
            def body(i, carry):
                ma, f = my_ma + i * stride // nf, my_f + i * stride % nf
                share(source, target, slot, turn, (lax.rem(ma, nma), lax.rem(f, nf)))
                return carry

            lax.fori_loop(1, n // stride, body, 0)
        else:
            for mask in sorted(range(stride, n, stride), key=lambda m: (-(m // nf // 2), m)):
                device = partner([bit for bit in range(bits) if mask >> bit & 1])
                share(source, target, slot, turn, device)

    def landed(target, sem, rows):
        if rows:
            rows = target.at[pl.ds(0, rows)]
            pltpu.make_async_copy(rows, rows, sem).wait()

    def lanes_of(x):
        x = jnp.sum(x, axis=0, keepdims=True)
        return sum(x[:, i:i + 128] for i in range(0, ell, 128))

    share_all(0, early_s, me, 0, 1)
    if paired:
        even_only([near_copy(2, g) for g in range(groups)])
    for f in matrix + vector:
        w_s[f] = w_s[f] + back(f, seen[f])

    late_rows = late_s.shape[0]
    if paired:
        @pl.when(helper)
        def _():
            cross = jnp.zeros((8, ell), F32)
            for g in range(groups):
                arrive(2, g)
                cross = cross + pull_s[group(g)] * halo_s[1, 0, group(g)]
            pull_copy().wait_recv()
            for g in range(groups):
                cross_copy(g).wait_recv()
                cross = cross + partner_s[group(g)] * cross_s[group(g)]
            message = lanes_of(cross)
            late_s[my_ma // 2] = message
            message_s[1] = message
            share_all(1, late_s, my_ma // 2, 1, nf)
            for g in range(groups):
                cross_copy(g).wait_send()

        @pl.when(jnp.logical_not(helper))
        def _():
            for g in range(groups):
                arrive(2, g)
            pull_copy().wait_send()
            for k in range(4):
                lend(k).wait_send()
            for g in range(groups):
                first_copy(g).wait_send()

        w_s[0] = w_s[0] - smooth * (halo_s[1, 0] - smooth * r_s[0])
    else:
        cross = jnp.zeros((8, ell), F32)
        nexts = []
        for g in range(groups):
            arrive(2, g)
            rows = group(g)
            for i, f in enumerate(edges):
                pull = beside(i, smooth * (halo_s[1, i, rows] - smooth * r_s[f, rows]))
                nexts.append((f, rows, pull))
                cross = cross + pull * u_s[f, rows]
        message = lanes_of(cross)
        late_s[me] = message
        message_s[1] = message
        share_all(1, late_s, me, 1, 1)
        for f, rows, pull in nexts:
            w_s[f, rows] = w_s[f, rows] - pull

    if paired:
        for g in range(groups):
            for kind in (1, 2):
                sent(kind, g)

        @pl.when(helper)
        def _():
            for g in range(groups):
                sent(0, g)
                hand_copy(g).wait_send()
    else:
        for kind in range(3):
            for g in range(groups):
                sent(kind, g)
    for source, target in ((r_s, r_out_s), (u_s, u_out_s), (w_s, w_out_s)):
        for f in range(freqs):
            value = source[f]
            for g in range(groups):
                for b in range(2):
                    start = 8 * g + 4 * b
                    target[4 * g:4 * g + 4, at(f), b, :] = value[start:start + 4]

    landed(early_s, sum_send.at[0], n - 1)
    landed(early_s, sum_recv.at[0], n - 1)
    def rows_total(ref):
        if ref.shape[0] > 64:
            return jnp.sum(ref[...], axis=0)
        return tree([ref[k] for k in range(ref.shape[0])])

    total = rows_total(early_s)
    m0, m1, m2, m3, known = (
        jnp.sum(jnp.where(lane == i, total, 0.0), axis=1, keepdims=True)
        for i in (0, 1, 2, 3, 4 + my_f)
    )
    inverse = 1.0 / m1
    step = m0 * inverse
    drop = step * m2 - m1
    growth = drop * inverse
    if paired:
        @pl.when(helper)
        def _():
            rows = early_s.at[pl.ds(0, nma - 1)]
            pltpu.make_async_copy(rows, rows, sum_send.at[1]).wait()
            landed(late_s, sum_recv.at[1], late_rows - 1)

        pl.when(jnp.logical_not(helper))(lambda: landed(late_s, sum_recv.at[1], late_rows))
    else:
        landed(late_s, sum_send.at[1], late_rows - 1)
        landed(late_s, sum_recv.at[1], late_rows - 1)
    crossed = jnp.sum(rows_total(late_s), axis=1, keepdims=True)
    m3 = m3 - 2.0 * (crossed - known) if paired else m3 - crossed
    curve_next = m1 - 2.0 * step * m2 + step * step * m3
    step_next = step * drop / (curve_next - growth * drop)
    c = step + step_next * (1.0 + growth)
    e = step * step_next
    for m in range(modes):
        r, u = r_out_s[m], u_out_s[m]
        sol_s[m] = x0_s[m] + c * r - e * u
        res_s[m] = r - c * u + e * w_out_s[m]


def scoped_kernel(nma, nf, sides, *refs):
    modes, freqs = refs[0].shape[:2]
    dma = pltpu.SemaphoreType.DMA
    pl.run_scoped(
        functools.partial(kernel, nma, nf, *refs),
        dma((7,)), dma((freqs,)), dma((3, modes // 4, sides)), dma((2 * (modes // 4) + 5,)),
        dma((modes // 4,)), dma((2,)),
    )


def write_out(sol_in, res_in, sol_out, res_out):
    def body(sem):
        copies = [
            pltpu.make_async_copy(sol_in, sol_out, sem.at[0]),
            pltpu.make_async_copy(res_in, res_out, sem.at[1]),
        ]
        for copy in copies:
            copy.start()
        for copy in copies:
            copy.wait()

    pl.run_scoped(body, pltpu.SemaphoreType.DMA((2,)))


def shards(right_side, start_field, beam, noise, inv_power, smooth):
    nma, nf = lax.axis_size("ma"), lax.axis_size("freq")
    modes, freqs, _, ell = right_side.shape
    rank = beam.shape[3]
    width = modes * rank
    sides = 2 if nf > 2 else 1
    vmem_spec = pl.BlockSpec(memory_space=pltpu.VMEM)
    any_spec = pl.BlockSpec(memory_space=pl.ANY)
    field = pltpu.VMEM(right_side.shape, F32)
    edge = pltpu.VMEM((sides, modes, 2, ell), F32)
    slab = pltpu.VMEM((freqs, 2 * modes, ell), F32)
    edge_field = pltpu.VMEM((2 * modes, ell), F32)
    edge_slab = pltpu.VMEM((sides, 2 * modes, ell), F32)
    vector = max(min(nf - 1, 2), freqs // 2)
    matrix = max(freqs - vector, 1)
    half = pltpu.VMEM((matrix, 2 * width, ell), BF16)
    outs = pl.pallas_call(
        functools.partial(scoped_kernel, nma, nf, sides),
        out_shape=[field] * 2,
        in_specs=[any_spec] * 6,
        out_specs=[vmem_spec] * 2,
        scratch_shapes=[
            field, field, edge,
            pltpu.VMEM((freqs, modes, 2, rank, ell), F32),
            pltpu.VMEM(noise.shape, F32),
            pltpu.VMEM((1, ell), F32), pltpu.VMEM((1, ell), F32),
            half, half,
            slab, edge_slab, slab, edge_slab, slab, slab,
            pltpu.VMEM((matrix, 2 * modes, width), F32),
            pltpu.VMEM((vector, modes, rank, 128), F32),
            edge,
            pltpu.VMEM((2, sides, 2 * modes, ell), F32),
            field, field, field,
            edge_field, edge_field, edge_field,
            pltpu.VMEM((modes, 2, rank, ell), F32), pltpu.VMEM((modes, rank, 128), F32),
            edge_field, edge_field, pltpu.VMEM((modes, 2, ell), F32), edge_field, edge_field,
            pltpu.VMEM((2, 1, 128), F32),
            pltpu.VMEM((nma * nf, 1, 128), F32),
            pltpu.VMEM((nma // 2 if nf == 2 and nma % 2 == 0 and freqs > 3 else nma * nf, 1, 128), F32),
            pltpu.SemaphoreType.DMA((3, modes // 4, sides)),
            pltpu.SemaphoreType.DMA((2 * (modes // 4) + 5,)),
            pltpu.SemaphoreType.DMA((2,)),
            pltpu.SemaphoreType.REGULAR((max((nma * nf).bit_length() - 4, 1),)),
        ],
        compiler_params=pltpu.CompilerParams(
            collective_id=0, has_side_effects=True, vmem_limit_bytes=67043328 - 2 * right_side.size * 4
        ),
        name="solve",
    )(right_side, start_field, beam, noise, inv_power[None], smooth[None])
    return pl.pallas_call(
        write_out,
        out_shape=[jax.ShapeDtypeStruct(right_side.shape, F32)] * 2,
        in_specs=[vmem_spec] * 2,
        out_specs=[any_spec] * 2,
        compiler_params=pltpu.CompilerParams(vmem_limit_bytes=1024 * 1024),
        name="write_out",
    )(*outs)


def solution(mesh):
    in_specs = (
        P("ma", "freq", None, None),
        P("ma", "freq", None, None),
        P("ma", "freq", None, None, None),
        P("ma", "freq", None),
        P(),
        P(),
    )
    out_specs = (P("ma", "freq", None, None), P("ma", "freq", None, None))
    return jax.shard_map(shards, mesh=mesh, in_specs=in_specs, out_specs=out_specs, check_vma=False)
```
